32 devices in a mesh: seq: 8 (over z, y), shard: 4 (over x, core).
Axes of the slice: x: 2, y: 2, z: 4, core: 2. Of those that a mesh axis runs over, the one named last changes fastest.
Arguments:
- tokens: bfloat16 [8, 4096, 768], P('shard', 'seq'), may hold values from -6 to 6
- segments: int32 [8, 4096], P('shard'), may hold values from 0 to 20, as said below
- positions: int32 [8, 4096], P('shard', 'seq'), may hold values from 0 to 1999, as said below
- cotangent: bfloat16 [8, 4096, 768], P('shard', 'seq'), may hold values from -6 to 6
- w_qkv: bfloat16 [768, 2304], P('shard'), may hold values from -0.21875 to 0.21875
- w_out: bfloat16 [768, 768], P('shard'), may hold values from -3 to 3
- w_gate: bfloat16 [768, 3072], P('shard'), may hold values from -0.21875 to 0.21875
- w_up: bfloat16 [768, 3072], P('shard'), may hold values from -0.21875 to 0.21875
- w_down: bfloat16 [3072, 768], P('shard'), may hold values from -0.109375 to 0.109375
- ln1_gain: bfloat16 [768], P('shard'), may hold values from 0.099609375 to 1.8984375
- ln1_bias: bfloat16 [768], P('shard'), may hold values from -3 to 3
- ln2_gain: bfloat16 [768], P('shard'), may hold values from 0.099609375 to 1.8984375
- ln2_bias: bfloat16 [768], P('shard'), may hold values from -3 to 3
Outputs:
- output: bfloat16 [8, 4096, 768], P('shard', 'seq')
- input_grad: bfloat16 [8, 4096, 768], P('shard', 'seq')
- grad_w_qkv: float32 [768, 2304], P('shard')
- grad_w_out: float32 [768, 768], P('shard')
- grad_w_gate: float32 [768, 3072], P('shard')
- grad_w_up: float32 [768, 3072], P('shard')
- grad_w_down: float32 [3072, 768], P('shard')
- grad_ln1_gain: float32 [768], P('shard')
- grad_ln1_bias: float32 [768], P('shard')
- grad_ln2_gain: float32 [768], P('shard')
- grad_ln2_bias: float32 [768], P('shard')
The draws below stay inside these ranges and needn't reach their ends.
Inputs may be any that keep to these rules, and one draw needn't show every extreme that they name: segments[s, t] numbers the documents of sequence s in order from 0 and never falls along t; every document has 200 to 2000 tokens, except that the end of the sequence may cut the last one short. positions[s, t] counts the earlier tokens of the same document of sequence s.
All inputs are finite; a program needn't handle non-finite values.
Results may differ from the reference program's by a relative error of at most 0.025.
Values may be sent and summed in bfloat16 or wider, within the bound.
A program may use at most 256 MiB of HBM per device.

```python
import math
import jax
import jax.numpy as jnp
from jax import lax

D = 768
HEADS = 12
HD = 64
FF = 3072
LEN = 4096
DOC_MIN = 200
DOC_MAX = 2000
SEQS = 8


def doc_layout(key):
    inner = jax.random.fold_in(key, 11)
    doc_count = LEN // DOC_MIN + 1
    lengths = jax.random.randint(inner, (SEQS, doc_count), DOC_MIN, DOC_MAX + 1).astype(jnp.int32)
    rows = jnp.arange(SEQS, dtype=jnp.int32)[:, None]
    cols = jnp.arange(doc_count, dtype=jnp.int32)[None, :]
    lengths = jnp.where(rows == SEQS - 1, DOC_MIN, lengths).astype(jnp.int32)
    lengths = jnp.where((rows == 0) & (cols == 0), DOC_MAX, lengths).astype(jnp.int32)
    second_row = (rows == 1) & (rows != SEQS - 1)
    lengths = jnp.where(second_row & (cols == 0), DOC_MIN, lengths).astype(jnp.int32)
    lengths = jnp.where(second_row & (cols == 1), DOC_MAX, lengths).astype(jnp.int32)
    ends = jnp.cumsum(lengths, axis=1).astype(jnp.int32)
    places = jnp.arange(LEN, dtype=jnp.int32)
    seg_ids = jnp.sum((places[None, :, None] >= ends[:, None, :]).astype(jnp.int32), axis=2).astype(jnp.int32)
    starts = ends - lengths
    first = jnp.take_along_axis(starts, seg_ids, axis=1)
    return (seg_ids, (places[None, :] - first).astype(jnp.int32))


def draw_segments(key, part):
    return doc_layout(key)[0]


def draw_positions(key, part):
    return doc_layout(key)[1]


def level_of(own_key, shape, pieces, least, high):
    loudness = 1.0
    for position, blocks in pieces:
        heights = jax.random.uniform(jax.random.fold_in(jax.random.fold_in(own_key, 6), position), (blocks,), jnp.float32, least / len(pieces), high / len(pieces))
        loudness = loudness * jnp.repeat(jnp.exp(heights), shape[position] // blocks).reshape((-1,) + (1,) * (len(shape) - 1 - position))
    return loudness


def scatter_about(own_key, dims, deviation, reach, split=(), held_as=jnp.bfloat16):
    drawn = deviation * jax.random.normal(own_key, dims, jnp.float32)
    if split:
        drawn = drawn * level_of(own_key, dims, split, -0.22, 0.18)
    return jnp.clip(drawn, -reach, reach).astype(held_as)


def setup_inputs(seed: int = 0) -> dict:
    streams_of = jax.random.split(jax.random.key(seed), 14)
    tokens = scatter_about(streams_of[0], (SEQS, LEN, D), 1.0, 6.0, ((0, 4), (1, 8)))
    segments = draw_segments(jax.random.fold_in(streams_of[13], 71), 0)
    positions = draw_positions(jax.random.fold_in(streams_of[13], 71), 0)
    cotangent = scatter_about(streams_of[3], (SEQS, LEN, D), 1.0, 6.0, ((0, 4), (1, 8)))
    w_qkv = scatter_about(streams_of[4], (D, 3 * D), D ** -0.5, 0.21875, ((0, 4),))
    w_out = scatter_about(streams_of[5], (D, D), 4 ** -0.5, 3.0, ((0, 4),))
    w_gate = scatter_about(streams_of[6], (D, FF), D ** -0.5, 0.21875, ((0, 4),))
    w_up = scatter_about(streams_of[7], (D, FF), D ** -0.5, 0.21875, ((0, 4),))
    w_down = scatter_about(streams_of[8], (FF, D), FF ** -0.5, 0.109375, ((0, 4),))
    ln1_gain = jnp.clip(1.0 + 0.18 * jax.random.normal(streams_of[9], (D,), jnp.float32), 0.099609375, 1.8984375).astype(jnp.bfloat16)
    ln1_bias = scatter_about(streams_of[10], (D,), 0.5, 3.0, ((0, 4),))
    ln2_gain = jnp.clip(1.0 + 0.18 * jax.random.normal(streams_of[11], (D,), jnp.float32), 0.099609375, 1.8984375).astype(jnp.bfloat16)
    ln2_bias = scatter_about(streams_of[12], (D,), 0.5, 3.0, ((0, 4),))
    return dict(tokens=tokens, segments=segments, positions=positions, cotangent=cotangent, w_qkv=w_qkv, w_out=w_out, w_gate=w_gate, w_up=w_up, w_down=w_down, ln1_gain=ln1_gain, ln1_bias=ln1_bias, ln2_gain=ln2_gain, ln2_bias=ln2_bias)


EPS = 1e-05
ROPE_BASE = 1000.0
HIGHEST_PRECISION = lax.Precision.HIGHEST

@jax.custom_vjp
def low(v):
    return lax.optimization_barrier(v.astype(jnp.bfloat16)).astype(jnp.float32)

@jax.custom_vjp
def low_back(v):
    return v

def low_keep(v):
    return (low(v), None)

def low_pass(kept, grad):
    return (grad,)

def back_keep(v):
    return (v, None)

def back_low(kept, grad):
    return (low(grad),)
low.defvjp(low_keep, low_pass)
low_back.defvjp(back_keep, back_low)

def rope_tables(pos_row):
    half_dim = HD // 2
    freqs = jnp.exp(jnp.arange(half_dim, dtype=jnp.float32) * (-math.log(ROPE_BASE) / half_dim))
    angle = pos_row.astype(jnp.float32)[:, None] * freqs[None, :]
    return (jnp.cos(angle), jnp.sin(angle))

def rotate(heads, cosine, sine):
    half_dim = heads.shape[-1] // 2
    first = heads[..., :half_dim]
    second = heads[..., half_dim:]
    cos_b = cosine[:, None, :]
    sin_b = sine[:, None, :]
    return jnp.concatenate([first * cos_b - second * sin_b, second * cos_b + first * sin_b], axis=-1)

def layer_norm(values, gain, bias):
    mean_val = lax.optimization_barrier(jnp.mean(values, axis=-1, keepdims=True))
    centered = values - mean_val
    variance = lax.optimization_barrier(jnp.mean(centered * centered, axis=-1, keepdims=True))
    return centered * lax.rsqrt(variance + EPS) * gain + bias

def layer_forward(tok_f, seg_row, cosine, sine, params):
    w_qkv, w_out, w_gate, w_up, w_down, gain_one, bias_one, gain_two, bias_two = params
    seq_len = tok_f.shape[0]
    model_width = tok_f.shape[1]
    score_scale = HD ** (-0.5)
    qkv_all = low_back(jnp.dot(tok_f, w_qkv, precision=HIGHEST_PRECISION))
    q_heads = low(rotate(qkv_all[:, :model_width].reshape(seq_len, HEADS, HD), cosine, sine))
    k_heads = low(rotate(qkv_all[:, model_width:2 * model_width].reshape(seq_len, HEADS, HD), cosine, sine))
    v_heads = low(qkv_all[:, 2 * model_width:].reshape(seq_len, HEADS, HD))
    block = math.gcd(512, seq_len)
    block_count = seq_len // block

    def attend_block(pair):
        q_part, seg_part = pair
        raw = jnp.einsum('qhd,khd->hqk', q_part, k_heads, precision=HIGHEST_PRECISION) * score_scale
        scores = low_back(raw)
        same_doc = seg_part[None, :, None] == seg_row[None, None, :]
        expo = jnp.where(same_doc, jnp.exp(scores), 0.0)
        row_total = lax.optimization_barrier(jnp.sum(expo, axis=-1))
        numer = low_back(jnp.einsum('hqk,khd->qhd', low(expo), v_heads, precision=HIGHEST_PRECISION))
        return numer / jnp.transpose(row_total)[:, :, None]
    attn_heads = lax.map(jax.checkpoint(attend_block), (q_heads.reshape(block_count, block, HEADS, HD), seg_row.reshape(block_count, block)))
    joined = low_back(low(attn_heads.reshape(seq_len, model_width)))
    h_one = tok_f + low_back(jnp.dot(joined, w_out, precision=HIGHEST_PRECISION))
    x_one = layer_norm(h_one, gain_one, bias_one)
    x_low = low(x_one)
    gate_pre = low_back(jnp.dot(x_low, w_gate, precision=HIGHEST_PRECISION))
    up_pre = low_back(jnp.dot(x_low, w_up, precision=HIGHEST_PRECISION))
    hidden = low(jax.nn.silu(gate_pre) * up_pre)
    h_two = x_one + low_back(jnp.dot(hidden, w_down, precision=HIGHEST_PRECISION))
    return layer_norm(h_two, gain_two, bias_two)

def reference(tokens, segments, positions, cotangent, w_qkv, w_out, w_gate, w_up, w_down, ln1_gain, ln1_bias, ln2_gain, ln2_bias):
    params = tuple((p.astype(jnp.float32) for p in (w_qkv, w_out, w_gate, w_up, w_down, ln1_gain, ln1_bias, ln2_gain, ln2_bias)))

    def one_seq(sums, item):
        tok_row, seg_row, pos_row, cot_row = item
        cosine, sine = rope_tables(pos_row)

        def forward(tok_f, params_in):
            return layer_forward(tok_f, seg_row, cosine, sine, params_in)
        result, pull = jax.vjp(forward, tok_row.astype(jnp.float32), params)
        tok_grad, param_grads = pull(cot_row.astype(jnp.float32))
        sums = tuple((a + b for a, b in zip(sums, param_grads)))
        return (sums, (result.astype(jnp.bfloat16), tok_grad.astype(jnp.bfloat16)))
    zeros = tuple((jnp.zeros(p.shape, jnp.float32) for p in params))
    sums, outs_pair = lax.scan(one_seq, zeros, (tokens, segments, positions, cotangent))
    output, input_grad = outs_pair
    return (output, input_grad, sums[0], sums[1], sums[2], sums[3], sums[4], sums[5], sums[6], sums[7], sums[8])
```

```python
import functools
import math

import jax
import jax.numpy as jnp
from jax import lax
from jax.experimental import pallas as pl
from jax.experimental.pallas import tpu as pltpu
from jax.sharding import PartitionSpec as P

HEADS = 12
HD = 64


EPS = 1e-05
ROPE_BASE = 1000.0


def rope_tables(pos_block):
    half_dim = HD // 2
    freqs = jnp.exp(jnp.arange(half_dim, dtype=jnp.float32) * (-math.log(ROPE_BASE) / half_dim))
    angle = pos_block.astype(jnp.float32)[..., None] * freqs
    return (jnp.cos(angle)[:, :, None, :], jnp.sin(angle)[:, :, None, :])


def rotate(heads, cos_b, sin_b):
    half_dim = heads.shape[-1] // 2
    first = heads[..., :half_dim]
    second = heads[..., half_dim:]
    return jnp.concatenate(
        [first * cos_b - second * sin_b, second * cos_b + first * sin_b], axis=-1
    )


def rotate_back(grads, cos_b, sin_b):
    half_dim = grads.shape[-1] // 2
    first = grads[..., :half_dim]
    second = grads[..., half_dim:]
    return jnp.concatenate(
        [first * cos_b + second * sin_b, second * cos_b - first * sin_b], axis=-1
    )


def norm_fwd(values, gain, bias):
    mean_val = jnp.mean(values, axis=-1, keepdims=True)
    centered = values - mean_val
    variance = jnp.mean(centered * centered, axis=-1, keepdims=True)
    inverse = lax.rsqrt(variance + EPS)
    normed = centered * inverse
    return (normed * gain + bias, normed, inverse)


def norm_back(grad_in, normed, inverse, gain):
    scaled = grad_in * gain
    return inverse * (
        scaled
        - jnp.mean(scaled, axis=-1, keepdims=True)
        - normed * jnp.mean(scaled * normed, axis=-1, keepdims=True)
    )


def head_split(block_rows, seq_count, row_count):
    return block_rows.reshape(seq_count, row_count, HEADS, HD)


def attend(q_heads, q_seg, k_full, v_full, seg_all, block, score_scale):
    seq_count, row_count = (q_heads.shape[0], q_heads.shape[1])
    block_count = k_full.shape[1] // block

    def attend_step(carry, index):
        row_total, value_sum = carry
        start = index * block
        k_part = head_split(lax.dynamic_slice_in_dim(k_full, start, block, 1), seq_count, block)
        v_part = head_split(lax.dynamic_slice_in_dim(v_full, start, block, 1), seq_count, block)
        seg_part = lax.dynamic_slice_in_dim(seg_all, start, block, 1)
        raw = (
            jnp.einsum("sqhd,skhd->shqk", q_heads, k_part, preferred_element_type=jnp.float32)
            * score_scale
        )
        same_doc = q_seg[:, None, :, None] == seg_part[:, None, None, :]
        expo = jnp.where(same_doc, jnp.exp(raw), 0.0)
        row_total = row_total + jnp.sum(expo, axis=-1)
        value_sum = value_sum + jnp.einsum(
            "shqk,skhd->sqhd", expo.astype(jnp.bfloat16), v_part, preferred_element_type=jnp.float32
        )
        return ((row_total, value_sum), None)

    start_carry = (
        jnp.zeros((seq_count, HEADS, row_count), jnp.float32),
        jnp.zeros((seq_count, row_count, HEADS, HD), jnp.float32),
    )
    final, unused = lax.scan(attend_step, start_carry, jnp.arange(block_count, dtype=jnp.int32))
    return final


def back_keys(q_heads, g_heads, delta, q_seg, k_full, v_full, seg_all, block, score_scale):
    seq_count, row_count = (q_heads.shape[0], q_heads.shape[1])
    full_len = k_full.shape[1]
    block_count = full_len // block

    def back_step(carry, index):
        start = index * block
        k_part = head_split(lax.dynamic_slice_in_dim(k_full, start, block, 1), seq_count, block)
        v_part = head_split(lax.dynamic_slice_in_dim(v_full, start, block, 1), seq_count, block)
        seg_part = lax.dynamic_slice_in_dim(seg_all, start, block, 1)
        raw = (
            jnp.einsum("sqhd,skhd->shqk", q_heads, k_part, preferred_element_type=jnp.float32)
            * score_scale
        )
        same_doc = q_seg[:, None, :, None] == seg_part[:, None, None, :]
        expo = jnp.where(same_doc, jnp.exp(raw), 0.0)
        prob_grad = jnp.einsum(
            "sqhd,skhd->shqk", g_heads, v_part, preferred_element_type=jnp.float32
        )
        d_score = (expo * (prob_grad - delta[..., None])).astype(jnp.bfloat16)
        q_grad = carry[0] + jnp.einsum(
            "shqk,skhd->sqhd", d_score, k_part, preferred_element_type=jnp.float32
        )
        k_grad = (
            jnp.einsum("shqk,sqhd->skhd", d_score, q_heads, preferred_element_type=jnp.float32)
            * score_scale
        )
        v_grad = jnp.einsum(
            "shqk,sqhd->skhd",
            expo.astype(jnp.bfloat16),
            g_heads,
            preferred_element_type=jnp.float32,
        )
        k_store = lax.dynamic_update_slice_in_dim(
            carry[1], k_grad.reshape(seq_count, block, HEADS * HD), start, 1
        )
        v_store = lax.dynamic_update_slice_in_dim(
            carry[2], v_grad.reshape(seq_count, block, HEADS * HD), start, 1
        )
        return ((q_grad, k_store, v_store), None)

    q_zero = jnp.zeros((seq_count, row_count, HEADS, HD), jnp.float32)
    kv_zero = jnp.zeros((seq_count, full_len, HEADS * HD), jnp.float32)
    start_carry = (q_zero, kv_zero, kv_zero)
    final, unused = lax.scan(back_step, start_carry, jnp.arange(block_count, dtype=jnp.int32))
    return (final[0] * score_scale,) + tuple(final[1:])


def local(
    tokens,
    segments,
    positions,
    cotangent,
    w_qkv,
    w_out,
    w_gate,
    w_up,
    w_down,
    ln1_gain,
    ln1_bias,
    ln2_gain,
    ln2_bias,
):
    seq_count, row_count, model_width = tokens.shape
    score_scale = HD ** (-0.5)
    q_seg = lax.dynamic_slice_in_dim(segments, lax.axis_index("seq") * row_count, row_count, 1)
    gathered = (
        lax.all_gather(w_qkv, "shard", axis=0, tiled=True),
        lax.all_gather(w_out, "shard", axis=0, tiled=True),
        lax.all_gather(w_gate, "shard", axis=0, tiled=True),
        lax.all_gather(w_up, "shard", axis=0, tiled=True),
        lax.all_gather(w_down, "shard", axis=0, tiled=True),
        lax.all_gather(ln1_gain, "shard", axis=0, tiled=True),
        lax.all_gather(ln1_bias, "shard", axis=0, tiled=True),
        lax.all_gather(ln2_gain, "shard", axis=0, tiled=True),
        lax.all_gather(ln2_bias, "shard", axis=0, tiled=True),
    )
    full_qkv, full_out, full_gate, full_up, full_down, gain_one, bias_one, gain_two, bias_two = (
        gathered
    )
    cos_b, sin_b = rope_tables(positions)
    qkv_all = jnp.einsum("scd,de->sce", tokens, full_qkv, preferred_element_type=jnp.float32)
    q_heads = rotate(
        head_split(qkv_all[..., :model_width], seq_count, row_count), cos_b, sin_b
    ).astype(jnp.bfloat16)
    k_heads = rotate(
        head_split(qkv_all[..., model_width : 2 * model_width], seq_count, row_count), cos_b, sin_b
    ).astype(jnp.bfloat16)
    v_heads = head_split(qkv_all[..., 2 * model_width :], seq_count, row_count).astype(jnp.bfloat16)
    k_local = k_heads.reshape(seq_count, row_count, model_width)
    v_local = v_heads.reshape(seq_count, row_count, model_width)
    k_full, v_full = (
        lax.all_gather(k_local, "seq", axis=1, tiled=True),
        lax.all_gather(v_local, "seq", axis=1, tiled=True),
    )
    row_total, value_sum = attend(q_heads, q_seg, k_full, v_full, segments, row_count, score_scale)
    denom = jnp.transpose(row_total, (0, 2, 1))[..., None]
    attn_out = value_sum / denom
    joined = attn_out.reshape(seq_count, row_count, model_width).astype(jnp.bfloat16)
    tokens_f = tokens.astype(jnp.float32)
    h_one = tokens_f + jnp.einsum(
        "sci,io->sco", joined, full_out, preferred_element_type=jnp.float32
    )
    x_one, normed_one, inverse_one = norm_fwd(
        h_one, gain_one.astype(jnp.float32), bias_one.astype(jnp.float32)
    )
    x_low = x_one.astype(jnp.bfloat16)
    gate_pre = jnp.einsum("scd,df->scf", x_low, full_gate, preferred_element_type=jnp.float32)
    up_pre = jnp.einsum("scd,df->scf", x_low, full_up, preferred_element_type=jnp.float32)
    sigma = jax.nn.sigmoid(gate_pre)
    smooth = gate_pre * sigma
    hidden = (smooth * up_pre).astype(jnp.bfloat16)
    h_two = x_one + jnp.einsum("scf,fd->scd", hidden, full_down, preferred_element_type=jnp.float32)
    result, normed_two, inverse_two = norm_fwd(
        h_two, gain_two.astype(jnp.float32), bias_two.astype(jnp.float32)
    )
    output = result.astype(jnp.bfloat16)
    regathered = (
        lax.all_gather(w_qkv, "shard", axis=0, tiled=True),
        lax.all_gather(w_out, "shard", axis=0, tiled=True),
        lax.all_gather(w_gate, "shard", axis=0, tiled=True),
        lax.all_gather(w_up, "shard", axis=0, tiled=True),
        lax.all_gather(w_down, "shard", axis=0, tiled=True),
        lax.all_gather(ln1_gain, "shard", axis=0, tiled=True),
        lax.all_gather(ln2_gain, "shard", axis=0, tiled=True),
    )
    back_qkv, back_out, back_gate, back_up, back_down, back_gain_one, back_gain_two = regathered
    back_k, back_v = (
        lax.all_gather(k_local, "seq", axis=1, tiled=True),
        lax.all_gather(v_local, "seq", axis=1, tiled=True),
    )
    cot_f = cotangent.astype(jnp.float32)
    grad_gain_two = jnp.sum(cot_f * normed_two, axis=(0, 1))
    grad_bias_two = jnp.sum(cot_f, axis=(0, 1))
    dh_two = norm_back(cot_f, normed_two, inverse_two, back_gain_two.astype(jnp.float32))
    dm_low = dh_two.astype(jnp.bfloat16)
    grad_down = jnp.einsum("scf,scd->fd", hidden, dm_low, preferred_element_type=jnp.float32)
    d_hidden = jnp.einsum("scd,fd->scf", dm_low, back_down, preferred_element_type=jnp.float32)
    d_up = (d_hidden * smooth).astype(jnp.bfloat16)
    d_gate = (d_hidden * up_pre * sigma * (1.0 + gate_pre * (1.0 - sigma))).astype(jnp.bfloat16)
    grad_gate = jnp.einsum("scd,scf->df", x_low, d_gate, preferred_element_type=jnp.float32)
    grad_up = jnp.einsum("scd,scf->df", x_low, d_up, preferred_element_type=jnp.float32)
    dx_one = (
        dh_two
        + jnp.einsum("scf,df->scd", d_gate, back_gate, preferred_element_type=jnp.float32)
        + jnp.einsum("scf,df->scd", d_up, back_up, preferred_element_type=jnp.float32)
    )
    grad_gain_one = jnp.sum(dx_one * normed_one, axis=(0, 1))
    grad_bias_one = jnp.sum(dx_one, axis=(0, 1))
    dh_one = norm_back(dx_one, normed_one, inverse_one, back_gain_one.astype(jnp.float32))
    d_attn = dh_one.astype(jnp.bfloat16)
    grad_out = jnp.einsum("sci,sco->io", joined, d_attn, preferred_element_type=jnp.float32)
    d_joined = jnp.einsum(
        "sco,io->sci", d_attn, back_out, preferred_element_type=jnp.float32
    ).astype(jnp.bfloat16)
    d_heads = head_split(d_joined, seq_count, row_count).astype(jnp.float32)
    g_heads = (d_heads / denom).astype(jnp.bfloat16)
    delta = jnp.transpose(jnp.sum(d_heads * attn_out, axis=-1) / denom[..., 0], (0, 2, 1))
    q_grad, k_all, v_all = back_keys(
        q_heads, g_heads, delta, q_seg, back_k, back_v, segments, row_count, score_scale
    )
    k_sum, v_sum = (
        lax.psum_scatter(k_all.astype(jnp.bfloat16), "seq", scatter_dimension=1, tiled=True).astype(
            jnp.float32
        ),
        lax.psum_scatter(v_all.astype(jnp.bfloat16), "seq", scatter_dimension=1, tiled=True).astype(
            jnp.float32
        ),
    )
    k_grad = head_split(k_sum, seq_count, row_count)
    v_grad = head_split(v_sum, seq_count, row_count)
    q_back = rotate_back(q_grad, cos_b, sin_b).reshape(seq_count, row_count, model_width)
    k_back = rotate_back(k_grad, cos_b, sin_b).reshape(seq_count, row_count, model_width)
    d_qkv = jnp.concatenate(
        [q_back, k_back, v_grad.reshape(seq_count, row_count, model_width)], axis=-1
    ).astype(jnp.bfloat16)
    grad_qkv = jnp.einsum("scd,sce->de", tokens, d_qkv, preferred_element_type=jnp.float32)
    d_tokens = dh_one + jnp.einsum(
        "sce,de->scd", d_qkv, back_qkv, preferred_element_type=jnp.float32
    )
    input_grad = d_tokens.astype(jnp.bfloat16)
    owned = (
        lax.psum_scatter(
            grad_qkv.astype(jnp.bfloat16), "shard", scatter_dimension=0, tiled=True
        ).astype(jnp.float32),
        lax.psum_scatter(
            grad_out.astype(jnp.bfloat16), "shard", scatter_dimension=0, tiled=True
        ).astype(jnp.float32),
        lax.psum_scatter(
            grad_gate.astype(jnp.bfloat16), "shard", scatter_dimension=0, tiled=True
        ).astype(jnp.float32),
        lax.psum_scatter(
            grad_up.astype(jnp.bfloat16), "shard", scatter_dimension=0, tiled=True
        ).astype(jnp.float32),
        lax.psum_scatter(
            grad_down.astype(jnp.bfloat16), "shard", scatter_dimension=0, tiled=True
        ).astype(jnp.float32),
        lax.psum_scatter(
            grad_gain_one.astype(jnp.bfloat16), "shard", scatter_dimension=0, tiled=True
        ).astype(jnp.float32),
        lax.psum_scatter(
            grad_bias_one.astype(jnp.bfloat16), "shard", scatter_dimension=0, tiled=True
        ).astype(jnp.float32),
        lax.psum_scatter(
            grad_gain_two.astype(jnp.bfloat16), "shard", scatter_dimension=0, tiled=True
        ).astype(jnp.float32),
        lax.psum_scatter(
            grad_bias_two.astype(jnp.bfloat16), "shard", scatter_dimension=0, tiled=True
        ).astype(jnp.float32),
    )
    summed = (
        lax.psum(owned[0].astype(jnp.bfloat16), "seq").astype(jnp.float32),
        lax.psum(owned[1].astype(jnp.bfloat16), "seq").astype(jnp.float32),
        lax.psum(owned[2].astype(jnp.bfloat16), "seq").astype(jnp.float32),
        lax.psum(owned[3].astype(jnp.bfloat16), "seq").astype(jnp.float32),
        lax.psum(owned[4].astype(jnp.bfloat16), "seq").astype(jnp.float32),
        lax.psum(owned[5].astype(jnp.bfloat16), "seq").astype(jnp.float32),
        lax.psum(owned[6].astype(jnp.bfloat16), "seq").astype(jnp.float32),
        lax.psum(owned[7].astype(jnp.bfloat16), "seq").astype(jnp.float32),
        lax.psum(owned[8].astype(jnp.bfloat16), "seq").astype(jnp.float32),
    )
    return (
        output,
        input_grad,
        summed[0],
        summed[1],
        summed[2],
        summed[3],
        summed[4],
        summed[5],
        summed[6],
        summed[7],
        summed[8],
    )


SEQS_HELD = 2
LANES = 128
LOG2E = 1.4426950408889634
LN2 = 0.6931471805599453
FAR = 2.0**30
F32 = jnp.float32
BF16 = jnp.bfloat16
VMEM_LIMIT = 60 * 1024 * 1024


def key_ranges(seg_row, rows, window, align):
    length = seg_row.shape[0]
    first = seg_row[::rows]
    last = seg_row[rows - 1 :: rows]
    low = jnp.sum((seg_row[None, :] < first[:, None]).astype(jnp.int32), axis=1)
    high = jnp.sum((seg_row[None, :] <= last[:, None]).astype(jnp.int32), axis=1)
    low = low // align * align
    count = (high - low + window - 1) // window
    low = jnp.minimum(low, length - count * window)
    return low.astype(jnp.int32), count.astype(jnp.int32)


def attend_kernel(window, align, low_ref, count_ref, q_ref, k_ref, v_ref, sum_ref):
    block = pl.program_id(0)
    low = low_ref[block]
    sum_ref[...] = jnp.zeros_like(sum_ref)

    def step(index, carry):
        start = pl.multiple_of(low + index * window, align)
        for head in range(q_ref.shape[0]):
            k_part = k_ref[head, pl.ds(start, window), :]
            v_part = v_ref[head, pl.ds(start, window), :]
            score = lax.dot_general(
                q_ref[head], k_part, (((1,), (1,)), ((), ())), preferred_element_type=F32
            )
            expo = jnp.exp2(score).astype(BF16)
            sum_ref[head] += jnp.dot(expo, v_part, preferred_element_type=F32)
        return carry

    lax.fori_loop(0, count_ref[block], step, 0)


def attend_heads(seg_row, q_ext, k_ext, v_ext, rows=512, window=1024, align=16):
    heads, length, lanes = q_ext.shape
    low, count = key_ranges(seg_row, rows, window, align)
    whole = pl.BlockSpec((heads, length, lanes), lambda i, *_: (0, 0, 0))
    part = pl.BlockSpec((heads, rows, lanes), lambda i, *_: (0, i, 0))
    return pl.pallas_call(
        functools.partial(attend_kernel, window, align),
        out_shape=jax.ShapeDtypeStruct((heads, length, lanes), F32),
        grid_spec=pltpu.PrefetchScalarGridSpec(
            num_scalar_prefetch=2,
            grid=(length // rows,),
            in_specs=[part, whole, whole],
            out_specs=part,
        ),
        compiler_params=pltpu.CompilerParams(vmem_limit_bytes=VMEM_LIMIT),
        cost_estimate=pl.CostEstimate(
            flops=heads * length * length * 4 * lanes // 2,
            bytes_accessed=heads * length * lanes * 10,
            transcendentals=heads * length * length // 2,
        ),
        name="attend_heads",
    )(low, count, q_ext, k_ext, v_ext)


def attend_back_kernel(
    window, align, low_ref, count_ref, q_ref, g_ref, qt_ref, gt_ref, k_ref, v_ref, dq_ref, dkt_ref, dvt_ref
):
    block = pl.program_id(0)

    @pl.when(block == 0)
    def _():
        dkt_ref[...] = jnp.zeros_like(dkt_ref)
        dvt_ref[...] = jnp.zeros_like(dvt_ref)

    dq_ref[...] = jnp.zeros_like(dq_ref)
    low = low_ref[block]
    by_lanes = (((1,), (1,)), ((), ()))

    def step(index, carry):
        start = pl.multiple_of(low + index * window, align)
        for head in range(q_ref.shape[0]):
            k_part = k_ref[head, pl.ds(start, window), :]
            v_part = v_ref[head, pl.ds(start, window), :]
            score = lax.dot_general(q_ref[head], k_part, by_lanes, preferred_element_type=F32)
            slope = lax.dot_general(g_ref[head], v_part, by_lanes, preferred_element_type=F32)
            expo = jnp.exp2(score)
            d_score = (expo * slope).astype(BF16)
            expo = expo.astype(BF16)
            dq_ref[head] += jnp.dot(d_score, k_part, preferred_element_type=F32)
            dvt_ref[head, :, pl.ds(start, window)] += jnp.dot(gt_ref[head], expo, preferred_element_type=F32)
            dkt_ref[head, :, pl.ds(start, window)] += jnp.dot(qt_ref[head], d_score, preferred_element_type=F32)
        return carry

    lax.fori_loop(0, count_ref[block], step, 0)


def attend_back_heads(seg_row, q_ext, k_ext, v_ext, g_ext, rows=512, window=512, align=128):
    heads, length, lanes = q_ext.shape
    low, count = key_ranges(seg_row, rows, window, align)
    q_turned = jnp.swapaxes(q_ext[:, :, :HD], 1, 2)
    g_turned = jnp.swapaxes(g_ext[:, :, :HD], 1, 2)
    whole = pl.BlockSpec((heads, length, lanes), lambda i, *_: (0, 0, 0))
    part = pl.BlockSpec((heads, rows, lanes), lambda i, *_: (0, i, 0))
    turned_part = pl.BlockSpec((heads, HD, rows), lambda i, *_: (0, 0, i))
    turned = pl.BlockSpec((heads, HD, length), lambda i, *_: (0, 0, 0))
    return pl.pallas_call(
        functools.partial(attend_back_kernel, window, align),
        out_shape=(
            jax.ShapeDtypeStruct((heads, length, lanes), F32),
            jax.ShapeDtypeStruct((heads, HD, length), F32),
            jax.ShapeDtypeStruct((heads, HD, length), F32),
        ),
        grid_spec=pltpu.PrefetchScalarGridSpec(
            num_scalar_prefetch=2,
            grid=(length // rows,),
            in_specs=[part, part, turned_part, turned_part, whole, whole],
            out_specs=(part, turned, turned),
        ),
        compiler_params=pltpu.CompilerParams(vmem_limit_bytes=VMEM_LIMIT),
        cost_estimate=pl.CostEstimate(
            flops=heads * length * length * 10 * lanes // 2,
            bytes_accessed=heads * length * lanes * 20,
            transcendentals=heads * length * length // 2,
        ),
        name="attend_back_heads",
    )(low, count, q_ext, g_ext, q_turned, g_turned, k_ext, v_ext)


def document_places(seg_row):
    length = seg_row.shape[0]
    ids = jnp.arange(LANES - HD, dtype=jnp.int32)
    starts = jnp.sum((seg_row[None, :] < ids[:, None]).astype(jnp.int32), axis=1)
    same = seg_row[:, None] == ids[None, :]
    start = jnp.sum(jnp.where(same, starts[None, :], 0), axis=1)
    return same, jnp.arange(length, dtype=jnp.int32) - start


def by_group(block_rows, groups):
    seqs, rows, width = block_rows.shape
    split = block_rows.reshape(seqs, rows, groups, width // groups)
    return jnp.transpose(split, (0, 2, 1, 3)).reshape(seqs * groups, rows, width // groups)


def from_group(blocks, groups):
    devices, rows, width = blocks.shape
    split = blocks.reshape(devices // groups, groups, rows, width)
    return jnp.transpose(split, (0, 2, 1, 3)).reshape(devices // groups, rows, groups * width)


def exchange(blocks):
    return lax.all_to_all(blocks, "seq", 0, 0, tiled=True)


def local_heads(
    seq_size,
    tokens,
    segments,
    positions,
    cotangent,
    w_qkv,
    w_out,
    w_gate,
    w_up,
    w_down,
    ln1_gain,
    ln1_bias,
    ln2_gain,
    ln2_bias,
):
    seq_count, row_count, model_width = tokens.shape
    groups = seq_size // seq_count
    held = HEADS // groups
    length = row_count * seq_size
    score_scale = HD ** (-0.5)
    my_seq = lax.axis_index("seq") // groups
    seg_row = lax.dynamic_index_in_dim(segments, my_seq, 0, keepdims=False)

    def gather(shard):
        return lax.all_gather(shard, "shard", axis=0, tiled=True)

    full_qkv = gather(w_qkv)
    norms = gather(jnp.stack([ln1_gain, ln1_bias, ln2_gain, ln2_bias], axis=1)).astype(F32)
    gain_one, bias_one, gain_two, bias_two = (norms[:, n] for n in range(4))
    full_out, full_gate, full_up, full_down = (gather(w) for w in (w_out, w_gate, w_up, w_down))

    cos_b, sin_b = rope_tables(positions)
    qkv_all = jnp.einsum("scd,de->sce", tokens, full_qkv, preferred_element_type=F32)
    q_heads = rotate(head_split(qkv_all[..., :model_width], seq_count, row_count), cos_b, sin_b)
    k_heads = rotate(
        head_split(qkv_all[..., model_width : 2 * model_width], seq_count, row_count), cos_b, sin_b
    )
    q_low = (q_heads * (score_scale * LOG2E)).astype(BF16).reshape(seq_count, row_count, model_width)
    k_low = k_heads.astype(BF16).reshape(seq_count, row_count, model_width)
    v_low = qkv_all[..., 2 * model_width :].astype(BF16)
    sent = jnp.concatenate([by_group(part, groups) for part in (q_low, k_low, v_low)], axis=-1)
    taken = exchange(sent).reshape(length, 3, held, HD)

    same, place = document_places(seg_row)
    own = jnp.broadcast_to(same.astype(BF16), (held, length, LANES - HD))
    other = jnp.broadcast_to(jnp.where(same, 0.0, -FAR).astype(BF16), (held, length, LANES - HD))
    ones = jnp.ones((held, length, LANES - HD), BF16)
    q_own, k_own, v_own = (jnp.transpose(taken[:, n], (1, 0, 2)) for n in range(3))
    q_ext = jnp.concatenate([q_own, own], axis=-1)
    k_ext = jnp.concatenate([k_own, other], axis=-1)
    v_ext = jnp.concatenate([v_own, ones], axis=-1)
    sums = attend_heads(seg_row, q_ext, k_ext, v_ext)
    total = sums[..., HD : HD + 1]
    o_own = sums[..., :HD] / total
    joined_own = jnp.transpose(o_own, (1, 0, 2)).astype(BF16).reshape(seq_size, row_count, held * HD)
    joined = from_group(exchange(joined_own), groups)

    tokens_f = tokens.astype(F32)
    h_one = tokens_f + jnp.einsum("sci,io->sco", joined, full_out, preferred_element_type=F32)
    x_one, normed_one, inverse_one = norm_fwd(h_one, gain_one, bias_one)
    x_low = x_one.astype(BF16)
    gate_pre = jnp.einsum("scd,df->scf", x_low, full_gate, preferred_element_type=F32)
    up_pre = jnp.einsum("scd,df->scf", x_low, full_up, preferred_element_type=F32)
    sigma = jax.nn.sigmoid(gate_pre)
    smooth = gate_pre * sigma
    hidden = (smooth * up_pre).astype(BF16)
    h_two = x_one + jnp.einsum("scf,fd->scd", hidden, full_down, preferred_element_type=F32)
    result, normed_two, inverse_two = norm_fwd(h_two, gain_two, bias_two)
    output = result.astype(BF16)

    cot_f = cotangent.astype(F32)
    grad_gain_two = jnp.sum(cot_f * normed_two, axis=(0, 1))
    grad_bias_two = jnp.sum(cot_f, axis=(0, 1))
    dh_two = norm_back(cot_f, normed_two, inverse_two, gain_two)
    dm_low = dh_two.astype(BF16)
    d_hidden = jnp.einsum("scd,fd->scf", dm_low, full_down, preferred_element_type=F32)
    d_up = (d_hidden * smooth).astype(BF16)
    d_gate = (d_hidden * up_pre * sigma * (1.0 + gate_pre * (1.0 - sigma))).astype(BF16)
    dx_one = (
        dh_two
        + jnp.einsum("scf,df->scd", d_gate, full_gate, preferred_element_type=F32)
        + jnp.einsum("scf,df->scd", d_up, full_up, preferred_element_type=F32)
    )
    grad_gain_one = jnp.sum(dx_one * normed_one, axis=(0, 1))
    grad_bias_one = jnp.sum(dx_one, axis=(0, 1))
    dh_one = norm_back(dx_one, normed_one, inverse_one, gain_one)
    d_attn = dh_one.astype(BF16)
    d_joined = jnp.einsum("sco,io->sci", d_attn, full_out, preferred_element_type=F32).astype(BF16)

    grad_down = jnp.einsum("scf,scd->fd", hidden, dm_low, preferred_element_type=F32).astype(BF16)
    grad_gate = jnp.einsum("scd,scf->df", x_low, d_gate, preferred_element_type=F32).astype(BF16)
    grad_up = jnp.einsum("scd,scf->df", x_low, d_up, preferred_element_type=F32).astype(BF16)
    grad_out = jnp.einsum("sci,sco->io", joined, d_attn, preferred_element_type=F32).astype(BF16)
    grad_norms = jnp.stack([grad_gain_one, grad_bias_one, grad_gain_two, grad_bias_two], axis=1)

    def reduce_shards(partial):
        return lax.psum_scatter(partial, "shard", scatter_dimension=0, tiled=True)

    d_joined, grad_down, grad_gate, grad_up, grad_out = lax.optimization_barrier(
        (d_joined, grad_down, grad_gate, grad_up, grad_out)
    )
    owned = [reduce_shards(g) for g in (grad_out, grad_gate, grad_up, grad_down)]

    dout = exchange(by_group(d_joined, groups)).reshape(length, held, HD)
    dout = jnp.transpose(dout, (1, 0, 2)).astype(F32)
    g_low = (dout / total).astype(BF16)
    delta = -jnp.sum(dout * o_own, axis=-1, keepdims=True) / total
    d_high = delta.astype(BF16)
    d_mid = (delta - d_high.astype(F32)).astype(BF16)
    d_small = (delta - d_high.astype(F32) - d_mid.astype(F32)).astype(BF16)
    g_ext = jnp.concatenate(
        [g_low, d_high, d_mid, d_small, jnp.zeros((held, length, LANES - HD - 3), BF16)], axis=-1
    )
    dq, dk_turned, dv_turned = attend_back_heads(seg_row, q_ext, k_ext, v_ext, g_ext)

    cos_f, sin_f = (t[0] for t in rope_tables(place[None]))
    dq_own = jnp.transpose(dq[..., :HD], (1, 0, 2)) * score_scale
    dk_own = jnp.transpose(dk_turned, (2, 0, 1)) * LN2
    dv_own = jnp.transpose(dv_turned, (2, 0, 1))
    d_parts = [
        part.astype(BF16).reshape(seq_size, row_count, held * HD)
        for part in (rotate_back(dq_own, cos_f, sin_f), rotate_back(dk_own, cos_f, sin_f), dv_own)
    ]
    d_taken = exchange(jnp.concatenate(d_parts, axis=-1))
    d_split = d_taken.reshape(seq_count, groups, row_count, 3, held * HD)
    d_qkv = jnp.transpose(d_split, (0, 2, 3, 1, 4)).reshape(seq_count, row_count, 3 * model_width)
    grad_qkv = jnp.einsum("scd,sce->de", tokens, d_qkv, preferred_element_type=F32).astype(BF16)
    d_tokens = dh_one + jnp.einsum("sce,de->scd", d_qkv, full_qkv, preferred_element_type=F32)
    input_grad = d_tokens.astype(BF16)

    grad_out, grad_gate, grad_up, grad_down = (lax.psum(g, "seq").astype(F32) for g in owned)
    grad_qkv = lax.psum(reduce_shards(grad_qkv), "seq").astype(F32)
    norm_sums = lax.psum(reduce_shards(grad_norms), "seq")
    return (
        output,
        input_grad,
        grad_qkv,
        grad_out,
        grad_gate,
        grad_up,
        grad_down,
        norm_sums[:, 0],
        norm_sums[:, 1],
        norm_sums[:, 2],
        norm_sums[:, 3],
    )


def solution(mesh):
    in_specs = (
        P("shard", "seq", None),
        P("shard", None),
        P("shard", "seq"),
        P("shard", "seq", None),
        P("shard", None),
        P("shard", None),
        P("shard", None),
        P("shard", None),
        P("shard", None),
        P("shard"),
        P("shard"),
        P("shard"),
        P("shard"),
    )
    out_specs = (
        P("shard", "seq", None),
        P("shard", "seq", None),
        P("shard", None),
        P("shard", None),
        P("shard", None),
        P("shard", None),
        P("shard", None),
        P("shard"),
        P("shard"),
        P("shard"),
        P("shard"),
    )
    heads_split = mesh.shape["seq"] % SEQS_HELD == 0 and HEADS % (mesh.shape["seq"] // SEQS_HELD) == 0
    body = functools.partial(local_heads, mesh.shape["seq"]) if heads_split else local
    return jax.shard_map(body, mesh=mesh, in_specs=in_specs, out_specs=out_specs, check_vma=False)
```

```python
import functools
import math

import jax
import jax.numpy as jnp
from jax import lax
from jax.experimental import pallas as pl
from jax.experimental.pallas import tpu as pltpu
from jax.sharding import PartitionSpec as P

HEADS = 12
HD = 64


EPS = 1e-05
ROPE_BASE = 1000.0


def rope_tables(pos_block):
    half_dim = HD // 2
    freqs = jnp.exp(jnp.arange(half_dim, dtype=jnp.float32) * (-math.log(ROPE_BASE) / half_dim))
    angle = pos_block.astype(jnp.float32)[..., None] * freqs
    return (jnp.cos(angle)[:, :, None, :], jnp.sin(angle)[:, :, None, :])


def rotate(heads, cos_b, sin_b):
    half_dim = heads.shape[-1] // 2
    first = heads[..., :half_dim]
    second = heads[..., half_dim:]
    return jnp.concatenate(
        [first * cos_b - second * sin_b, second * cos_b + first * sin_b], axis=-1
    )


def rotate_back(grads, cos_b, sin_b):
    half_dim = grads.shape[-1] // 2
    first = grads[..., :half_dim]
    second = grads[..., half_dim:]
    return jnp.concatenate(
        [first * cos_b + second * sin_b, second * cos_b - first * sin_b], axis=-1
    )


def norm_fwd(values, gain, bias):
    mean_val = jnp.mean(values, axis=-1, keepdims=True)
    centered = values - mean_val
    variance = jnp.mean(centered * centered, axis=-1, keepdims=True)
    inverse = lax.rsqrt(variance + EPS)
    normed = centered * inverse
    return (normed * gain + bias, normed, inverse)


def norm_back(grad_in, normed, inverse, gain):
    scaled = grad_in * gain
    return inverse * (
        scaled
        - jnp.mean(scaled, axis=-1, keepdims=True)
        - normed * jnp.mean(scaled * normed, axis=-1, keepdims=True)
    )


def head_split(block_rows, seq_count, row_count):
    return block_rows.reshape(seq_count, row_count, HEADS, HD)


def attend(q_heads, q_seg, k_full, v_full, seg_all, block, score_scale):
    seq_count, row_count = (q_heads.shape[0], q_heads.shape[1])
    block_count = k_full.shape[1] // block

    def attend_step(carry, index):
        row_total, value_sum = carry
        start = index * block
        k_part = head_split(lax.dynamic_slice_in_dim(k_full, start, block, 1), seq_count, block)
        v_part = head_split(lax.dynamic_slice_in_dim(v_full, start, block, 1), seq_count, block)
        seg_part = lax.dynamic_slice_in_dim(seg_all, start, block, 1)
        raw = (
            jnp.einsum("sqhd,skhd->shqk", q_heads, k_part, preferred_element_type=jnp.float32)
            * score_scale
        )
        same_doc = q_seg[:, None, :, None] == seg_part[:, None, None, :]
        expo = jnp.where(same_doc, jnp.exp(raw), 0.0)
        row_total = row_total + jnp.sum(expo, axis=-1)
        value_sum = value_sum + jnp.einsum(
            "shqk,skhd->sqhd", expo.astype(jnp.bfloat16), v_part, preferred_element_type=jnp.float32
        )
        return ((row_total, value_sum), None)

    start_carry = (
        jnp.zeros((seq_count, HEADS, row_count), jnp.float32),
        jnp.zeros((seq_count, row_count, HEADS, HD), jnp.float32),
    )
    final, unused = lax.scan(attend_step, start_carry, jnp.arange(block_count, dtype=jnp.int32))
    return final


def back_keys(q_heads, g_heads, delta, q_seg, k_full, v_full, seg_all, block, score_scale):
    seq_count, row_count = (q_heads.shape[0], q_heads.shape[1])
    full_len = k_full.shape[1]
    block_count = full_len // block

    def back_step(carry, index):
        start = index * block
        k_part = head_split(lax.dynamic_slice_in_dim(k_full, start, block, 1), seq_count, block)
        v_part = head_split(lax.dynamic_slice_in_dim(v_full, start, block, 1), seq_count, block)
        seg_part = lax.dynamic_slice_in_dim(seg_all, start, block, 1)
        raw = (
            jnp.einsum("sqhd,skhd->shqk", q_heads, k_part, preferred_element_type=jnp.float32)
            * score_scale
        )
        same_doc = q_seg[:, None, :, None] == seg_part[:, None, None, :]
        expo = jnp.where(same_doc, jnp.exp(raw), 0.0)
        prob_grad = jnp.einsum(
            "sqhd,skhd->shqk", g_heads, v_part, preferred_element_type=jnp.float32
        )
        d_score = (expo * (prob_grad - delta[..., None])).astype(jnp.bfloat16)
        q_grad = carry[0] + jnp.einsum(
            "shqk,skhd->sqhd", d_score, k_part, preferred_element_type=jnp.float32
        )
        k_grad = (
            jnp.einsum("shqk,sqhd->skhd", d_score, q_heads, preferred_element_type=jnp.float32)
            * score_scale
        )
        v_grad = jnp.einsum(
            "shqk,sqhd->skhd",
            expo.astype(jnp.bfloat16),
            g_heads,
            preferred_element_type=jnp.float32,
        )
        k_store = lax.dynamic_update_slice_in_dim(
            carry[1], k_grad.reshape(seq_count, block, HEADS * HD), start, 1
        )
        v_store = lax.dynamic_update_slice_in_dim(
            carry[2], v_grad.reshape(seq_count, block, HEADS * HD), start, 1
        )
        return ((q_grad, k_store, v_store), None)

    q_zero = jnp.zeros((seq_count, row_count, HEADS, HD), jnp.float32)
    kv_zero = jnp.zeros((seq_count, full_len, HEADS * HD), jnp.float32)
    start_carry = (q_zero, kv_zero, kv_zero)
    final, unused = lax.scan(back_step, start_carry, jnp.arange(block_count, dtype=jnp.int32))
    return (final[0] * score_scale,) + tuple(final[1:])


def local(
    tokens,
    segments,
    positions,
    cotangent,
    w_qkv,
    w_out,
    w_gate,
    w_up,
    w_down,
    ln1_gain,
    ln1_bias,
    ln2_gain,
    ln2_bias,
):
    seq_count, row_count, model_width = tokens.shape
    score_scale = HD ** (-0.5)
    q_seg = lax.dynamic_slice_in_dim(segments, lax.axis_index("seq") * row_count, row_count, 1)
    gathered = (
        lax.all_gather(w_qkv, "shard", axis=0, tiled=True),
        lax.all_gather(w_out, "shard", axis=0, tiled=True),
        lax.all_gather(w_gate, "shard", axis=0, tiled=True),
        lax.all_gather(w_up, "shard", axis=0, tiled=True),
        lax.all_gather(w_down, "shard", axis=0, tiled=True),
        lax.all_gather(ln1_gain, "shard", axis=0, tiled=True),
        lax.all_gather(ln1_bias, "shard", axis=0, tiled=True),
        lax.all_gather(ln2_gain, "shard", axis=0, tiled=True),
        lax.all_gather(ln2_bias, "shard", axis=0, tiled=True),
    )
    full_qkv, full_out, full_gate, full_up, full_down, gain_one, bias_one, gain_two, bias_two = (
        gathered
    )
    cos_b, sin_b = rope_tables(positions)
    qkv_all = jnp.einsum("scd,de->sce", tokens, full_qkv, preferred_element_type=jnp.float32)
    q_heads = rotate(
        head_split(qkv_all[..., :model_width], seq_count, row_count), cos_b, sin_b
    ).astype(jnp.bfloat16)
    k_heads = rotate(
        head_split(qkv_all[..., model_width : 2 * model_width], seq_count, row_count), cos_b, sin_b
    ).astype(jnp.bfloat16)
    v_heads = head_split(qkv_all[..., 2 * model_width :], seq_count, row_count).astype(jnp.bfloat16)
    k_local = k_heads.reshape(seq_count, row_count, model_width)
    v_local = v_heads.reshape(seq_count, row_count, model_width)
    k_full, v_full = (
        lax.all_gather(k_local, "seq", axis=1, tiled=True),
        lax.all_gather(v_local, "seq", axis=1, tiled=True),
    )
    row_total, value_sum = attend(q_heads, q_seg, k_full, v_full, segments, row_count, score_scale)
    denom = jnp.transpose(row_total, (0, 2, 1))[..., None]
    attn_out = value_sum / denom
    joined = attn_out.reshape(seq_count, row_count, model_width).astype(jnp.bfloat16)
    tokens_f = tokens.astype(jnp.float32)
    h_one = tokens_f + jnp.einsum(
        "sci,io->sco", joined, full_out, preferred_element_type=jnp.float32
    )
    x_one, normed_one, inverse_one = norm_fwd(
        h_one, gain_one.astype(jnp.float32), bias_one.astype(jnp.float32)
    )
    x_low = x_one.astype(jnp.bfloat16)
    gate_pre = jnp.einsum("scd,df->scf", x_low, full_gate, preferred_element_type=jnp.float32)
    up_pre = jnp.einsum("scd,df->scf", x_low, full_up, preferred_element_type=jnp.float32)
    sigma = jax.nn.sigmoid(gate_pre)
    smooth = gate_pre * sigma
    hidden = (smooth * up_pre).astype(jnp.bfloat16)
    h_two = x_one + jnp.einsum("scf,fd->scd", hidden, full_down, preferred_element_type=jnp.float32)
    result, normed_two, inverse_two = norm_fwd(
        h_two, gain_two.astype(jnp.float32), bias_two.astype(jnp.float32)
    )
    output = result.astype(jnp.bfloat16)
    regathered = (
        lax.all_gather(w_qkv, "shard", axis=0, tiled=True),
        lax.all_gather(w_out, "shard", axis=0, tiled=True),
        lax.all_gather(w_gate, "shard", axis=0, tiled=True),
        lax.all_gather(w_up, "shard", axis=0, tiled=True),
        lax.all_gather(w_down, "shard", axis=0, tiled=True),
        lax.all_gather(ln1_gain, "shard", axis=0, tiled=True),
        lax.all_gather(ln2_gain, "shard", axis=0, tiled=True),
    )
    back_qkv, back_out, back_gate, back_up, back_down, back_gain_one, back_gain_two = regathered
    back_k, back_v = (
        lax.all_gather(k_local, "seq", axis=1, tiled=True),
        lax.all_gather(v_local, "seq", axis=1, tiled=True),
    )
    cot_f = cotangent.astype(jnp.float32)
    grad_gain_two = jnp.sum(cot_f * normed_two, axis=(0, 1))
    grad_bias_two = jnp.sum(cot_f, axis=(0, 1))
    dh_two = norm_back(cot_f, normed_two, inverse_two, back_gain_two.astype(jnp.float32))
    dm_low = dh_two.astype(jnp.bfloat16)
    grad_down = jnp.einsum("scf,scd->fd", hidden, dm_low, preferred_element_type=jnp.float32)
    d_hidden = jnp.einsum("scd,fd->scf", dm_low, back_down, preferred_element_type=jnp.float32)
    d_up = (d_hidden * smooth).astype(jnp.bfloat16)
    d_gate = (d_hidden * up_pre * sigma * (1.0 + gate_pre * (1.0 - sigma))).astype(jnp.bfloat16)
    grad_gate = jnp.einsum("scd,scf->df", x_low, d_gate, preferred_element_type=jnp.float32)
    grad_up = jnp.einsum("scd,scf->df", x_low, d_up, preferred_element_type=jnp.float32)
    dx_one = (
        dh_two
        + jnp.einsum("scf,df->scd", d_gate, back_gate, preferred_element_type=jnp.float32)
        + jnp.einsum("scf,df->scd", d_up, back_up, preferred_element_type=jnp.float32)
    )
    grad_gain_one = jnp.sum(dx_one * normed_one, axis=(0, 1))
    grad_bias_one = jnp.sum(dx_one, axis=(0, 1))
    dh_one = norm_back(dx_one, normed_one, inverse_one, back_gain_one.astype(jnp.float32))
    d_attn = dh_one.astype(jnp.bfloat16)
    grad_out = jnp.einsum("sci,sco->io", joined, d_attn, preferred_element_type=jnp.float32)
    d_joined = jnp.einsum(
        "sco,io->sci", d_attn, back_out, preferred_element_type=jnp.float32
    ).astype(jnp.bfloat16)
    d_heads = head_split(d_joined, seq_count, row_count).astype(jnp.float32)
    g_heads = (d_heads / denom).astype(jnp.bfloat16)
    delta = jnp.transpose(jnp.sum(d_heads * attn_out, axis=-1) / denom[..., 0], (0, 2, 1))
    q_grad, k_all, v_all = back_keys(
        q_heads, g_heads, delta, q_seg, back_k, back_v, segments, row_count, score_scale
    )
    k_sum, v_sum = (
        lax.psum_scatter(k_all.astype(jnp.bfloat16), "seq", scatter_dimension=1, tiled=True).astype(
            jnp.float32
        ),
        lax.psum_scatter(v_all.astype(jnp.bfloat16), "seq", scatter_dimension=1, tiled=True).astype(
            jnp.float32
        ),
    )
    k_grad = head_split(k_sum, seq_count, row_count)
    v_grad = head_split(v_sum, seq_count, row_count)
    q_back = rotate_back(q_grad, cos_b, sin_b).reshape(seq_count, row_count, model_width)
    k_back = rotate_back(k_grad, cos_b, sin_b).reshape(seq_count, row_count, model_width)
    d_qkv = jnp.concatenate(
        [q_back, k_back, v_grad.reshape(seq_count, row_count, model_width)], axis=-1
    ).astype(jnp.bfloat16)
    grad_qkv = jnp.einsum("scd,sce->de", tokens, d_qkv, preferred_element_type=jnp.float32)
    d_tokens = dh_one + jnp.einsum(
        "sce,de->scd", d_qkv, back_qkv, preferred_element_type=jnp.float32
    )
    input_grad = d_tokens.astype(jnp.bfloat16)
    owned = (
        lax.psum_scatter(
            grad_qkv.astype(jnp.bfloat16), "shard", scatter_dimension=0, tiled=True
        ).astype(jnp.float32),
        lax.psum_scatter(
            grad_out.astype(jnp.bfloat16), "shard", scatter_dimension=0, tiled=True
        ).astype(jnp.float32),
        lax.psum_scatter(
            grad_gate.astype(jnp.bfloat16), "shard", scatter_dimension=0, tiled=True
        ).astype(jnp.float32),
        lax.psum_scatter(
            grad_up.astype(jnp.bfloat16), "shard", scatter_dimension=0, tiled=True
        ).astype(jnp.float32),
        lax.psum_scatter(
            grad_down.astype(jnp.bfloat16), "shard", scatter_dimension=0, tiled=True
        ).astype(jnp.float32),
        lax.psum_scatter(
            grad_gain_one.astype(jnp.bfloat16), "shard", scatter_dimension=0, tiled=True
        ).astype(jnp.float32),
        lax.psum_scatter(
            grad_bias_one.astype(jnp.bfloat16), "shard", scatter_dimension=0, tiled=True
        ).astype(jnp.float32),
        lax.psum_scatter(
            grad_gain_two.astype(jnp.bfloat16), "shard", scatter_dimension=0, tiled=True
        ).astype(jnp.float32),
        lax.psum_scatter(
            grad_bias_two.astype(jnp.bfloat16), "shard", scatter_dimension=0, tiled=True
        ).astype(jnp.float32),
    )
    summed = (
        lax.psum(owned[0].astype(jnp.bfloat16), "seq").astype(jnp.float32),
        lax.psum(owned[1].astype(jnp.bfloat16), "seq").astype(jnp.float32),
        lax.psum(owned[2].astype(jnp.bfloat16), "seq").astype(jnp.float32),
        lax.psum(owned[3].astype(jnp.bfloat16), "seq").astype(jnp.float32),
        lax.psum(owned[4].astype(jnp.bfloat16), "seq").astype(jnp.float32),
        lax.psum(owned[5].astype(jnp.bfloat16), "seq").astype(jnp.float32),
        lax.psum(owned[6].astype(jnp.bfloat16), "seq").astype(jnp.float32),
        lax.psum(owned[7].astype(jnp.bfloat16), "seq").astype(jnp.float32),
        lax.psum(owned[8].astype(jnp.bfloat16), "seq").astype(jnp.float32),
    )
    return (
        output,
        input_grad,
        summed[0],
        summed[1],
        summed[2],
        summed[3],
        summed[4],
        summed[5],
        summed[6],
        summed[7],
        summed[8],
    )


SEQS_HELD = 2
SEQ_SIZE = 8
GROUPS = 4
LANES = 128
LOG2E = 1.4426950408889634
LN2 = 0.6931471805599453
FAR = 2.0**30
F32 = jnp.float32
BF16 = jnp.bfloat16
VMEM_LIMIT = 60 * 1024 * 1024
BY_MESH = pl.DeviceIdType.MESH
BY_LANES = (((1,), (1,)), ((), ()))


def flip(index, bit):
    return index + bit - 2 * bit * lax.rem(lax.div(index, bit), 2)


def gather_kernel(chunks, by_z, tok_ref, w_ref, all_ref, w_all_ref, send, recv, kept, w_send, w_recv):
    me = lax.axis_index("seq")
    shard = lax.axis_index("shard")
    shards = w_all_ref.shape[0]
    half = lax.div(me, GROUPS)
    y_near, z_near, partner = flip(me, 1), flip(me, 2), flip(me, 4)
    barrier = pltpu.get_barrier_semaphore()
    for device in (y_near, z_near, partner):
        pl.semaphore_signal(barrier, inc=1, device_id={"seq": device}, device_id_type=BY_MESH)
    for step in range(1, shards):
        pl.semaphore_signal(
            barrier, inc=1, device_id={"shard": lax.rem(shard + step, shards)}, device_id_type=BY_MESH
        )
    pl.semaphore_wait(barrier, 2 + shards)

    part = tok_ref.shape[1] // chunks
    started = []

    def go(source, target, slot, device):
        copy = pltpu.make_async_remote_copy(
            src_ref=source,
            dst_ref=target,
            send_sem=send.at[slot],
            recv_sem=recv.at[slot],
            device_id={"seq": device},
            device_id_type=BY_MESH,
        )
        copy.start()
        started.append(copy)
        return copy

    def rows(chunk):
        return pl.ds(chunk * part, part)

    def relay(piece, chunk, slot, device):
        return go(all_ref.at[piece, rows(chunk)], all_ref.at[piece, rows(chunk)], slot * chunks + chunk, device)

    def own(which, chunk, slot, device):
        return go(tok_ref.at[which, rows(chunk)], all_ref.at[me, rows(chunk)], slot * chunks + chunk, device)

    crossing = [own(1 - half, chunk, 0, partner) for chunk in range(chunks)]
    own_y, own_z = [], []
    for chunk in range(chunks):
        own_y.append(own(half, chunk, 1, y_near))
        own_z.append(own(half, chunk, 2, z_near))
    weights = []
    for step in range(1, shards):
        copy = pltpu.make_async_remote_copy(
            src_ref=w_ref,
            dst_ref=w_all_ref.at[shard],
            send_sem=w_send.at[step],
            recv_sem=w_recv.at[step],
            device_id={"shard": lax.rem(shard + step, shards)},
            device_id_type=BY_MESH,
        )
        copy.start()
        weights.append(copy)
    keep_tok = pltpu.make_async_copy(tok_ref.at[half], all_ref.at[me], kept.at[0])
    keep_tok.start()
    keep_w = pltpu.make_async_copy(w_ref, w_all_ref.at[shard], kept.at[1])
    keep_w.start()

    cross_y, cross_z, corner = [], [], []
    for chunk in range(chunks):
        own_y[chunk].wait_recv()
        if chunk < by_z:
            corner.append(relay(y_near, chunk, 5, z_near))
        own_z[chunk].wait_recv()
        if chunk >= by_z:
            corner.append(relay(z_near, chunk, 5, y_near))
        crossing[chunk].wait_recv()
        cross_y.append(relay(partner, chunk, 3, y_near))
        cross_z.append(relay(partner, chunk, 4, z_near))
    for chunk in range(chunks):
        cross_y[chunk].wait_recv()
        if chunk < by_z:
            corner.append(relay(flip(y_near, 4), chunk, 6, z_near))
        cross_z[chunk].wait_recv()
        if chunk >= by_z:
            corner.append(relay(flip(z_near, 4), chunk, 6, y_near))
    for copy in corner:
        copy.wait_recv()
    for copy in weights:
        copy.wait()
    keep_tok.wait()
    keep_w.wait()
    for copy in started:
        copy.wait_send()


def gather_tokens(tokens, w_part, shards, chunks=8, by_z=3):
    seqs, rows, width = tokens.shape
    anywhere = pl.BlockSpec(memory_space=pl.ANY)
    return pl.pallas_call(
        functools.partial(gather_kernel, chunks, by_z),
        out_shape=(
            jax.ShapeDtypeStruct((SEQ_SIZE, rows, width), tokens.dtype),
            jax.ShapeDtypeStruct((shards,) + w_part.shape, w_part.dtype),
        ),
        in_specs=[anywhere, anywhere],
        out_specs=(anywhere, anywhere),
        scratch_shapes=[
            pltpu.SemaphoreType.DMA((7 * chunks,)),
            pltpu.SemaphoreType.DMA((7 * chunks,)),
            pltpu.SemaphoreType.DMA((2,)),
            pltpu.SemaphoreType.DMA((shards,)),
            pltpu.SemaphoreType.DMA((shards,)),
        ],
        compiler_params=pltpu.CompilerParams(collective_id=1, has_side_effects=True),
        name="gather_tokens",
    )(tokens, w_part)


def project_kernel(seg_ref, place_ref, freq_ref, x_ref, w_ref, q_ref, k_ref, v_ref, turn_ref):
    rows = x_ref.shape[1]
    held = q_ref.shape[0]
    lane = lax.broadcasted_iota(jnp.int32, (rows, LANES), 1)
    seg = jnp.transpose(jnp.broadcast_to(seg_ref[0], (LANES, rows)))
    place = jnp.transpose(jnp.broadcast_to(place_ref[0], (LANES, rows)))
    turn = jnp.where(lane < HD, jnp.cos(place * freq_ref[...]), jnp.sin(place * freq_ref[...]))
    turn_ref[...] = turn
    cos_b = jnp.where(lane < HD, turn, 0.0)
    sin_b = jnp.where(lane < HD, pltpu.roll(turn, HD, 1), 0.0)
    sin_b = jnp.where(lane < HD // 2, -sin_b, sin_b)
    same = seg == (lane - HD).astype(F32)
    q_tail = jnp.where(same, 1.0, 0.0)
    k_tail = jnp.where(same | (lane < HD), 0.0, -FAR)
    v_tail = jnp.where(lane < HD, 0.0, 1.0)
    scale = HD ** (-0.5) * LOG2E
    q_cos, q_sin = cos_b * scale, sin_b * scale
    width = held * LANES
    for part in range(3):
        mixed = jnp.dot(x_ref[0], w_ref[:, part * width : (part + 1) * width], preferred_element_type=F32)
        for head in range(held):
            value = mixed[:, head * LANES : (head + 1) * LANES]
            if part == 0:
                value = value * q_cos + pltpu.roll(value, HD // 2, 1) * q_sin + q_tail
                q_ref[head] = value.astype(BF16)
            elif part == 1:
                value = value * cos_b + pltpu.roll(value, HD // 2, 1) * sin_b + k_tail
                k_ref[head] = value.astype(BF16)
            else:
                v_ref[head] = (value + v_tail).astype(BF16)


def project_heads(seg_row, place_row, freq, pieces, w_full, held):
    count, rows, width = pieces.shape
    length = count * rows
    row_spec = pl.BlockSpec((1, 1, rows), lambda i: (i, 0, 0))
    head_spec = pl.BlockSpec((held, rows, LANES), lambda i: (0, i, 0))
    head_shape = jax.ShapeDtypeStruct((held, length, LANES), BF16)
    return pl.pallas_call(
        project_kernel,
        out_shape=(head_shape, head_shape, head_shape, jax.ShapeDtypeStruct((length, LANES), F32)),
        grid=(count,),
        in_specs=[
            row_spec,
            row_spec,
            pl.BlockSpec((1, LANES), lambda i: (0, 0)),
            pl.BlockSpec((1, rows, width), lambda i: (i, 0, 0)),
            pl.BlockSpec(w_full.shape, lambda i: (0, 0)),
        ],
        out_specs=(head_spec, head_spec, head_spec, pl.BlockSpec((rows, LANES), lambda i: (i, 0))),
        compiler_params=pltpu.CompilerParams(vmem_limit_bytes=VMEM_LIMIT),
        cost_estimate=pl.CostEstimate(
            flops=2 * length * width * w_full.shape[1],
            bytes_accessed=length * (width * 2 + held * LANES * 6 + LANES * 4),
            transcendentals=length * LANES,
        ),
        name="project_heads",
    )(seg_row.reshape(count, 1, rows), place_row.reshape(count, 1, rows), freq, pieces, w_full)


def document_bounds(seg_row, rows):
    first = seg_row[::rows]
    last = seg_row[rows - 1 :: rows]
    low = jnp.sum((seg_row[None, :] < first[:, None]).astype(jnp.int32), axis=1)
    high = jnp.sum((seg_row[None, :] <= last[:, None]).astype(jnp.int32), axis=1)
    return low, high


def windows(bounds, length, window, align):
    low = bounds[0] // align * align
    count = (bounds[1] - low + window - 1) // window
    return jnp.minimum(low, length - count * window), count


def attend_kernel(window, align, low_ref, count_ref, q_ref, k_ref, v_ref, sum_ref, joined_ref):
    block = pl.program_id(0)
    low = low_ref[block]
    sum_ref[...] = jnp.zeros_like(sum_ref)

    def step(index, carry):
        start = pl.multiple_of(low + index * window, align)
        for head in range(q_ref.shape[0]):
            k_part = k_ref[head, pl.ds(start, window), :]
            v_part = v_ref[head, pl.ds(start, window), :]
            score = lax.dot_general(q_ref[head], k_part, BY_LANES, preferred_element_type=F32)
            expo = jnp.exp2(score).astype(BF16)
            sum_ref[head] += jnp.dot(expo, v_part, preferred_element_type=F32)
        return carry

    lax.fori_loop(0, count_ref[block], step, 0)
    for head in range(q_ref.shape[0]):
        sums = sum_ref[head]
        joined_ref[0, :, head * HD : (head + 1) * HD] = (sums[:, :HD] / sums[:, HD : HD + 1]).astype(BF16)


def attend_heads(bounds, q_ext, k_ext, v_ext, rows, window=1024, align=16):
    heads, length, lanes = q_ext.shape
    low, count = windows(bounds, length, window, align)
    whole = pl.BlockSpec((heads, length, lanes), lambda i, *_: (0, 0, 0))
    part = pl.BlockSpec((heads, rows, lanes), lambda i, *_: (0, i, 0))
    return pl.pallas_call(
        functools.partial(attend_kernel, window, align),
        out_shape=(
            jax.ShapeDtypeStruct((heads, length, lanes), F32),
            jax.ShapeDtypeStruct((length // rows, rows, heads * HD), BF16),
        ),
        grid_spec=pltpu.PrefetchScalarGridSpec(
            num_scalar_prefetch=2,
            grid=(length // rows,),
            in_specs=[part, whole, whole],
            out_specs=(part, pl.BlockSpec((1, rows, heads * HD), lambda i, *_: (i, 0, 0))),
        ),
        compiler_params=pltpu.CompilerParams(vmem_limit_bytes=VMEM_LIMIT),
        cost_estimate=pl.CostEstimate(
            flops=heads * length * length * 4 * lanes // 2,
            bytes_accessed=heads * length * lanes * 10,
            transcendentals=heads * length * length // 2,
        ),
        name="attend_heads",
    )(low, count, q_ext, k_ext, v_ext)


def attend_back_kernel(
    window,
    align,
    low_ref,
    count_ref,
    q_ref,
    sum_ref,
    dout_ref,
    turn_ref,
    k_ref,
    v_ref,
    d_ref,
    dq_ref,
    dkv_ref,
    g_ref,
    gt_ref,
    qt_ref,
):
    block = pl.program_id(0)
    heads, rows, lanes = q_ref.shape
    width = heads * HD

    @pl.when(block == 0)
    def _():
        dkv_ref[...] = jnp.zeros_like(dkv_ref)

    dq_ref[...] = jnp.zeros_like(dq_ref)
    half_lane = lax.broadcasted_iota(jnp.int32, (rows, HD), 1)
    for head in range(heads):
        dout = dout_ref[0, :, head * HD : (head + 1) * HD].astype(F32)
        sums = sum_ref[head]
        total = sums[:, HD : HD + 1]
        g_low = dout / total
        delta = -jnp.sum(dout * sums[:, :HD], axis=1, keepdims=True) / (total * total)
        high = delta.astype(BF16).astype(F32)
        middle = (delta - high).astype(BF16).astype(F32)
        tail = jnp.where(
            half_lane == 0,
            high,
            jnp.where(half_lane == 1, middle, jnp.where(half_lane == 2, delta - high - middle, 0.0)),
        )
        g_ext = jnp.concatenate([g_low, tail], axis=1)
        g_ref[head] = g_ext.astype(BF16)
        gt_ref[head] = jnp.transpose(g_ext)[:HD].astype(BF16)
        qt_ref[head] = jnp.transpose(q_ref[head].astype(F32))[:HD].astype(BF16)

    low = low_ref[block]

    def step(index, carry):
        start = pl.multiple_of(low + index * window, align)
        for head in range(heads):
            k_part = k_ref[head, pl.ds(start, window), :]
            v_part = v_ref[head, pl.ds(start, window), :]
            score = lax.dot_general(q_ref[head], k_part, BY_LANES, preferred_element_type=F32)
            slope = lax.dot_general(g_ref[head], v_part, BY_LANES, preferred_element_type=F32)
            expo = jnp.exp2(score)
            d_score = (expo * slope).astype(BF16)
            expo = expo.astype(BF16)
            dq_ref[head] += jnp.dot(d_score, k_part, preferred_element_type=F32)
            dkv_ref[head, :HD, pl.ds(start, window)] += jnp.dot(qt_ref[head], d_score, preferred_element_type=F32)
            dkv_ref[head, HD:, pl.ds(start, window)] += jnp.dot(gt_ref[head], expo, preferred_element_type=F32)
        return carry

    lax.fori_loop(0, count_ref[block], step, 0)

    lane = lax.broadcasted_iota(jnp.int32, (rows, lanes), 1)

    def turn_back(value, turn):
        swapped = jnp.where(lane < HD // 2, pltpu.roll(value, lanes - HD // 2, 1), pltpu.roll(value, HD // 2, 1))
        sine = pltpu.roll(turn, HD, 1)
        sine = jnp.where(lane < HD // 2, sine, -sine)
        return (value * turn + swapped * sine)[:, :HD]

    here = turn_ref[pl.ds(pl.multiple_of(block * rows, rows), rows), :]
    for head in range(heads):
        turned = turn_back(dq_ref[head] * HD ** (-0.5), here)
        d_ref[block, :, head * HD : (head + 1) * HD] = turned.astype(BF16)

    @pl.when(block == pl.num_programs(0) - 1)
    def _():
        def finish(piece, carry):
            start = pl.multiple_of(piece * rows, rows)
            turn = turn_ref[pl.ds(start, rows), :]
            for head in range(heads):
                both = jnp.transpose(dkv_ref[head, :, pl.ds(start, rows)])
                at = width + head * HD
                d_ref[piece, :, at : at + HD] = (turn_back(both, turn) * LN2).astype(BF16)
                d_ref[piece, :, width + at : width + at + HD] = both[:, HD:].astype(BF16)
            return carry

        lax.fori_loop(0, d_ref.shape[0], finish, 0)


def attend_back_heads(bounds, q_ext, k_ext, v_ext, sums, dout, turn, window=512, align=128):
    heads, length, lanes = q_ext.shape
    count_blocks, rows, width = dout.shape
    low, count = windows(bounds, length, window, align)
    whole = pl.BlockSpec((heads, length, lanes), lambda i, *_: (0, 0, 0))
    part = pl.BlockSpec((heads, rows, lanes), lambda i, *_: (0, i, 0))
    return pl.pallas_call(
        functools.partial(attend_back_kernel, window, align),
        out_shape=jax.ShapeDtypeStruct((count_blocks, rows, 3 * width), BF16),
        grid_spec=pltpu.PrefetchScalarGridSpec(
            num_scalar_prefetch=2,
            grid=(count_blocks,),
            in_specs=[
                part,
                part,
                pl.BlockSpec((1, rows, width), lambda i, *_: (i, 0, 0)),
                pl.BlockSpec((length, lanes), lambda i, *_: (0, 0)),
                whole,
                whole,
            ],
            out_specs=pl.BlockSpec((count_blocks, rows, 3 * width), lambda i, *_: (0, 0, 0)),
            scratch_shapes=[
                pltpu.VMEM((heads, rows, lanes), F32),
                pltpu.VMEM((heads, 2 * HD, length), F32),
                pltpu.VMEM((heads, rows, lanes), BF16),
                pltpu.VMEM((heads, HD, rows), BF16),
                pltpu.VMEM((heads, HD, rows), BF16),
            ],
        ),
        compiler_params=pltpu.CompilerParams(vmem_limit_bytes=VMEM_LIMIT),
        cost_estimate=pl.CostEstimate(
            flops=heads * length * length * 10 * lanes // 2,
            bytes_accessed=heads * length * lanes * 20,
            transcendentals=heads * length * length // 2,
        ),
        name="attend_back_heads",
    )(low, count, q_ext, sums, dout, turn, k_ext, v_ext)


def document_places(seg_row):
    length = seg_row.shape[0]
    ids = jnp.arange(LANES - HD, dtype=jnp.int32)[:, None]
    starts = jnp.sum((seg_row[None, :] < ids).astype(jnp.int32), axis=1, keepdims=True)
    start = jnp.sum(jnp.where(seg_row[None, :] == ids, starts, 0), axis=0)
    return jnp.arange(length, dtype=jnp.int32) - start


def by_group(block_rows):
    seqs, rows, width = block_rows.shape
    split = block_rows.reshape(seqs, rows, GROUPS, width // GROUPS)
    return jnp.transpose(split, (0, 2, 1, 3)).reshape(seqs * GROUPS, rows, width // GROUPS)


def from_group(blocks):
    devices, rows, width = blocks.shape
    split = blocks.reshape(devices // GROUPS, GROUPS, rows, width)
    return jnp.transpose(split, (0, 2, 1, 3)).reshape(devices // GROUPS, rows, GROUPS * width)


def exchange(blocks):
    return lax.all_to_all(blocks, "seq", 0, 0, tiled=True)


def head_columns(w_qkv, group, held):
    depth = w_qkv.shape[0]
    split = w_qkv.reshape(depth, 3, GROUPS, held, HD)
    mine = lax.dynamic_index_in_dim(split, group, 2, keepdims=False)
    second = mine * jnp.array([1, 1, 0], w_qkv.dtype)[None, :, None, None]
    return jnp.concatenate([mine, second], axis=-1).reshape(depth, 3 * held * 2 * HD)


def local_heads(
    shards,
    tokens,
    segments,
    positions,
    cotangent,
    w_qkv,
    w_out,
    w_gate,
    w_up,
    w_down,
    ln1_gain,
    ln1_bias,
    ln2_gain,
    ln2_bias,
):
    seq_count, row_count, model_width = tokens.shape
    held = HEADS // GROUPS
    length = row_count * SEQ_SIZE
    me = lax.axis_index("seq")
    seg_row = lax.dynamic_index_in_dim(segments, me // GROUPS, 0, keepdims=False)

    def gather(shard):
        return lax.all_gather(shard, "shard", axis=0, tiled=True)

    pieces, w_heads = gather_tokens(tokens, head_columns(w_qkv, me % GROUPS, held), shards)
    full_qkv = gather(w_qkv)
    norms = gather(jnp.stack([ln1_gain, ln1_bias, ln2_gain, ln2_bias], axis=1)).astype(F32)
    gain_one, bias_one, gain_two, bias_two = (norms[:, n] for n in range(4))
    full_out, full_gate, full_up, full_down = (gather(w) for w in (w_out, w_gate, w_up, w_down))
    freqs = jnp.exp(jnp.arange(HD // 2, dtype=F32) * (-math.log(ROPE_BASE) / (HD // 2)))
    freq = jnp.tile(freqs, LANES // (HD // 2))[None]
    place = document_places(seg_row).astype(F32)
    bounds = document_bounds(seg_row, row_count)
    q_ext, k_ext, v_ext, turn = project_heads(
        seg_row.astype(F32), place, freq, pieces, w_heads.reshape(model_width, -1), held
    )
    sums, joined_own = attend_heads(bounds, q_ext, k_ext, v_ext, row_count)
    joined = from_group(exchange(joined_own))

    tokens_f = tokens.astype(F32)
    h_one = tokens_f + jnp.einsum("sci,io->sco", joined, full_out, preferred_element_type=F32)
    x_one, normed_one, inverse_one = norm_fwd(h_one, gain_one, bias_one)
    x_low = x_one.astype(BF16)
    gate_pre = jnp.einsum("scd,df->scf", x_low, full_gate, preferred_element_type=F32)
    up_pre = jnp.einsum("scd,df->scf", x_low, full_up, preferred_element_type=F32)
    sigma = jax.nn.sigmoid(gate_pre)
    smooth = gate_pre * sigma
    hidden = (smooth * up_pre).astype(BF16)
    h_two = x_one + jnp.einsum("scf,fd->scd", hidden, full_down, preferred_element_type=F32)
    result, normed_two, inverse_two = norm_fwd(h_two, gain_two, bias_two)
    output = result.astype(BF16)

    cot_f = cotangent.astype(F32)
    grad_gain_two = jnp.sum(cot_f * normed_two, axis=(0, 1))
    grad_bias_two = jnp.sum(cot_f, axis=(0, 1))
    dh_two = norm_back(cot_f, normed_two, inverse_two, gain_two)
    dm_low = dh_two.astype(BF16)
    d_hidden = jnp.einsum("scd,fd->scf", dm_low, full_down, preferred_element_type=F32)
    d_up = (d_hidden * smooth).astype(BF16)
    d_gate = (d_hidden * up_pre * sigma * (1.0 + gate_pre * (1.0 - sigma))).astype(BF16)
    dx_one = (
        dh_two
        + jnp.einsum("scf,df->scd", d_gate, full_gate, preferred_element_type=F32)
        + jnp.einsum("scf,df->scd", d_up, full_up, preferred_element_type=F32)
    )
    grad_gain_one = jnp.sum(dx_one * normed_one, axis=(0, 1))
    grad_bias_one = jnp.sum(dx_one, axis=(0, 1))
    dh_one = norm_back(dx_one, normed_one, inverse_one, gain_one)
    d_attn = dh_one.astype(BF16)
    d_joined = jnp.einsum("sco,io->sci", d_attn, full_out, preferred_element_type=F32).astype(BF16)

    grad_down = jnp.einsum("scf,scd->fd", hidden, dm_low, preferred_element_type=F32).astype(BF16)
    grad_gate = jnp.einsum("scd,scf->df", x_low, d_gate, preferred_element_type=F32).astype(BF16)
    grad_up = jnp.einsum("scd,scf->df", x_low, d_up, preferred_element_type=F32).astype(BF16)
    grad_out = jnp.einsum("sci,sco->io", joined, d_attn, preferred_element_type=F32).astype(BF16)
    grad_norms = jnp.stack([grad_gain_one, grad_bias_one, grad_gain_two, grad_bias_two], axis=1)

    def reduce_shards(partial):
        return lax.psum_scatter(partial, "shard", scatter_dimension=0, tiled=True)

    d_joined, grad_down, grad_gate, grad_up, grad_out = lax.optimization_barrier(
        (d_joined, grad_down, grad_gate, grad_up, grad_out)
    )
    owned = [reduce_shards(g) for g in (grad_out, grad_gate, grad_up, grad_down)]

    dout = exchange(by_group(d_joined))
    d_heads = attend_back_heads(bounds, q_ext, k_ext, v_ext, sums, dout, turn)
    d_heads, *owned = lax.optimization_barrier((d_heads, *owned))
    summed = [lax.psum(g, "seq") for g in owned]
    d_taken = exchange(d_heads)
    d_taken, *summed = lax.optimization_barrier((d_taken, *summed))
    d_split = d_taken.reshape(seq_count, GROUPS, row_count, 3, held * HD)
    d_qkv = jnp.transpose(d_split, (0, 2, 3, 1, 4)).reshape(seq_count, row_count, 3 * model_width)
    grad_qkv = jnp.einsum("scd,sce->de", tokens, d_qkv, preferred_element_type=F32).astype(BF16)
    d_tokens = dh_one + jnp.einsum("sce,de->scd", d_qkv, full_qkv, preferred_element_type=F32)
    input_grad = d_tokens.astype(BF16)

    grad_out, grad_gate, grad_up, grad_down = (g.astype(F32) for g in summed)
    grad_qkv = lax.psum(reduce_shards(grad_qkv), "seq").astype(F32)
    norm_sums = lax.psum(reduce_shards(grad_norms), "seq")
    return (
        output,
        input_grad,
        grad_qkv,
        grad_out,
        grad_gate,
        grad_up,
        grad_down,
        norm_sums[:, 0],
        norm_sums[:, 1],
        norm_sums[:, 2],
        norm_sums[:, 3],
    )


def solution(mesh):
    in_specs = (
        P("shard", "seq", None),
        P("shard", None),
        P("shard", "seq"),
        P("shard", "seq", None),
        P("shard", None),
        P("shard", None),
        P("shard", None),
        P("shard", None),
        P("shard", None),
        P("shard"),
        P("shard"),
        P("shard"),
        P("shard"),
    )
    out_specs = (
        P("shard", "seq", None),
        P("shard", "seq", None),
        P("shard", None),
        P("shard", None),
        P("shard", None),
        P("shard", None),
        P("shard", None),
        P("shard"),
        P("shard"),
        P("shard"),
        P("shard"),
    )
    body = functools.partial(local_heads, mesh.shape["shard"]) if mesh.shape["seq"] == SEQ_SIZE else local
    return jax.shard_map(body, mesh=mesh, in_specs=in_specs, out_specs=out_specs, check_vma=False)
```

```python
import functools
import math

import jax
import jax.numpy as jnp
from jax import lax
from jax.experimental import pallas as pl
from jax.experimental.pallas import tpu as pltpu
from jax.sharding import PartitionSpec as P

HEADS = 12
HD = 64


EPS = 1e-05
ROPE_BASE = 1000.0


def rope_tables(pos_block):
    half_dim = HD // 2
    freqs = jnp.exp(jnp.arange(half_dim, dtype=jnp.float32) * (-math.log(ROPE_BASE) / half_dim))
    angle = pos_block.astype(jnp.float32)[..., None] * freqs
    return (jnp.cos(angle)[:, :, None, :], jnp.sin(angle)[:, :, None, :])


def rotate(heads, cos_b, sin_b):
    half_dim = heads.shape[-1] // 2
    first = heads[..., :half_dim]
    second = heads[..., half_dim:]
    return jnp.concatenate(
        [first * cos_b - second * sin_b, second * cos_b + first * sin_b], axis=-1
    )


def rotate_back(grads, cos_b, sin_b):
    half_dim = grads.shape[-1] // 2
    first = grads[..., :half_dim]
    second = grads[..., half_dim:]
    return jnp.concatenate(
        [first * cos_b + second * sin_b, second * cos_b - first * sin_b], axis=-1
    )


def norm_fwd(values, gain, bias):
    mean_val = jnp.mean(values, axis=-1, keepdims=True)
    centered = values - mean_val
    variance = jnp.mean(centered * centered, axis=-1, keepdims=True)
    inverse = lax.rsqrt(variance + EPS)
    normed = centered * inverse
    return (normed * gain + bias, normed, inverse)


def norm_back(grad_in, normed, inverse, gain):
    scaled = grad_in * gain
    return inverse * (
        scaled
        - jnp.mean(scaled, axis=-1, keepdims=True)
        - normed * jnp.mean(scaled * normed, axis=-1, keepdims=True)
    )


def head_split(block_rows, seq_count, row_count):
    return block_rows.reshape(seq_count, row_count, HEADS, HD)


def attend(q_heads, q_seg, k_full, v_full, seg_all, block, score_scale):
    seq_count, row_count = (q_heads.shape[0], q_heads.shape[1])
    block_count = k_full.shape[1] // block

    def attend_step(carry, index):
        row_total, value_sum = carry
        start = index * block
        k_part = head_split(lax.dynamic_slice_in_dim(k_full, start, block, 1), seq_count, block)
        v_part = head_split(lax.dynamic_slice_in_dim(v_full, start, block, 1), seq_count, block)
        seg_part = lax.dynamic_slice_in_dim(seg_all, start, block, 1)
        raw = (
            jnp.einsum("sqhd,skhd->shqk", q_heads, k_part, preferred_element_type=jnp.float32)
            * score_scale
        )
        same_doc = q_seg[:, None, :, None] == seg_part[:, None, None, :]
        expo = jnp.where(same_doc, jnp.exp(raw), 0.0)
        row_total = row_total + jnp.sum(expo, axis=-1)
        value_sum = value_sum + jnp.einsum(
            "shqk,skhd->sqhd", expo.astype(jnp.bfloat16), v_part, preferred_element_type=jnp.float32
        )
        return ((row_total, value_sum), None)

    start_carry = (
        jnp.zeros((seq_count, HEADS, row_count), jnp.float32),
        jnp.zeros((seq_count, row_count, HEADS, HD), jnp.float32),
    )
    final, unused = lax.scan(attend_step, start_carry, jnp.arange(block_count, dtype=jnp.int32))
    return final


def back_keys(q_heads, g_heads, delta, q_seg, k_full, v_full, seg_all, block, score_scale):
    seq_count, row_count = (q_heads.shape[0], q_heads.shape[1])
    full_len = k_full.shape[1]
    block_count = full_len // block

    def back_step(carry, index):
        start = index * block
        k_part = head_split(lax.dynamic_slice_in_dim(k_full, start, block, 1), seq_count, block)
        v_part = head_split(lax.dynamic_slice_in_dim(v_full, start, block, 1), seq_count, block)
        seg_part = lax.dynamic_slice_in_dim(seg_all, start, block, 1)
        raw = (
            jnp.einsum("sqhd,skhd->shqk", q_heads, k_part, preferred_element_type=jnp.float32)
            * score_scale
        )
        same_doc = q_seg[:, None, :, None] == seg_part[:, None, None, :]
        expo = jnp.where(same_doc, jnp.exp(raw), 0.0)
        prob_grad = jnp.einsum(
            "sqhd,skhd->shqk", g_heads, v_part, preferred_element_type=jnp.float32
        )
        d_score = (expo * (prob_grad - delta[..., None])).astype(jnp.bfloat16)
        q_grad = carry[0] + jnp.einsum(
            "shqk,skhd->sqhd", d_score, k_part, preferred_element_type=jnp.float32
        )
        k_grad = (
            jnp.einsum("shqk,sqhd->skhd", d_score, q_heads, preferred_element_type=jnp.float32)
            * score_scale
        )
        v_grad = jnp.einsum(
            "shqk,sqhd->skhd",
            expo.astype(jnp.bfloat16),
            g_heads,
            preferred_element_type=jnp.float32,
        )
        k_store = lax.dynamic_update_slice_in_dim(
            carry[1], k_grad.reshape(seq_count, block, HEADS * HD), start, 1
        )
        v_store = lax.dynamic_update_slice_in_dim(
            carry[2], v_grad.reshape(seq_count, block, HEADS * HD), start, 1
        )
        return ((q_grad, k_store, v_store), None)

    q_zero = jnp.zeros((seq_count, row_count, HEADS, HD), jnp.float32)
    kv_zero = jnp.zeros((seq_count, full_len, HEADS * HD), jnp.float32)
    start_carry = (q_zero, kv_zero, kv_zero)
    final, unused = lax.scan(back_step, start_carry, jnp.arange(block_count, dtype=jnp.int32))
    return (final[0] * score_scale,) + tuple(final[1:])


def local(
    tokens,
    segments,
    positions,
    cotangent,
    w_qkv,
    w_out,
    w_gate,
    w_up,
    w_down,
    ln1_gain,
    ln1_bias,
    ln2_gain,
    ln2_bias,
):
    seq_count, row_count, model_width = tokens.shape
    score_scale = HD ** (-0.5)
    q_seg = lax.dynamic_slice_in_dim(segments, lax.axis_index("seq") * row_count, row_count, 1)
    gathered = (
        lax.all_gather(w_qkv, "shard", axis=0, tiled=True),
        lax.all_gather(w_out, "shard", axis=0, tiled=True),
        lax.all_gather(w_gate, "shard", axis=0, tiled=True),
        lax.all_gather(w_up, "shard", axis=0, tiled=True),
        lax.all_gather(w_down, "shard", axis=0, tiled=True),
        lax.all_gather(ln1_gain, "shard", axis=0, tiled=True),
        lax.all_gather(ln1_bias, "shard", axis=0, tiled=True),
        lax.all_gather(ln2_gain, "shard", axis=0, tiled=True),
        lax.all_gather(ln2_bias, "shard", axis=0, tiled=True),
    )
    full_qkv, full_out, full_gate, full_up, full_down, gain_one, bias_one, gain_two, bias_two = (
        gathered
    )
    cos_b, sin_b = rope_tables(positions)
    qkv_all = jnp.einsum("scd,de->sce", tokens, full_qkv, preferred_element_type=jnp.float32)
    q_heads = rotate(
        head_split(qkv_all[..., :model_width], seq_count, row_count), cos_b, sin_b
    ).astype(jnp.bfloat16)
    k_heads = rotate(
        head_split(qkv_all[..., model_width : 2 * model_width], seq_count, row_count), cos_b, sin_b
    ).astype(jnp.bfloat16)
    v_heads = head_split(qkv_all[..., 2 * model_width :], seq_count, row_count).astype(jnp.bfloat16)
    k_local = k_heads.reshape(seq_count, row_count, model_width)
    v_local = v_heads.reshape(seq_count, row_count, model_width)
    k_full, v_full = (
        lax.all_gather(k_local, "seq", axis=1, tiled=True),
        lax.all_gather(v_local, "seq", axis=1, tiled=True),
    )
    row_total, value_sum = attend(q_heads, q_seg, k_full, v_full, segments, row_count, score_scale)
    denom = jnp.transpose(row_total, (0, 2, 1))[..., None]
    attn_out = value_sum / denom
    joined = attn_out.reshape(seq_count, row_count, model_width).astype(jnp.bfloat16)
    tokens_f = tokens.astype(jnp.float32)
    h_one = tokens_f + jnp.einsum(
        "sci,io->sco", joined, full_out, preferred_element_type=jnp.float32
    )
    x_one, normed_one, inverse_one = norm_fwd(
        h_one, gain_one.astype(jnp.float32), bias_one.astype(jnp.float32)
    )
    x_low = x_one.astype(jnp.bfloat16)
    gate_pre = jnp.einsum("scd,df->scf", x_low, full_gate, preferred_element_type=jnp.float32)
    up_pre = jnp.einsum("scd,df->scf", x_low, full_up, preferred_element_type=jnp.float32)
    sigma = jax.nn.sigmoid(gate_pre)
    smooth = gate_pre * sigma
    hidden = (smooth * up_pre).astype(jnp.bfloat16)
    h_two = x_one + jnp.einsum("scf,fd->scd", hidden, full_down, preferred_element_type=jnp.float32)
    result, normed_two, inverse_two = norm_fwd(
        h_two, gain_two.astype(jnp.float32), bias_two.astype(jnp.float32)
    )
    output = result.astype(jnp.bfloat16)
    regathered = (
        lax.all_gather(w_qkv, "shard", axis=0, tiled=True),
        lax.all_gather(w_out, "shard", axis=0, tiled=True),
        lax.all_gather(w_gate, "shard", axis=0, tiled=True),
        lax.all_gather(w_up, "shard", axis=0, tiled=True),
        lax.all_gather(w_down, "shard", axis=0, tiled=True),
        lax.all_gather(ln1_gain, "shard", axis=0, tiled=True),
        lax.all_gather(ln2_gain, "shard", axis=0, tiled=True),
    )
    back_qkv, back_out, back_gate, back_up, back_down, back_gain_one, back_gain_two = regathered
    back_k, back_v = (
        lax.all_gather(k_local, "seq", axis=1, tiled=True),
        lax.all_gather(v_local, "seq", axis=1, tiled=True),
    )
    cot_f = cotangent.astype(jnp.float32)
    grad_gain_two = jnp.sum(cot_f * normed_two, axis=(0, 1))
    grad_bias_two = jnp.sum(cot_f, axis=(0, 1))
    dh_two = norm_back(cot_f, normed_two, inverse_two, back_gain_two.astype(jnp.float32))
    dm_low = dh_two.astype(jnp.bfloat16)
    grad_down = jnp.einsum("scf,scd->fd", hidden, dm_low, preferred_element_type=jnp.float32)
    d_hidden = jnp.einsum("scd,fd->scf", dm_low, back_down, preferred_element_type=jnp.float32)
    d_up = (d_hidden * smooth).astype(jnp.bfloat16)
    d_gate = (d_hidden * up_pre * sigma * (1.0 + gate_pre * (1.0 - sigma))).astype(jnp.bfloat16)
    grad_gate = jnp.einsum("scd,scf->df", x_low, d_gate, preferred_element_type=jnp.float32)
    grad_up = jnp.einsum("scd,scf->df", x_low, d_up, preferred_element_type=jnp.float32)
    dx_one = (
        dh_two
        + jnp.einsum("scf,df->scd", d_gate, back_gate, preferred_element_type=jnp.float32)
        + jnp.einsum("scf,df->scd", d_up, back_up, preferred_element_type=jnp.float32)
    )
    grad_gain_one = jnp.sum(dx_one * normed_one, axis=(0, 1))
    grad_bias_one = jnp.sum(dx_one, axis=(0, 1))
    dh_one = norm_back(dx_one, normed_one, inverse_one, back_gain_one.astype(jnp.float32))
    d_attn = dh_one.astype(jnp.bfloat16)
    grad_out = jnp.einsum("sci,sco->io", joined, d_attn, preferred_element_type=jnp.float32)
    d_joined = jnp.einsum(
        "sco,io->sci", d_attn, back_out, preferred_element_type=jnp.float32
    ).astype(jnp.bfloat16)
    d_heads = head_split(d_joined, seq_count, row_count).astype(jnp.float32)
    g_heads = (d_heads / denom).astype(jnp.bfloat16)
    delta = jnp.transpose(jnp.sum(d_heads * attn_out, axis=-1) / denom[..., 0], (0, 2, 1))
    q_grad, k_all, v_all = back_keys(
        q_heads, g_heads, delta, q_seg, back_k, back_v, segments, row_count, score_scale
    )
    k_sum, v_sum = (
        lax.psum_scatter(k_all.astype(jnp.bfloat16), "seq", scatter_dimension=1, tiled=True).astype(
            jnp.float32
        ),
        lax.psum_scatter(v_all.astype(jnp.bfloat16), "seq", scatter_dimension=1, tiled=True).astype(
            jnp.float32
        ),
    )
    k_grad = head_split(k_sum, seq_count, row_count)
    v_grad = head_split(v_sum, seq_count, row_count)
    q_back = rotate_back(q_grad, cos_b, sin_b).reshape(seq_count, row_count, model_width)
    k_back = rotate_back(k_grad, cos_b, sin_b).reshape(seq_count, row_count, model_width)
    d_qkv = jnp.concatenate(
        [q_back, k_back, v_grad.reshape(seq_count, row_count, model_width)], axis=-1
    ).astype(jnp.bfloat16)
    grad_qkv = jnp.einsum("scd,sce->de", tokens, d_qkv, preferred_element_type=jnp.float32)
    d_tokens = dh_one + jnp.einsum(
        "sce,de->scd", d_qkv, back_qkv, preferred_element_type=jnp.float32
    )
    input_grad = d_tokens.astype(jnp.bfloat16)
    owned = (
        lax.psum_scatter(
            grad_qkv.astype(jnp.bfloat16), "shard", scatter_dimension=0, tiled=True
        ).astype(jnp.float32),
        lax.psum_scatter(
            grad_out.astype(jnp.bfloat16), "shard", scatter_dimension=0, tiled=True
        ).astype(jnp.float32),
        lax.psum_scatter(
            grad_gate.astype(jnp.bfloat16), "shard", scatter_dimension=0, tiled=True
        ).astype(jnp.float32),
        lax.psum_scatter(
            grad_up.astype(jnp.bfloat16), "shard", scatter_dimension=0, tiled=True
        ).astype(jnp.float32),
        lax.psum_scatter(
            grad_down.astype(jnp.bfloat16), "shard", scatter_dimension=0, tiled=True
        ).astype(jnp.float32),
        lax.psum_scatter(
            grad_gain_one.astype(jnp.bfloat16), "shard", scatter_dimension=0, tiled=True
        ).astype(jnp.float32),
        lax.psum_scatter(
            grad_bias_one.astype(jnp.bfloat16), "shard", scatter_dimension=0, tiled=True
        ).astype(jnp.float32),
        lax.psum_scatter(
            grad_gain_two.astype(jnp.bfloat16), "shard", scatter_dimension=0, tiled=True
        ).astype(jnp.float32),
        lax.psum_scatter(
            grad_bias_two.astype(jnp.bfloat16), "shard", scatter_dimension=0, tiled=True
        ).astype(jnp.float32),
    )
    summed = (
        lax.psum(owned[0].astype(jnp.bfloat16), "seq").astype(jnp.float32),
        lax.psum(owned[1].astype(jnp.bfloat16), "seq").astype(jnp.float32),
        lax.psum(owned[2].astype(jnp.bfloat16), "seq").astype(jnp.float32),
        lax.psum(owned[3].astype(jnp.bfloat16), "seq").astype(jnp.float32),
        lax.psum(owned[4].astype(jnp.bfloat16), "seq").astype(jnp.float32),
        lax.psum(owned[5].astype(jnp.bfloat16), "seq").astype(jnp.float32),
        lax.psum(owned[6].astype(jnp.bfloat16), "seq").astype(jnp.float32),
        lax.psum(owned[7].astype(jnp.bfloat16), "seq").astype(jnp.float32),
        lax.psum(owned[8].astype(jnp.bfloat16), "seq").astype(jnp.float32),
    )
    return (
        output,
        input_grad,
        summed[0],
        summed[1],
        summed[2],
        summed[3],
        summed[4],
        summed[5],
        summed[6],
        summed[7],
        summed[8],
    )


SEQS_HELD = 2
SEQ_SIZE = 8
GROUPS = 4
LANES = 128
LOG2E = 1.4426950408889634
LN2 = 0.6931471805599453
FAR = 2.0**30
F32 = jnp.float32
BF16 = jnp.bfloat16
VMEM_LIMIT = 60 * 1024 * 1024
BY_MESH = pl.DeviceIdType.MESH
BY_LANES = (((1,), (1,)), ((), ()))


def flip(index, bit):
    return index + bit - 2 * bit * lax.rem(lax.div(index, bit), 2)


def gather_kernel(chunks, by_z, tok_ref, w_ref, all_ref, w_all_ref, send, recv, kept, w_send, w_recv):
    me = lax.axis_index("seq")
    shard = lax.axis_index("shard")
    shards = w_all_ref.shape[0]
    half = lax.div(me, GROUPS)
    y_near, z_near, partner = flip(me, 1), flip(me, 2), flip(me, 4)
    barrier = pltpu.get_barrier_semaphore()
    for device in (y_near, z_near, partner):
        pl.semaphore_signal(barrier, inc=1, device_id={"seq": device}, device_id_type=BY_MESH)
    for step in range(1, shards):
        pl.semaphore_signal(
            barrier, inc=1, device_id={"shard": lax.rem(shard + step, shards)}, device_id_type=BY_MESH
        )
    pl.semaphore_wait(barrier, 2 + shards)

    part = tok_ref.shape[1] // chunks
    started = []

    def go(source, target, slot, device):
        copy = pltpu.make_async_remote_copy(
            src_ref=source,
            dst_ref=target,
            send_sem=send.at[slot],
            recv_sem=recv.at[slot],
            device_id={"seq": device},
            device_id_type=BY_MESH,
        )
        copy.start()
        started.append(copy)
        return copy

    def rows(chunk):
        return pl.ds(chunk * part, part)

    def relay(piece, chunk, slot, device):
        return go(all_ref.at[piece, rows(chunk)], all_ref.at[piece, rows(chunk)], slot * chunks + chunk, device)

    def own(which, chunk, slot, device):
        return go(tok_ref.at[which, rows(chunk)], all_ref.at[me, rows(chunk)], slot * chunks + chunk, device)

    crossing = [own(1 - half, chunk, 0, partner) for chunk in range(chunks)]
    own_y, own_z = [], []
    for chunk in range(chunks):
        own_y.append(own(half, chunk, 1, y_near))
        own_z.append(own(half, chunk, 2, z_near))
    weights = []
    for step in range(1, shards):
        copy = pltpu.make_async_remote_copy(
            src_ref=w_ref,
            dst_ref=w_all_ref.at[shard],
            send_sem=w_send.at[step],
            recv_sem=w_recv.at[step],
            device_id={"shard": lax.rem(shard + step, shards)},
            device_id_type=BY_MESH,
        )
        copy.start()
        weights.append(copy)
    keep_tok = pltpu.make_async_copy(tok_ref.at[half], all_ref.at[me], kept.at[0])
    keep_tok.start()
    keep_w = pltpu.make_async_copy(w_ref, w_all_ref.at[shard], kept.at[1])
    keep_w.start()

    cross_y, cross_z, corner = [], [], []
    for chunk in range(chunks):
        own_y[chunk].wait_recv()
        if chunk < by_z:
            corner.append(relay(y_near, chunk, 5, z_near))
        own_z[chunk].wait_recv()
        if chunk >= by_z:
            corner.append(relay(z_near, chunk, 5, y_near))
        crossing[chunk].wait_recv()
        cross_y.append(relay(partner, chunk, 3, y_near))
        cross_z.append(relay(partner, chunk, 4, z_near))
    for chunk in range(chunks):
        cross_y[chunk].wait_recv()
        if chunk < by_z:
            corner.append(relay(flip(y_near, 4), chunk, 6, z_near))
        cross_z[chunk].wait_recv()
        if chunk >= by_z:
            corner.append(relay(flip(z_near, 4), chunk, 6, y_near))
    for copy in corner:
        copy.wait_recv()
    for copy in weights:
        copy.wait()
    keep_tok.wait()
    keep_w.wait()
    for copy in started:
        copy.wait_send()


def gather_tokens(tokens, w_part, shards, chunks=8, by_z=3):
    seqs, rows, width = tokens.shape
    anywhere = pl.BlockSpec(memory_space=pl.ANY)
    return pl.pallas_call(
        functools.partial(gather_kernel, chunks, by_z),
        out_shape=(
            jax.ShapeDtypeStruct((SEQ_SIZE, rows, width), tokens.dtype),
            jax.ShapeDtypeStruct((shards,) + w_part.shape, w_part.dtype),
        ),
        in_specs=[anywhere, anywhere],
        out_specs=(anywhere, anywhere),
        scratch_shapes=[
            pltpu.SemaphoreType.DMA((7 * chunks,)),
            pltpu.SemaphoreType.DMA((7 * chunks,)),
            pltpu.SemaphoreType.DMA((2,)),
            pltpu.SemaphoreType.DMA((shards,)),
            pltpu.SemaphoreType.DMA((shards,)),
        ],
        compiler_params=pltpu.CompilerParams(collective_id=1, has_side_effects=True),
        name="gather_tokens",
    )(tokens, w_part)


def project_kernel(seg_ref, place_ref, freq_ref, x_ref, w_ref, q_ref, k_ref, v_ref, turn_ref):
    rows = x_ref.shape[1]
    held = q_ref.shape[0]
    lane = lax.broadcasted_iota(jnp.int32, (rows, LANES), 1)
    seg = jnp.transpose(jnp.broadcast_to(seg_ref[0], (LANES, rows)))
    place = jnp.transpose(jnp.broadcast_to(place_ref[0], (LANES, rows)))
    turn = jnp.where(lane < HD, jnp.cos(place * freq_ref[...]), jnp.sin(place * freq_ref[...]))
    turn_ref[...] = turn
    cos_b = jnp.where(lane < HD, turn, 0.0)
    sin_b = jnp.where(lane < HD, pltpu.roll(turn, HD, 1), 0.0)
    sin_b = jnp.where(lane < HD // 2, -sin_b, sin_b)
    same = seg == (lane - HD).astype(F32)
    q_tail = jnp.where(same, 1.0, 0.0)
    k_tail = jnp.where(same | (lane < HD), 0.0, -FAR)
    v_tail = jnp.where(lane < HD, 0.0, 1.0)
    scale = HD ** (-0.5) * LOG2E
    q_cos, q_sin = cos_b * scale, sin_b * scale
    width = held * LANES
    for part in range(3):
        mixed = jnp.dot(x_ref[0], w_ref[:, part * width : (part + 1) * width], preferred_element_type=F32)
        for head in range(held):
            value = mixed[:, head * LANES : (head + 1) * LANES]
            if part == 0:
                value = value * q_cos + pltpu.roll(value, HD // 2, 1) * q_sin + q_tail
                q_ref[head] = value.astype(BF16)
            elif part == 1:
                value = value * cos_b + pltpu.roll(value, HD // 2, 1) * sin_b + k_tail
                k_ref[head] = value.astype(BF16)
            else:
                v_ref[head] = (value + v_tail).astype(BF16)


def project_heads(seg_row, place_row, freq, pieces, w_full, held):
    count, rows, width = pieces.shape
    length = count * rows
    row_spec = pl.BlockSpec((1, 1, rows), lambda i: (i, 0, 0))
    head_spec = pl.BlockSpec((held, rows, LANES), lambda i: (0, i, 0))
    head_shape = jax.ShapeDtypeStruct((held, length, LANES), BF16)
    return pl.pallas_call(
        project_kernel,
        out_shape=(head_shape, head_shape, head_shape, jax.ShapeDtypeStruct((length, LANES), F32)),
        grid=(count,),
        in_specs=[
            row_spec,
            row_spec,
            pl.BlockSpec((1, LANES), lambda i: (0, 0)),
            pl.BlockSpec((1, rows, width), lambda i: (i, 0, 0)),
            pl.BlockSpec(w_full.shape, lambda i: (0, 0)),
        ],
        out_specs=(head_spec, head_spec, head_spec, pl.BlockSpec((rows, LANES), lambda i: (i, 0))),
        compiler_params=pltpu.CompilerParams(vmem_limit_bytes=VMEM_LIMIT),
        cost_estimate=pl.CostEstimate(
            flops=2 * length * width * w_full.shape[1],
            bytes_accessed=length * (width * 2 + held * LANES * 6 + LANES * 4),
            transcendentals=length * LANES,
        ),
        name="project_heads",
    )(seg_row.reshape(count, 1, rows), place_row.reshape(count, 1, rows), freq, pieces, w_full)


def document_bounds(seg_row, rows):
    first = seg_row[::rows]
    last = seg_row[rows - 1 :: rows]
    low = jnp.sum((seg_row[None, :] < first[:, None]).astype(jnp.int32), axis=1)
    high = jnp.sum((seg_row[None, :] <= last[:, None]).astype(jnp.int32), axis=1)
    return low, high


def windows(bounds, length, window, align):
    low = bounds[0] // align * align
    count = (bounds[1] - low + window - 1) // window
    return jnp.minimum(low, length - count * window), count


def attend_kernel(window, align, low_ref, count_ref, q_ref, k_ref, v_ref, sum_ref, joined_ref):
    block = pl.program_id(0)
    low = low_ref[block]
    sum_ref[...] = jnp.zeros_like(sum_ref)

    def step(index, carry):
        start = pl.multiple_of(low + index * window, align)
        for head in range(q_ref.shape[0]):
            k_part = k_ref[head, pl.ds(start, window), :]
            v_part = v_ref[head, pl.ds(start, window), :]
            score = lax.dot_general(q_ref[head], k_part, BY_LANES, preferred_element_type=F32)
            expo = jnp.exp2(score).astype(BF16)
            sum_ref[head] += jnp.dot(expo, v_part, preferred_element_type=F32)
        return carry

    lax.fori_loop(0, count_ref[block], step, 0)
    for head in range(q_ref.shape[0]):
        sums = sum_ref[head]
        joined_ref[0, :, head * HD : (head + 1) * HD] = (sums[:, :HD] / sums[:, HD : HD + 1]).astype(BF16)


def attend_heads(bounds, q_ext, k_ext, v_ext, rows, window=1024, align=16):
    heads, length, lanes = q_ext.shape
    low, count = windows(bounds, length, window, align)
    whole = pl.BlockSpec((heads, length, lanes), lambda i, *_: (0, 0, 0))
    part = pl.BlockSpec((heads, rows, lanes), lambda i, *_: (0, i, 0))
    return pl.pallas_call(
        functools.partial(attend_kernel, window, align),
        out_shape=(
            jax.ShapeDtypeStruct((heads, length, lanes), F32),
            jax.ShapeDtypeStruct((length // rows, rows, heads * HD), BF16),
        ),
        grid_spec=pltpu.PrefetchScalarGridSpec(
            num_scalar_prefetch=2,
            grid=(length // rows,),
            in_specs=[part, whole, whole],
            out_specs=(part, pl.BlockSpec((1, rows, heads * HD), lambda i, *_: (i, 0, 0))),
        ),
        compiler_params=pltpu.CompilerParams(vmem_limit_bytes=VMEM_LIMIT),
        cost_estimate=pl.CostEstimate(
            flops=heads * length * length * 4 * lanes // 2,
            bytes_accessed=heads * length * lanes * 10,
            transcendentals=heads * length * length // 2,
        ),
        name="attend_heads",
    )(low, count, q_ext, k_ext, v_ext)


def attend_back_kernel(
    window,
    align,
    low_ref,
    count_ref,
    q_ref,
    sum_ref,
    dout_ref,
    turn_ref,
    k_ref,
    v_ref,
    d_ref,
    dq_ref,
    dkv_ref,
    g_ref,
    gt_ref,
    qt_ref,
):
    block = pl.program_id(0)
    heads, rows, lanes = q_ref.shape
    width = heads * HD

    @pl.when(block == 0)
    def _():
        dkv_ref[...] = jnp.zeros_like(dkv_ref)

    dq_ref[...] = jnp.zeros_like(dq_ref)
    half_lane = lax.broadcasted_iota(jnp.int32, (rows, HD), 1)
    for head in range(heads):
        dout = dout_ref[0, :, head * HD : (head + 1) * HD].astype(F32)
        sums = sum_ref[head]
        total = sums[:, HD : HD + 1]
        g_low = dout / total
        delta = -jnp.sum(dout * sums[:, :HD], axis=1, keepdims=True) / (total * total)
        high = delta.astype(BF16).astype(F32)
        middle = (delta - high).astype(BF16).astype(F32)
        tail = jnp.where(
            half_lane == 0,
            high,
            jnp.where(half_lane == 1, middle, jnp.where(half_lane == 2, delta - high - middle, 0.0)),
        )
        g_ext = jnp.concatenate([g_low, tail], axis=1)
        g_ref[head] = g_ext.astype(BF16)
        gt_ref[head] = jnp.transpose(g_ext)[:HD].astype(BF16)
        qt_ref[head] = jnp.transpose(q_ref[head].astype(F32))[:HD].astype(BF16)

    low = low_ref[block]

    def step(index, carry):
        start = pl.multiple_of(low + index * window, align)
        for head in range(heads):
            k_part = k_ref[head, pl.ds(start, window), :]
            v_part = v_ref[head, pl.ds(start, window), :]
            score = lax.dot_general(q_ref[head], k_part, BY_LANES, preferred_element_type=F32)
            slope = lax.dot_general(g_ref[head], v_part, BY_LANES, preferred_element_type=F32)
            expo = jnp.exp2(score)
            d_score = (expo * slope).astype(BF16)
            expo = expo.astype(BF16)
            dq_ref[head] += jnp.dot(d_score, k_part, preferred_element_type=F32)
            dkv_ref[head, :HD, pl.ds(start, window)] += jnp.dot(qt_ref[head], d_score, preferred_element_type=F32)
            dkv_ref[head, HD:, pl.ds(start, window)] += jnp.dot(gt_ref[head], expo, preferred_element_type=F32)
        return carry

    lax.fori_loop(0, count_ref[block], step, 0)

    lane = lax.broadcasted_iota(jnp.int32, (rows, lanes), 1)

    def turn_back(value, turn):
        swapped = jnp.where(lane < HD // 2, pltpu.roll(value, lanes - HD // 2, 1), pltpu.roll(value, HD // 2, 1))
        sine = pltpu.roll(turn, HD, 1)
        sine = jnp.where(lane < HD // 2, sine, -sine)
        return (value * turn + swapped * sine)[:, :HD]

    here = turn_ref[pl.ds(pl.multiple_of(block * rows, rows), rows), :]
    for head in range(heads):
        turned = turn_back(dq_ref[head] * HD ** (-0.5), here)
        d_ref[block, :, head * HD : (head + 1) * HD] = turned.astype(BF16)

    @pl.when(block == pl.num_programs(0) - 1)
    def _():
        def finish(piece, carry):
            start = pl.multiple_of(piece * rows, rows)
            turn = turn_ref[pl.ds(start, rows), :]
            for head in range(heads):
                both = jnp.transpose(dkv_ref[head, :, pl.ds(start, rows)])
                at = width + head * HD
                d_ref[piece, :, at : at + HD] = (turn_back(both, turn) * LN2).astype(BF16)
                d_ref[piece, :, width + at : width + at + HD] = both[:, HD:].astype(BF16)
            return carry

        lax.fori_loop(0, d_ref.shape[0], finish, 0)


def attend_back_heads(bounds, q_ext, k_ext, v_ext, sums, dout, turn, window=512, align=128):
    heads, length, lanes = q_ext.shape
    count_blocks, rows, width = dout.shape
    low, count = windows(bounds, length, window, align)
    whole = pl.BlockSpec((heads, length, lanes), lambda i, *_: (0, 0, 0))
    part = pl.BlockSpec((heads, rows, lanes), lambda i, *_: (0, i, 0))
    return pl.pallas_call(
        functools.partial(attend_back_kernel, window, align),
        out_shape=jax.ShapeDtypeStruct((count_blocks, rows, 3 * width), BF16),
        grid_spec=pltpu.PrefetchScalarGridSpec(
            num_scalar_prefetch=2,
            grid=(count_blocks,),
            in_specs=[
                part,
                part,
                pl.BlockSpec((1, rows, width), lambda i, *_: (i, 0, 0)),
                pl.BlockSpec((length, lanes), lambda i, *_: (0, 0)),
                whole,
                whole,
            ],
            out_specs=pl.BlockSpec((count_blocks, rows, 3 * width), lambda i, *_: (0, 0, 0)),
            scratch_shapes=[
                pltpu.VMEM((heads, rows, lanes), F32),
                pltpu.VMEM((heads, 2 * HD, length), F32),
                pltpu.VMEM((heads, rows, lanes), BF16),
                pltpu.VMEM((heads, HD, rows), BF16),
                pltpu.VMEM((heads, HD, rows), BF16),
            ],
        ),
        compiler_params=pltpu.CompilerParams(vmem_limit_bytes=VMEM_LIMIT),
        cost_estimate=pl.CostEstimate(
            flops=heads * length * length * 10 * lanes // 2,
            bytes_accessed=heads * length * lanes * 20,
            transcendentals=heads * length * length // 2,
        ),
        name="attend_back_heads",
    )(low, count, q_ext, sums, dout, turn, k_ext, v_ext)


def scatter_kernel(
    chunks,
    by_z,
    part_ref,
    dh_ref,
    gw_ref,
    norm_ref,
    out_ref,
    gw_all_ref,
    norm_out_ref,
    got_y,
    got_z,
    relay_y,
    relay_z,
    sent_y,
    sent_z,
    cross_out,
    cross_in,
    gw_got,
    gw_mine,
    gw_pair,
    gw_final,
    norm_got,
    norm_sent,
    send,
    recv,
    gw_send,
    gw_recv,
    norm_send,
    norm_recv,
    kept,
):
    me = lax.axis_index("seq")
    shard = lax.axis_index("shard")
    shards = gw_ref.shape[0]
    half = lax.div(me, GROUPS)
    y_near, z_near, partner = flip(me, 1), flip(me, 2), flip(me, 4)
    corner = flip(y_near, 2)
    barrier = pltpu.get_barrier_semaphore()
    for device in (y_near, z_near, partner, corner):
        pl.semaphore_signal(barrier, inc=1, device_id={"seq": device}, device_id_type=BY_MESH)
    for step in range(1, shards):
        pl.semaphore_signal(
            barrier, inc=1, device_id={"shard": lax.rem(shard + step, shards)}, device_id_type=BY_MESH
        )
    pl.semaphore_wait(barrier, 3 + shards)

    started = []

    def go(source, target, sends, receives, slot, where):
        copy = pltpu.make_async_remote_copy(
            src_ref=source,
            dst_ref=target,
            send_sem=sends.at[slot],
            recv_sem=receives.at[slot],
            device_id=where,
            device_id_type=BY_MESH,
        )
        copy.start()
        started.append(copy)
        return copy

    rows = part_ref.shape[1] // chunks

    def band(chunk):
        return pl.ds(chunk * rows, rows)

    def piece(device, far):
        return flip(device, 4) if far else device

    def slot(kind, far, chunk):
        return (kind * 2 + (0 if far else 1)) * chunks + chunk

    gw_one = [
        go(
            gw_ref.at[lax.rem(shard + step, shards)],
            gw_got.at[step - 1],
            gw_send,
            gw_recv,
            step - 1,
            {"shard": lax.rem(shard + step, shards)},
        )
        for step in range(1, shards)
    ]
    pairs = [
        {"shard": flip(shard, 1)},
        {"shard": flip(shard, 2)},
        {"seq": y_near},
        {"seq": z_near},
        {"seq": partner},
    ]
    norm_sent[0] = norm_ref[...]

    from_corner, direct = {}, {}
    for far in (True, False):
        for chunk in range(chunks):
            over_z = chunk < by_z
            from_corner[far, chunk] = go(
                part_ref.at[piece(corner, far), band(chunk)],
                (relay_y if over_z else relay_z).at[0 if far else 1, chunk if over_z else chunk - by_z],
                send,
                recv,
                slot(0, far, chunk),
                {"seq": y_near if over_z else z_near},
            )
        for chunk in range(chunks):
            over_z = chunk < by_z
            near = y_near if over_z else z_near
            direct[far, chunk] = go(
                part_ref.at[piece(near, far), band(chunk)],
                (got_y if over_z else got_z).at[0 if far else 1, band(chunk)],
                send,
                recv,
                slot(1 if over_z else 2, far, chunk),
                {"seq": near},
            )

    norm_copies = [go(norm_sent.at[0], norm_got.at[0], norm_send, norm_recv, 0, pairs[0])]
    done_norm = 0

    def norm_step(index):
        norm_copies[index].wait_recv()
        total = norm_sent[index] + norm_got[index]
        if index + 1 < len(pairs):
            norm_sent[index + 1] = total
            norm_copies.append(
                go(norm_sent.at[index + 1], norm_got.at[index + 1], norm_send, norm_recv, index + 1, pairs[index + 1])
            )
        else:
            norm_out_ref[...] = total

    relayed = {}

    def relay(far, chunk):
        over_z = chunk < by_z
        target = z_near if over_z else y_near
        index = chunk if over_z else chunk - by_z
        which = 0 if far else 1
        from_corner[far, chunk].wait_recv()
        source = relay_y if over_z else relay_z
        buffer = sent_y if over_z else sent_z
        mine = part_ref[piece(target, far), band(chunk)].astype(F32)
        buffer[which, index] = (source[which, index].astype(F32) + mine).astype(BF16)
        relayed[far, chunk] = go(
            buffer.at[which, index],
            (got_z if over_z else got_y).at[which, band(chunk)],
            send,
            recv,
            slot(2 if over_z else 1, far, chunk),
            {"seq": target},
        )

    def total(far, chunk):
        which = 0 if far else 1
        direct[far, chunk].wait_recv()
        relayed[far, chunk].wait_recv()
        mine = part_ref[piece(me, far), band(chunk)].astype(F32)
        return mine + got_y[which, band(chunk)].astype(F32) + got_z[which, band(chunk)].astype(F32)

    for chunk in range(chunks):
        relay(True, chunk)
    norm_step(0)
    for copy in gw_one:
        copy.wait_recv()
    summed = gw_ref[shard].astype(F32)
    for step in range(1, shards):
        summed = summed + gw_got[step - 1].astype(F32)
    gw_mine[...] = summed.astype(BF16)
    norm_step(1)
    gw_two = go(gw_mine, gw_pair, gw_send, gw_recv, shards - 1, {"seq": partner})
    crossing = []
    for chunk in range(chunks):
        cross_out[band(chunk)] = total(True, chunk).astype(BF16)
        crossing.append(
            go(cross_out.at[band(chunk)], cross_in.at[band(chunk)], send, recv, slot(3, True, chunk), {"seq": partner})
        )
        relay(False, chunk)
    norm_step(2)
    gw_two.wait_recv()
    gw_final[...] = (gw_mine[...].astype(F32) + gw_pair[...].astype(F32)).astype(BF16)
    norm_step(3)
    group = lax.rem(me, GROUPS)
    gw_three = [
        go(gw_final, gw_all_ref.at[group], gw_send, gw_recv, shards + n, {"seq": device})
        for n, device in enumerate((y_near, z_near, corner))
    ]
    keep = pltpu.make_async_copy(gw_final, gw_all_ref.at[group], kept.at[0])
    keep.start()
    for chunk in range(chunks):
        out_ref[half, band(chunk)] = (total(False, chunk) + dh_ref[half, band(chunk)]).astype(BF16)
    norm_step(4)
    for chunk in range(chunks):
        crossing[chunk].wait_recv()
        other = 1 - half
        out_ref[other, band(chunk)] = (cross_in[band(chunk)].astype(F32) + dh_ref[other, band(chunk)]).astype(BF16)
    for copy in gw_three:
        copy.wait_recv()
    keep.wait()
    for copy in started:
        copy.wait_send()


def scatter_gradients(partial, dh_one, grad_columns, norms, chunks=4, by_z=3):
    _, rows, width = partial.shape
    shards, depth, columns = grad_columns.shape
    part = rows // chunks
    vmem = pl.BlockSpec(memory_space=pltpu.VMEM)
    dma = pltpu.SemaphoreType.DMA
    return pl.pallas_call(
        functools.partial(scatter_kernel, chunks, by_z),
        out_shape=(
            jax.ShapeDtypeStruct(dh_one.shape, BF16),
            jax.ShapeDtypeStruct((GROUPS, depth, columns), BF16),
            jax.ShapeDtypeStruct(norms.shape, F32),
        ),
        in_specs=[vmem] * 4,
        out_specs=(vmem,) * 3,
        scratch_shapes=[
            pltpu.VMEM((2, rows, width), BF16),
            pltpu.VMEM((2, rows, width), BF16),
            pltpu.VMEM((2, by_z, part, width), BF16),
            pltpu.VMEM((2, chunks - by_z, part, width), BF16),
            pltpu.VMEM((2, by_z, part, width), BF16),
            pltpu.VMEM((2, chunks - by_z, part, width), BF16),
            pltpu.VMEM((rows, width), BF16),
            pltpu.VMEM((rows, width), BF16),
            pltpu.VMEM((shards - 1, depth, columns), BF16),
            pltpu.VMEM((depth, columns), BF16),
            pltpu.VMEM((depth, columns), BF16),
            pltpu.VMEM((depth, columns), BF16),
            pltpu.VMEM((5,) + norms.shape, F32),
            pltpu.VMEM((5,) + norms.shape, F32),
            dma((7 * chunks,)),
            dma((7 * chunks,)),
            dma((shards + 3,)),
            dma((shards + 3,)),
            dma((5,)),
            dma((5,)),
            dma((1,)),
        ],
        compiler_params=pltpu.CompilerParams(
            collective_id=2, has_side_effects=True, vmem_limit_bytes=VMEM_LIMIT
        ),
        cost_estimate=pl.CostEstimate(flops=60 * 10**9, bytes_accessed=64 * 2**20, transcendentals=0),
        name="scatter_gradients",
    )(partial, dh_one, grad_columns, norms)


def document_places(seg_row):
    length = seg_row.shape[0]
    ids = jnp.arange(LANES - HD, dtype=jnp.int32)[:, None]
    starts = jnp.sum((seg_row[None, :] < ids).astype(jnp.int32), axis=1, keepdims=True)
    start = jnp.sum(jnp.where(seg_row[None, :] == ids, starts, 0), axis=0)
    return jnp.arange(length, dtype=jnp.int32) - start


def by_group(block_rows):
    seqs, rows, width = block_rows.shape
    split = block_rows.reshape(seqs, rows, GROUPS, width // GROUPS)
    return jnp.transpose(split, (0, 2, 1, 3)).reshape(seqs * GROUPS, rows, width // GROUPS)


def from_group(blocks):
    devices, rows, width = blocks.shape
    split = blocks.reshape(devices // GROUPS, GROUPS, rows, width)
    return jnp.transpose(split, (0, 2, 1, 3)).reshape(devices // GROUPS, rows, GROUPS * width)


def exchange(blocks):
    return lax.all_to_all(blocks, "seq", 0, 0, tiled=True)


def head_columns(w_qkv, group, held):
    depth = w_qkv.shape[0]
    split = w_qkv.reshape(depth, 3, GROUPS, held, HD)
    mine = lax.dynamic_index_in_dim(split, group, 2, keepdims=False)
    second = mine * jnp.array([1, 1, 0], w_qkv.dtype)[None, :, None, None]
    return jnp.concatenate([mine, second], axis=-1).reshape(depth, 3 * held * 2 * HD)


def local_heads(
    shards,
    tokens,
    segments,
    positions,
    cotangent,
    w_qkv,
    w_out,
    w_gate,
    w_up,
    w_down,
    ln1_gain,
    ln1_bias,
    ln2_gain,
    ln2_bias,
):
    seq_count, row_count, model_width = tokens.shape
    held = HEADS // GROUPS
    length = row_count * SEQ_SIZE
    me = lax.axis_index("seq")
    seg_row = lax.dynamic_index_in_dim(segments, me // GROUPS, 0, keepdims=False)

    def gather(shard):
        return lax.all_gather(shard, "shard", axis=0, tiled=True)

    pieces, w_heads = gather_tokens(tokens, head_columns(w_qkv, me % GROUPS, held), shards)
    norms = gather(jnp.stack([ln1_gain, ln1_bias, ln2_gain, ln2_bias], axis=1)).astype(F32)
    gain_one, bias_one, gain_two, bias_two = (norms[:, n] for n in range(4))
    full_out, full_gate, full_up, full_down = (gather(w) for w in (w_out, w_gate, w_up, w_down))
    freqs = jnp.exp(jnp.arange(HD // 2, dtype=F32) * (-math.log(ROPE_BASE) / (HD // 2)))
    freq = jnp.tile(freqs, LANES // (HD // 2))[None]
    place = document_places(seg_row).astype(F32)
    bounds = document_bounds(seg_row, row_count)
    q_ext, k_ext, v_ext, turn = project_heads(
        seg_row.astype(F32), place, freq, pieces, w_heads.reshape(model_width, -1), held
    )
    sums, joined_own = attend_heads(bounds, q_ext, k_ext, v_ext, row_count)
    joined = from_group(exchange(joined_own))

    tokens_f = tokens.astype(F32)
    h_one = tokens_f + jnp.einsum("sci,io->sco", joined, full_out, preferred_element_type=F32)
    x_one, normed_one, inverse_one = norm_fwd(h_one, gain_one, bias_one)
    x_low = x_one.astype(BF16)
    gate_pre = jnp.einsum("scd,df->scf", x_low, full_gate, preferred_element_type=F32)
    up_pre = jnp.einsum("scd,df->scf", x_low, full_up, preferred_element_type=F32)
    sigma = jax.nn.sigmoid(gate_pre)
    smooth = gate_pre * sigma
    hidden = (smooth * up_pre).astype(BF16)
    h_two = x_one + jnp.einsum("scf,fd->scd", hidden, full_down, preferred_element_type=F32)
    result, normed_two, inverse_two = norm_fwd(h_two, gain_two, bias_two)
    output = result.astype(BF16)

    cot_f = cotangent.astype(F32)
    grad_gain_two = jnp.sum(cot_f * normed_two, axis=(0, 1))
    grad_bias_two = jnp.sum(cot_f, axis=(0, 1))
    dh_two = norm_back(cot_f, normed_two, inverse_two, gain_two)
    dm_low = dh_two.astype(BF16)
    d_hidden = jnp.einsum("scd,fd->scf", dm_low, full_down, preferred_element_type=F32)
    d_up = (d_hidden * smooth).astype(BF16)
    d_gate = (d_hidden * up_pre * sigma * (1.0 + gate_pre * (1.0 - sigma))).astype(BF16)
    dx_one = (
        dh_two
        + jnp.einsum("scf,df->scd", d_gate, full_gate, preferred_element_type=F32)
        + jnp.einsum("scf,df->scd", d_up, full_up, preferred_element_type=F32)
    )
    grad_gain_one = jnp.sum(dx_one * normed_one, axis=(0, 1))
    grad_bias_one = jnp.sum(dx_one, axis=(0, 1))
    dh_one = norm_back(dx_one, normed_one, inverse_one, gain_one)
    d_attn = dh_one.astype(BF16)
    d_joined = jnp.einsum("sco,io->sci", d_attn, full_out, preferred_element_type=F32).astype(BF16)

    grad_down = jnp.einsum("scf,scd->fd", hidden, dm_low, preferred_element_type=F32).astype(BF16)
    grad_gate = jnp.einsum("scd,scf->df", x_low, d_gate, preferred_element_type=F32).astype(BF16)
    grad_up = jnp.einsum("scd,scf->df", x_low, d_up, preferred_element_type=F32).astype(BF16)
    grad_out = jnp.einsum("sci,sco->io", joined, d_attn, preferred_element_type=F32).astype(BF16)
    norms_part = jnp.stack([grad_gain_one, grad_bias_one, grad_gain_two, grad_bias_two])
    depth = model_width // shards
    ff_blocks = grad_gate.shape[1] // model_width

    def by_shard(grad):
        split = grad.reshape(shards, -1, grad.shape[1] // model_width, model_width)
        return jnp.transpose(split, (0, 2, 1, 3)).reshape(shards, -1, model_width)

    packed = jnp.concatenate([by_shard(g) for g in (grad_gate, grad_up, grad_down, grad_out)], axis=1)
    d_joined, packed = lax.optimization_barrier((d_joined, packed))
    owned = lax.psum_scatter(
        packed.reshape(-1, model_width), ("shard", "seq"), scatter_dimension=0, tiled=True
    )

    dout = exchange(by_group(d_joined))
    d_heads = attend_back_heads(bounds, q_ext, k_ext, v_ext, sums, dout, turn)
    w_own = w_heads.reshape(model_width, -1, LANES)[:, :, :HD].reshape(model_width, -1)
    partial = jnp.einsum("prc,dc->prd", d_heads, w_own, preferred_element_type=F32).astype(BF16)
    grad_columns = jnp.einsum("prd,prc->dc", pieces, d_heads, preferred_element_type=F32).astype(BF16)
    partial, grad_columns, owned = lax.optimization_barrier((partial, grad_columns, owned))
    shared = lax.all_gather(owned, "seq", axis=0, tiled=True)
    input_grad, columns, norm_sums = scatter_gradients(
        partial, dh_one, grad_columns.reshape(shards, depth, -1), norms_part
    )
    grad_qkv = jnp.transpose(columns.reshape(GROUPS, depth, 3, held * HD), (1, 2, 0, 3))
    grad_qkv = grad_qkv.reshape(depth, 3 * model_width).astype(F32)

    def taken(start, blocks):
        rows = shared[start : start + blocks * depth].reshape(blocks, depth, model_width)
        return jnp.transpose(rows, (1, 0, 2)).reshape(depth, blocks * model_width).astype(F32)

    ff_rows = ff_blocks * depth
    grad_gate, grad_up = taken(0, ff_blocks), taken(ff_rows, ff_blocks)
    grad_down = shared[2 * ff_rows : 3 * ff_rows].astype(F32)
    grad_out = taken(3 * ff_rows, 1)
    shard = lax.axis_index("shard")
    norm_sums = lax.dynamic_slice_in_dim(norm_sums, shard * depth, depth, 1)
    return (
        output,
        input_grad,
        grad_qkv,
        grad_out,
        grad_gate,
        grad_up,
        grad_down,
        norm_sums[0],
        norm_sums[1],
        norm_sums[2],
        norm_sums[3],
    )


def solution(mesh):
    in_specs = (
        P("shard", "seq", None),
        P("shard", None),
        P("shard", "seq"),
        P("shard", "seq", None),
        P("shard", None),
        P("shard", None),
        P("shard", None),
        P("shard", None),
        P("shard", None),
        P("shard"),
        P("shard"),
        P("shard"),
        P("shard"),
    )
    out_specs = (
        P("shard", "seq", None),
        P("shard", "seq", None),
        P("shard", None),
        P("shard", None),
        P("shard", None),
        P("shard", None),
        P("shard", None),
        P("shard"),
        P("shard"),
        P("shard"),
        P("shard"),
    )
    body = functools.partial(local_heads, mesh.shape["shard"]) if (mesh.shape["seq"], mesh.shape["shard"]) == (SEQ_SIZE, GROUPS) else local
    return jax.shard_map(body, mesh=mesh, in_specs=in_specs, out_specs=out_specs, check_vma=False)
```

```python
import functools
import math

import jax
import jax.numpy as jnp
from jax import lax
from jax.experimental import pallas as pl
from jax.experimental.pallas import tpu as pltpu
from jax.sharding import PartitionSpec as P

HEADS = 12
HD = 64


EPS = 1e-05
ROPE_BASE = 1000.0


def rope_tables(pos_block):
    half_dim = HD // 2
    freqs = jnp.exp(jnp.arange(half_dim, dtype=jnp.float32) * (-math.log(ROPE_BASE) / half_dim))
    angle = pos_block.astype(jnp.float32)[..., None] * freqs
    return (jnp.cos(angle)[:, :, None, :], jnp.sin(angle)[:, :, None, :])


def rotate(heads, cos_b, sin_b):
    half_dim = heads.shape[-1] // 2
    first = heads[..., :half_dim]
    second = heads[..., half_dim:]
    return jnp.concatenate(
        [first * cos_b - second * sin_b, second * cos_b + first * sin_b], axis=-1
    )


def rotate_back(grads, cos_b, sin_b):
    half_dim = grads.shape[-1] // 2
    first = grads[..., :half_dim]
    second = grads[..., half_dim:]
    return jnp.concatenate(
        [first * cos_b + second * sin_b, second * cos_b - first * sin_b], axis=-1
    )


def norm_fwd(values, gain, bias):
    mean_val = jnp.mean(values, axis=-1, keepdims=True)
    centered = values - mean_val
    variance = jnp.mean(centered * centered, axis=-1, keepdims=True)
    inverse = lax.rsqrt(variance + EPS)
    normed = centered * inverse
    return (normed * gain + bias, normed, inverse)


def norm_back(grad_in, normed, inverse, gain):
    scaled = grad_in * gain
    return inverse * (
        scaled
        - jnp.mean(scaled, axis=-1, keepdims=True)
        - normed * jnp.mean(scaled * normed, axis=-1, keepdims=True)
    )


def head_split(block_rows, seq_count, row_count):
    return block_rows.reshape(seq_count, row_count, HEADS, HD)


def attend(q_heads, q_seg, k_full, v_full, seg_all, block, score_scale):
    seq_count, row_count = (q_heads.shape[0], q_heads.shape[1])
    block_count = k_full.shape[1] // block

    def attend_step(carry, index):
        row_total, value_sum = carry
        start = index * block
        k_part = head_split(lax.dynamic_slice_in_dim(k_full, start, block, 1), seq_count, block)
        v_part = head_split(lax.dynamic_slice_in_dim(v_full, start, block, 1), seq_count, block)
        seg_part = lax.dynamic_slice_in_dim(seg_all, start, block, 1)
        raw = (
            jnp.einsum("sqhd,skhd->shqk", q_heads, k_part, preferred_element_type=jnp.float32)
            * score_scale
        )
        same_doc = q_seg[:, None, :, None] == seg_part[:, None, None, :]
        expo = jnp.where(same_doc, jnp.exp(raw), 0.0)
        row_total = row_total + jnp.sum(expo, axis=-1)
        value_sum = value_sum + jnp.einsum(
            "shqk,skhd->sqhd", expo.astype(jnp.bfloat16), v_part, preferred_element_type=jnp.float32
        )
        return ((row_total, value_sum), None)

    start_carry = (
        jnp.zeros((seq_count, HEADS, row_count), jnp.float32),
        jnp.zeros((seq_count, row_count, HEADS, HD), jnp.float32),
    )
    final, unused = lax.scan(attend_step, start_carry, jnp.arange(block_count, dtype=jnp.int32))
    return final


def back_keys(q_heads, g_heads, delta, q_seg, k_full, v_full, seg_all, block, score_scale):
    seq_count, row_count = (q_heads.shape[0], q_heads.shape[1])
    full_len = k_full.shape[1]
    block_count = full_len // block

    def back_step(carry, index):
        start = index * block
        k_part = head_split(lax.dynamic_slice_in_dim(k_full, start, block, 1), seq_count, block)
        v_part = head_split(lax.dynamic_slice_in_dim(v_full, start, block, 1), seq_count, block)
        seg_part = lax.dynamic_slice_in_dim(seg_all, start, block, 1)
        raw = (
            jnp.einsum("sqhd,skhd->shqk", q_heads, k_part, preferred_element_type=jnp.float32)
            * score_scale
        )
        same_doc = q_seg[:, None, :, None] == seg_part[:, None, None, :]
        expo = jnp.where(same_doc, jnp.exp(raw), 0.0)
        prob_grad = jnp.einsum(
            "sqhd,skhd->shqk", g_heads, v_part, preferred_element_type=jnp.float32
        )
        d_score = (expo * (prob_grad - delta[..., None])).astype(jnp.bfloat16)
        q_grad = carry[0] + jnp.einsum(
            "shqk,skhd->sqhd", d_score, k_part, preferred_element_type=jnp.float32
        )
        k_grad = (
            jnp.einsum("shqk,sqhd->skhd", d_score, q_heads, preferred_element_type=jnp.float32)
            * score_scale
        )
        v_grad = jnp.einsum(
            "shqk,sqhd->skhd",
            expo.astype(jnp.bfloat16),
            g_heads,
            preferred_element_type=jnp.float32,
        )
        k_store = lax.dynamic_update_slice_in_dim(
            carry[1], k_grad.reshape(seq_count, block, HEADS * HD), start, 1
        )
        v_store = lax.dynamic_update_slice_in_dim(
            carry[2], v_grad.reshape(seq_count, block, HEADS * HD), start, 1
        )
        return ((q_grad, k_store, v_store), None)

    q_zero = jnp.zeros((seq_count, row_count, HEADS, HD), jnp.float32)
    kv_zero = jnp.zeros((seq_count, full_len, HEADS * HD), jnp.float32)
    start_carry = (q_zero, kv_zero, kv_zero)
    final, unused = lax.scan(back_step, start_carry, jnp.arange(block_count, dtype=jnp.int32))
    return (final[0] * score_scale,) + tuple(final[1:])


def local(
    tokens,
    segments,
    positions,
    cotangent,
    w_qkv,
    w_out,
    w_gate,
    w_up,
    w_down,
    ln1_gain,
    ln1_bias,
    ln2_gain,
    ln2_bias,
):
    seq_count, row_count, model_width = tokens.shape
    score_scale = HD ** (-0.5)
    q_seg = lax.dynamic_slice_in_dim(segments, lax.axis_index("seq") * row_count, row_count, 1)
    gathered = (
        lax.all_gather(w_qkv, "shard", axis=0, tiled=True),
        lax.all_gather(w_out, "shard", axis=0, tiled=True),
        lax.all_gather(w_gate, "shard", axis=0, tiled=True),
        lax.all_gather(w_up, "shard", axis=0, tiled=True),
        lax.all_gather(w_down, "shard", axis=0, tiled=True),
        lax.all_gather(ln1_gain, "shard", axis=0, tiled=True),
        lax.all_gather(ln1_bias, "shard", axis=0, tiled=True),
        lax.all_gather(ln2_gain, "shard", axis=0, tiled=True),
        lax.all_gather(ln2_bias, "shard", axis=0, tiled=True),
    )
    full_qkv, full_out, full_gate, full_up, full_down, gain_one, bias_one, gain_two, bias_two = (
        gathered
    )
    cos_b, sin_b = rope_tables(positions)
    qkv_all = jnp.einsum("scd,de->sce", tokens, full_qkv, preferred_element_type=jnp.float32)
    q_heads = rotate(
        head_split(qkv_all[..., :model_width], seq_count, row_count), cos_b, sin_b
    ).astype(jnp.bfloat16)
    k_heads = rotate(
        head_split(qkv_all[..., model_width : 2 * model_width], seq_count, row_count), cos_b, sin_b
    ).astype(jnp.bfloat16)
    v_heads = head_split(qkv_all[..., 2 * model_width :], seq_count, row_count).astype(jnp.bfloat16)
    k_local = k_heads.reshape(seq_count, row_count, model_width)
    v_local = v_heads.reshape(seq_count, row_count, model_width)
    k_full, v_full = (
        lax.all_gather(k_local, "seq", axis=1, tiled=True),
        lax.all_gather(v_local, "seq", axis=1, tiled=True),
    )
    row_total, value_sum = attend(q_heads, q_seg, k_full, v_full, segments, row_count, score_scale)
    denom = jnp.transpose(row_total, (0, 2, 1))[..., None]
    attn_out = value_sum / denom
    joined = attn_out.reshape(seq_count, row_count, model_width).astype(jnp.bfloat16)
    tokens_f = tokens.astype(jnp.float32)
    h_one = tokens_f + jnp.einsum(
        "sci,io->sco", joined, full_out, preferred_element_type=jnp.float32
    )
    x_one, normed_one, inverse_one = norm_fwd(
        h_one, gain_one.astype(jnp.float32), bias_one.astype(jnp.float32)
    )
    x_low = x_one.astype(jnp.bfloat16)
    gate_pre = jnp.einsum("scd,df->scf", x_low, full_gate, preferred_element_type=jnp.float32)
    up_pre = jnp.einsum("scd,df->scf", x_low, full_up, preferred_element_type=jnp.float32)
    sigma = jax.nn.sigmoid(gate_pre)
    smooth = gate_pre * sigma
    hidden = (smooth * up_pre).astype(jnp.bfloat16)
    h_two = x_one + jnp.einsum("scf,fd->scd", hidden, full_down, preferred_element_type=jnp.float32)
    result, normed_two, inverse_two = norm_fwd(
        h_two, gain_two.astype(jnp.float32), bias_two.astype(jnp.float32)
    )
    output = result.astype(jnp.bfloat16)
    regathered = (
        lax.all_gather(w_qkv, "shard", axis=0, tiled=True),
        lax.all_gather(w_out, "shard", axis=0, tiled=True),
        lax.all_gather(w_gate, "shard", axis=0, tiled=True),
        lax.all_gather(w_up, "shard", axis=0, tiled=True),
        lax.all_gather(w_down, "shard", axis=0, tiled=True),
        lax.all_gather(ln1_gain, "shard", axis=0, tiled=True),
        lax.all_gather(ln2_gain, "shard", axis=0, tiled=True),
    )
    back_qkv, back_out, back_gate, back_up, back_down, back_gain_one, back_gain_two = regathered
    back_k, back_v = (
        lax.all_gather(k_local, "seq", axis=1, tiled=True),
        lax.all_gather(v_local, "seq", axis=1, tiled=True),
    )
    cot_f = cotangent.astype(jnp.float32)
    grad_gain_two = jnp.sum(cot_f * normed_two, axis=(0, 1))
    grad_bias_two = jnp.sum(cot_f, axis=(0, 1))
    dh_two = norm_back(cot_f, normed_two, inverse_two, back_gain_two.astype(jnp.float32))
    dm_low = dh_two.astype(jnp.bfloat16)
    grad_down = jnp.einsum("scf,scd->fd", hidden, dm_low, preferred_element_type=jnp.float32)
    d_hidden = jnp.einsum("scd,fd->scf", dm_low, back_down, preferred_element_type=jnp.float32)
    d_up = (d_hidden * smooth).astype(jnp.bfloat16)
    d_gate = (d_hidden * up_pre * sigma * (1.0 + gate_pre * (1.0 - sigma))).astype(jnp.bfloat16)
    grad_gate = jnp.einsum("scd,scf->df", x_low, d_gate, preferred_element_type=jnp.float32)
    grad_up = jnp.einsum("scd,scf->df", x_low, d_up, preferred_element_type=jnp.float32)
    dx_one = (
        dh_two
        + jnp.einsum("scf,df->scd", d_gate, back_gate, preferred_element_type=jnp.float32)
        + jnp.einsum("scf,df->scd", d_up, back_up, preferred_element_type=jnp.float32)
    )
    grad_gain_one = jnp.sum(dx_one * normed_one, axis=(0, 1))
    grad_bias_one = jnp.sum(dx_one, axis=(0, 1))
    dh_one = norm_back(dx_one, normed_one, inverse_one, back_gain_one.astype(jnp.float32))
    d_attn = dh_one.astype(jnp.bfloat16)
    grad_out = jnp.einsum("sci,sco->io", joined, d_attn, preferred_element_type=jnp.float32)
    d_joined = jnp.einsum(
        "sco,io->sci", d_attn, back_out, preferred_element_type=jnp.float32
    ).astype(jnp.bfloat16)
    d_heads = head_split(d_joined, seq_count, row_count).astype(jnp.float32)
    g_heads = (d_heads / denom).astype(jnp.bfloat16)
    delta = jnp.transpose(jnp.sum(d_heads * attn_out, axis=-1) / denom[..., 0], (0, 2, 1))
    q_grad, k_all, v_all = back_keys(
        q_heads, g_heads, delta, q_seg, back_k, back_v, segments, row_count, score_scale
    )
    k_sum, v_sum = (
        lax.psum_scatter(k_all.astype(jnp.bfloat16), "seq", scatter_dimension=1, tiled=True).astype(
            jnp.float32
        ),
        lax.psum_scatter(v_all.astype(jnp.bfloat16), "seq", scatter_dimension=1, tiled=True).astype(
            jnp.float32
        ),
    )
    k_grad = head_split(k_sum, seq_count, row_count)
    v_grad = head_split(v_sum, seq_count, row_count)
    q_back = rotate_back(q_grad, cos_b, sin_b).reshape(seq_count, row_count, model_width)
    k_back = rotate_back(k_grad, cos_b, sin_b).reshape(seq_count, row_count, model_width)
    d_qkv = jnp.concatenate(
        [q_back, k_back, v_grad.reshape(seq_count, row_count, model_width)], axis=-1
    ).astype(jnp.bfloat16)
    grad_qkv = jnp.einsum("scd,sce->de", tokens, d_qkv, preferred_element_type=jnp.float32)
    d_tokens = dh_one + jnp.einsum(
        "sce,de->scd", d_qkv, back_qkv, preferred_element_type=jnp.float32
    )
    input_grad = d_tokens.astype(jnp.bfloat16)
    owned = (
        lax.psum_scatter(
            grad_qkv.astype(jnp.bfloat16), "shard", scatter_dimension=0, tiled=True
        ).astype(jnp.float32),
        lax.psum_scatter(
            grad_out.astype(jnp.bfloat16), "shard", scatter_dimension=0, tiled=True
        ).astype(jnp.float32),
        lax.psum_scatter(
            grad_gate.astype(jnp.bfloat16), "shard", scatter_dimension=0, tiled=True
        ).astype(jnp.float32),
        lax.psum_scatter(
            grad_up.astype(jnp.bfloat16), "shard", scatter_dimension=0, tiled=True
        ).astype(jnp.float32),
        lax.psum_scatter(
            grad_down.astype(jnp.bfloat16), "shard", scatter_dimension=0, tiled=True
        ).astype(jnp.float32),
        lax.psum_scatter(
            grad_gain_one.astype(jnp.bfloat16), "shard", scatter_dimension=0, tiled=True
        ).astype(jnp.float32),
        lax.psum_scatter(
            grad_bias_one.astype(jnp.bfloat16), "shard", scatter_dimension=0, tiled=True
        ).astype(jnp.float32),
        lax.psum_scatter(
            grad_gain_two.astype(jnp.bfloat16), "shard", scatter_dimension=0, tiled=True
        ).astype(jnp.float32),
        lax.psum_scatter(
            grad_bias_two.astype(jnp.bfloat16), "shard", scatter_dimension=0, tiled=True
        ).astype(jnp.float32),
    )
    summed = (
        lax.psum(owned[0].astype(jnp.bfloat16), "seq").astype(jnp.float32),
        lax.psum(owned[1].astype(jnp.bfloat16), "seq").astype(jnp.float32),
        lax.psum(owned[2].astype(jnp.bfloat16), "seq").astype(jnp.float32),
        lax.psum(owned[3].astype(jnp.bfloat16), "seq").astype(jnp.float32),
        lax.psum(owned[4].astype(jnp.bfloat16), "seq").astype(jnp.float32),
        lax.psum(owned[5].astype(jnp.bfloat16), "seq").astype(jnp.float32),
        lax.psum(owned[6].astype(jnp.bfloat16), "seq").astype(jnp.float32),
        lax.psum(owned[7].astype(jnp.bfloat16), "seq").astype(jnp.float32),
        lax.psum(owned[8].astype(jnp.bfloat16), "seq").astype(jnp.float32),
    )
    return (
        output,
        input_grad,
        summed[0],
        summed[1],
        summed[2],
        summed[3],
        summed[4],
        summed[5],
        summed[6],
        summed[7],
        summed[8],
    )


SEQS_HELD = 2
SEQ_SIZE = 8
GROUPS = 4
LANES = 128
LOG2E = 1.4426950408889634
LN2 = 0.6931471805599453
FAR = 2.0**30
F32 = jnp.float32
BF16 = jnp.bfloat16
VMEM_LIMIT = 60 * 1024 * 1024
FEED_LIMIT = 63 * 1024 * 1024
BY_MESH = pl.DeviceIdType.MESH
BY_LANES = (((1,), (1,)), ((), ()))


def flip(index, bit):
    return index + bit - 2 * bit * lax.rem(lax.div(index, bit), 2)


def gather_kernel(chunks, by_z, tok_ref, w_ref, all_ref, w_all_ref, send, recv, kept, w_send, w_recv):
    me = lax.axis_index("seq")
    shard = lax.axis_index("shard")
    shards = w_all_ref.shape[0]
    half = lax.div(me, GROUPS)
    y_near, z_near, partner = flip(me, 1), flip(me, 2), flip(me, 4)
    barrier = pltpu.get_barrier_semaphore()
    for device in (y_near, z_near, partner):
        pl.semaphore_signal(barrier, inc=1, device_id={"seq": device}, device_id_type=BY_MESH)
    for step in range(1, shards):
        pl.semaphore_signal(
            barrier, inc=1, device_id={"shard": lax.rem(shard + step, shards)}, device_id_type=BY_MESH
        )
    pl.semaphore_wait(barrier, 2 + shards)

    part = tok_ref.shape[1] // chunks
    started = []

    def go(source, target, slot, device):
        copy = pltpu.make_async_remote_copy(
            src_ref=source,
            dst_ref=target,
            send_sem=send.at[slot],
            recv_sem=recv.at[slot],
            device_id={"seq": device},
            device_id_type=BY_MESH,
        )
        copy.start()
        started.append(copy)
        return copy

    def rows(chunk):
        return pl.ds(chunk * part, part)

    def relay(piece, chunk, slot, device):
        return go(all_ref.at[piece, rows(chunk)], all_ref.at[piece, rows(chunk)], slot * chunks + chunk, device)

    def own(which, chunk, slot, device):
        return go(tok_ref.at[which, rows(chunk)], all_ref.at[me, rows(chunk)], slot * chunks + chunk, device)

    crossing = [own(1 - half, chunk, 0, partner) for chunk in range(chunks)]
    own_y, own_z = [], []
    for chunk in range(chunks):
        own_y.append(own(half, chunk, 1, y_near))
        own_z.append(own(half, chunk, 2, z_near))
    weights = []
    for step in range(1, shards):
        copy = pltpu.make_async_remote_copy(
            src_ref=w_ref,
            dst_ref=w_all_ref.at[shard],
            send_sem=w_send.at[step],
            recv_sem=w_recv.at[step],
            device_id={"shard": lax.rem(shard + step, shards)},
            device_id_type=BY_MESH,
        )
        copy.start()
        weights.append(copy)
    keep_tok = pltpu.make_async_copy(tok_ref.at[half], all_ref.at[me], kept.at[0])
    keep_tok.start()
    keep_w = pltpu.make_async_copy(w_ref, w_all_ref.at[shard], kept.at[1])
    keep_w.start()

    cross_y, cross_z, corner = [], [], []
    for chunk in range(chunks):
        own_y[chunk].wait_recv()
        if chunk < by_z:
            corner.append(relay(y_near, chunk, 5, z_near))
        own_z[chunk].wait_recv()
        if chunk >= by_z:
            corner.append(relay(z_near, chunk, 5, y_near))
        crossing[chunk].wait_recv()
        cross_y.append(relay(partner, chunk, 3, y_near))
        cross_z.append(relay(partner, chunk, 4, z_near))
    for chunk in range(chunks):
        cross_y[chunk].wait_recv()
        if chunk < by_z:
            corner.append(relay(flip(y_near, 4), chunk, 6, z_near))
        cross_z[chunk].wait_recv()
        if chunk >= by_z:
            corner.append(relay(flip(z_near, 4), chunk, 6, y_near))
    for copy in corner:
        copy.wait_recv()
    for copy in weights:
        copy.wait()
    keep_tok.wait()
    keep_w.wait()
    for copy in started:
        copy.wait_send()


def gather_tokens(tokens, w_part, shards, chunks=8, by_z=3):
    seqs, rows, width = tokens.shape
    anywhere = pl.BlockSpec(memory_space=pl.ANY)
    return pl.pallas_call(
        functools.partial(gather_kernel, chunks, by_z),
        out_shape=(
            jax.ShapeDtypeStruct((SEQ_SIZE, rows, width), tokens.dtype),
            jax.ShapeDtypeStruct((shards,) + w_part.shape, w_part.dtype),
        ),
        in_specs=[anywhere, anywhere],
        out_specs=(anywhere, anywhere),
        scratch_shapes=[
            pltpu.SemaphoreType.DMA((7 * chunks,)),
            pltpu.SemaphoreType.DMA((7 * chunks,)),
            pltpu.SemaphoreType.DMA((2,)),
            pltpu.SemaphoreType.DMA((shards,)),
            pltpu.SemaphoreType.DMA((shards,)),
        ],
        compiler_params=pltpu.CompilerParams(collective_id=1, has_side_effects=True),
        name="gather_tokens",
    )(tokens, w_part)


def project_kernel(seg_ref, place_ref, freq_ref, x_ref, w_ref, q_ref, k_ref, v_ref, turn_ref):
    rows = x_ref.shape[1]
    held = q_ref.shape[0]
    lane = lax.broadcasted_iota(jnp.int32, (rows, LANES), 1)
    seg = jnp.transpose(jnp.broadcast_to(seg_ref[0], (LANES, rows)))
    place = jnp.transpose(jnp.broadcast_to(place_ref[0], (LANES, rows)))
    turn = jnp.where(lane < HD, jnp.cos(place * freq_ref[...]), jnp.sin(place * freq_ref[...]))
    turn_ref[...] = turn
    cos_b = jnp.where(lane < HD, turn, 0.0)
    sin_b = jnp.where(lane < HD, pltpu.roll(turn, HD, 1), 0.0)
    sin_b = jnp.where(lane < HD // 2, -sin_b, sin_b)
    same = seg == (lane - HD).astype(F32)
    q_tail = jnp.where(same, 1.0, 0.0)
    k_tail = jnp.where(same | (lane < HD), 0.0, -FAR)
    v_tail = jnp.where(lane < HD, 0.0, 1.0)
    scale = HD ** (-0.5) * LOG2E
    q_cos, q_sin = cos_b * scale, sin_b * scale
    width = held * LANES
    for part in range(3):
        mixed = jnp.dot(x_ref[0], w_ref[:, part * width : (part + 1) * width], preferred_element_type=F32)
        for head in range(held):
            value = mixed[:, head * LANES : (head + 1) * LANES]
            if part == 0:
                value = value * q_cos + pltpu.roll(value, HD // 2, 1) * q_sin + q_tail
                q_ref[head] = value.astype(BF16)
            elif part == 1:
                value = value * cos_b + pltpu.roll(value, HD // 2, 1) * sin_b + k_tail
                k_ref[head] = value.astype(BF16)
            else:
                v_ref[head] = (value + v_tail).astype(BF16)


def project_heads(seg_row, place_row, freq, pieces, w_full, held):
    count, rows, width = pieces.shape
    length = count * rows
    row_spec = pl.BlockSpec((1, 1, rows), lambda i: (i, 0, 0))
    head_spec = pl.BlockSpec((held, rows, LANES), lambda i: (0, i, 0))
    head_shape = jax.ShapeDtypeStruct((held, length, LANES), BF16)
    return pl.pallas_call(
        project_kernel,
        out_shape=(head_shape, head_shape, head_shape, jax.ShapeDtypeStruct((length, LANES), F32)),
        grid=(count,),
        in_specs=[
            row_spec,
            row_spec,
            pl.BlockSpec((1, LANES), lambda i: (0, 0)),
            pl.BlockSpec((1, rows, width), lambda i: (i, 0, 0)),
            pl.BlockSpec(w_full.shape, lambda i: (0, 0)),
        ],
        out_specs=(head_spec, head_spec, head_spec, pl.BlockSpec((rows, LANES), lambda i: (i, 0))),
        compiler_params=pltpu.CompilerParams(vmem_limit_bytes=VMEM_LIMIT),
        cost_estimate=pl.CostEstimate(
            flops=2 * length * width * w_full.shape[1],
            bytes_accessed=length * (width * 2 + held * LANES * 6 + LANES * 4),
            transcendentals=length * LANES,
        ),
        name="project_heads",
    )(seg_row.reshape(count, 1, rows), place_row.reshape(count, 1, rows), freq, pieces, w_full)


def document_bounds(seg_row, rows):
    first = seg_row[::rows]
    last = seg_row[rows - 1 :: rows]
    low = jnp.sum((seg_row[None, :] < first[:, None]).astype(jnp.int32), axis=1)
    high = jnp.sum((seg_row[None, :] <= last[:, None]).astype(jnp.int32), axis=1)
    return low, high


def windows(bounds, length, window, align):
    low = bounds[0] // align * align
    count = (bounds[1] - low + window - 1) // window
    return jnp.minimum(low, length - count * window), count


def attend_kernel(window, align, low_ref, count_ref, q_ref, k_ref, v_ref, sum_ref, joined_ref):
    block = pl.program_id(0)
    low = low_ref[block]
    sum_ref[...] = jnp.zeros_like(sum_ref)

    def step(index, carry):
        start = pl.multiple_of(low + index * window, align)
        for head in range(q_ref.shape[0]):
            k_part = k_ref[head, pl.ds(start, window), :]
            v_part = v_ref[head, pl.ds(start, window), :]
            score = lax.dot_general(q_ref[head], k_part, BY_LANES, preferred_element_type=F32)
            expo = jnp.exp2(score).astype(BF16)
            sum_ref[head] += jnp.dot(expo, v_part, preferred_element_type=F32)
        return carry

    lax.fori_loop(0, count_ref[block], step, 0)
    for head in range(q_ref.shape[0]):
        sums = sum_ref[head]
        joined_ref[0, :, head * HD : (head + 1) * HD] = (sums[:, :HD] / sums[:, HD : HD + 1]).astype(BF16)


def attend_heads(bounds, q_ext, k_ext, v_ext, rows, window=1024, align=16):
    heads, length, lanes = q_ext.shape
    low, count = windows(bounds, length, window, align)
    whole = pl.BlockSpec((heads, length, lanes), lambda i, *_: (0, 0, 0))
    part = pl.BlockSpec((heads, rows, lanes), lambda i, *_: (0, i, 0))
    return pl.pallas_call(
        functools.partial(attend_kernel, window, align),
        out_shape=(
            jax.ShapeDtypeStruct((heads, length, lanes), F32),
            jax.ShapeDtypeStruct((length // rows, rows, heads * HD), BF16),
        ),
        grid_spec=pltpu.PrefetchScalarGridSpec(
            num_scalar_prefetch=2,
            grid=(length // rows,),
            in_specs=[part, whole, whole],
            out_specs=(part, pl.BlockSpec((1, rows, heads * HD), lambda i, *_: (i, 0, 0))),
        ),
        compiler_params=pltpu.CompilerParams(vmem_limit_bytes=VMEM_LIMIT),
        cost_estimate=pl.CostEstimate(
            flops=heads * length * length * 4 * lanes // 2,
            bytes_accessed=heads * length * lanes * 10,
            transcendentals=heads * length * length // 2,
        ),
        name="attend_heads",
    )(low, count, q_ext, k_ext, v_ext)


def attend_back_kernel(
    window,
    align,
    low_ref,
    count_ref,
    q_ref,
    sum_ref,
    dout_ref,
    turn_ref,
    k_ref,
    v_ref,
    d_ref,
    dq_ref,
    dkv_ref,
    g_ref,
    gt_ref,
    qt_ref,
):
    block = pl.program_id(0)
    heads, rows, lanes = q_ref.shape
    width = heads * HD

    @pl.when(block == 0)
    def _():
        dkv_ref[...] = jnp.zeros_like(dkv_ref)

    dq_ref[...] = jnp.zeros_like(dq_ref)
    half_lane = lax.broadcasted_iota(jnp.int32, (rows, HD), 1)
    for head in range(heads):
        dout = dout_ref[0, :, head * HD : (head + 1) * HD].astype(F32)
        sums = sum_ref[head]
        total = sums[:, HD : HD + 1]
        g_low = dout / total
        delta = -jnp.sum(dout * sums[:, :HD], axis=1, keepdims=True) / (total * total)
        high = delta.astype(BF16).astype(F32)
        middle = (delta - high).astype(BF16).astype(F32)
        tail = jnp.where(
            half_lane == 0,
            high,
            jnp.where(half_lane == 1, middle, jnp.where(half_lane == 2, delta - high - middle, 0.0)),
        )
        g_ext = jnp.concatenate([g_low, tail], axis=1)
        g_ref[head] = g_ext.astype(BF16)
        gt_ref[head] = jnp.transpose(g_ext)[:HD].astype(BF16)
        qt_ref[head] = jnp.transpose(q_ref[head].astype(F32))[:HD].astype(BF16)

    low = low_ref[block]

    def step(index, carry):
        start = pl.multiple_of(low + index * window, align)
        for head in range(heads):
            k_part = k_ref[head, pl.ds(start, window), :]
            v_part = v_ref[head, pl.ds(start, window), :]
            score = lax.dot_general(q_ref[head], k_part, BY_LANES, preferred_element_type=F32)
            slope = lax.dot_general(g_ref[head], v_part, BY_LANES, preferred_element_type=F32)
            expo = jnp.exp2(score)
            d_score = (expo * slope).astype(BF16)
            expo = expo.astype(BF16)
            dq_ref[head] += jnp.dot(d_score, k_part, preferred_element_type=F32)
            dkv_ref[head, :HD, pl.ds(start, window)] += jnp.dot(qt_ref[head], d_score, preferred_element_type=F32)
            dkv_ref[head, HD:, pl.ds(start, window)] += jnp.dot(gt_ref[head], expo, preferred_element_type=F32)
        return carry

    lax.fori_loop(0, count_ref[block], step, 0)

    lane = lax.broadcasted_iota(jnp.int32, (rows, lanes), 1)

    def turn_back(value, turn):
        swapped = jnp.where(lane < HD // 2, pltpu.roll(value, lanes - HD // 2, 1), pltpu.roll(value, HD // 2, 1))
        sine = pltpu.roll(turn, HD, 1)
        sine = jnp.where(lane < HD // 2, sine, -sine)
        return (value * turn + swapped * sine)[:, :HD]

    here = turn_ref[pl.ds(pl.multiple_of(block * rows, rows), rows), :]
    for head in range(heads):
        turned = turn_back(dq_ref[head] * HD ** (-0.5), here)
        d_ref[block, :, head * HD : (head + 1) * HD] = turned.astype(BF16)

    @pl.when(block == pl.num_programs(0) - 1)
    def _():
        def finish(piece, carry):
            start = pl.multiple_of(piece * rows, rows)
            turn = turn_ref[pl.ds(start, rows), :]
            for head in range(heads):
                both = jnp.transpose(dkv_ref[head, :, pl.ds(start, rows)])
                at = width + head * HD
                d_ref[piece, :, at : at + HD] = (turn_back(both, turn) * LN2).astype(BF16)
                d_ref[piece, :, width + at : width + at + HD] = both[:, HD:].astype(BF16)
            return carry

        lax.fori_loop(0, d_ref.shape[0], finish, 0)


def attend_back_heads(bounds, q_ext, k_ext, v_ext, sums, dout, turn, window=512, align=128):
    heads, length, lanes = q_ext.shape
    count_blocks, rows, width = dout.shape
    low, count = windows(bounds, length, window, align)
    whole = pl.BlockSpec((heads, length, lanes), lambda i, *_: (0, 0, 0))
    part = pl.BlockSpec((heads, rows, lanes), lambda i, *_: (0, i, 0))
    return pl.pallas_call(
        functools.partial(attend_back_kernel, window, align),
        out_shape=jax.ShapeDtypeStruct((count_blocks, rows, 3 * width), BF16),
        grid_spec=pltpu.PrefetchScalarGridSpec(
            num_scalar_prefetch=2,
            grid=(count_blocks,),
            in_specs=[
                part,
                part,
                pl.BlockSpec((1, rows, width), lambda i, *_: (i, 0, 0)),
                pl.BlockSpec((length, lanes), lambda i, *_: (0, 0)),
                whole,
                whole,
            ],
            out_specs=pl.BlockSpec((count_blocks, rows, 3 * width), lambda i, *_: (0, 0, 0)),
            scratch_shapes=[
                pltpu.VMEM((heads, rows, lanes), F32),
                pltpu.VMEM((heads, 2 * HD, length), F32),
                pltpu.VMEM((heads, rows, lanes), BF16),
                pltpu.VMEM((heads, HD, rows), BF16),
                pltpu.VMEM((heads, HD, rows), BF16),
            ],
        ),
        compiler_params=pltpu.CompilerParams(vmem_limit_bytes=VMEM_LIMIT),
        cost_estimate=pl.CostEstimate(
            flops=heads * length * length * 10 * lanes // 2,
            bytes_accessed=heads * length * lanes * 20,
            transcendentals=heads * length * length // 2,
        ),
        name="attend_back_heads",
    )(low, count, q_ext, sums, dout, turn, k_ext, v_ext)


def scatter_kernel(
    chunks,
    by_z,
    part_ref,
    dh_ref,
    gw_ref,
    norm_ref,
    out_ref,
    gw_all_ref,
    norm_out_ref,
    got_y,
    got_z,
    relay_y,
    relay_z,
    sent_y,
    sent_z,
    cross_out,
    cross_in,
    gw_got,
    gw_mine,
    gw_pair,
    gw_final,
    norm_got,
    norm_sent,
    send,
    recv,
    gw_send,
    gw_recv,
    norm_send,
    norm_recv,
    kept,
):
    me = lax.axis_index("seq")
    shard = lax.axis_index("shard")
    shards = gw_ref.shape[0]
    half = lax.div(me, GROUPS)
    y_near, z_near, partner = flip(me, 1), flip(me, 2), flip(me, 4)
    corner = flip(y_near, 2)
    barrier = pltpu.get_barrier_semaphore()
    for device in (y_near, z_near, partner, corner):
        pl.semaphore_signal(barrier, inc=1, device_id={"seq": device}, device_id_type=BY_MESH)
    for step in range(1, shards):
        pl.semaphore_signal(
            barrier, inc=1, device_id={"shard": lax.rem(shard + step, shards)}, device_id_type=BY_MESH
        )
    pl.semaphore_wait(barrier, 3 + shards)

    started = []

    def go(source, target, sends, receives, slot, where):
        copy = pltpu.make_async_remote_copy(
            src_ref=source,
            dst_ref=target,
            send_sem=sends.at[slot],
            recv_sem=receives.at[slot],
            device_id=where,
            device_id_type=BY_MESH,
        )
        copy.start()
        started.append(copy)
        return copy

    rows = part_ref.shape[1] // chunks

    def band(chunk):
        return pl.ds(chunk * rows, rows)

    def piece(device, far):
        return flip(device, 4) if far else device

    def slot(kind, far, chunk):
        return (kind * 2 + (0 if far else 1)) * chunks + chunk

    gw_one = [
        go(
            gw_ref.at[lax.rem(shard + step, shards)],
            gw_got.at[step - 1],
            gw_send,
            gw_recv,
            step - 1,
            {"shard": lax.rem(shard + step, shards)},
        )
        for step in range(1, shards)
    ]
    pairs = [
        {"shard": flip(shard, 1)},
        {"shard": flip(shard, 2)},
        {"seq": y_near},
        {"seq": z_near},
        {"seq": partner},
    ]
    norm_sent[0] = norm_ref[...]

    from_corner, direct = {}, {}
    for far in (True, False):
        for chunk in range(chunks):
            over_z = chunk < by_z
            from_corner[far, chunk] = go(
                part_ref.at[piece(corner, far), band(chunk)],
                (relay_y if over_z else relay_z).at[0 if far else 1, chunk if over_z else chunk - by_z],
                send,
                recv,
                slot(0, far, chunk),
                {"seq": y_near if over_z else z_near},
            )
        for chunk in range(chunks):
            over_z = chunk < by_z
            near = y_near if over_z else z_near
            direct[far, chunk] = go(
                part_ref.at[piece(near, far), band(chunk)],
                (got_y if over_z else got_z).at[0 if far else 1, band(chunk)],
                send,
                recv,
                slot(1 if over_z else 2, far, chunk),
                {"seq": near},
            )

    norm_copies = [go(norm_sent.at[0], norm_got.at[0], norm_send, norm_recv, 0, pairs[0])]
    done_norm = 0

    def norm_step(index):
        norm_copies[index].wait_recv()
        total = norm_sent[index] + norm_got[index]
        if index + 1 < len(pairs):
            norm_sent[index + 1] = total
            norm_copies.append(
                go(norm_sent.at[index + 1], norm_got.at[index + 1], norm_send, norm_recv, index + 1, pairs[index + 1])
            )
        else:
            norm_out_ref[...] = total

    relayed = {}

    def relay(far, chunk):
        over_z = chunk < by_z
        target = z_near if over_z else y_near
        index = chunk if over_z else chunk - by_z
        which = 0 if far else 1
        from_corner[far, chunk].wait_recv()
        source = relay_y if over_z else relay_z
        buffer = sent_y if over_z else sent_z
        mine = part_ref[piece(target, far), band(chunk)].astype(F32)
        buffer[which, index] = (source[which, index].astype(F32) + mine).astype(BF16)
        relayed[far, chunk] = go(
            buffer.at[which, index],
            (got_z if over_z else got_y).at[which, band(chunk)],
            send,
            recv,
            slot(2 if over_z else 1, far, chunk),
            {"seq": target},
        )

    def total(far, chunk):
        which = 0 if far else 1
        direct[far, chunk].wait_recv()
        relayed[far, chunk].wait_recv()
        mine = part_ref[piece(me, far), band(chunk)].astype(F32)
        return mine + got_y[which, band(chunk)].astype(F32) + got_z[which, band(chunk)].astype(F32)

    for chunk in range(chunks):
        relay(True, chunk)
    norm_step(0)
    for copy in gw_one:
        copy.wait_recv()
    summed = gw_ref[shard].astype(F32)
    for step in range(1, shards):
        summed = summed + gw_got[step - 1].astype(F32)
    gw_mine[...] = summed.astype(BF16)
    norm_step(1)
    gw_two = go(gw_mine, gw_pair, gw_send, gw_recv, shards - 1, {"seq": partner})
    crossing = []
    for chunk in range(chunks):
        cross_out[band(chunk)] = total(True, chunk).astype(BF16)
        crossing.append(
            go(cross_out.at[band(chunk)], cross_in.at[band(chunk)], send, recv, slot(3, True, chunk), {"seq": partner})
        )
        relay(False, chunk)
    norm_step(2)
    gw_two.wait_recv()
    gw_final[...] = (gw_mine[...].astype(F32) + gw_pair[...].astype(F32)).astype(BF16)
    norm_step(3)
    group = lax.rem(me, GROUPS)
    gw_three = [
        go(gw_final, gw_all_ref.at[group], gw_send, gw_recv, shards + n, {"seq": device})
        for n, device in enumerate((y_near, z_near, corner))
    ]
    keep = pltpu.make_async_copy(gw_final, gw_all_ref.at[group], kept.at[0])
    keep.start()
    for chunk in range(chunks):
        out_ref[half, band(chunk)] = (total(False, chunk) + dh_ref[half, band(chunk)]).astype(BF16)
    norm_step(4)
    for chunk in range(chunks):
        crossing[chunk].wait_recv()
        other = 1 - half
        out_ref[other, band(chunk)] = (cross_in[band(chunk)].astype(F32) + dh_ref[other, band(chunk)]).astype(BF16)
    for copy in gw_three:
        copy.wait_recv()
    keep.wait()
    for copy in started:
        copy.wait_send()


def scatter_gradients(partial, dh_one, grad_columns, norms, chunks=4, by_z=3):
    _, rows, width = partial.shape
    shards, depth, columns = grad_columns.shape
    part = rows // chunks
    vmem = pl.BlockSpec(memory_space=pltpu.VMEM)
    dma = pltpu.SemaphoreType.DMA
    return pl.pallas_call(
        functools.partial(scatter_kernel, chunks, by_z),
        out_shape=(
            jax.ShapeDtypeStruct(dh_one.shape, BF16),
            jax.ShapeDtypeStruct((GROUPS, depth, columns), BF16),
            jax.ShapeDtypeStruct(norms.shape, F32),
        ),
        in_specs=[vmem] * 4,
        out_specs=(vmem,) * 3,
        scratch_shapes=[
            pltpu.VMEM((2, rows, width), BF16),
            pltpu.VMEM((2, rows, width), BF16),
            pltpu.VMEM((2, by_z, part, width), BF16),
            pltpu.VMEM((2, chunks - by_z, part, width), BF16),
            pltpu.VMEM((2, by_z, part, width), BF16),
            pltpu.VMEM((2, chunks - by_z, part, width), BF16),
            pltpu.VMEM((rows, width), BF16),
            pltpu.VMEM((rows, width), BF16),
            pltpu.VMEM((shards - 1, depth, columns), BF16),
            pltpu.VMEM((depth, columns), BF16),
            pltpu.VMEM((depth, columns), BF16),
            pltpu.VMEM((depth, columns), BF16),
            pltpu.VMEM((5,) + norms.shape, F32),
            pltpu.VMEM((5,) + norms.shape, F32),
            dma((7 * chunks,)),
            dma((7 * chunks,)),
            dma((shards + 3,)),
            dma((shards + 3,)),
            dma((5,)),
            dma((5,)),
            dma((1,)),
        ],
        compiler_params=pltpu.CompilerParams(
            collective_id=2, has_side_effects=True, vmem_limit_bytes=VMEM_LIMIT
        ),
        cost_estimate=pl.CostEstimate(flops=60 * 10**9, bytes_accessed=64 * 2**20, transcendentals=0),
        name="scatter_gradients",
    )(partial, dh_one, grad_columns, norms)


def feed_forward_kernel(
    tokens_ref,
    joined_ref,
    cot_ref,
    out_hbm,
    gate_hbm,
    up_hbm,
    down_hbm,
    norms_ref,
    output_ref,
    dout_ref,
    dh_ref,
    norm_sums_ref,
    packed_ref,
    w_out,
    w_gate,
    w_up,
    w_down,
    flow,
    hat_one,
    inverse_one,
    x_low,
    x_turned,
    dm_low,
    gate_kept,
    up_kept,
    d_gate,
    d_up,
    hidden_kept,
    staged,
    loads,
    stores,
):
    seqs, rows, width = dh_ref.shape
    shards = packed_ref.shape[0]
    depth = width // shards
    blocks = gate_hbm.shape[1] // width
    weights = ((out_hbm, w_out), (gate_hbm, w_gate), (up_hbm, w_up), (down_hbm, w_down))
    fetch = [pltpu.make_async_copy(src, dst, loads.at[n]) for n, (src, dst) in enumerate(weights)]
    tokens_in = pltpu.make_async_copy(tokens_ref, flow, loads.at[4])
    tokens_in.start()
    for copy in fetch:
        copy.start()
    gain_one, bias_one, gain_two, bias_two = (norms_ref[n : n + 1, :] for n in range(4))

    def mean(value):
        return jnp.sum(value, axis=-1, keepdims=True) * (1.0 / width)

    fetch[0].wait()
    tokens_in.wait()
    for seq in range(seqs):
        h_one = flow[seq].astype(F32)
        for group in range(GROUPS):
            h_one = h_one + jnp.dot(
                joined_ref[seq * GROUPS + group],
                w_out[group * depth : (group + 1) * depth, :],
                preferred_element_type=F32,
            )
        centered = h_one - mean(h_one)
        inverse = lax.rsqrt(mean(centered * centered) + EPS)
        normed = centered * inverse
        hat_one[seq] = normed
        inverse_one[seq] = inverse
        x_one = normed * gain_one + bias_one
        dh_ref[seq] = x_one
        x_low[seq] = x_one.astype(BF16)
        x_turned[:, seq * rows : (seq + 1) * rows] = jnp.transpose(x_one).astype(BF16)
    cot_in = pltpu.make_async_copy(cot_ref, flow, loads.at[4])
    cot_in.start()
    for copy in fetch[1:]:
        copy.wait()

    def forward(block, carry):
        at = pl.ds(pl.multiple_of(block * width, width), width)
        for seq in range(seqs):
            gate = jnp.dot(x_low[seq], w_gate[:, at], preferred_element_type=F32)
            up = jnp.dot(x_low[seq], w_up[:, at], preferred_element_type=F32)
            gate_kept[block, seq] = gate.astype(gate_kept.dtype)
            up_kept[block, seq] = up.astype(up_kept.dtype)
            hidden = (gate * jax.nn.sigmoid(gate) * up).astype(BF16)
            dh_ref[seq] += jnp.dot(hidden, w_down[at, :], preferred_element_type=F32)
        return carry

    lax.fori_loop(0, blocks, forward, 0)

    cot_in.wait()
    gain_two_sum = jnp.zeros((1, width), F32)
    bias_two_sum = jnp.zeros((1, width), F32)
    for seq in range(seqs):
        h_two = dh_ref[seq]
        centered = h_two - mean(h_two)
        inverse = lax.rsqrt(mean(centered * centered) + EPS)
        normed = centered * inverse
        cot = flow[seq].astype(F32)
        flow[seq] = (normed * gain_two + bias_two).astype(BF16)
        gain_two_sum = gain_two_sum + jnp.sum(cot * normed, axis=0, keepdims=True)
        bias_two_sum = bias_two_sum + jnp.sum(cot, axis=0, keepdims=True)
        scaled = cot * gain_two
        dh_two = inverse * (scaled - mean(scaled) - normed * mean(scaled * normed))
        dh_ref[seq] = dh_two
        dm_low[seq * rows : (seq + 1) * rows, :] = dh_two.astype(BF16)
    output_out = pltpu.make_async_copy(flow, output_ref, loads.at[4])
    output_out.start()

    def store(kind, block):
        if kind < 2:
            start = pl.multiple_of((kind * blocks + block) * depth, depth)
            return [
                pltpu.make_async_copy(
                    staged.at[kind, pl.ds(shard * depth, depth)],
                    packed_ref.at[shard, pl.ds(start, depth)],
                    stores.at[kind, shard],
                )
                for shard in range(shards)
            ]
        start = 2 * blocks * depth
        return [
            pltpu.make_async_copy(
                staged.at[2], packed_ref.at[block, pl.ds(start, width)], stores.at[2, 0]
            )
        ]

    def backward(block, carry):
        at = pl.ds(pl.multiple_of(block * width, width), width)
        for seq in range(seqs):
            here = slice(seq * rows, (seq + 1) * rows)
            d_hidden = lax.dot_general(dm_low[here, :], w_down[at, :], BY_LANES, preferred_element_type=F32)
            gate = gate_kept[block, seq].astype(F32)
            up = up_kept[block, seq].astype(F32)
            sigma = jax.nn.sigmoid(gate)
            smooth = gate * sigma
            hidden_kept[here, :] = (smooth * up).astype(BF16)
            dg = (d_hidden * up * (sigma + smooth * (1.0 - sigma))).astype(BF16)
            du = (d_hidden * smooth).astype(BF16)
            d_gate[here, :] = dg
            d_up[here, :] = du
            dh_ref[seq] += lax.dot_general(dg, w_gate[:, at], BY_LANES, preferred_element_type=F32)
            dh_ref[seq] += lax.dot_general(du, w_up[:, at], BY_LANES, preferred_element_type=F32)

        @pl.when(block > 0)
        def _():
            for kind in range(3):
                for copy in store(kind, block - 1):
                    copy.wait()

        staged[0] = jnp.dot(x_turned[...], d_gate[...], preferred_element_type=F32).astype(BF16)
        staged[1] = jnp.dot(x_turned[...], d_up[...], preferred_element_type=F32).astype(BF16)
        staged[2] = lax.dot_general(
            hidden_kept[...], dm_low[...], (((0,), (0,)), ((), ())), preferred_element_type=F32
        ).astype(BF16)
        for kind in range(3):
            for copy in store(kind, block):
                copy.start()
        return carry

    lax.fori_loop(0, blocks, backward, 0)

    gain_one_sum = jnp.zeros((1, width), F32)
    bias_one_sum = jnp.zeros((1, width), F32)
    for seq in range(seqs):
        here = slice(seq * rows, (seq + 1) * rows)
        dx_one = dh_ref[seq]
        normed = hat_one[seq]
        gain_one_sum = gain_one_sum + jnp.sum(dx_one * normed, axis=0, keepdims=True)
        bias_one_sum = bias_one_sum + jnp.sum(dx_one, axis=0, keepdims=True)
        scaled = dx_one * gain_one
        dh_one = inverse_one[seq] * (scaled - mean(scaled) - normed * mean(scaled * normed))
        dh_ref[seq] = dh_one
        d_attn = dh_one.astype(BF16)
        d_gate[here, :] = d_attn
        for group in range(GROUPS):
            dout_ref[seq * GROUPS + group] = lax.dot_general(
                d_attn, w_out[group * depth : (group + 1) * depth, :], BY_LANES, preferred_element_type=F32
            ).astype(BF16)
    for kind in range(3):
        for copy in store(kind, blocks - 1):
            copy.wait()
    for group in range(GROUPS):
        grad = jnp.zeros((depth, width), F32)
        for seq in range(seqs):
            grad = grad + lax.dot_general(
                joined_ref[seq * GROUPS + group],
                d_gate[seq * rows : (seq + 1) * rows, :],
                (((0,), (0,)), ((), ())),
                preferred_element_type=F32,
            )
        staged[0, group * depth : (group + 1) * depth, :] = grad.astype(BF16)
    last = [
        pltpu.make_async_copy(
            staged.at[0, pl.ds(shard * depth, depth)],
            packed_ref.at[shard, pl.ds(3 * blocks * depth, depth)],
            stores.at[0, shard],
        )
        for shard in range(shards)
    ]
    for copy in last:
        copy.start()
    norm_sums_ref[0:1, :] = gain_one_sum
    norm_sums_ref[1:2, :] = bias_one_sum
    norm_sums_ref[2:3, :] = gain_two_sum
    norm_sums_ref[3:4, :] = bias_two_sum
    for copy in last:
        copy.wait()
    output_out.wait()


def feed_forward(tokens, joined, cotangent, w_out, w_gate, w_up, w_down, norms, kept=BF16):
    seqs, rows, width = tokens.shape
    total = seqs * rows
    hidden = w_gate.shape[1]
    blocks = hidden // width
    depth = width // GROUPS
    vmem = pl.BlockSpec(memory_space=pltpu.VMEM)
    hbm = pl.BlockSpec(memory_space=pltpu.HBM)
    dma = pltpu.SemaphoreType.DMA
    return pl.pallas_call(
        feed_forward_kernel,
        out_shape=(
            jax.ShapeDtypeStruct(tokens.shape, BF16),
            jax.ShapeDtypeStruct(joined.shape, BF16),
            jax.ShapeDtypeStruct(tokens.shape, F32),
            jax.ShapeDtypeStruct((4, width), F32),
            jax.ShapeDtypeStruct((GROUPS, (3 * blocks + 1) * depth, width), BF16),
        ),
        in_specs=[hbm, vmem, hbm, hbm, hbm, hbm, hbm, vmem],
        out_specs=(hbm, vmem, vmem, vmem, hbm),
        scratch_shapes=[
            pltpu.VMEM(w_out.shape, BF16),
            pltpu.VMEM(w_gate.shape, BF16),
            pltpu.VMEM(w_up.shape, BF16),
            pltpu.VMEM(w_down.shape, BF16),
            pltpu.VMEM(tokens.shape, BF16),
            pltpu.VMEM(tokens.shape, F32),
            pltpu.VMEM((seqs, rows, 1), F32),
            pltpu.VMEM(tokens.shape, BF16),
            pltpu.VMEM((width, total), BF16),
            pltpu.VMEM((total, width), BF16),
            pltpu.VMEM((blocks, seqs, rows, width), kept),
            pltpu.VMEM((blocks, seqs, rows, width), kept),
            pltpu.VMEM((total, width), BF16),
            pltpu.VMEM((total, width), BF16),
            pltpu.VMEM((total, width), BF16),
            pltpu.VMEM((3, width, width), BF16),
            dma((5,)),
            dma((3, GROUPS)),
        ],
        compiler_params=pltpu.CompilerParams(vmem_limit_bytes=FEED_LIMIT),
        cost_estimate=pl.CostEstimate(
            flops=6 * total * width * (3 * hidden + width),
            bytes_accessed=2 * 2 * (3 * hidden + width) * width + 20 * total * width,
            transcendentals=2 * total * hidden,
        ),
        name="feed_forward",
    )(tokens, joined, cotangent, w_out, w_gate, w_up, w_down, norms)


def document_places(seg_row):
    length = seg_row.shape[0]
    ids = jnp.arange(LANES - HD, dtype=jnp.int32)[:, None]
    starts = jnp.sum((seg_row[None, :] < ids).astype(jnp.int32), axis=1, keepdims=True)
    start = jnp.sum(jnp.where(seg_row[None, :] == ids, starts, 0), axis=0)
    return jnp.arange(length, dtype=jnp.int32) - start


def exchange(blocks):
    return lax.all_to_all(blocks, "seq", 0, 0, tiled=True)


def head_columns(w_qkv, group, held):
    depth = w_qkv.shape[0]
    split = w_qkv.reshape(depth, 3, GROUPS, held, HD)
    mine = lax.dynamic_index_in_dim(split, group, 2, keepdims=False)
    second = mine * jnp.array([1, 1, 0], w_qkv.dtype)[None, :, None, None]
    return jnp.concatenate([mine, second], axis=-1).reshape(depth, 3 * held * 2 * HD)


def local_heads(
    shards,
    tokens,
    segments,
    positions,
    cotangent,
    w_qkv,
    w_out,
    w_gate,
    w_up,
    w_down,
    ln1_gain,
    ln1_bias,
    ln2_gain,
    ln2_bias,
):
    seq_count, row_count, model_width = tokens.shape
    held = HEADS // GROUPS
    length = row_count * SEQ_SIZE
    me = lax.axis_index("seq")
    seg_row = lax.dynamic_index_in_dim(segments, me // GROUPS, 0, keepdims=False)

    def gather(shard):
        return lax.all_gather(shard, "shard", axis=0, tiled=True)

    pieces, w_heads = gather_tokens(tokens, head_columns(w_qkv, me % GROUPS, held), shards)
    norms = lax.all_gather(jnp.stack([ln1_gain, ln1_bias, ln2_gain, ln2_bias]), "shard", axis=1, tiled=True).astype(F32)
    full_out, full_gate, full_up, full_down = (gather(w) for w in (w_out, w_gate, w_up, w_down))
    freqs = jnp.exp(jnp.arange(HD // 2, dtype=F32) * (-math.log(ROPE_BASE) / (HD // 2)))
    freq = jnp.tile(freqs, LANES // (HD // 2))[None]
    place = document_places(seg_row).astype(F32)
    bounds = document_bounds(seg_row, row_count)
    q_ext, k_ext, v_ext, turn = project_heads(
        seg_row.astype(F32), place, freq, pieces, w_heads.reshape(model_width, -1), held
    )
    sums, joined_own = attend_heads(bounds, q_ext, k_ext, v_ext, row_count)
    output, d_joined, dh_one, norms_part, packed = feed_forward(
        tokens, exchange(joined_own), cotangent, full_out, full_gate, full_up, full_down, norms
    )
    depth = model_width // shards
    ff_blocks = full_gate.shape[1] // model_width
    owned = lax.psum_scatter(
        packed.reshape(-1, model_width), ("shard", "seq"), scatter_dimension=0, tiled=True
    )

    dout = exchange(d_joined)
    d_heads = attend_back_heads(bounds, q_ext, k_ext, v_ext, sums, dout, turn)
    w_own = w_heads.reshape(model_width, -1, LANES)[:, :, :HD].reshape(model_width, -1)
    partial = jnp.einsum("prc,dc->prd", d_heads, w_own, preferred_element_type=F32).astype(BF16)
    grad_columns = jnp.einsum("prd,prc->dc", pieces, d_heads, preferred_element_type=F32).astype(BF16)
    partial, grad_columns, owned = lax.optimization_barrier((partial, grad_columns, owned))
    shared = lax.all_gather(owned, "seq", axis=0, tiled=True)
    input_grad, columns, norm_sums = scatter_gradients(
        partial, dh_one, grad_columns.reshape(shards, depth, -1), norms_part
    )
    grad_qkv = jnp.transpose(columns.reshape(GROUPS, depth, 3, held * HD), (1, 2, 0, 3))
    grad_qkv = grad_qkv.reshape(depth, 3 * model_width).astype(F32)

    def taken(start, blocks):
        rows = shared[start : start + blocks * depth].reshape(blocks, depth, model_width)
        return jnp.transpose(rows, (1, 0, 2)).reshape(depth, blocks * model_width).astype(F32)

    ff_rows = ff_blocks * depth
    grad_gate, grad_up = taken(0, ff_blocks), taken(ff_rows, ff_blocks)
    grad_down = shared[2 * ff_rows : 3 * ff_rows].astype(F32)
    grad_out = taken(3 * ff_rows, 1)
    shard = lax.axis_index("shard")
    norm_sums = lax.dynamic_slice_in_dim(norm_sums, shard * depth, depth, 1)
    return (
        output,
        input_grad,
        grad_qkv,
        grad_out,
        grad_gate,
        grad_up,
        grad_down,
        norm_sums[0],
        norm_sums[1],
        norm_sums[2],
        norm_sums[3],
    )


def solution(mesh):
    in_specs = (
        P("shard", "seq", None),
        P("shard", None),
        P("shard", "seq"),
        P("shard", "seq", None),
        P("shard", None),
        P("shard", None),
        P("shard", None),
        P("shard", None),
        P("shard", None),
        P("shard"),
        P("shard"),
        P("shard"),
        P("shard"),
    )
    out_specs = (
        P("shard", "seq", None),
        P("shard", "seq", None),
        P("shard", None),
        P("shard", None),
        P("shard", None),
        P("shard", None),
        P("shard", None),
        P("shard"),
        P("shard"),
        P("shard"),
        P("shard"),
    )
    body = functools.partial(local_heads, mesh.shape["shard"]) if (mesh.shape["seq"], mesh.shape["shard"]) == (SEQ_SIZE, GROUPS) else local
    return jax.shard_map(body, mesh=mesh, in_specs=in_specs, out_specs=out_specs, check_vma=False)
```

```python
import functools
import math

import jax
import jax.numpy as jnp
from jax import lax
from jax.experimental import pallas as pl
from jax.experimental.pallas import tpu as pltpu
from jax.sharding import PartitionSpec as P

HEADS = 12
HD = 64


EPS = 1e-05
ROPE_BASE = 1000.0


def rope_tables(pos_block):
    half_dim = HD // 2
    freqs = jnp.exp(jnp.arange(half_dim, dtype=jnp.float32) * (-math.log(ROPE_BASE) / half_dim))
    angle = pos_block.astype(jnp.float32)[..., None] * freqs
    return (jnp.cos(angle)[:, :, None, :], jnp.sin(angle)[:, :, None, :])


def rotate(heads, cos_b, sin_b):
    half_dim = heads.shape[-1] // 2
    first = heads[..., :half_dim]
    second = heads[..., half_dim:]
    return jnp.concatenate(
        [first * cos_b - second * sin_b, second * cos_b + first * sin_b], axis=-1
    )


def rotate_back(grads, cos_b, sin_b):
    half_dim = grads.shape[-1] // 2
    first = grads[..., :half_dim]
    second = grads[..., half_dim:]
    return jnp.concatenate(
        [first * cos_b + second * sin_b, second * cos_b - first * sin_b], axis=-1
    )


def norm_fwd(values, gain, bias):
    mean_val = jnp.mean(values, axis=-1, keepdims=True)
    centered = values - mean_val
    variance = jnp.mean(centered * centered, axis=-1, keepdims=True)
    inverse = lax.rsqrt(variance + EPS)
    normed = centered * inverse
    return (normed * gain + bias, normed, inverse)


def norm_back(grad_in, normed, inverse, gain):
    scaled = grad_in * gain
    return inverse * (
        scaled
        - jnp.mean(scaled, axis=-1, keepdims=True)
        - normed * jnp.mean(scaled * normed, axis=-1, keepdims=True)
    )


def head_split(block_rows, seq_count, row_count):
    return block_rows.reshape(seq_count, row_count, HEADS, HD)


def attend(q_heads, q_seg, k_full, v_full, seg_all, block, score_scale):
    seq_count, row_count = (q_heads.shape[0], q_heads.shape[1])
    block_count = k_full.shape[1] // block

    def attend_step(carry, index):
        row_total, value_sum = carry
        start = index * block
        k_part = head_split(lax.dynamic_slice_in_dim(k_full, start, block, 1), seq_count, block)
        v_part = head_split(lax.dynamic_slice_in_dim(v_full, start, block, 1), seq_count, block)
        seg_part = lax.dynamic_slice_in_dim(seg_all, start, block, 1)
        raw = (
            jnp.einsum("sqhd,skhd->shqk", q_heads, k_part, preferred_element_type=jnp.float32)
            * score_scale
        )
        same_doc = q_seg[:, None, :, None] == seg_part[:, None, None, :]
        expo = jnp.where(same_doc, jnp.exp(raw), 0.0)
        row_total = row_total + jnp.sum(expo, axis=-1)
        value_sum = value_sum + jnp.einsum(
            "shqk,skhd->sqhd", expo.astype(jnp.bfloat16), v_part, preferred_element_type=jnp.float32
        )
        return ((row_total, value_sum), None)

    start_carry = (
        jnp.zeros((seq_count, HEADS, row_count), jnp.float32),
        jnp.zeros((seq_count, row_count, HEADS, HD), jnp.float32),
    )
    final, unused = lax.scan(attend_step, start_carry, jnp.arange(block_count, dtype=jnp.int32))
    return final


def back_keys(q_heads, g_heads, delta, q_seg, k_full, v_full, seg_all, block, score_scale):
    seq_count, row_count = (q_heads.shape[0], q_heads.shape[1])
    full_len = k_full.shape[1]
    block_count = full_len // block

    def back_step(carry, index):
        start = index * block
        k_part = head_split(lax.dynamic_slice_in_dim(k_full, start, block, 1), seq_count, block)
        v_part = head_split(lax.dynamic_slice_in_dim(v_full, start, block, 1), seq_count, block)
        seg_part = lax.dynamic_slice_in_dim(seg_all, start, block, 1)
        raw = (
            jnp.einsum("sqhd,skhd->shqk", q_heads, k_part, preferred_element_type=jnp.float32)
            * score_scale
        )
        same_doc = q_seg[:, None, :, None] == seg_part[:, None, None, :]
        expo = jnp.where(same_doc, jnp.exp(raw), 0.0)
        prob_grad = jnp.einsum(
            "sqhd,skhd->shqk", g_heads, v_part, preferred_element_type=jnp.float32
        )
        d_score = (expo * (prob_grad - delta[..., None])).astype(jnp.bfloat16)
        q_grad = carry[0] + jnp.einsum(
            "shqk,skhd->sqhd", d_score, k_part, preferred_element_type=jnp.float32
        )
        k_grad = (
            jnp.einsum("shqk,sqhd->skhd", d_score, q_heads, preferred_element_type=jnp.float32)
            * score_scale
        )
        v_grad = jnp.einsum(
            "shqk,sqhd->skhd",
            expo.astype(jnp.bfloat16),
            g_heads,
            preferred_element_type=jnp.float32,
        )
        k_store = lax.dynamic_update_slice_in_dim(
            carry[1], k_grad.reshape(seq_count, block, HEADS * HD), start, 1
        )
        v_store = lax.dynamic_update_slice_in_dim(
            carry[2], v_grad.reshape(seq_count, block, HEADS * HD), start, 1
        )
        return ((q_grad, k_store, v_store), None)

    q_zero = jnp.zeros((seq_count, row_count, HEADS, HD), jnp.float32)
    kv_zero = jnp.zeros((seq_count, full_len, HEADS * HD), jnp.float32)
    start_carry = (q_zero, kv_zero, kv_zero)
    final, unused = lax.scan(back_step, start_carry, jnp.arange(block_count, dtype=jnp.int32))
    return (final[0] * score_scale,) + tuple(final[1:])


def local(
    tokens,
    segments,
    positions,
    cotangent,
    w_qkv,
    w_out,
    w_gate,
    w_up,
    w_down,
    ln1_gain,
    ln1_bias,
    ln2_gain,
    ln2_bias,
):
    seq_count, row_count, model_width = tokens.shape
    score_scale = HD ** (-0.5)
    q_seg = lax.dynamic_slice_in_dim(segments, lax.axis_index("seq") * row_count, row_count, 1)
    gathered = (
        lax.all_gather(w_qkv, "shard", axis=0, tiled=True),
        lax.all_gather(w_out, "shard", axis=0, tiled=True),
        lax.all_gather(w_gate, "shard", axis=0, tiled=True),
        lax.all_gather(w_up, "shard", axis=0, tiled=True),
        lax.all_gather(w_down, "shard", axis=0, tiled=True),
        lax.all_gather(ln1_gain, "shard", axis=0, tiled=True),
        lax.all_gather(ln1_bias, "shard", axis=0, tiled=True),
        lax.all_gather(ln2_gain, "shard", axis=0, tiled=True),
        lax.all_gather(ln2_bias, "shard", axis=0, tiled=True),
    )
    full_qkv, full_out, full_gate, full_up, full_down, gain_one, bias_one, gain_two, bias_two = (
        gathered
    )
    cos_b, sin_b = rope_tables(positions)
    qkv_all = jnp.einsum("scd,de->sce", tokens, full_qkv, preferred_element_type=jnp.float32)
    q_heads = rotate(
        head_split(qkv_all[..., :model_width], seq_count, row_count), cos_b, sin_b
    ).astype(jnp.bfloat16)
    k_heads = rotate(
        head_split(qkv_all[..., model_width : 2 * model_width], seq_count, row_count), cos_b, sin_b
    ).astype(jnp.bfloat16)
    v_heads = head_split(qkv_all[..., 2 * model_width :], seq_count, row_count).astype(jnp.bfloat16)
    k_local = k_heads.reshape(seq_count, row_count, model_width)
    v_local = v_heads.reshape(seq_count, row_count, model_width)
    k_full, v_full = (
        lax.all_gather(k_local, "seq", axis=1, tiled=True),
        lax.all_gather(v_local, "seq", axis=1, tiled=True),
    )
    row_total, value_sum = attend(q_heads, q_seg, k_full, v_full, segments, row_count, score_scale)
    denom = jnp.transpose(row_total, (0, 2, 1))[..., None]
    attn_out = value_sum / denom
    joined = attn_out.reshape(seq_count, row_count, model_width).astype(jnp.bfloat16)
    tokens_f = tokens.astype(jnp.float32)
    h_one = tokens_f + jnp.einsum(
        "sci,io->sco", joined, full_out, preferred_element_type=jnp.float32
    )
    x_one, normed_one, inverse_one = norm_fwd(
        h_one, gain_one.astype(jnp.float32), bias_one.astype(jnp.float32)
    )
    x_low = x_one.astype(jnp.bfloat16)
    gate_pre = jnp.einsum("scd,df->scf", x_low, full_gate, preferred_element_type=jnp.float32)
    up_pre = jnp.einsum("scd,df->scf", x_low, full_up, preferred_element_type=jnp.float32)
    sigma = jax.nn.sigmoid(gate_pre)
    smooth = gate_pre * sigma
    hidden = (smooth * up_pre).astype(jnp.bfloat16)
    h_two = x_one + jnp.einsum("scf,fd->scd", hidden, full_down, preferred_element_type=jnp.float32)
    result, normed_two, inverse_two = norm_fwd(
        h_two, gain_two.astype(jnp.float32), bias_two.astype(jnp.float32)
    )
    output = result.astype(jnp.bfloat16)
    regathered = (
        lax.all_gather(w_qkv, "shard", axis=0, tiled=True),
        lax.all_gather(w_out, "shard", axis=0, tiled=True),
        lax.all_gather(w_gate, "shard", axis=0, tiled=True),
        lax.all_gather(w_up, "shard", axis=0, tiled=True),
        lax.all_gather(w_down, "shard", axis=0, tiled=True),
        lax.all_gather(ln1_gain, "shard", axis=0, tiled=True),
        lax.all_gather(ln2_gain, "shard", axis=0, tiled=True),
    )
    back_qkv, back_out, back_gate, back_up, back_down, back_gain_one, back_gain_two = regathered
    back_k, back_v = (
        lax.all_gather(k_local, "seq", axis=1, tiled=True),
        lax.all_gather(v_local, "seq", axis=1, tiled=True),
    )
    cot_f = cotangent.astype(jnp.float32)
    grad_gain_two = jnp.sum(cot_f * normed_two, axis=(0, 1))
    grad_bias_two = jnp.sum(cot_f, axis=(0, 1))
    dh_two = norm_back(cot_f, normed_two, inverse_two, back_gain_two.astype(jnp.float32))
    dm_low = dh_two.astype(jnp.bfloat16)
    grad_down = jnp.einsum("scf,scd->fd", hidden, dm_low, preferred_element_type=jnp.float32)
    d_hidden = jnp.einsum("scd,fd->scf", dm_low, back_down, preferred_element_type=jnp.float32)
    d_up = (d_hidden * smooth).astype(jnp.bfloat16)
    d_gate = (d_hidden * up_pre * sigma * (1.0 + gate_pre * (1.0 - sigma))).astype(jnp.bfloat16)
    grad_gate = jnp.einsum("scd,scf->df", x_low, d_gate, preferred_element_type=jnp.float32)
    grad_up = jnp.einsum("scd,scf->df", x_low, d_up, preferred_element_type=jnp.float32)
    dx_one = (
        dh_two
        + jnp.einsum("scf,df->scd", d_gate, back_gate, preferred_element_type=jnp.float32)
        + jnp.einsum("scf,df->scd", d_up, back_up, preferred_element_type=jnp.float32)
    )
    grad_gain_one = jnp.sum(dx_one * normed_one, axis=(0, 1))
    grad_bias_one = jnp.sum(dx_one, axis=(0, 1))
    dh_one = norm_back(dx_one, normed_one, inverse_one, back_gain_one.astype(jnp.float32))
    d_attn = dh_one.astype(jnp.bfloat16)
    grad_out = jnp.einsum("sci,sco->io", joined, d_attn, preferred_element_type=jnp.float32)
    d_joined = jnp.einsum(
        "sco,io->sci", d_attn, back_out, preferred_element_type=jnp.float32
    ).astype(jnp.bfloat16)
    d_heads = head_split(d_joined, seq_count, row_count).astype(jnp.float32)
    g_heads = (d_heads / denom).astype(jnp.bfloat16)
    delta = jnp.transpose(jnp.sum(d_heads * attn_out, axis=-1) / denom[..., 0], (0, 2, 1))
    q_grad, k_all, v_all = back_keys(
        q_heads, g_heads, delta, q_seg, back_k, back_v, segments, row_count, score_scale
    )
    k_sum, v_sum = (
        lax.psum_scatter(k_all.astype(jnp.bfloat16), "seq", scatter_dimension=1, tiled=True).astype(
            jnp.float32
        ),
        lax.psum_scatter(v_all.astype(jnp.bfloat16), "seq", scatter_dimension=1, tiled=True).astype(
            jnp.float32
        ),
    )
    k_grad = head_split(k_sum, seq_count, row_count)
    v_grad = head_split(v_sum, seq_count, row_count)
    q_back = rotate_back(q_grad, cos_b, sin_b).reshape(seq_count, row_count, model_width)
    k_back = rotate_back(k_grad, cos_b, sin_b).reshape(seq_count, row_count, model_width)
    d_qkv = jnp.concatenate(
        [q_back, k_back, v_grad.reshape(seq_count, row_count, model_width)], axis=-1
    ).astype(jnp.bfloat16)
    grad_qkv = jnp.einsum("scd,sce->de", tokens, d_qkv, preferred_element_type=jnp.float32)
    d_tokens = dh_one + jnp.einsum(
        "sce,de->scd", d_qkv, back_qkv, preferred_element_type=jnp.float32
    )
    input_grad = d_tokens.astype(jnp.bfloat16)
    owned = (
        lax.psum_scatter(
            grad_qkv.astype(jnp.bfloat16), "shard", scatter_dimension=0, tiled=True
        ).astype(jnp.float32),
        lax.psum_scatter(
            grad_out.astype(jnp.bfloat16), "shard", scatter_dimension=0, tiled=True
        ).astype(jnp.float32),
        lax.psum_scatter(
            grad_gate.astype(jnp.bfloat16), "shard", scatter_dimension=0, tiled=True
        ).astype(jnp.float32),
        lax.psum_scatter(
            grad_up.astype(jnp.bfloat16), "shard", scatter_dimension=0, tiled=True
        ).astype(jnp.float32),
        lax.psum_scatter(
            grad_down.astype(jnp.bfloat16), "shard", scatter_dimension=0, tiled=True
        ).astype(jnp.float32),
        lax.psum_scatter(
            grad_gain_one.astype(jnp.bfloat16), "shard", scatter_dimension=0, tiled=True
        ).astype(jnp.float32),
        lax.psum_scatter(
            grad_bias_one.astype(jnp.bfloat16), "shard", scatter_dimension=0, tiled=True
        ).astype(jnp.float32),
        lax.psum_scatter(
            grad_gain_two.astype(jnp.bfloat16), "shard", scatter_dimension=0, tiled=True
        ).astype(jnp.float32),
        lax.psum_scatter(
            grad_bias_two.astype(jnp.bfloat16), "shard", scatter_dimension=0, tiled=True
        ).astype(jnp.float32),
    )
    summed = (
        lax.psum(owned[0].astype(jnp.bfloat16), "seq").astype(jnp.float32),
        lax.psum(owned[1].astype(jnp.bfloat16), "seq").astype(jnp.float32),
        lax.psum(owned[2].astype(jnp.bfloat16), "seq").astype(jnp.float32),
        lax.psum(owned[3].astype(jnp.bfloat16), "seq").astype(jnp.float32),
        lax.psum(owned[4].astype(jnp.bfloat16), "seq").astype(jnp.float32),
        lax.psum(owned[5].astype(jnp.bfloat16), "seq").astype(jnp.float32),
        lax.psum(owned[6].astype(jnp.bfloat16), "seq").astype(jnp.float32),
        lax.psum(owned[7].astype(jnp.bfloat16), "seq").astype(jnp.float32),
        lax.psum(owned[8].astype(jnp.bfloat16), "seq").astype(jnp.float32),
    )
    return (
        output,
        input_grad,
        summed[0],
        summed[1],
        summed[2],
        summed[3],
        summed[4],
        summed[5],
        summed[6],
        summed[7],
        summed[8],
    )


SEQS_HELD = 2
SEQ_SIZE = 8
GROUPS = 4
LANES = 128
LOG2E = 1.4426950408889634
LN2 = 0.6931471805599453
FAR = 2.0**30
F32 = jnp.float32
BF16 = jnp.bfloat16
VMEM_LIMIT = 60 * 1024 * 1024
FEED_LIMIT = 63 * 1024 * 1024
BY_MESH = pl.DeviceIdType.MESH
BY_LANES = (((1,), (1,)), ((), ()))


def packed_heads(rows):
    return rows + rows // 2


def unpack_heads(block):
    rows = block.shape[0] * 2 // 3
    last = block[rows:]
    third = jnp.concatenate([last[:, :HD], last[:, HD:]], axis=0)
    return jnp.concatenate([block[:rows], third], axis=1)


def pack_heads(value):
    rows = value.shape[0]
    third = value[:, 2 * HD :]
    return value[:, : 2 * HD], jnp.concatenate([third[: rows // 2], third[rows // 2 :]], axis=1)


def flip(index, bit):
    return index + bit - 2 * bit * lax.rem(lax.div(index, bit), 2)


def gather_kernel(
    chunks, by_z, tok_ref, w_ref, n_ref, place_ref, freq_ref, all_ref, w_all_ref, n_all_ref, turn_ref, send, recv, kept, w_send, w_recv
):
    me = lax.axis_index("seq")
    shard = lax.axis_index("shard")
    shards = w_all_ref.shape[0]
    half = lax.div(me, GROUPS)
    y_near, z_near, partner = flip(me, 1), flip(me, 2), flip(me, 4)
    barrier = pltpu.get_barrier_semaphore()
    for device in (y_near, z_near, partner):
        pl.semaphore_signal(barrier, inc=1, device_id={"seq": device}, device_id_type=BY_MESH)
    for step in range(1, shards):
        pl.semaphore_signal(
            barrier, inc=1, device_id={"shard": lax.rem(shard + step, shards)}, device_id_type=BY_MESH
        )
    pl.semaphore_wait(barrier, 2 + shards)

    part = tok_ref.shape[1] // chunks
    started = []

    def go(source, target, slot, device):
        copy = pltpu.make_async_remote_copy(
            src_ref=source,
            dst_ref=target,
            send_sem=send.at[slot],
            recv_sem=recv.at[slot],
            device_id={"seq": device},
            device_id_type=BY_MESH,
        )
        copy.start()
        started.append(copy)
        return copy

    def rows(chunk):
        return pl.ds(chunk * part, part)

    def relay(piece, chunk, slot, device):
        return go(all_ref.at[piece, rows(chunk)], all_ref.at[piece, rows(chunk)], slot * chunks + chunk, device)

    def own(which, chunk, slot, device):
        return go(tok_ref.at[which, rows(chunk)], all_ref.at[me, rows(chunk)], slot * chunks + chunk, device)

    crossing = [own(1 - half, chunk, 0, partner) for chunk in range(chunks)]
    own_y, own_z = [], []
    for chunk in range(chunks):
        own_y.append(own(half, chunk, 1, y_near))
        own_z.append(own(half, chunk, 2, z_near))
    weights = []
    for step in range(1, shards):
        copy = pltpu.make_async_remote_copy(
            src_ref=w_ref,
            dst_ref=w_all_ref.at[shard],
            send_sem=w_send.at[step],
            recv_sem=w_recv.at[step],
            device_id={"shard": lax.rem(shard + step, shards)},
            device_id_type=BY_MESH,
        )
        copy.start()
        weights.append(copy)
        copy = pltpu.make_async_remote_copy(
            src_ref=n_ref,
            dst_ref=n_all_ref.at[shard],
            send_sem=w_send.at[shards + step],
            recv_sem=w_recv.at[shards + step],
            device_id={"shard": lax.rem(shard + step, shards)},
            device_id_type=BY_MESH,
        )
        copy.start()
        weights.append(copy)
    keep_n = pltpu.make_async_copy(n_ref, n_all_ref.at[shard], kept.at[2])
    keep_n.start()
    keep_tok = pltpu.make_async_copy(tok_ref.at[half], all_ref.at[me], kept.at[0])
    keep_tok.start()
    keep_w = pltpu.make_async_copy(w_ref, w_all_ref.at[shard], kept.at[1])
    keep_w.start()

    def turn_piece(index, carry):
        count = turn_ref.shape[0] // place_ref.shape[0]
        lane = lax.broadcasted_iota(jnp.int32, (count, LANES), 1)
        place = jnp.transpose(jnp.broadcast_to(place_ref[index], (LANES, count)))
        angle = place * freq_ref[...]
        turn_ref[pl.ds(pl.multiple_of(index * count, count), count), :] = jnp.where(
            lane < HD, jnp.cos(angle), jnp.sin(angle)
        )
        return carry

    lax.fori_loop(0, place_ref.shape[0], turn_piece, 0)

    cross_y, cross_z, corner = [], [], []
    for chunk in range(chunks):
        own_y[chunk].wait_recv()
        if chunk < by_z:
            corner.append(relay(y_near, chunk, 5, z_near))
        own_z[chunk].wait_recv()
        if chunk >= by_z:
            corner.append(relay(z_near, chunk, 5, y_near))
        crossing[chunk].wait_recv()
        cross_y.append(relay(partner, chunk, 3, y_near))
        cross_z.append(relay(partner, chunk, 4, z_near))
    for chunk in range(chunks):
        cross_y[chunk].wait_recv()
        if chunk < by_z:
            corner.append(relay(flip(y_near, 4), chunk, 6, z_near))
        cross_z[chunk].wait_recv()
        if chunk >= by_z:
            corner.append(relay(flip(z_near, 4), chunk, 6, y_near))
    for copy in corner:
        copy.wait_recv()
    for copy in weights:
        copy.wait()
    keep_tok.wait()
    keep_w.wait()
    keep_n.wait()
    for copy in started:
        copy.wait_send()


def gather_tokens(tokens, w_part, norms, place, freq, shards, chunks=8, by_z=3):
    seqs, rows, width = tokens.shape
    anywhere = pl.BlockSpec(memory_space=pl.ANY)
    vmem = pl.BlockSpec(memory_space=pltpu.VMEM)
    return pl.pallas_call(
        functools.partial(gather_kernel, chunks, by_z),
        out_shape=(
            jax.ShapeDtypeStruct((SEQ_SIZE, rows, width), tokens.dtype),
            jax.ShapeDtypeStruct((shards,) + w_part.shape, w_part.dtype),
            jax.ShapeDtypeStruct((shards,) + norms.shape, norms.dtype),
            jax.ShapeDtypeStruct((place.shape[0] * place.shape[2], LANES), F32),
        ),
        in_specs=[anywhere, anywhere, anywhere, vmem, vmem],
        out_specs=(anywhere, anywhere, anywhere, vmem),
        scratch_shapes=[
            pltpu.SemaphoreType.DMA((7 * chunks,)),
            pltpu.SemaphoreType.DMA((7 * chunks,)),
            pltpu.SemaphoreType.DMA((3,)),
            pltpu.SemaphoreType.DMA((2 * shards,)),
            pltpu.SemaphoreType.DMA((2 * shards,)),
        ],
        compiler_params=pltpu.CompilerParams(collective_id=1, has_side_effects=True),
        name="gather_tokens",
    )(tokens, w_part, norms, place, freq)


def project_kernel(seg_ref, turn_ref, x_ref, w_ref, q_ref, k_ref, v_ref):
    rows = x_ref.shape[1]
    held = q_ref.shape[0]
    lane = lax.broadcasted_iota(jnp.int32, (rows, LANES), 1)
    seg = jnp.transpose(jnp.broadcast_to(seg_ref[0], (LANES, rows)))
    turn = turn_ref[...]
    cos_b = jnp.where(lane < HD, turn, 0.0)
    sin_b = jnp.where(lane < HD, pltpu.roll(turn, HD, 1), 0.0)
    sin_b = jnp.where(lane < HD // 2, -sin_b, sin_b)
    same = seg == (lane - HD).astype(F32)
    q_tail = jnp.where(same, 1.0, 0.0)
    k_tail = jnp.where(same | (lane < HD), 0.0, -FAR)
    v_tail = jnp.where(lane < HD, 0.0, 1.0)
    scale = HD ** (-0.5) * LOG2E
    q_cos, q_sin = cos_b * scale, sin_b * scale
    width = held * LANES
    for part in range(3):
        mixed = jnp.dot(x_ref[0], w_ref[:, part * width : (part + 1) * width], preferred_element_type=F32)
        for head in range(held):
            value = mixed[:, head * LANES : (head + 1) * LANES]
            if part == 0:
                value = value * q_cos + pltpu.roll(value, HD // 2, 1) * q_sin + q_tail
                q_ref[head] = value.astype(BF16)
            elif part == 1:
                value = value * cos_b + pltpu.roll(value, HD // 2, 1) * sin_b + k_tail
                k_ref[head] = value.astype(BF16)
            else:
                v_ref[head] = (value + v_tail).astype(BF16)


def project_heads(seg_row, turn, pieces, w_full, held):
    count, rows, width = pieces.shape
    length = count * rows
    row_spec = pl.BlockSpec((1, 1, rows), lambda i: (i, 0, 0))
    head_spec = pl.BlockSpec((held, rows, LANES), lambda i: (0, i, 0))
    head_shape = jax.ShapeDtypeStruct((held, length, LANES), BF16)
    return pl.pallas_call(
        project_kernel,
        out_shape=(head_shape, head_shape, head_shape),
        grid=(count,),
        in_specs=[
            row_spec,
            pl.BlockSpec((rows, LANES), lambda i: (i, 0)),
            pl.BlockSpec((1, rows, width), lambda i: (i, 0, 0)),
            pl.BlockSpec(w_full.shape, lambda i: (0, 0)),
        ],
        out_specs=(head_spec, head_spec, head_spec),
        compiler_params=pltpu.CompilerParams(vmem_limit_bytes=VMEM_LIMIT),
        cost_estimate=pl.CostEstimate(
            flops=2 * length * width * w_full.shape[1],
            bytes_accessed=length * (width * 2 + held * LANES * 6 + LANES * 4),
            transcendentals=length * LANES,
        ),
        name="project_heads",
    )(seg_row.reshape(count, 1, rows), turn, pieces, w_full)


def document_bounds(seg_row, rows):
    first = seg_row[::rows]
    last = seg_row[rows - 1 :: rows]
    low = jnp.sum((seg_row[None, :] < first[:, None]).astype(jnp.int32), axis=1)
    high = jnp.sum((seg_row[None, :] <= last[:, None]).astype(jnp.int32), axis=1)
    return low, high


def windows(bounds, length, window, align):
    low = bounds[0] // align * align
    count = (bounds[1] - low + window - 1) // window
    return jnp.minimum(low, length - count * window), count


def attend_kernel(window, align, low_ref, count_ref, q_ref, k_ref, v_ref, sum_ref, joined_ref):
    block = pl.program_id(0)
    low = low_ref[block]
    sum_ref[...] = jnp.zeros_like(sum_ref)

    def step(index, carry):
        start = pl.multiple_of(low + index * window, align)
        for head in range(q_ref.shape[0]):
            k_part = k_ref[head, pl.ds(start, window), :]
            v_part = v_ref[head, pl.ds(start, window), :]
            score = lax.dot_general(q_ref[head], k_part, BY_LANES, preferred_element_type=F32)
            expo = jnp.exp2(score).astype(BF16)
            sum_ref[head] += jnp.dot(expo, v_part, preferred_element_type=F32)
        return carry

    lax.fori_loop(0, count_ref[block], step, 0)
    rows = q_ref.shape[1]
    parts = [sum_ref[head][:, :HD] / sum_ref[head][:, HD : HD + 1] for head in range(q_ref.shape[0])]
    first, last = pack_heads(jnp.concatenate(parts, axis=1))
    joined_ref[0, :rows] = first.astype(BF16)
    joined_ref[0, rows:] = last.astype(BF16)


def attend_heads(bounds, q_ext, k_ext, v_ext, rows, window=1024, align=16):
    heads, length, lanes = q_ext.shape
    low, count = windows(bounds, length, window, align)
    whole = pl.BlockSpec((heads, length, lanes), lambda i, *_: (0, 0, 0))
    part = pl.BlockSpec((heads, rows, lanes), lambda i, *_: (0, i, 0))
    return pl.pallas_call(
        functools.partial(attend_kernel, window, align),
        out_shape=(
            jax.ShapeDtypeStruct((heads, length, lanes), F32),
            jax.ShapeDtypeStruct((length // rows, packed_heads(rows), LANES), BF16),
        ),
        grid_spec=pltpu.PrefetchScalarGridSpec(
            num_scalar_prefetch=2,
            grid=(length // rows,),
            in_specs=[part, whole, whole],
            out_specs=(part, pl.BlockSpec((1, packed_heads(rows), LANES), lambda i, *_: (i, 0, 0))),
        ),
        compiler_params=pltpu.CompilerParams(vmem_limit_bytes=VMEM_LIMIT),
        cost_estimate=pl.CostEstimate(
            flops=heads * length * length * 4 * lanes // 2,
            bytes_accessed=heads * length * lanes * 10,
            transcendentals=heads * length * length // 2,
        ),
        name="attend_heads",
    )(low, count, q_ext, k_ext, v_ext)


def attend_back_kernel(
    window,
    align,
    low_ref,
    count_ref,
    q_ref,
    sum_ref,
    dout_ref,
    turn_ref,
    k_ref,
    v_ref,
    d_ref,
    dq_ref,
    dkv_ref,
    g_ref,
    gt_ref,
    qt_ref,
):
    block = pl.program_id(0)
    heads, rows, lanes = q_ref.shape
    width = heads * HD

    @pl.when(block == 0)
    def _():
        dkv_ref[...] = jnp.zeros_like(dkv_ref)

    dq_ref[...] = jnp.zeros_like(dq_ref)
    half_lane = lax.broadcasted_iota(jnp.int32, (rows, HD), 1)
    dout_all = unpack_heads(dout_ref[0].astype(F32))
    for head in range(heads):
        dout = dout_all[:, head * HD : (head + 1) * HD]
        sums = sum_ref[head]
        total = sums[:, HD : HD + 1]
        g_low = dout / total
        delta = -jnp.sum(dout * sums[:, :HD], axis=1, keepdims=True) / (total * total)
        high = delta.astype(BF16).astype(F32)
        middle = (delta - high).astype(BF16).astype(F32)
        tail = jnp.where(
            half_lane == 0,
            high,
            jnp.where(half_lane == 1, middle, jnp.where(half_lane == 2, delta - high - middle, 0.0)),
        )
        g_ext = jnp.concatenate([g_low, tail], axis=1)
        g_ref[head] = g_ext.astype(BF16)
        gt_ref[head] = jnp.transpose(g_ext)[:HD].astype(BF16)
        qt_ref[head] = jnp.transpose(q_ref[head].astype(F32))[:HD].astype(BF16)

    low = low_ref[block]

    def step(index, carry):
        start = pl.multiple_of(low + index * window, align)
        for head in range(heads):
            k_part = k_ref[head, pl.ds(start, window), :]
            v_part = v_ref[head, pl.ds(start, window), :]
            score = lax.dot_general(q_ref[head], k_part, BY_LANES, preferred_element_type=F32)
            slope = lax.dot_general(g_ref[head], v_part, BY_LANES, preferred_element_type=F32)
            expo = jnp.exp2(score)
            d_score = (expo * slope).astype(BF16)
            expo = expo.astype(BF16)
            dq_ref[head] += jnp.dot(d_score, k_part, preferred_element_type=F32)
            dkv_ref[head, :HD, pl.ds(start, window)] += jnp.dot(qt_ref[head], d_score, preferred_element_type=F32)
            dkv_ref[head, HD:, pl.ds(start, window)] += jnp.dot(gt_ref[head], expo, preferred_element_type=F32)
        return carry

    lax.fori_loop(0, count_ref[block], step, 0)

    lane = lax.broadcasted_iota(jnp.int32, (rows, lanes), 1)

    def turn_back(value, turn):
        swapped = jnp.where(lane < HD // 2, pltpu.roll(value, lanes - HD // 2, 1), pltpu.roll(value, HD // 2, 1))
        sine = pltpu.roll(turn, HD, 1)
        sine = jnp.where(lane < HD // 2, sine, -sine)
        return (value * turn + swapped * sine)[:, :HD]

    here = turn_ref[pl.ds(pl.multiple_of(block * rows, rows), rows), :]
    for head in range(heads):
        turned = turn_back(dq_ref[head] * HD ** (-0.5), here)
        d_ref[block, :, head * HD : (head + 1) * HD] = turned.astype(BF16)

    @pl.when(block == pl.num_programs(0) - 1)
    def _():
        def finish(piece, carry):
            start = pl.multiple_of(piece * rows, rows)
            turn = turn_ref[pl.ds(start, rows), :]
            for head in range(heads):
                both = jnp.transpose(dkv_ref[head, :, pl.ds(start, rows)])
                at = width + head * HD
                d_ref[piece, :, at : at + HD] = (turn_back(both, turn) * LN2).astype(BF16)
                d_ref[piece, :, width + at : width + at + HD] = both[:, HD:].astype(BF16)
            return carry

        lax.fori_loop(0, d_ref.shape[0], finish, 0)


def attend_back_heads(bounds, q_ext, k_ext, v_ext, sums, dout, turn, window=512, align=128):
    heads, length, lanes = q_ext.shape
    count_blocks = dout.shape[0]
    rows, width = length // count_blocks, heads * HD
    low, count = windows(bounds, length, window, align)
    whole = pl.BlockSpec((heads, length, lanes), lambda i, *_: (0, 0, 0))
    part = pl.BlockSpec((heads, rows, lanes), lambda i, *_: (0, i, 0))
    return pl.pallas_call(
        functools.partial(attend_back_kernel, window, align),
        out_shape=jax.ShapeDtypeStruct((count_blocks, rows, 3 * width), BF16),
        grid_spec=pltpu.PrefetchScalarGridSpec(
            num_scalar_prefetch=2,
            grid=(count_blocks,),
            in_specs=[
                part,
                part,
                pl.BlockSpec((1,) + dout.shape[1:], lambda i, *_: (i, 0, 0)),
                pl.BlockSpec((length, lanes), lambda i, *_: (0, 0)),
                whole,
                whole,
            ],
            out_specs=pl.BlockSpec((count_blocks, rows, 3 * width), lambda i, *_: (0, 0, 0)),
            scratch_shapes=[
                pltpu.VMEM((heads, rows, lanes), F32),
                pltpu.VMEM((heads, 2 * HD, length), F32),
                pltpu.VMEM((heads, rows, lanes), BF16),
                pltpu.VMEM((heads, HD, rows), BF16),
                pltpu.VMEM((heads, HD, rows), BF16),
            ],
        ),
        compiler_params=pltpu.CompilerParams(vmem_limit_bytes=VMEM_LIMIT),
        cost_estimate=pl.CostEstimate(
            flops=heads * length * length * 10 * lanes // 2,
            bytes_accessed=heads * length * lanes * 20,
            transcendentals=heads * length * length // 2,
        ),
        name="attend_back_heads",
    )(low, count, q_ext, sums, dout, turn, k_ext, v_ext)


def scatter_kernel(
    chunks,
    by_z,
    part_ref,
    dh_hbm,
    gw_ref,
    norm_ref,
    own_ref,
    out_hbm,
    gw_all_ref,
    norm_out_ref,
    rows_ref,
    mine,
    pass_z,
    pass_y,
    dh_ref,
    out_ref,
    got_y,
    got_z,
    relay_y,
    relay_z,
    sent_y,
    sent_z,
    cross_out,
    cross_in,
    gw_got,
    gw_mine,
    gw_pair,
    gw_final,
    norm_got,
    norm_sent,
    send,
    recv,
    gw_send,
    gw_recv,
    norm_send,
    norm_recv,
    own_send,
    own_recv,
    kept,
):
    me = lax.axis_index("seq")
    shard = lax.axis_index("shard")
    shards = gw_ref.shape[0]
    half = lax.div(me, GROUPS)
    y_near, z_near, partner = flip(me, 1), flip(me, 2), flip(me, 4)
    corner = flip(y_near, 2)
    barrier = pltpu.get_barrier_semaphore()
    for n in range(1, SEQ_SIZE):
        pl.semaphore_signal(
            barrier, inc=1, device_id={"seq": lax.rem(me + n, SEQ_SIZE)}, device_id_type=BY_MESH
        )
    for step in range(1, shards):
        pl.semaphore_signal(
            barrier, inc=1, device_id={"shard": lax.rem(shard + step, shards)}, device_id_type=BY_MESH
        )
    pl.semaphore_wait(barrier, SEQ_SIZE + shards - 2)

    started = []

    def go(source, target, sends, receives, slot, where):
        copy = pltpu.make_async_remote_copy(
            src_ref=source,
            dst_ref=target,
            send_sem=sends.at[slot],
            recv_sem=receives.at[slot],
            device_id=where,
            device_id_type=BY_MESH,
        )
        copy.start()
        started.append(copy)
        return copy

    rows = part_ref.shape[1] // chunks

    def band(chunk):
        return pl.ds(chunk * rows, rows)

    def piece(device, far):
        return flip(device, 4) if far else device

    def slot(kind, far, chunk):
        return (kind * 2 + (0 if far else 1)) * chunks + chunk

    loads = [pltpu.make_async_copy(dh_hbm, dh_ref, kept.at[8])]
    for which, far in enumerate((True, False)):
        device = piece(z_near, far)
        split = by_z * rows
        loads += [
            pltpu.make_async_copy(part_ref.at[device, pl.ds(0, split)], pass_z.at[which], kept.at[2 + which]),
            pltpu.make_async_copy(
                part_ref.at[piece(y_near, far), pl.ds(split, (chunks - by_z) * rows)], pass_y.at[which], kept.at[4 + which]
            ),
            pltpu.make_async_copy(part_ref.at[piece(me, far)], mine.at[which], kept.at[6 + which]),
        ]

    gw_one = [
        go(
            gw_ref.at[lax.rem(shard + step, shards)],
            gw_got.at[step - 1],
            gw_send,
            gw_recv,
            step - 1,
            {"shard": lax.rem(shard + step, shards)},
        )
        for step in range(1, shards)
    ]
    norm_seq = [
        go(norm_ref, norm_got.at[n], norm_send, norm_recv, n, {"seq": lax.rem(me + n + 1, SEQ_SIZE)})
        for n in range(SEQ_SIZE - 1)
    ]

    from_corner, direct = {}, {}

    own_rows = own_ref.shape[0] // chunks
    all_rows = own_ref.shape[0]

    def own_band(device, chunk):
        return rows_ref.at[pl.ds(device * all_rows + chunk * own_rows, own_rows)]

    def spread(device, chunk, kind, where):
        source = own_band(device, chunk)
        return go(source, source, own_send, own_recv, kind * chunks + chunk, {"seq": where})

    def spread_own(kind, where):
        return [
            go(
                own_ref.at[pl.ds(chunk * own_rows, own_rows)],
                own_band(me, chunk),
                own_send,
                own_recv,
                kind * chunks + chunk,
                {"seq": where},
            )
            for chunk in range(chunks)
        ]

    def send_pieces(far):
        for chunk in range(chunks):
            over_z = chunk < by_z
            from_corner[far, chunk] = go(
                part_ref.at[piece(corner, far), band(chunk)],
                (relay_y if over_z else relay_z).at[0 if far else 1, chunk if over_z else chunk - by_z],
                send,
                recv,
                slot(0, far, chunk),
                {"seq": y_near if over_z else z_near},
            )
        for chunk in range(chunks):
            over_z = chunk < by_z
            direct[far, chunk] = go(
                part_ref.at[piece(y_near if over_z else z_near, far), band(chunk)],
                (got_y if over_z else got_z).at[0 if far else 1, band(chunk)],
                send,
                recv,
                slot(1 if over_z else 2, far, chunk),
                {"seq": y_near if over_z else z_near},
            )

    send_pieces(True)
    for copy in loads:
        copy.start()
    keep_rows = pltpu.make_async_copy(own_ref, rows_ref.at[pl.ds(me * all_rows, all_rows)], kept.at[1])
    keep_rows.start()
    relayed = {}

    def relay(far, chunk):
        over_z = chunk < by_z
        target = z_near if over_z else y_near
        index = chunk if over_z else chunk - by_z
        which = 0 if far else 1
        from_corner[far, chunk].wait_recv()
        source = relay_y if over_z else relay_z
        buffer = sent_y if over_z else sent_z
        passed = (pass_z if over_z else pass_y)[which, band(index)].astype(F32)
        buffer[which, index] = (source[which, index].astype(F32) + passed).astype(BF16)
        relayed[far, chunk] = go(
            buffer.at[which, index],
            (got_z if over_z else got_y).at[which, band(chunk)],
            send,
            recv,
            slot(2 if over_z else 1, far, chunk),
            {"seq": target},
        )

    def total(far, chunk):
        which = 0 if far else 1
        direct[far, chunk].wait_recv()
        relayed[far, chunk].wait_recv()
        return mine[which, band(chunk)].astype(F32) + got_y[which, band(chunk)].astype(F32) + got_z[which, band(chunk)].astype(F32)

    for copy in loads:
        copy.wait()
    for chunk in range(chunks):
        relay(True, chunk)
    send_pieces(False)
    norm_total = norm_ref[...]
    for n, copy in enumerate(norm_seq):
        copy.wait_recv()
        norm_total = norm_total + norm_got[n]
    norm_sent[...] = norm_total
    for copy in gw_one:
        copy.wait_recv()
    summed = gw_ref[shard].astype(F32)
    for step in range(1, shards):
        summed = summed + gw_got[step - 1].astype(F32)
    gw_mine[...] = summed.astype(BF16)
    gw_two = go(gw_mine, gw_pair, gw_send, gw_recv, shards - 1, {"seq": partner})
    norm_shard = [
        go(
            norm_sent,
            norm_got.at[SEQ_SIZE - 2 + step],
            norm_send,
            norm_recv,
            SEQ_SIZE - 2 + step,
            {"shard": lax.rem(shard + step, shards)},
        )
        for step in range(1, shards)
    ]
    crossing = []
    for chunk in range(chunks):
        cross_out[band(chunk)] = total(True, chunk).astype(BF16)
        crossing.append(
            go(cross_out.at[band(chunk)], cross_in.at[band(chunk)], send, recv, slot(3, True, chunk), {"seq": partner})
        )
    rows_cross, rows_y, rows_z = spread_own(0, partner), spread_own(1, y_near), spread_own(2, z_near)
    for chunk in range(chunks):
        relay(False, chunk)
    rows_cross_y, rows_cross_z, rows_corner = [], [], []
    for chunk in range(chunks):
        rows_y[chunk].wait_recv()
        if chunk >= by_z:
            rows_corner.append(spread(y_near, chunk, 5, z_near))
        rows_z[chunk].wait_recv()
        if chunk < by_z:
            rows_corner.append(spread(z_near, chunk, 5, y_near))
        rows_cross[chunk].wait_recv()
        rows_cross_y.append(spread(partner, chunk, 3, y_near))
        rows_cross_z.append(spread(partner, chunk, 4, z_near))
    gw_two.wait_recv()
    gw_final[...] = (gw_mine[...].astype(F32) + gw_pair[...].astype(F32)).astype(BF16)
    group = lax.rem(me, GROUPS)
    gw_three = [
        go(gw_final, gw_all_ref.at[group], gw_send, gw_recv, shards + n, {"seq": device})
        for n, device in enumerate((y_near, z_near, corner))
    ]
    keep = pltpu.make_async_copy(gw_final, gw_all_ref.at[group], kept.at[0])
    keep.start()
    for chunk in range(chunks):
        rows_cross_y[chunk].wait_recv()
        if chunk >= by_z:
            rows_corner.append(spread(flip(y_near, 4), chunk, 6, z_near))
        rows_cross_z[chunk].wait_recv()
        if chunk < by_z:
            rows_corner.append(spread(flip(z_near, 4), chunk, 6, y_near))
    for chunk in range(chunks):
        out_ref[0, band(chunk)] = (total(False, chunk) + dh_ref[half, band(chunk)]).astype(BF16)
    out_near = pltpu.make_async_copy(out_ref.at[0], out_hbm.at[half], kept.at[2])
    out_near.start()
    norm_total = norm_sent[...]
    for step, copy in enumerate(norm_shard):
        copy.wait_recv()
        norm_total = norm_total + norm_got[SEQ_SIZE - 1 + step]
    norm_out_ref[...] = norm_total
    for chunk in range(chunks):
        crossing[chunk].wait_recv()
        other = 1 - half
        out_ref[1, band(chunk)] = (cross_in[band(chunk)].astype(F32) + dh_ref[other, band(chunk)]).astype(BF16)
    out_far = pltpu.make_async_copy(out_ref.at[1], out_hbm.at[1 - half], kept.at[3])
    out_far.start()
    for copy in gw_three + rows_corner:
        copy.wait_recv()
    keep.wait()
    keep_rows.wait()
    out_near.wait()
    out_far.wait()
    for copy in started:
        copy.wait_send()


def scatter_gradients(partial, dh_one, grad_columns, norms, owned, chunks=4, by_z=3):
    _, rows, width = partial.shape
    shards, depth, columns = grad_columns.shape
    part = rows // chunks
    hbm = pl.BlockSpec(memory_space=pltpu.HBM)
    vmem = pl.BlockSpec(memory_space=pltpu.VMEM)
    dma = pltpu.SemaphoreType.DMA
    return pl.pallas_call(
        functools.partial(scatter_kernel, chunks, by_z),
        out_shape=(
            jax.ShapeDtypeStruct(dh_one.shape, BF16),
            jax.ShapeDtypeStruct((GROUPS, depth, columns), BF16),
            jax.ShapeDtypeStruct(norms.shape, F32),
            jax.ShapeDtypeStruct((SEQ_SIZE * owned.shape[0], width), BF16),
        ),
        in_specs=[hbm, hbm, vmem, vmem, hbm],
        out_specs=(hbm, vmem, vmem, hbm),
        scratch_shapes=[
            pltpu.VMEM((2, rows, width), BF16),
            pltpu.VMEM((2, by_z * part, width), BF16),
            pltpu.VMEM((2, (chunks - by_z) * part, width), BF16),
            pltpu.VMEM(dh_one.shape, F32),
            pltpu.VMEM((2, rows, width), BF16),
            pltpu.VMEM((2, rows, width), BF16),
            pltpu.VMEM((2, rows, width), BF16),
            pltpu.VMEM((2, by_z, part, width), BF16),
            pltpu.VMEM((2, chunks - by_z, part, width), BF16),
            pltpu.VMEM((2, by_z, part, width), BF16),
            pltpu.VMEM((2, chunks - by_z, part, width), BF16),
            pltpu.VMEM((rows, width), BF16),
            pltpu.VMEM((rows, width), BF16),
            pltpu.VMEM((shards - 1, depth, columns), BF16),
            pltpu.VMEM((depth, columns), BF16),
            pltpu.VMEM((depth, columns), BF16),
            pltpu.VMEM((depth, columns), BF16),
            pltpu.VMEM((SEQ_SIZE + shards - 2,) + norms.shape, F32),
            pltpu.VMEM(norms.shape, F32),
            dma((7 * chunks,)),
            dma((7 * chunks,)),
            dma((shards + 3,)),
            dma((shards + 3,)),
            dma((SEQ_SIZE + shards - 2,)),
            dma((SEQ_SIZE + shards - 2,)),
            dma((7 * chunks,)),
            dma((7 * chunks,)),
            dma((9,)),
        ],
        compiler_params=pltpu.CompilerParams(
            collective_id=2, has_side_effects=True, vmem_limit_bytes=VMEM_LIMIT
        ),
        cost_estimate=pl.CostEstimate(flops=60 * 10**9, bytes_accessed=64 * 2**20, transcendentals=0),
        name="scatter_gradients",
    )(partial, dh_one, grad_columns, norms, owned)


def padded_rows(blocks, depth):
    return pl.cdiv((3 * blocks + 1) * depth, SEQ_SIZE * 16) * SEQ_SIZE * 16


def feed_forward_kernel(
    tokens_ref,
    joined_ref,
    cot_ref,
    out_hbm,
    gate_hbm,
    up_hbm,
    down_hbm,
    norms_ref,
    output_ref,
    dout_ref,
    dh_ref,
    norm_sums_ref,
    packed_ref,
    w_out,
    w_gate,
    w_up,
    w_down,
    flow,
    hat_one,
    inverse_one,
    x_low,
    x_turned,
    dm_low,
    gate_kept,
    up_kept,
    d_gate,
    d_up,
    hidden_kept,
    staged,
    loads,
    stores,
):
    seqs, rows, width = dh_ref.shape
    shards = packed_ref.shape[0]
    depth = width // shards
    blocks = gate_hbm.shape[1] // width
    weights = ((out_hbm, w_out), (gate_hbm, w_gate), (up_hbm, w_up), (down_hbm, w_down))
    fetch = [pltpu.make_async_copy(src, dst, loads.at[n]) for n, (src, dst) in enumerate(weights)]
    tokens_in = pltpu.make_async_copy(tokens_ref, flow, loads.at[4])
    tokens_in.start()
    for copy in fetch:
        copy.start()
    gain_one, bias_one, gain_two, bias_two = (norms_ref[n : n + 1, :] for n in range(4))

    def mean(value):
        return jnp.sum(value, axis=-1, keepdims=True) * (1.0 / width)

    fetch[0].wait()
    tokens_in.wait()
    for seq in range(seqs):
        h_one = flow[seq].astype(F32)
        for group in range(GROUPS):
            h_one = h_one + jnp.dot(
                unpack_heads(joined_ref[seq * GROUPS + group]),
                w_out[group * depth : (group + 1) * depth, :],
                preferred_element_type=F32,
            )
        centered = h_one - mean(h_one)
        inverse = lax.rsqrt(mean(centered * centered) + EPS)
        normed = centered * inverse
        hat_one[seq] = normed
        inverse_one[seq] = inverse
        x_one = normed * gain_one + bias_one
        dh_ref[seq] = x_one
        x_low[seq] = x_one.astype(BF16)
        x_turned[:, seq * rows : (seq + 1) * rows] = jnp.transpose(x_one).astype(BF16)
    cot_in = pltpu.make_async_copy(cot_ref, flow, loads.at[4])
    cot_in.start()
    for copy in fetch[1:]:
        copy.wait()

    def forward(block, carry):
        at = pl.ds(pl.multiple_of(block * width, width), width)
        for seq in range(seqs):
            gate = jnp.dot(x_low[seq], w_gate[:, at], preferred_element_type=F32)
            up = jnp.dot(x_low[seq], w_up[:, at], preferred_element_type=F32)
            gate_kept[block, seq] = gate.astype(gate_kept.dtype)
            up_kept[block, seq] = up.astype(up_kept.dtype)
            hidden = (gate * jax.nn.sigmoid(gate) * up).astype(BF16)
            dh_ref[seq] += jnp.dot(hidden, w_down[at, :], preferred_element_type=F32)
        return carry

    lax.fori_loop(0, blocks, forward, 0)

    cot_in.wait()
    gain_two_sum = jnp.zeros((1, width), F32)
    bias_two_sum = jnp.zeros((1, width), F32)
    for seq in range(seqs):
        h_two = dh_ref[seq]
        centered = h_two - mean(h_two)
        inverse = lax.rsqrt(mean(centered * centered) + EPS)
        normed = centered * inverse
        cot = flow[seq].astype(F32)
        flow[seq] = (normed * gain_two + bias_two).astype(BF16)
        gain_two_sum = gain_two_sum + jnp.sum(cot * normed, axis=0, keepdims=True)
        bias_two_sum = bias_two_sum + jnp.sum(cot, axis=0, keepdims=True)
        scaled = cot * gain_two
        dh_two = inverse * (scaled - mean(scaled) - normed * mean(scaled * normed))
        dh_ref[seq] = dh_two
        dm_low[seq * rows : (seq + 1) * rows, :] = dh_two.astype(BF16)
    output_out = pltpu.make_async_copy(flow, output_ref, loads.at[4])
    output_out.start()

    def store(kind, block):
        if kind < 2:
            start = pl.multiple_of((kind * blocks + block) * depth, depth)
            return [
                pltpu.make_async_copy(
                    staged.at[kind, pl.ds(shard * depth, depth)],
                    packed_ref.at[shard, pl.ds(start, depth)],
                    stores.at[kind, shard],
                )
                for shard in range(shards)
            ]
        start = 2 * blocks * depth
        return [
            pltpu.make_async_copy(
                staged.at[2], packed_ref.at[block, pl.ds(start, width)], stores.at[2, 0]
            )
        ]

    def backward(block, carry):
        at = pl.ds(pl.multiple_of(block * width, width), width)
        for seq in range(seqs):
            here = slice(seq * rows, (seq + 1) * rows)
            d_hidden = lax.dot_general(dm_low[here, :], w_down[at, :], BY_LANES, preferred_element_type=F32)
            gate = gate_kept[block, seq].astype(F32)
            up = up_kept[block, seq].astype(F32)
            sigma = jax.nn.sigmoid(gate)
            smooth = gate * sigma
            hidden_kept[here, :] = (smooth * up).astype(BF16)
            dg = (d_hidden * up * (sigma + smooth * (1.0 - sigma))).astype(BF16)
            du = (d_hidden * smooth).astype(BF16)
            d_gate[here, :] = dg
            d_up[here, :] = du
            dh_ref[seq] += lax.dot_general(dg, w_gate[:, at], BY_LANES, preferred_element_type=F32)
            dh_ref[seq] += lax.dot_general(du, w_up[:, at], BY_LANES, preferred_element_type=F32)

        @pl.when(block > 0)
        def _():
            for kind in range(3):
                for copy in store(kind, block - 1):
                    copy.wait()

        staged[0] = jnp.dot(x_turned[...], d_gate[...], preferred_element_type=F32).astype(BF16)
        staged[1] = jnp.dot(x_turned[...], d_up[...], preferred_element_type=F32).astype(BF16)
        staged[2] = lax.dot_general(
            hidden_kept[...], dm_low[...], (((0,), (0,)), ((), ())), preferred_element_type=F32
        ).astype(BF16)
        for kind in range(3):
            for copy in store(kind, block):
                copy.start()
        return carry

    lax.fori_loop(0, blocks, backward, 0)

    gain_one_sum = jnp.zeros((1, width), F32)
    bias_one_sum = jnp.zeros((1, width), F32)
    for seq in range(seqs):
        here = slice(seq * rows, (seq + 1) * rows)
        dx_one = dh_ref[seq]
        normed = hat_one[seq]
        gain_one_sum = gain_one_sum + jnp.sum(dx_one * normed, axis=0, keepdims=True)
        bias_one_sum = bias_one_sum + jnp.sum(dx_one, axis=0, keepdims=True)
        scaled = dx_one * gain_one
        dh_one = inverse_one[seq] * (scaled - mean(scaled) - normed * mean(scaled * normed))
        dh_ref[seq] = dh_one
        d_attn = dh_one.astype(BF16)
        d_gate[here, :] = d_attn
        for group in range(GROUPS):
            dout = lax.dot_general(
                d_attn, w_out[group * depth : (group + 1) * depth, :], BY_LANES, preferred_element_type=F32
            )
            first, last = pack_heads(dout)
            dout_ref[seq * GROUPS + group, :rows] = first.astype(BF16)
            dout_ref[seq * GROUPS + group, rows:] = last.astype(BF16)
    for kind in range(3):
        for copy in store(kind, blocks - 1):
            copy.wait()
    for group in range(GROUPS):
        grad = jnp.zeros((depth, width), F32)
        for seq in range(seqs):
            grad = grad + lax.dot_general(
                unpack_heads(joined_ref[seq * GROUPS + group]),
                d_gate[seq * rows : (seq + 1) * rows, :],
                (((0,), (0,)), ((), ())),
                preferred_element_type=F32,
            )
        staged[0, group * depth : (group + 1) * depth, :] = grad.astype(BF16)
    last = [
        pltpu.make_async_copy(
            staged.at[0, pl.ds(shard * depth, depth)],
            packed_ref.at[shard, pl.ds(3 * blocks * depth, depth)],
            stores.at[0, shard],
        )
        for shard in range(shards)
    ]
    used = (3 * blocks + 1) * depth
    rest = packed_ref.shape[1] - used
    staged[1, :rest, :] = jnp.zeros((rest, width), BF16)
    last += [
        pltpu.make_async_copy(
            staged.at[1, pl.ds(0, rest)], packed_ref.at[shard, pl.ds(used, rest)], stores.at[1, shard]
        )
        for shard in range(shards)
    ]
    for copy in last:
        copy.start()
    norm_sums_ref[0:1, :] = gain_one_sum
    norm_sums_ref[1:2, :] = bias_one_sum
    norm_sums_ref[2:3, :] = gain_two_sum
    norm_sums_ref[3:4, :] = bias_two_sum
    for copy in last:
        copy.wait()
    output_out.wait()


def feed_forward(tokens, joined, cotangent, w_out, w_gate, w_up, w_down, norms, kept=BF16):
    seqs, rows, width = tokens.shape
    total = seqs * rows
    hidden = w_gate.shape[1]
    blocks = hidden // width
    depth = width // GROUPS
    vmem = pl.BlockSpec(memory_space=pltpu.VMEM)
    hbm = pl.BlockSpec(memory_space=pltpu.HBM)
    dma = pltpu.SemaphoreType.DMA
    return pl.pallas_call(
        feed_forward_kernel,
        out_shape=(
            jax.ShapeDtypeStruct(tokens.shape, BF16),
            jax.ShapeDtypeStruct(joined.shape, BF16),
            jax.ShapeDtypeStruct(tokens.shape, F32),
            jax.ShapeDtypeStruct((4, width), F32),
            jax.ShapeDtypeStruct((GROUPS, padded_rows(blocks, depth), width), BF16),
        ),
        in_specs=[hbm, vmem, hbm, hbm, hbm, hbm, hbm, vmem],
        out_specs=(hbm, vmem, vmem, vmem, hbm),
        scratch_shapes=[
            pltpu.VMEM(w_out.shape, BF16),
            pltpu.VMEM(w_gate.shape, BF16),
            pltpu.VMEM(w_up.shape, BF16),
            pltpu.VMEM(w_down.shape, BF16),
            pltpu.VMEM(tokens.shape, BF16),
            pltpu.VMEM(tokens.shape, F32),
            pltpu.VMEM((seqs, rows, 1), F32),
            pltpu.VMEM(tokens.shape, BF16),
            pltpu.VMEM((width, total), BF16),
            pltpu.VMEM((total, width), BF16),
            pltpu.VMEM((blocks, seqs, rows, width), kept),
            pltpu.VMEM((blocks, seqs, rows, width), kept),
            pltpu.VMEM((total, width), BF16),
            pltpu.VMEM((total, width), BF16),
            pltpu.VMEM((total, width), BF16),
            pltpu.VMEM((3, width, width), BF16),
            dma((5,)),
            dma((3, GROUPS)),
        ],
        compiler_params=pltpu.CompilerParams(vmem_limit_bytes=FEED_LIMIT),
        cost_estimate=pl.CostEstimate(
            flops=6 * total * width * (3 * hidden + width),
            bytes_accessed=2 * 2 * (3 * hidden + width) * width + 20 * total * width,
            transcendentals=2 * total * hidden,
        ),
        name="feed_forward",
    )(tokens, joined, cotangent, w_out, w_gate, w_up, w_down, norms)


def unpack_kernel(gate_rows, up_rows, down_rows, out_rows, columns, gate_ref, up_ref, down_ref, out_ref, qkv_ref):
    gate_ref[...] = gate_rows[...].astype(F32)
    up_ref[...] = up_rows[...].astype(F32)
    down_ref[...] = down_rows[...].astype(F32)

    @pl.when(pl.program_id(0) == 0)
    def _():
        out_ref[...] = out_rows[...].astype(F32)
        groups, _, width = columns.shape
        width = width // 3
        for group in range(groups):
            for part in range(3):
                at = (part * groups + group) * width
                qkv_ref[:, at : at + width] = columns[group, :, part * width : (part + 1) * width].astype(F32)


def unpack_gradients(rows, columns, blocks):
    groups, depth, thirds = columns.shape
    width = rows.shape[1]
    piece = [
        pl.BlockSpec((depth, width), lambda i, first=first, step=step: (first + step * i, 0))
        for first, step in ((0, 1), (blocks, 1), (2 * blocks, 1), (3 * blocks, 0))
    ]
    return pl.pallas_call(
        unpack_kernel,
        out_shape=(
            jax.ShapeDtypeStruct((depth, blocks * width), F32),
            jax.ShapeDtypeStruct((depth, blocks * width), F32),
            jax.ShapeDtypeStruct((blocks * depth, width), F32),
            jax.ShapeDtypeStruct((depth, width), F32),
            jax.ShapeDtypeStruct((depth, groups * thirds), F32),
        ),
        grid=(blocks,),
        in_specs=piece + [pl.BlockSpec(columns.shape, lambda i: (0, 0, 0))],
        out_specs=(
            pl.BlockSpec((depth, width), lambda i: (0, i)),
            pl.BlockSpec((depth, width), lambda i: (0, i)),
            pl.BlockSpec((depth, width), lambda i: (i, 0)),
            pl.BlockSpec((depth, width), lambda i: (0, 0)),
            pl.BlockSpec((depth, groups * thirds), lambda i: (0, 0)),
        ),
        name="unpack_gradients",
    )(rows, rows, rows, rows, columns)


def document_places(seg_row):
    length = seg_row.shape[0]
    ids = jnp.arange(LANES - HD, dtype=jnp.int32)[:, None]
    starts = jnp.sum((seg_row[None, :] < ids).astype(jnp.int32), axis=1, keepdims=True)
    start = jnp.sum(jnp.where(seg_row[None, :] == ids, starts, 0), axis=0)
    return jnp.arange(length, dtype=jnp.int32) - start


def exchange_kernel(sent_ref, taken_ref, send, recv, kept):
    me = lax.axis_index("seq")
    barrier = pltpu.get_barrier_semaphore()
    others = [lax.rem(me + step, SEQ_SIZE) for step in range(1, SEQ_SIZE)]
    for device in others:
        pl.semaphore_signal(barrier, inc=1, device_id={"seq": device}, device_id_type=BY_MESH)
    pl.semaphore_wait(barrier, SEQ_SIZE - 1)
    copies = []
    for step, device in enumerate(others):
        copy = pltpu.make_async_remote_copy(
            src_ref=sent_ref.at[device],
            dst_ref=taken_ref.at[me],
            send_sem=send.at[step],
            recv_sem=recv.at[step],
            device_id={"seq": device},
            device_id_type=BY_MESH,
        )
        copy.start()
        copies.append(copy)
    keep = pltpu.make_async_copy(sent_ref.at[me], taken_ref.at[me], kept)
    keep.start()
    keep.wait()
    for copy in copies:
        copy.wait()


def exchange(blocks, collective_id):
    hbm = pl.BlockSpec(memory_space=pltpu.HBM)
    dma = pltpu.SemaphoreType.DMA
    return pl.pallas_call(
        exchange_kernel,
        out_shape=jax.ShapeDtypeStruct(blocks.shape, blocks.dtype),
        in_specs=[hbm],
        out_specs=hbm,
        scratch_shapes=[dma((SEQ_SIZE - 1,)), dma((SEQ_SIZE - 1,)), dma],
        compiler_params=pltpu.CompilerParams(collective_id=collective_id, has_side_effects=True),
        name="exchange",
    )(blocks)


def head_columns(w_qkv, group, held):
    depth = w_qkv.shape[0]
    split = w_qkv.reshape(depth, 3, GROUPS, held, HD)
    mine = lax.dynamic_index_in_dim(split, group, 2, keepdims=False)
    second = mine * jnp.array([1, 1, 0], w_qkv.dtype)[None, :, None, None]
    return jnp.concatenate([mine, second], axis=-1).reshape(depth, 3 * held * 2 * HD)


def local_heads(
    shards,
    tokens,
    segments,
    positions,
    cotangent,
    w_qkv,
    w_out,
    w_gate,
    w_up,
    w_down,
    ln1_gain,
    ln1_bias,
    ln2_gain,
    ln2_bias,
):
    seq_count, row_count, model_width = tokens.shape
    held = HEADS // GROUPS
    length = row_count * SEQ_SIZE
    me = lax.axis_index("seq")
    seg_row = lax.dynamic_index_in_dim(segments, me // GROUPS, 0, keepdims=False)

    def gather(shard):
        return lax.all_gather(shard, "shard", axis=0, tiled=True)

    freqs = jnp.exp(jnp.arange(HD // 2, dtype=F32) * (-math.log(ROPE_BASE) / (HD // 2)))
    freq = jnp.tile(freqs, LANES // (HD // 2))[None]
    place = document_places(seg_row).astype(F32).reshape(SEQ_SIZE, 1, row_count)
    norm_rows = jnp.stack([ln1_gain, ln1_bias, ln2_gain, ln2_bias]).astype(F32)
    pieces, w_heads, norms, turn = gather_tokens(
        tokens, head_columns(w_qkv, me % GROUPS, held), norm_rows, place, freq, shards
    )
    norms = jnp.transpose(norms, (1, 0, 2)).reshape(4, model_width)
    full_out, full_gate, full_up, full_down = (gather(w) for w in (w_out, w_gate, w_up, w_down))
    bounds = document_bounds(seg_row, row_count)
    q_ext, k_ext, v_ext = project_heads(
        seg_row.astype(F32), turn, pieces, w_heads.reshape(model_width, -1), held
    )
    sums, joined_own = attend_heads(bounds, q_ext, k_ext, v_ext, row_count)
    output, d_joined, dh_one, norms_part, packed = feed_forward(
        tokens, exchange(joined_own, 3), cotangent, full_out, full_gate, full_up, full_down, norms
    )
    depth = model_width // shards
    ff_blocks = full_gate.shape[1] // model_width
    owned = lax.psum_scatter(
        packed.reshape(-1, model_width), ("shard", "seq"), scatter_dimension=0, tiled=True
    )

    dout = exchange(d_joined, 4)
    d_heads = attend_back_heads(bounds, q_ext, k_ext, v_ext, sums, dout, turn)
    w_lanes = w_heads.reshape(model_width, -1)
    w_own = jnp.concatenate(
        [w_lanes[:, at : at + HD] for at in range(0, w_lanes.shape[1], LANES)], axis=1
    )
    partial = jnp.einsum("prc,dc->prd", d_heads, w_own, preferred_element_type=F32).astype(BF16)
    grad_columns = jnp.einsum("prd,prc->dc", pieces, d_heads, preferred_element_type=F32).astype(BF16)
    input_grad, columns, norm_sums, shared = scatter_gradients(
        partial, dh_one, grad_columns.reshape(shards, depth, -1), norms_part, owned
    )
    grad_gate, grad_up, grad_down, grad_out, grad_qkv = unpack_gradients(shared, columns, ff_blocks)
    shard = lax.axis_index("shard")
    norm_sums = lax.dynamic_slice_in_dim(norm_sums, shard * depth, depth, 1)
    return (
        output,
        input_grad,
        grad_qkv,
        grad_out,
        grad_gate,
        grad_up,
        grad_down,
        norm_sums[0],
        norm_sums[1],
        norm_sums[2],
        norm_sums[3],
    )


def solution(mesh):
    in_specs = (
        P("shard", "seq", None),
        P("shard", None),
        P("shard", "seq"),
        P("shard", "seq", None),
        P("shard", None),
        P("shard", None),
        P("shard", None),
        P("shard", None),
        P("shard", None),
        P("shard"),
        P("shard"),
        P("shard"),
        P("shard"),
    )
    out_specs = (
        P("shard", "seq", None),
        P("shard", "seq", None),
        P("shard", None),
        P("shard", None),
        P("shard", None),
        P("shard", None),
        P("shard", None),
        P("shard"),
        P("shard"),
        P("shard"),
        P("shard"),
    )
    body = functools.partial(local_heads, mesh.shape["shard"]) if (mesh.shape["seq"], mesh.shape["shard"]) == (SEQ_SIZE, GROUPS) else local
    return jax.shard_map(body, mesh=mesh, in_specs=in_specs, out_specs=out_specs, check_vma=False)
```

```python
import functools
import math

import jax
import jax.numpy as jnp
from jax import lax
from jax.experimental import pallas as pl
from jax.experimental.pallas import tpu as pltpu
from jax.sharding import PartitionSpec as P

HEADS = 12
HD = 64


EPS = 1e-05
ROPE_BASE = 1000.0


def rope_tables(pos_block):
    half_dim = HD // 2
    freqs = jnp.exp(jnp.arange(half_dim, dtype=jnp.float32) * (-math.log(ROPE_BASE) / half_dim))
    angle = pos_block.astype(jnp.float32)[..., None] * freqs
    return (jnp.cos(angle)[:, :, None, :], jnp.sin(angle)[:, :, None, :])


def rotate(heads, cos_b, sin_b):
    half_dim = heads.shape[-1] // 2
    first = heads[..., :half_dim]
    second = heads[..., half_dim:]
    return jnp.concatenate(
        [first * cos_b - second * sin_b, second * cos_b + first * sin_b], axis=-1
    )


def rotate_back(grads, cos_b, sin_b):
    half_dim = grads.shape[-1] // 2
    first = grads[..., :half_dim]
    second = grads[..., half_dim:]
    return jnp.concatenate(
        [first * cos_b + second * sin_b, second * cos_b - first * sin_b], axis=-1
    )


def norm_fwd(values, gain, bias):
    mean_val = jnp.mean(values, axis=-1, keepdims=True)
    centered = values - mean_val
    variance = jnp.mean(centered * centered, axis=-1, keepdims=True)
    inverse = lax.rsqrt(variance + EPS)
    normed = centered * inverse
    return (normed * gain + bias, normed, inverse)


def norm_back(grad_in, normed, inverse, gain):
    scaled = grad_in * gain
    return inverse * (
        scaled
        - jnp.mean(scaled, axis=-1, keepdims=True)
        - normed * jnp.mean(scaled * normed, axis=-1, keepdims=True)
    )


def head_split(block_rows, seq_count, row_count):
    return block_rows.reshape(seq_count, row_count, HEADS, HD)


def attend(q_heads, q_seg, k_full, v_full, seg_all, block, score_scale):
    seq_count, row_count = (q_heads.shape[0], q_heads.shape[1])
    block_count = k_full.shape[1] // block

    def attend_step(carry, index):
        row_total, value_sum = carry
        start = index * block
        k_part = head_split(lax.dynamic_slice_in_dim(k_full, start, block, 1), seq_count, block)
        v_part = head_split(lax.dynamic_slice_in_dim(v_full, start, block, 1), seq_count, block)
        seg_part = lax.dynamic_slice_in_dim(seg_all, start, block, 1)
        raw = (
            jnp.einsum("sqhd,skhd->shqk", q_heads, k_part, preferred_element_type=jnp.float32)
            * score_scale
        )
        same_doc = q_seg[:, None, :, None] == seg_part[:, None, None, :]
        expo = jnp.where(same_doc, jnp.exp(raw), 0.0)
        row_total = row_total + jnp.sum(expo, axis=-1)
        value_sum = value_sum + jnp.einsum(
            "shqk,skhd->sqhd", expo.astype(jnp.bfloat16), v_part, preferred_element_type=jnp.float32
        )
        return ((row_total, value_sum), None)

    start_carry = (
        jnp.zeros((seq_count, HEADS, row_count), jnp.float32),
        jnp.zeros((seq_count, row_count, HEADS, HD), jnp.float32),
    )
    final, unused = lax.scan(attend_step, start_carry, jnp.arange(block_count, dtype=jnp.int32))
    return final


def back_keys(q_heads, g_heads, delta, q_seg, k_full, v_full, seg_all, block, score_scale):
    seq_count, row_count = (q_heads.shape[0], q_heads.shape[1])
    full_len = k_full.shape[1]
    block_count = full_len // block

    def back_step(carry, index):
        start = index * block
        k_part = head_split(lax.dynamic_slice_in_dim(k_full, start, block, 1), seq_count, block)
        v_part = head_split(lax.dynamic_slice_in_dim(v_full, start, block, 1), seq_count, block)
        seg_part = lax.dynamic_slice_in_dim(seg_all, start, block, 1)
        raw = (
            jnp.einsum("sqhd,skhd->shqk", q_heads, k_part, preferred_element_type=jnp.float32)
            * score_scale
        )
        same_doc = q_seg[:, None, :, None] == seg_part[:, None, None, :]
        expo = jnp.where(same_doc, jnp.exp(raw), 0.0)
        prob_grad = jnp.einsum(
            "sqhd,skhd->shqk", g_heads, v_part, preferred_element_type=jnp.float32
        )
        d_score = (expo * (prob_grad - delta[..., None])).astype(jnp.bfloat16)
        q_grad = carry[0] + jnp.einsum(
            "shqk,skhd->sqhd", d_score, k_part, preferred_element_type=jnp.float32
        )
        k_grad = (
            jnp.einsum("shqk,sqhd->skhd", d_score, q_heads, preferred_element_type=jnp.float32)
            * score_scale
        )
        v_grad = jnp.einsum(
            "shqk,sqhd->skhd",
            expo.astype(jnp.bfloat16),
            g_heads,
            preferred_element_type=jnp.float32,
        )
        k_store = lax.dynamic_update_slice_in_dim(
            carry[1], k_grad.reshape(seq_count, block, HEADS * HD), start, 1
        )
        v_store = lax.dynamic_update_slice_in_dim(
            carry[2], v_grad.reshape(seq_count, block, HEADS * HD), start, 1
        )
        return ((q_grad, k_store, v_store), None)

    q_zero = jnp.zeros((seq_count, row_count, HEADS, HD), jnp.float32)
    kv_zero = jnp.zeros((seq_count, full_len, HEADS * HD), jnp.float32)
    start_carry = (q_zero, kv_zero, kv_zero)
    final, unused = lax.scan(back_step, start_carry, jnp.arange(block_count, dtype=jnp.int32))
    return (final[0] * score_scale,) + tuple(final[1:])


def local(
    tokens,
    segments,
    positions,
    cotangent,
    w_qkv,
    w_out,
    w_gate,
    w_up,
    w_down,
    ln1_gain,
    ln1_bias,
    ln2_gain,
    ln2_bias,
):
    seq_count, row_count, model_width = tokens.shape
    score_scale = HD ** (-0.5)
    q_seg = lax.dynamic_slice_in_dim(segments, lax.axis_index("seq") * row_count, row_count, 1)
    gathered = (
        lax.all_gather(w_qkv, "shard", axis=0, tiled=True),
        lax.all_gather(w_out, "shard", axis=0, tiled=True),
        lax.all_gather(w_gate, "shard", axis=0, tiled=True),
        lax.all_gather(w_up, "shard", axis=0, tiled=True),
        lax.all_gather(w_down, "shard", axis=0, tiled=True),
        lax.all_gather(ln1_gain, "shard", axis=0, tiled=True),
        lax.all_gather(ln1_bias, "shard", axis=0, tiled=True),
        lax.all_gather(ln2_gain, "shard", axis=0, tiled=True),
        lax.all_gather(ln2_bias, "shard", axis=0, tiled=True),
    )
    full_qkv, full_out, full_gate, full_up, full_down, gain_one, bias_one, gain_two, bias_two = (
        gathered
    )
    cos_b, sin_b = rope_tables(positions)
    qkv_all = jnp.einsum("scd,de->sce", tokens, full_qkv, preferred_element_type=jnp.float32)
    q_heads = rotate(
        head_split(qkv_all[..., :model_width], seq_count, row_count), cos_b, sin_b
    ).astype(jnp.bfloat16)
    k_heads = rotate(
        head_split(qkv_all[..., model_width : 2 * model_width], seq_count, row_count), cos_b, sin_b
    ).astype(jnp.bfloat16)
    v_heads = head_split(qkv_all[..., 2 * model_width :], seq_count, row_count).astype(jnp.bfloat16)
    k_local = k_heads.reshape(seq_count, row_count, model_width)
    v_local = v_heads.reshape(seq_count, row_count, model_width)
    k_full, v_full = (
        lax.all_gather(k_local, "seq", axis=1, tiled=True),
        lax.all_gather(v_local, "seq", axis=1, tiled=True),
    )
    row_total, value_sum = attend(q_heads, q_seg, k_full, v_full, segments, row_count, score_scale)
    denom = jnp.transpose(row_total, (0, 2, 1))[..., None]
    attn_out = value_sum / denom
    joined = attn_out.reshape(seq_count, row_count, model_width).astype(jnp.bfloat16)
    tokens_f = tokens.astype(jnp.float32)
    h_one = tokens_f + jnp.einsum(
        "sci,io->sco", joined, full_out, preferred_element_type=jnp.float32
    )
    x_one, normed_one, inverse_one = norm_fwd(
        h_one, gain_one.astype(jnp.float32), bias_one.astype(jnp.float32)
    )
    x_low = x_one.astype(jnp.bfloat16)
    gate_pre = jnp.einsum("scd,df->scf", x_low, full_gate, preferred_element_type=jnp.float32)
    up_pre = jnp.einsum("scd,df->scf", x_low, full_up, preferred_element_type=jnp.float32)
    sigma = jax.nn.sigmoid(gate_pre)
    smooth = gate_pre * sigma
    hidden = (smooth * up_pre).astype(jnp.bfloat16)
    h_two = x_one + jnp.einsum("scf,fd->scd", hidden, full_down, preferred_element_type=jnp.float32)
    result, normed_two, inverse_two = norm_fwd(
        h_two, gain_two.astype(jnp.float32), bias_two.astype(jnp.float32)
    )
    output = result.astype(jnp.bfloat16)
    regathered = (
        lax.all_gather(w_qkv, "shard", axis=0, tiled=True),
        lax.all_gather(w_out, "shard", axis=0, tiled=True),
        lax.all_gather(w_gate, "shard", axis=0, tiled=True),
        lax.all_gather(w_up, "shard", axis=0, tiled=True),
        lax.all_gather(w_down, "shard", axis=0, tiled=True),
        lax.all_gather(ln1_gain, "shard", axis=0, tiled=True),
        lax.all_gather(ln2_gain, "shard", axis=0, tiled=True),
    )
    back_qkv, back_out, back_gate, back_up, back_down, back_gain_one, back_gain_two = regathered
    back_k, back_v = (
        lax.all_gather(k_local, "seq", axis=1, tiled=True),
        lax.all_gather(v_local, "seq", axis=1, tiled=True),
    )
    cot_f = cotangent.astype(jnp.float32)
    grad_gain_two = jnp.sum(cot_f * normed_two, axis=(0, 1))
    grad_bias_two = jnp.sum(cot_f, axis=(0, 1))
    dh_two = norm_back(cot_f, normed_two, inverse_two, back_gain_two.astype(jnp.float32))
    dm_low = dh_two.astype(jnp.bfloat16)
    grad_down = jnp.einsum("scf,scd->fd", hidden, dm_low, preferred_element_type=jnp.float32)
    d_hidden = jnp.einsum("scd,fd->scf", dm_low, back_down, preferred_element_type=jnp.float32)
    d_up = (d_hidden * smooth).astype(jnp.bfloat16)
    d_gate = (d_hidden * up_pre * sigma * (1.0 + gate_pre * (1.0 - sigma))).astype(jnp.bfloat16)
    grad_gate = jnp.einsum("scd,scf->df", x_low, d_gate, preferred_element_type=jnp.float32)
    grad_up = jnp.einsum("scd,scf->df", x_low, d_up, preferred_element_type=jnp.float32)
    dx_one = (
        dh_two
        + jnp.einsum("scf,df->scd", d_gate, back_gate, preferred_element_type=jnp.float32)
        + jnp.einsum("scf,df->scd", d_up, back_up, preferred_element_type=jnp.float32)
    )
    grad_gain_one = jnp.sum(dx_one * normed_one, axis=(0, 1))
    grad_bias_one = jnp.sum(dx_one, axis=(0, 1))
    dh_one = norm_back(dx_one, normed_one, inverse_one, back_gain_one.astype(jnp.float32))
    d_attn = dh_one.astype(jnp.bfloat16)
    grad_out = jnp.einsum("sci,sco->io", joined, d_attn, preferred_element_type=jnp.float32)
    d_joined = jnp.einsum(
        "sco,io->sci", d_attn, back_out, preferred_element_type=jnp.float32
    ).astype(jnp.bfloat16)
    d_heads = head_split(d_joined, seq_count, row_count).astype(jnp.float32)
    g_heads = (d_heads / denom).astype(jnp.bfloat16)
    delta = jnp.transpose(jnp.sum(d_heads * attn_out, axis=-1) / denom[..., 0], (0, 2, 1))
    q_grad, k_all, v_all = back_keys(
        q_heads, g_heads, delta, q_seg, back_k, back_v, segments, row_count, score_scale
    )
    k_sum, v_sum = (
        lax.psum_scatter(k_all.astype(jnp.bfloat16), "seq", scatter_dimension=1, tiled=True).astype(
            jnp.float32
        ),
        lax.psum_scatter(v_all.astype(jnp.bfloat16), "seq", scatter_dimension=1, tiled=True).astype(
            jnp.float32
        ),
    )
    k_grad = head_split(k_sum, seq_count, row_count)
    v_grad = head_split(v_sum, seq_count, row_count)
    q_back = rotate_back(q_grad, cos_b, sin_b).reshape(seq_count, row_count, model_width)
    k_back = rotate_back(k_grad, cos_b, sin_b).reshape(seq_count, row_count, model_width)
    d_qkv = jnp.concatenate(
        [q_back, k_back, v_grad.reshape(seq_count, row_count, model_width)], axis=-1
    ).astype(jnp.bfloat16)
    grad_qkv = jnp.einsum("scd,sce->de", tokens, d_qkv, preferred_element_type=jnp.float32)
    d_tokens = dh_one + jnp.einsum(
        "sce,de->scd", d_qkv, back_qkv, preferred_element_type=jnp.float32
    )
    input_grad = d_tokens.astype(jnp.bfloat16)
    owned = (
        lax.psum_scatter(
            grad_qkv.astype(jnp.bfloat16), "shard", scatter_dimension=0, tiled=True
        ).astype(jnp.float32),
        lax.psum_scatter(
            grad_out.astype(jnp.bfloat16), "shard", scatter_dimension=0, tiled=True
        ).astype(jnp.float32),
        lax.psum_scatter(
            grad_gate.astype(jnp.bfloat16), "shard", scatter_dimension=0, tiled=True
        ).astype(jnp.float32),
        lax.psum_scatter(
            grad_up.astype(jnp.bfloat16), "shard", scatter_dimension=0, tiled=True
        ).astype(jnp.float32),
        lax.psum_scatter(
            grad_down.astype(jnp.bfloat16), "shard", scatter_dimension=0, tiled=True
        ).astype(jnp.float32),
        lax.psum_scatter(
            grad_gain_one.astype(jnp.bfloat16), "shard", scatter_dimension=0, tiled=True
        ).astype(jnp.float32),
        lax.psum_scatter(
            grad_bias_one.astype(jnp.bfloat16), "shard", scatter_dimension=0, tiled=True
        ).astype(jnp.float32),
        lax.psum_scatter(
            grad_gain_two.astype(jnp.bfloat16), "shard", scatter_dimension=0, tiled=True
        ).astype(jnp.float32),
        lax.psum_scatter(
            grad_bias_two.astype(jnp.bfloat16), "shard", scatter_dimension=0, tiled=True
        ).astype(jnp.float32),
    )
    summed = (
        lax.psum(owned[0].astype(jnp.bfloat16), "seq").astype(jnp.float32),
        lax.psum(owned[1].astype(jnp.bfloat16), "seq").astype(jnp.float32),
        lax.psum(owned[2].astype(jnp.bfloat16), "seq").astype(jnp.float32),
        lax.psum(owned[3].astype(jnp.bfloat16), "seq").astype(jnp.float32),
        lax.psum(owned[4].astype(jnp.bfloat16), "seq").astype(jnp.float32),
        lax.psum(owned[5].astype(jnp.bfloat16), "seq").astype(jnp.float32),
        lax.psum(owned[6].astype(jnp.bfloat16), "seq").astype(jnp.float32),
        lax.psum(owned[7].astype(jnp.bfloat16), "seq").astype(jnp.float32),
        lax.psum(owned[8].astype(jnp.bfloat16), "seq").astype(jnp.float32),
    )
    return (
        output,
        input_grad,
        summed[0],
        summed[1],
        summed[2],
        summed[3],
        summed[4],
        summed[5],
        summed[6],
        summed[7],
        summed[8],
    )


SEQS_HELD = 2
SEQ_SIZE = 8
GROUPS = 4
LANES = 128
LOG2E = 1.4426950408889634
LN2 = 0.6931471805599453
FAR = 2.0**30
F32 = jnp.float32
BF16 = jnp.bfloat16
VMEM_LIMIT = 60 * 1024 * 1024
FEED_LIMIT = 63 * 1024 * 1024
BY_MESH = pl.DeviceIdType.MESH
BY_LANES = (((1,), (1,)), ((), ()))


def packed_heads(rows):
    return rows + rows // 2


def unpack_heads(block):
    rows = block.shape[0] * 2 // 3
    last = block[rows:]
    third = jnp.concatenate([last[:, :HD], last[:, HD:]], axis=0)
    return jnp.concatenate([block[:rows], third], axis=1)


def pack_heads(value):
    rows = value.shape[0]
    third = value[:, 2 * HD :]
    return value[:, : 2 * HD], jnp.concatenate([third[: rows // 2], third[rows // 2 :]], axis=1)


def flip(index, bit):
    return index + bit - 2 * bit * lax.rem(lax.div(index, bit), 2)


def gather_kernel(
    chunks, by_z, tok_ref, w_ref, n_ref, place_ref, freq_ref, all_ref, w_all_ref, n_all_ref, turn_ref, send, recv, kept, w_send, w_recv
):
    me = lax.axis_index("seq")
    shard = lax.axis_index("shard")
    shards = w_all_ref.shape[0]
    half = lax.div(me, GROUPS)
    y_near, z_near, partner = flip(me, 1), flip(me, 2), flip(me, 4)
    barrier = pltpu.get_barrier_semaphore()
    for device in (y_near, z_near, partner):
        pl.semaphore_signal(barrier, inc=1, device_id={"seq": device}, device_id_type=BY_MESH)
    for step in range(1, shards):
        pl.semaphore_signal(
            barrier, inc=1, device_id={"shard": lax.rem(shard + step, shards)}, device_id_type=BY_MESH
        )
    pl.semaphore_wait(barrier, 2 + shards)

    part = tok_ref.shape[1] // chunks
    started = []

    def go(source, target, slot, device):
        copy = pltpu.make_async_remote_copy(
            src_ref=source,
            dst_ref=target,
            send_sem=send.at[slot],
            recv_sem=recv.at[slot],
            device_id={"seq": device},
            device_id_type=BY_MESH,
        )
        copy.start()
        started.append(copy)
        return copy

    def rows(chunk):
        return pl.ds(chunk * part, part)

    def relay(piece, chunk, slot, device):
        return go(all_ref.at[piece, rows(chunk)], all_ref.at[piece, rows(chunk)], slot * chunks + chunk, device)

    def own(which, chunk, slot, device):
        return go(tok_ref.at[which, rows(chunk)], all_ref.at[me, rows(chunk)], slot * chunks + chunk, device)

    crossing = [own(1 - half, chunk, 0, partner) for chunk in range(chunks)]
    own_y, own_z = [], []
    for chunk in range(chunks):
        own_y.append(own(half, chunk, 1, y_near))
        own_z.append(own(half, chunk, 2, z_near))
    weights = []
    for step in range(1, shards):
        copy = pltpu.make_async_remote_copy(
            src_ref=w_ref,
            dst_ref=w_all_ref.at[shard],
            send_sem=w_send.at[step],
            recv_sem=w_recv.at[step],
            device_id={"shard": lax.rem(shard + step, shards)},
            device_id_type=BY_MESH,
        )
        copy.start()
        weights.append(copy)
        copy = pltpu.make_async_remote_copy(
            src_ref=n_ref,
            dst_ref=n_all_ref.at[shard],
            send_sem=w_send.at[shards + step],
            recv_sem=w_recv.at[shards + step],
            device_id={"shard": lax.rem(shard + step, shards)},
            device_id_type=BY_MESH,
        )
        copy.start()
        weights.append(copy)
    keep_n = pltpu.make_async_copy(n_ref, n_all_ref.at[shard], kept.at[2])
    keep_n.start()
    keep_tok = pltpu.make_async_copy(tok_ref.at[half], all_ref.at[me], kept.at[0])
    keep_tok.start()
    keep_w = pltpu.make_async_copy(w_ref, w_all_ref.at[shard], kept.at[1])
    keep_w.start()

    def turn_piece(index, carry):
        count = turn_ref.shape[0] // place_ref.shape[0]
        lane = lax.broadcasted_iota(jnp.int32, (count, LANES), 1)
        place = jnp.transpose(jnp.broadcast_to(place_ref[index], (LANES, count)))
        angle = place * freq_ref[...]
        turn_ref[pl.ds(pl.multiple_of(index * count, count), count), :] = jnp.where(
            lane < HD, jnp.cos(angle), jnp.sin(angle)
        )
        return carry

    lax.fori_loop(0, place_ref.shape[0], turn_piece, 0)

    cross_y, cross_z, corner = [], [], []
    for chunk in range(chunks):
        own_y[chunk].wait_recv()
        if chunk < by_z:
            corner.append(relay(y_near, chunk, 5, z_near))
        own_z[chunk].wait_recv()
        if chunk >= by_z:
            corner.append(relay(z_near, chunk, 5, y_near))
        crossing[chunk].wait_recv()
        cross_y.append(relay(partner, chunk, 3, y_near))
        cross_z.append(relay(partner, chunk, 4, z_near))
    for chunk in range(chunks):
        cross_y[chunk].wait_recv()
        if chunk < by_z:
            corner.append(relay(flip(y_near, 4), chunk, 6, z_near))
        cross_z[chunk].wait_recv()
        if chunk >= by_z:
            corner.append(relay(flip(z_near, 4), chunk, 6, y_near))
    for copy in corner:
        copy.wait_recv()
    for copy in weights:
        copy.wait()
    keep_tok.wait()
    keep_w.wait()
    keep_n.wait()
    for copy in started:
        copy.wait_send()


def gather_tokens(tokens, w_part, norms, place, freq, shards, chunks=8, by_z=3):
    seqs, rows, width = tokens.shape
    anywhere = pl.BlockSpec(memory_space=pl.ANY)
    vmem = pl.BlockSpec(memory_space=pltpu.VMEM)
    return pl.pallas_call(
        functools.partial(gather_kernel, chunks, by_z),
        out_shape=(
            jax.ShapeDtypeStruct((SEQ_SIZE, rows, width), tokens.dtype),
            jax.ShapeDtypeStruct((shards,) + w_part.shape, w_part.dtype),
            jax.ShapeDtypeStruct((shards,) + norms.shape, norms.dtype),
            jax.ShapeDtypeStruct((place.shape[0] * place.shape[2], LANES), F32),
        ),
        in_specs=[anywhere, anywhere, anywhere, vmem, vmem],
        out_specs=(anywhere, anywhere, anywhere, vmem),
        scratch_shapes=[
            pltpu.SemaphoreType.DMA((7 * chunks,)),
            pltpu.SemaphoreType.DMA((7 * chunks,)),
            pltpu.SemaphoreType.DMA((3,)),
            pltpu.SemaphoreType.DMA((2 * shards,)),
            pltpu.SemaphoreType.DMA((2 * shards,)),
        ],
        compiler_params=pltpu.CompilerParams(collective_id=1, has_side_effects=True),
        name="gather_tokens",
    )(tokens, w_part, norms, place, freq)


def project_kernel(seg_ref, turn_ref, x_ref, w_ref, q_ref, k_ref, v_ref):
    rows = x_ref.shape[1]
    held = q_ref.shape[0]
    lane = lax.broadcasted_iota(jnp.int32, (rows, LANES), 1)
    seg = jnp.transpose(jnp.broadcast_to(seg_ref[0], (LANES, rows)))
    turn = turn_ref[...]
    cos_b = jnp.where(lane < HD, turn, 0.0)
    sin_b = jnp.where(lane < HD, pltpu.roll(turn, HD, 1), 0.0)
    sin_b = jnp.where(lane < HD // 2, -sin_b, sin_b)
    same = seg == (lane - HD).astype(F32)
    q_tail = jnp.where(same, 1.0, 0.0)
    k_tail = jnp.where(same | (lane < HD), 0.0, -FAR)
    v_tail = jnp.where(lane < HD, 0.0, 1.0)
    scale = HD ** (-0.5) * LOG2E
    q_cos, q_sin = cos_b * scale, sin_b * scale
    width = held * LANES
    for part in range(3):
        mixed = jnp.dot(x_ref[0], w_ref[:, part * width : (part + 1) * width], preferred_element_type=F32)
        for head in range(held):
            value = mixed[:, head * LANES : (head + 1) * LANES]
            if part == 0:
                value = value * q_cos + pltpu.roll(value, HD // 2, 1) * q_sin + q_tail
                q_ref[head] = value.astype(BF16)
            elif part == 1:
                value = value * cos_b + pltpu.roll(value, HD // 2, 1) * sin_b + k_tail
                k_ref[head] = value.astype(BF16)
            else:
                v_ref[head] = (value + v_tail).astype(BF16)


def project_heads(seg_row, turn, pieces, w_full, held):
    count, rows, width = pieces.shape
    length = count * rows
    row_spec = pl.BlockSpec((1, 1, rows), lambda i: (i, 0, 0))
    head_spec = pl.BlockSpec((held, rows, LANES), lambda i: (0, i, 0))
    head_shape = jax.ShapeDtypeStruct((held, length, LANES), BF16)
    return pl.pallas_call(
        project_kernel,
        out_shape=(head_shape, head_shape, head_shape),
        grid=(count,),
        in_specs=[
            row_spec,
            pl.BlockSpec((rows, LANES), lambda i: (i, 0)),
            pl.BlockSpec((1, rows, width), lambda i: (i, 0, 0)),
            pl.BlockSpec(w_full.shape, lambda i: (0, 0)),
        ],
        out_specs=(head_spec, head_spec, head_spec),
        compiler_params=pltpu.CompilerParams(vmem_limit_bytes=VMEM_LIMIT),
        cost_estimate=pl.CostEstimate(
            flops=2 * length * width * w_full.shape[1],
            bytes_accessed=length * (width * 2 + held * LANES * 6 + LANES * 4),
            transcendentals=length * LANES,
        ),
        name="project_heads",
    )(seg_row.reshape(count, 1, rows), turn, pieces, w_full)


def document_bounds(seg_row, rows):
    first = seg_row[::rows]
    last = seg_row[rows - 1 :: rows]
    low = jnp.sum((seg_row[None, :] < first[:, None]).astype(jnp.int32), axis=1)
    high = jnp.sum((seg_row[None, :] <= last[:, None]).astype(jnp.int32), axis=1)
    return low, high


def windows(bounds, length, window, align):
    low = bounds[0] // align * align
    count = (bounds[1] - low + window - 1) // window
    return jnp.minimum(low, length - count * window), count


def attend_kernel(window, align, low_ref, count_ref, q_ref, k_ref, v_ref, sum_ref, joined_ref):
    block = pl.program_id(0)
    low = low_ref[block]
    sum_ref[...] = jnp.zeros_like(sum_ref)

    def step(index, carry):
        start = pl.multiple_of(low + index * window, align)
        for head in range(q_ref.shape[0]):
            k_part = k_ref[head, pl.ds(start, window), :]
            v_part = v_ref[head, pl.ds(start, window), :]
            score = lax.dot_general(q_ref[head], k_part, BY_LANES, preferred_element_type=F32)
            expo = jnp.exp2(score).astype(BF16)
            sum_ref[head] += jnp.dot(expo, v_part, preferred_element_type=F32)
        return carry

    lax.fori_loop(0, count_ref[block], step, 0)
    rows = q_ref.shape[1]
    parts = [sum_ref[head][:, :HD] / sum_ref[head][:, HD : HD + 1] for head in range(q_ref.shape[0])]
    first, last = pack_heads(jnp.concatenate(parts, axis=1))
    joined_ref[0, :rows] = first.astype(BF16)
    joined_ref[0, rows:] = last.astype(BF16)


def attend_heads(bounds, q_ext, k_ext, v_ext, rows, window=1024, align=16):
    heads, length, lanes = q_ext.shape
    low, count = windows(bounds, length, window, align)
    whole = pl.BlockSpec((heads, length, lanes), lambda i, *_: (0, 0, 0))
    part = pl.BlockSpec((heads, rows, lanes), lambda i, *_: (0, i, 0))
    return pl.pallas_call(
        functools.partial(attend_kernel, window, align),
        out_shape=(
            jax.ShapeDtypeStruct((heads, length, lanes), F32),
            jax.ShapeDtypeStruct((length // rows, packed_heads(rows), LANES), BF16),
        ),
        grid_spec=pltpu.PrefetchScalarGridSpec(
            num_scalar_prefetch=2,
            grid=(length // rows,),
            in_specs=[part, whole, whole],
            out_specs=(part, pl.BlockSpec((1, packed_heads(rows), LANES), lambda i, *_: (i, 0, 0))),
        ),
        compiler_params=pltpu.CompilerParams(vmem_limit_bytes=VMEM_LIMIT),
        cost_estimate=pl.CostEstimate(
            flops=heads * length * length * 4 * lanes // 2,
            bytes_accessed=heads * length * lanes * 10,
            transcendentals=heads * length * length // 2,
        ),
        name="attend_heads",
    )(low, count, q_ext, k_ext, v_ext)


def attend_back_kernel(
    align,
    low_ref,
    count_ref,
    q_ref,
    sum_ref,
    dout_ref,
    turn_ref,
    k_ref,
    v_ref,
    d_ref,
    dq_ref,
    dkv_ref,
    g_ref,
    gt_ref,
    qt_ref,
):
    block = pl.program_id(0)
    heads, rows, lanes = q_ref.shape
    width = heads * HD

    @pl.when(block == 0)
    def _():
        dkv_ref[...] = jnp.zeros_like(dkv_ref)

    dq_ref[...] = jnp.zeros_like(dq_ref)
    half_lane = lax.broadcasted_iota(jnp.int32, (rows, HD), 1)
    dout_all = unpack_heads(dout_ref[0].astype(F32))
    for head in range(heads):
        dout = dout_all[:, head * HD : (head + 1) * HD]
        sums = sum_ref[head]
        total = sums[:, HD : HD + 1]
        g_low = dout / total
        delta = -jnp.sum(dout * sums[:, :HD], axis=1, keepdims=True) / (total * total)
        high = delta.astype(BF16).astype(F32)
        middle = (delta - high).astype(BF16).astype(F32)
        tail = jnp.where(
            half_lane == 0,
            high,
            jnp.where(half_lane == 1, middle, jnp.where(half_lane == 2, delta - high - middle, 0.0)),
        )
        g_ext = jnp.concatenate([g_low, tail], axis=1)
        g_ref[head] = g_ext.astype(BF16)
        gt_ref[head] = jnp.transpose(g_ext)[:HD].astype(BF16)
        qt_ref[head] = jnp.transpose(q_ref[head].astype(F32))[:HD].astype(BF16)

    low = low_ref[block]

    def step(window, low, index, carry):
        start = pl.multiple_of(low + index * window, align)
        for head in range(heads):
            k_part = k_ref[head, pl.ds(start, window), :]
            v_part = v_ref[head, pl.ds(start, window), :]
            score = lax.dot_general(q_ref[head], k_part, BY_LANES, preferred_element_type=F32)
            slope = lax.dot_general(g_ref[head], v_part, BY_LANES, preferred_element_type=F32)
            expo = jnp.exp2(score)
            d_score = (expo * slope).astype(BF16)
            expo = expo.astype(BF16)
            dq_ref[head] += jnp.dot(d_score, k_part, preferred_element_type=F32)
            dkv_ref[head, :HD, pl.ds(start, window)] += jnp.dot(qt_ref[head], d_score, preferred_element_type=F32)
            dkv_ref[head, HD:, pl.ds(start, window)] += jnp.dot(gt_ref[head], expo, preferred_element_type=F32)
        return carry

    units = count_ref[block]
    many = lax.div(units, 4)
    rest = lax.rem(units, 4)
    lax.fori_loop(0, many, functools.partial(step, 4 * align, low), 0)
    low = low + many * 4 * align

    @pl.when(rest >= 2)
    def _():
        step(2 * align, low, 0, 0)

    @pl.when(lax.rem(rest, 2) == 1)
    def _():
        step(align, low + lax.div(rest, 2) * 2 * align, 0, 0)

    lane = lax.broadcasted_iota(jnp.int32, (rows, lanes), 1)

    def turn_back(value, turn):
        swapped = jnp.where(lane < HD // 2, pltpu.roll(value, lanes - HD // 2, 1), pltpu.roll(value, HD // 2, 1))
        sine = pltpu.roll(turn, HD, 1)
        sine = jnp.where(lane < HD // 2, sine, -sine)
        return (value * turn + swapped * sine)[:, :HD]

    here = turn_ref[pl.ds(pl.multiple_of(block * rows, rows), rows), :]
    for head in range(heads):
        turned = turn_back(dq_ref[head] * HD ** (-0.5), here)
        d_ref[block, :, head * HD : (head + 1) * HD] = turned.astype(BF16)

    @pl.when(block == pl.num_programs(0) - 1)
    def _():
        def finish(piece, carry):
            start = pl.multiple_of(piece * rows, rows)
            turn = turn_ref[pl.ds(start, rows), :]
            for head in range(heads):
                both = jnp.transpose(dkv_ref[head, :, pl.ds(start, rows)])
                at = width + head * HD
                d_ref[piece, :, at : at + HD] = (turn_back(both, turn) * LN2).astype(BF16)
                d_ref[piece, :, width + at : width + at + HD] = both[:, HD:].astype(BF16)
            return carry

        lax.fori_loop(0, d_ref.shape[0], finish, 0)


def attend_back_heads(bounds, q_ext, k_ext, v_ext, sums, dout, turn, align=128):
    heads, length, lanes = q_ext.shape
    count_blocks = dout.shape[0]
    rows, width = length // count_blocks, heads * HD
    low, count = windows(bounds, length, align, align)
    whole = pl.BlockSpec((heads, length, lanes), lambda i, *_: (0, 0, 0))
    part = pl.BlockSpec((heads, rows, lanes), lambda i, *_: (0, i, 0))
    return pl.pallas_call(
        functools.partial(attend_back_kernel, align),
        out_shape=jax.ShapeDtypeStruct((count_blocks, rows, 3 * width), BF16),
        grid_spec=pltpu.PrefetchScalarGridSpec(
            num_scalar_prefetch=2,
            grid=(count_blocks,),
            in_specs=[
                part,
                part,
                pl.BlockSpec((1,) + dout.shape[1:], lambda i, *_: (i, 0, 0)),
                pl.BlockSpec((length, lanes), lambda i, *_: (0, 0)),
                whole,
                whole,
            ],
            out_specs=pl.BlockSpec((count_blocks, rows, 3 * width), lambda i, *_: (0, 0, 0)),
            scratch_shapes=[
                pltpu.VMEM((heads, rows, lanes), F32),
                pltpu.VMEM((heads, 2 * HD, length), F32),
                pltpu.VMEM((heads, rows, lanes), BF16),
                pltpu.VMEM((heads, HD, rows), BF16),
                pltpu.VMEM((heads, HD, rows), BF16),
            ],
        ),
        compiler_params=pltpu.CompilerParams(vmem_limit_bytes=VMEM_LIMIT),
        cost_estimate=pl.CostEstimate(
            flops=heads * length * length * 10 * lanes // 2,
            bytes_accessed=heads * length * lanes * 20,
            transcendentals=heads * length * length // 2,
        ),
        name="attend_back_heads",
    )(low, count, q_ext, sums, dout, turn, k_ext, v_ext)


def scatter_kernel(
    chunks,
    by_z,
    d_hbm,
    x_hbm,
    w_ref,
    dh_hbm,
    norm_ref,
    out_hbm,
    gw_all_ref,
    norm_out_ref,
    d_ref,
    x_ref,
    part_ref,
    gw_sum,
    gw_ref,
    dh_ref,
    out_ref,
    got_y,
    got_z,
    relay_y,
    relay_z,
    sent_y,
    sent_z,
    cross_out,
    cross_in,
    gw_got,
    gw_mine,
    gw_pair,
    gw_final,
    norm_got,
    norm_sent,
    send,
    recv,
    gw_send,
    gw_recv,
    norm_send,
    norm_recv,
    kept,
):
    me = lax.axis_index("seq")
    shard = lax.axis_index("shard")
    shards = gw_ref.shape[0]
    half = lax.div(me, GROUPS)
    y_near, z_near, partner = flip(me, 1), flip(me, 2), flip(me, 4)
    corner = flip(y_near, 2)
    barrier = pltpu.get_barrier_semaphore()
    for n in range(1, SEQ_SIZE):
        pl.semaphore_signal(
            barrier, inc=1, device_id={"seq": lax.rem(me + n, SEQ_SIZE)}, device_id_type=BY_MESH
        )
    for step in range(1, shards):
        pl.semaphore_signal(
            barrier, inc=1, device_id={"shard": lax.rem(shard + step, shards)}, device_id_type=BY_MESH
        )
    pl.semaphore_wait(barrier, SEQ_SIZE + shards - 2)

    started = []

    def go(source, target, sends, receives, slot, where):
        copy = pltpu.make_async_remote_copy(
            src_ref=source,
            dst_ref=target,
            send_sem=sends.at[slot],
            recv_sem=receives.at[slot],
            device_id=where,
            device_id_type=BY_MESH,
        )
        copy.start()
        started.append(copy)
        return copy

    rows = part_ref.shape[1] // chunks

    def band(chunk):
        return pl.ds(chunk * rows, rows)

    def piece(device, far):
        return flip(device, 4) if far else device

    def slot(kind, far, chunk):
        return (kind * 2 + (0 if far else 1)) * chunks + chunk

    def other(mask):
        index = 0
        for bit in (1, 2, 4):
            here, there = lax.rem(lax.div(me, bit), 2), lax.rem(lax.div(mask, bit), 2)
            index = index + bit * (here + there - 2 * here * there)
        return index

    masks = (7, 6, 5, 3, 2, 1, 4, 0)

    def fetch(mask, place):
        return pltpu.make_async_copy(d_hbm.at[other(mask)], d_ref.at[other(mask)], kept.at[8 + place])

    for place, mask in enumerate(masks):
        fetch(mask, place).start()
    loads = [
        pltpu.make_async_copy(dh_hbm, dh_ref, kept.at[4]),
        pltpu.make_async_copy(x_hbm, x_ref, kept.at[5]),
    ]
    for copy in loads:
        copy.start()

    def project(count, first, place):
        def body(n, carry):
            mask = first(n)
            fetch(mask, place + n).wait()
            index = other(mask)
            part_ref[index] = lax.dot_general(
                d_ref[index], w_ref[...], BY_LANES, preferred_element_type=F32
            ).astype(BF16)
            return carry

        lax.fori_loop(0, count, body, 0)

    norm_seq = [
        go(norm_ref, norm_got.at[n], norm_send, norm_recv, n, {"seq": lax.rem(me + n + 1, SEQ_SIZE)})
        for n in range(SEQ_SIZE - 1)
    ]

    from_corner, direct = {}, {}

    def send_pieces(far):
        for chunk in range(chunks):
            over_z = chunk < by_z
            from_corner[far, chunk] = go(
                part_ref.at[piece(corner, far), band(chunk)],
                (relay_y if over_z else relay_z).at[0 if far else 1, chunk if over_z else chunk - by_z],
                send,
                recv,
                slot(0, far, chunk),
                {"seq": y_near if over_z else z_near},
            )
        for chunk in range(chunks):
            over_z = chunk < by_z
            direct[far, chunk] = go(
                part_ref.at[piece(y_near if over_z else z_near, far), band(chunk)],
                (got_y if over_z else got_z).at[0 if far else 1, band(chunk)],
                send,
                recv,
                slot(1 if over_z else 2, far, chunk),
                {"seq": y_near if over_z else z_near},
            )

    project(3, lambda n: 7 - n, 0)
    send_pieces(True)
    project(3, lambda n: 3 - n, 3)
    project(2, lambda n: 4 - 4 * n, 6)
    relayed = {}

    def relay(far, chunk):
        over_z = chunk < by_z
        target = z_near if over_z else y_near
        index = chunk if over_z else chunk - by_z
        which = 0 if far else 1
        from_corner[far, chunk].wait_recv()
        source = relay_y if over_z else relay_z
        buffer = sent_y if over_z else sent_z
        passed = part_ref[piece(target, far), band(chunk)].astype(F32)
        buffer[which, index] = (source[which, index].astype(F32) + passed).astype(BF16)
        relayed[far, chunk] = go(
            buffer.at[which, index],
            (got_z if over_z else got_y).at[which, band(chunk)],
            send,
            recv,
            slot(2 if over_z else 1, far, chunk),
            {"seq": target},
        )

    def total(far, chunk):
        which = 0 if far else 1
        direct[far, chunk].wait_recv()
        relayed[far, chunk].wait_recv()
        return part_ref[piece(me, far), band(chunk)].astype(F32) + got_y[which, band(chunk)].astype(F32) + got_z[which, band(chunk)].astype(F32)

    for chunk in range(chunks):
        relay(True, chunk)
    send_pieces(False)
    for copy in loads:
        copy.wait()
    gw_sum[...] = jnp.zeros_like(gw_sum)

    def grow(n, carry):
        gw_sum[...] += lax.dot_general(
            x_ref[n], d_ref[n], (((0,), (0,)), ((), ())), preferred_element_type=F32
        )
        return carry

    lax.fori_loop(0, d_ref.shape[0], grow, 0)
    depth = gw_ref.shape[1]
    for owner in range(shards):
        gw_ref[owner] = gw_sum[owner * depth : (owner + 1) * depth, :].astype(BF16)
    gw_one = [
        go(
            gw_ref.at[lax.rem(shard + step, shards)],
            gw_got.at[step - 1],
            gw_send,
            gw_recv,
            step - 1,
            {"shard": lax.rem(shard + step, shards)},
        )
        for step in range(1, shards)
    ]
    norm_total = norm_ref[...]
    for n, copy in enumerate(norm_seq):
        copy.wait_recv()
        norm_total = norm_total + norm_got[n]
    norm_sent[...] = norm_total
    for copy in gw_one:
        copy.wait_recv()
    summed = gw_ref[shard].astype(F32)
    for step in range(1, shards):
        summed = summed + gw_got[step - 1].astype(F32)
    gw_mine[...] = summed.astype(BF16)
    gw_two = go(gw_mine, gw_pair, gw_send, gw_recv, shards - 1, {"seq": partner})
    norm_shard = [
        go(
            norm_sent,
            norm_got.at[SEQ_SIZE - 2 + step],
            norm_send,
            norm_recv,
            SEQ_SIZE - 2 + step,
            {"shard": lax.rem(shard + step, shards)},
        )
        for step in range(1, shards)
    ]
    crossing = []
    for chunk in range(chunks):
        cross_out[band(chunk)] = total(True, chunk).astype(BF16)
        crossing.append(
            go(cross_out.at[band(chunk)], cross_in.at[band(chunk)], send, recv, slot(3, True, chunk), {"seq": partner})
        )
    for chunk in range(chunks):
        relay(False, chunk)
    gw_two.wait_recv()
    gw_final[...] = (gw_mine[...].astype(F32) + gw_pair[...].astype(F32)).astype(BF16)
    group = lax.rem(me, GROUPS)
    gw_three = [
        go(gw_final, gw_all_ref.at[group], gw_send, gw_recv, shards + n, {"seq": device})
        for n, device in enumerate((y_near, z_near, corner))
    ]
    keep = pltpu.make_async_copy(gw_final, gw_all_ref.at[group], kept.at[0])
    keep.start()
    for chunk in range(chunks):
        out_ref[0, band(chunk)] = (total(False, chunk) + dh_ref[half, band(chunk)]).astype(BF16)
    out_near = pltpu.make_async_copy(out_ref.at[0], out_hbm.at[half], kept.at[2])
    out_near.start()
    norm_total = norm_sent[...]
    for step, copy in enumerate(norm_shard):
        copy.wait_recv()
        norm_total = norm_total + norm_got[SEQ_SIZE - 1 + step]
    norm_out_ref[...] = norm_total
    for chunk in range(chunks):
        crossing[chunk].wait_recv()
        other = 1 - half
        out_ref[1, band(chunk)] = (cross_in[band(chunk)].astype(F32) + dh_ref[other, band(chunk)]).astype(BF16)
    out_far = pltpu.make_async_copy(out_ref.at[1], out_hbm.at[1 - half], kept.at[3])
    out_far.start()
    for copy in gw_three:
        copy.wait_recv()
    keep.wait()
    out_near.wait()
    out_far.wait()
    for copy in started:
        copy.wait_send()


def scatter_gradients(d_heads, pieces, w_own, dh_one, norms, shards, chunks=4, by_z=3):
    _, rows, width = pieces.shape
    columns = d_heads.shape[2]
    depth = width // shards
    part = rows // chunks
    hbm = pl.BlockSpec(memory_space=pltpu.HBM)
    vmem = pl.BlockSpec(memory_space=pltpu.VMEM)
    dma = pltpu.SemaphoreType.DMA
    return pl.pallas_call(
        functools.partial(scatter_kernel, chunks, by_z),
        out_shape=(
            jax.ShapeDtypeStruct(dh_one.shape, BF16),
            jax.ShapeDtypeStruct((GROUPS, depth, columns), BF16),
            jax.ShapeDtypeStruct(norms.shape, F32),
        ),
        in_specs=[hbm, hbm, vmem, hbm, vmem],
        out_specs=(hbm, vmem, vmem),
        scratch_shapes=[
            pltpu.VMEM(d_heads.shape, BF16),
            pltpu.VMEM(pieces.shape, BF16),
            pltpu.VMEM(pieces.shape, BF16),
            pltpu.VMEM((width, columns), F32),
            pltpu.VMEM((shards, depth, columns), BF16),
            pltpu.VMEM(dh_one.shape, F32),
            pltpu.VMEM((2, rows, width), BF16),
            pltpu.VMEM((2, rows, width), BF16),
            pltpu.VMEM((2, rows, width), BF16),
            pltpu.VMEM((2, by_z, part, width), BF16),
            pltpu.VMEM((2, chunks - by_z, part, width), BF16),
            pltpu.VMEM((2, by_z, part, width), BF16),
            pltpu.VMEM((2, chunks - by_z, part, width), BF16),
            pltpu.VMEM((rows, width), BF16),
            pltpu.VMEM((rows, width), BF16),
            pltpu.VMEM((shards - 1, depth, columns), BF16),
            pltpu.VMEM((depth, columns), BF16),
            pltpu.VMEM((depth, columns), BF16),
            pltpu.VMEM((depth, columns), BF16),
            pltpu.VMEM((SEQ_SIZE + shards - 2,) + norms.shape, F32),
            pltpu.VMEM(norms.shape, F32),
            dma((7 * chunks,)),
            dma((7 * chunks,)),
            dma((shards + 3,)),
            dma((shards + 3,)),
            dma((SEQ_SIZE + shards - 2,)),
            dma((SEQ_SIZE + shards - 2,)),
            dma((8 + SEQ_SIZE,)),
        ],
        compiler_params=pltpu.CompilerParams(
            collective_id=2, has_side_effects=True, vmem_limit_bytes=VMEM_LIMIT
        ),
        cost_estimate=pl.CostEstimate(flops=60 * 10**9, bytes_accessed=64 * 2**20, transcendentals=0),
        name="scatter_gradients",
    )(d_heads, pieces, w_own, dh_one, norms)


def padded_rows(blocks, depth):
    return pl.cdiv((3 * blocks + 1) * depth, SEQ_SIZE * 16) * SEQ_SIZE * 16


def feed_forward_kernel(
    tokens_ref,
    joined_ref,
    cot_ref,
    out_hbm,
    gate_hbm,
    up_hbm,
    down_hbm,
    norms_ref,
    output_ref,
    dout_ref,
    dh_ref,
    norm_sums_ref,
    packed_ref,
    w_out,
    w_gate,
    w_up,
    w_down,
    flow,
    hat_one,
    inverse_one,
    x_low,
    x_turned,
    dm_low,
    gate_kept,
    up_kept,
    d_gate,
    d_up,
    hidden_kept,
    staged,
    loads,
    stores,
):
    seqs, rows, width = dh_ref.shape
    shards = packed_ref.shape[0]
    depth = width // shards
    blocks = gate_hbm.shape[1] // width
    weights = ((out_hbm, w_out), (gate_hbm, w_gate), (up_hbm, w_up), (down_hbm, w_down))
    fetch = [pltpu.make_async_copy(src, dst, loads.at[n]) for n, (src, dst) in enumerate(weights)]
    tokens_in = pltpu.make_async_copy(tokens_ref, flow, loads.at[4])
    tokens_in.start()
    for copy in fetch:
        copy.start()
    gain_one, bias_one, gain_two, bias_two = (norms_ref[n : n + 1, :] for n in range(4))

    def mean(value):
        return jnp.sum(value, axis=-1, keepdims=True) * (1.0 / width)

    fetch[0].wait()
    tokens_in.wait()
    for seq in range(seqs):
        h_one = flow[seq].astype(F32)
        for group in range(GROUPS):
            h_one = h_one + jnp.dot(
                unpack_heads(joined_ref[seq * GROUPS + group]),
                w_out[group * depth : (group + 1) * depth, :],
                preferred_element_type=F32,
            )
        centered = h_one - mean(h_one)
        inverse = lax.rsqrt(mean(centered * centered) + EPS)
        normed = centered * inverse
        hat_one[seq] = normed
        inverse_one[seq] = inverse
        x_one = normed * gain_one + bias_one
        dh_ref[seq] = x_one
        x_low[seq] = x_one.astype(BF16)
        x_turned[:, seq * rows : (seq + 1) * rows] = jnp.transpose(x_one).astype(BF16)
    cot_in = pltpu.make_async_copy(cot_ref, flow, loads.at[4])
    cot_in.start()
    for copy in fetch[1:]:
        copy.wait()

    def forward(block, carry):
        at = pl.ds(pl.multiple_of(block * width, width), width)
        for seq in range(seqs):
            gate = jnp.dot(x_low[seq], w_gate[:, at], preferred_element_type=F32)
            up = jnp.dot(x_low[seq], w_up[:, at], preferred_element_type=F32)
            gate_kept[block, seq] = gate.astype(gate_kept.dtype)
            up_kept[block, seq] = up.astype(up_kept.dtype)
            hidden = (gate * jax.nn.sigmoid(gate) * up).astype(BF16)
            dh_ref[seq] += jnp.dot(hidden, w_down[at, :], preferred_element_type=F32)
        return carry

    lax.fori_loop(0, blocks, forward, 0)

    cot_in.wait()
    gain_two_sum = jnp.zeros((1, width), F32)
    bias_two_sum = jnp.zeros((1, width), F32)
    for seq in range(seqs):
        h_two = dh_ref[seq]
        centered = h_two - mean(h_two)
        inverse = lax.rsqrt(mean(centered * centered) + EPS)
        normed = centered * inverse
        cot = flow[seq].astype(F32)
        flow[seq] = (normed * gain_two + bias_two).astype(BF16)
        gain_two_sum = gain_two_sum + jnp.sum(cot * normed, axis=0, keepdims=True)
        bias_two_sum = bias_two_sum + jnp.sum(cot, axis=0, keepdims=True)
        scaled = cot * gain_two
        dh_two = inverse * (scaled - mean(scaled) - normed * mean(scaled * normed))
        dh_ref[seq] = dh_two
        dm_low[seq * rows : (seq + 1) * rows, :] = dh_two.astype(BF16)
    output_out = pltpu.make_async_copy(flow, output_ref, loads.at[4])
    output_out.start()

    def store(kind, block):
        if kind < 2:
            start = pl.multiple_of((kind * blocks + block) * depth, depth)
            return [
                pltpu.make_async_copy(
                    staged.at[kind, pl.ds(shard * depth, depth)],
                    packed_ref.at[shard, pl.ds(start, depth)],
                    stores.at[kind, shard],
                )
                for shard in range(shards)
            ]
        start = 2 * blocks * depth
        return [
            pltpu.make_async_copy(
                staged.at[2], packed_ref.at[block, pl.ds(start, width)], stores.at[2, 0]
            )
        ]

    def backward(block, carry):
        at = pl.ds(pl.multiple_of(block * width, width), width)
        for seq in range(seqs):
            here = slice(seq * rows, (seq + 1) * rows)
            d_hidden = lax.dot_general(dm_low[here, :], w_down[at, :], BY_LANES, preferred_element_type=F32)
            gate = gate_kept[block, seq].astype(F32)
            up = up_kept[block, seq].astype(F32)
            sigma = jax.nn.sigmoid(gate)
            smooth = gate * sigma
            hidden_kept[here, :] = (smooth * up).astype(BF16)
            dg = (d_hidden * up * (sigma + smooth * (1.0 - sigma))).astype(BF16)
            du = (d_hidden * smooth).astype(BF16)
            d_gate[here, :] = dg
            d_up[here, :] = du
            dh_ref[seq] += lax.dot_general(dg, w_gate[:, at], BY_LANES, preferred_element_type=F32)
            dh_ref[seq] += lax.dot_general(du, w_up[:, at], BY_LANES, preferred_element_type=F32)

        @pl.when(block > 0)
        def _():
            for kind in range(3):
                for copy in store(kind, block - 1):
                    copy.wait()

        staged[0] = jnp.dot(x_turned[...], d_gate[...], preferred_element_type=F32).astype(BF16)
        staged[1] = jnp.dot(x_turned[...], d_up[...], preferred_element_type=F32).astype(BF16)
        staged[2] = lax.dot_general(
            hidden_kept[...], dm_low[...], (((0,), (0,)), ((), ())), preferred_element_type=F32
        ).astype(BF16)
        for kind in range(3):
            for copy in store(kind, block):
                copy.start()
        return carry

    lax.fori_loop(0, blocks, backward, 0)

    gain_one_sum = jnp.zeros((1, width), F32)
    bias_one_sum = jnp.zeros((1, width), F32)
    for seq in range(seqs):
        here = slice(seq * rows, (seq + 1) * rows)
        dx_one = dh_ref[seq]
        normed = hat_one[seq]
        gain_one_sum = gain_one_sum + jnp.sum(dx_one * normed, axis=0, keepdims=True)
        bias_one_sum = bias_one_sum + jnp.sum(dx_one, axis=0, keepdims=True)
        scaled = dx_one * gain_one
        dh_one = inverse_one[seq] * (scaled - mean(scaled) - normed * mean(scaled * normed))
        dh_ref[seq] = dh_one
        d_attn = dh_one.astype(BF16)
        d_gate[here, :] = d_attn
        for group in range(GROUPS):
            dout = lax.dot_general(
                d_attn, w_out[group * depth : (group + 1) * depth, :], BY_LANES, preferred_element_type=F32
            )
            first, last = pack_heads(dout)
            dout_ref[seq * GROUPS + group, :rows] = first.astype(BF16)
            dout_ref[seq * GROUPS + group, rows:] = last.astype(BF16)
    for kind in range(3):
        for copy in store(kind, blocks - 1):
            copy.wait()
    for group in range(GROUPS):
        grad = jnp.zeros((depth, width), F32)
        for seq in range(seqs):
            grad = grad + lax.dot_general(
                unpack_heads(joined_ref[seq * GROUPS + group]),
                d_gate[seq * rows : (seq + 1) * rows, :],
                (((0,), (0,)), ((), ())),
                preferred_element_type=F32,
            )
        staged[0, group * depth : (group + 1) * depth, :] = grad.astype(BF16)
    last = [
        pltpu.make_async_copy(
            staged.at[0, pl.ds(shard * depth, depth)],
            packed_ref.at[shard, pl.ds(3 * blocks * depth, depth)],
            stores.at[0, shard],
        )
        for shard in range(shards)
    ]
    used = (3 * blocks + 1) * depth
    rest = packed_ref.shape[1] - used
    staged[1, :rest, :] = jnp.zeros((rest, width), BF16)
    last += [
        pltpu.make_async_copy(
            staged.at[1, pl.ds(0, rest)], packed_ref.at[shard, pl.ds(used, rest)], stores.at[1, shard]
        )
        for shard in range(shards)
    ]
    for copy in last:
        copy.start()
    norm_sums_ref[0:1, :] = gain_one_sum
    norm_sums_ref[1:2, :] = bias_one_sum
    norm_sums_ref[2:3, :] = gain_two_sum
    norm_sums_ref[3:4, :] = bias_two_sum
    for copy in last:
        copy.wait()
    output_out.wait()


def feed_forward(tokens, joined, cotangent, w_out, w_gate, w_up, w_down, norms, kept=BF16):
    seqs, rows, width = tokens.shape
    total = seqs * rows
    hidden = w_gate.shape[1]
    blocks = hidden // width
    depth = width // GROUPS
    vmem = pl.BlockSpec(memory_space=pltpu.VMEM)
    hbm = pl.BlockSpec(memory_space=pltpu.HBM)
    dma = pltpu.SemaphoreType.DMA
    return pl.pallas_call(
        feed_forward_kernel,
        out_shape=(
            jax.ShapeDtypeStruct(tokens.shape, BF16),
            jax.ShapeDtypeStruct(joined.shape, BF16),
            jax.ShapeDtypeStruct(tokens.shape, F32),
            jax.ShapeDtypeStruct((4, width), F32),
            jax.ShapeDtypeStruct((GROUPS, padded_rows(blocks, depth), width), BF16),
        ),
        in_specs=[hbm, vmem, hbm, hbm, hbm, hbm, hbm, vmem],
        out_specs=(hbm, vmem, vmem, vmem, hbm),
        scratch_shapes=[
            pltpu.VMEM(w_out.shape, BF16),
            pltpu.VMEM(w_gate.shape, BF16),
            pltpu.VMEM(w_up.shape, BF16),
            pltpu.VMEM(w_down.shape, BF16),
            pltpu.VMEM(tokens.shape, BF16),
            pltpu.VMEM(tokens.shape, F32),
            pltpu.VMEM((seqs, rows, 1), F32),
            pltpu.VMEM(tokens.shape, BF16),
            pltpu.VMEM((width, total), BF16),
            pltpu.VMEM((total, width), BF16),
            pltpu.VMEM((blocks, seqs, rows, width), kept),
            pltpu.VMEM((blocks, seqs, rows, width), kept),
            pltpu.VMEM((total, width), BF16),
            pltpu.VMEM((total, width), BF16),
            pltpu.VMEM((total, width), BF16),
            pltpu.VMEM((3, width, width), BF16),
            dma((5,)),
            dma((3, GROUPS)),
        ],
        compiler_params=pltpu.CompilerParams(vmem_limit_bytes=FEED_LIMIT),
        cost_estimate=pl.CostEstimate(
            flops=6 * total * width * (3 * hidden + width),
            bytes_accessed=2 * 2 * (3 * hidden + width) * width + 20 * total * width,
            transcendentals=2 * total * hidden,
        ),
        name="feed_forward",
    )(tokens, joined, cotangent, w_out, w_gate, w_up, w_down, norms)


def gather_rows_kernel(chunks, by_z, own_ref, rows_ref, send, recv, kept):
    me = lax.axis_index("seq")
    y_near, z_near, partner = flip(me, 1), flip(me, 2), flip(me, 4)
    barrier = pltpu.get_barrier_semaphore()
    for device in (y_near, z_near, partner):
        pl.semaphore_signal(barrier, inc=1, device_id={"seq": device}, device_id_type=BY_MESH)
    pl.semaphore_wait(barrier, 3)
    count = own_ref.shape[0]
    part = count // chunks
    started = []

    def go(source, target, slot, device):
        copy = pltpu.make_async_remote_copy(
            src_ref=source,
            dst_ref=target,
            send_sem=send.at[slot],
            recv_sem=recv.at[slot],
            device_id={"seq": device},
            device_id_type=BY_MESH,
        )
        copy.start()
        started.append(copy)
        return copy

    def band(device, chunk):
        return rows_ref.at[pl.ds(device * count + chunk * part, part)]

    def own(chunk, slot, device):
        return go(own_ref.at[pl.ds(chunk * part, part)], band(me, chunk), slot * chunks + chunk, device)

    def relay(device, chunk, slot, target):
        return go(band(device, chunk), band(device, chunk), slot * chunks + chunk, target)

    crossing = [own(chunk, 0, partner) for chunk in range(chunks)]
    own_y, own_z = [], []
    for chunk in range(chunks):
        own_y.append(own(chunk, 1, y_near))
        own_z.append(own(chunk, 2, z_near))
    keep = pltpu.make_async_copy(own_ref, rows_ref.at[pl.ds(me * count, count)], kept)
    keep.start()
    cross_y, cross_z, corner = [], [], []
    for chunk in range(chunks):
        own_y[chunk].wait_recv()
        if chunk < by_z:
            corner.append(relay(y_near, chunk, 5, z_near))
        own_z[chunk].wait_recv()
        if chunk >= by_z:
            corner.append(relay(z_near, chunk, 5, y_near))
        crossing[chunk].wait_recv()
        cross_y.append(relay(partner, chunk, 3, y_near))
        cross_z.append(relay(partner, chunk, 4, z_near))
    for chunk in range(chunks):
        cross_y[chunk].wait_recv()
        if chunk < by_z:
            corner.append(relay(flip(y_near, 4), chunk, 6, z_near))
        cross_z[chunk].wait_recv()
        if chunk >= by_z:
            corner.append(relay(flip(z_near, 4), chunk, 6, y_near))
    for copy in corner:
        copy.wait_recv()
    keep.wait()
    for copy in started:
        copy.wait_send()


def gather_rows(owned, chunks=8, by_z=3):
    hbm = pl.BlockSpec(memory_space=pltpu.HBM)
    dma = pltpu.SemaphoreType.DMA
    return pl.pallas_call(
        functools.partial(gather_rows_kernel, chunks, by_z),
        out_shape=jax.ShapeDtypeStruct((SEQ_SIZE * owned.shape[0], owned.shape[1]), BF16),
        in_specs=[hbm],
        out_specs=hbm,
        scratch_shapes=[dma((7 * chunks,)), dma((7 * chunks,)), dma],
        compiler_params=pltpu.CompilerParams(collective_id=5, has_side_effects=True),
        name="gather_rows",
    )(owned)


def unpack_kernel(gate_rows, up_rows, down_rows, out_rows, columns, gate_ref, up_ref, down_ref, out_ref, qkv_ref):
    gate_ref[...] = gate_rows[...].astype(F32)
    up_ref[...] = up_rows[...].astype(F32)
    down_ref[...] = down_rows[...].astype(F32)

    @pl.when(pl.program_id(0) == 0)
    def _():
        out_ref[...] = out_rows[...].astype(F32)
        groups, _, width = columns.shape
        width = width // 3
        for group in range(groups):
            for part in range(3):
                at = (part * groups + group) * width
                qkv_ref[:, at : at + width] = columns[group, :, part * width : (part + 1) * width].astype(F32)


def unpack_gradients(rows, columns, blocks):
    groups, depth, thirds = columns.shape
    width = rows.shape[1]
    piece = [
        pl.BlockSpec((depth, width), lambda i, first=first, step=step: (first + step * i, 0))
        for first, step in ((0, 1), (blocks, 1), (2 * blocks, 1), (3 * blocks, 0))
    ]
    return pl.pallas_call(
        unpack_kernel,
        out_shape=(
            jax.ShapeDtypeStruct((depth, blocks * width), F32),
            jax.ShapeDtypeStruct((depth, blocks * width), F32),
            jax.ShapeDtypeStruct((blocks * depth, width), F32),
            jax.ShapeDtypeStruct((depth, width), F32),
            jax.ShapeDtypeStruct((depth, groups * thirds), F32),
        ),
        grid=(blocks,),
        in_specs=piece + [pl.BlockSpec(columns.shape, lambda i: (0, 0, 0))],
        out_specs=(
            pl.BlockSpec((depth, width), lambda i: (0, i)),
            pl.BlockSpec((depth, width), lambda i: (0, i)),
            pl.BlockSpec((depth, width), lambda i: (i, 0)),
            pl.BlockSpec((depth, width), lambda i: (0, 0)),
            pl.BlockSpec((depth, groups * thirds), lambda i: (0, 0)),
        ),
        name="unpack_gradients",
    )(rows, rows, rows, rows, columns)


def document_places(seg_row):
    length = seg_row.shape[0]
    ids = jnp.arange(LANES - HD, dtype=jnp.int32)[:, None]
    starts = jnp.sum((seg_row[None, :] < ids).astype(jnp.int32), axis=1, keepdims=True)
    start = jnp.sum(jnp.where(seg_row[None, :] == ids, starts, 0), axis=0)
    return jnp.arange(length, dtype=jnp.int32) - start


def exchange_kernel(sent_ref, taken_ref, send, recv, kept):
    me = lax.axis_index("seq")
    barrier = pltpu.get_barrier_semaphore()
    others = [lax.rem(me + step, SEQ_SIZE) for step in range(1, SEQ_SIZE)]
    for device in others:
        pl.semaphore_signal(barrier, inc=1, device_id={"seq": device}, device_id_type=BY_MESH)
    pl.semaphore_wait(barrier, SEQ_SIZE - 1)
    copies = []
    for step, device in enumerate(others):
        copy = pltpu.make_async_remote_copy(
            src_ref=sent_ref.at[device],
            dst_ref=taken_ref.at[me],
            send_sem=send.at[step],
            recv_sem=recv.at[step],
            device_id={"seq": device},
            device_id_type=BY_MESH,
        )
        copy.start()
        copies.append(copy)
    keep = pltpu.make_async_copy(sent_ref.at[me], taken_ref.at[me], kept)
    keep.start()
    keep.wait()
    for copy in copies:
        copy.wait()


def exchange(blocks, collective_id):
    hbm = pl.BlockSpec(memory_space=pltpu.HBM)
    dma = pltpu.SemaphoreType.DMA
    return pl.pallas_call(
        exchange_kernel,
        out_shape=jax.ShapeDtypeStruct(blocks.shape, blocks.dtype),
        in_specs=[hbm],
        out_specs=hbm,
        scratch_shapes=[dma((SEQ_SIZE - 1,)), dma((SEQ_SIZE - 1,)), dma],
        compiler_params=pltpu.CompilerParams(collective_id=collective_id, has_side_effects=True),
        name="exchange",
    )(blocks)


def head_columns(w_qkv, group, held):
    depth = w_qkv.shape[0]
    split = w_qkv.reshape(depth, 3, GROUPS, held, HD)
    mine = lax.dynamic_index_in_dim(split, group, 2, keepdims=False)
    second = mine * jnp.array([1, 1, 0], w_qkv.dtype)[None, :, None, None]
    return jnp.concatenate([mine, second], axis=-1).reshape(depth, 3 * held * 2 * HD)


def local_heads(
    shards,
    tokens,
    segments,
    positions,
    cotangent,
    w_qkv,
    w_out,
    w_gate,
    w_up,
    w_down,
    ln1_gain,
    ln1_bias,
    ln2_gain,
    ln2_bias,
):
    seq_count, row_count, model_width = tokens.shape
    held = HEADS // GROUPS
    length = row_count * SEQ_SIZE
    me = lax.axis_index("seq")
    seg_row = lax.dynamic_index_in_dim(segments, me // GROUPS, 0, keepdims=False)

    def gather(shard):
        return lax.all_gather(shard, "shard", axis=0, tiled=True)

    freqs = jnp.exp(jnp.arange(HD // 2, dtype=F32) * (-math.log(ROPE_BASE) / (HD // 2)))
    freq = jnp.tile(freqs, LANES // (HD // 2))[None]
    place = document_places(seg_row).astype(F32).reshape(SEQ_SIZE, 1, row_count)
    norm_rows = jnp.stack([ln1_gain, ln1_bias, ln2_gain, ln2_bias]).astype(F32)
    pieces, w_heads, norms, turn = gather_tokens(
        tokens, head_columns(w_qkv, me % GROUPS, held), norm_rows, place, freq, shards
    )
    norms = jnp.transpose(norms, (1, 0, 2)).reshape(4, model_width)
    full_out, full_gate, full_up, full_down = (gather(w) for w in (w_out, w_gate, w_up, w_down))
    bounds = document_bounds(seg_row, row_count)
    q_ext, k_ext, v_ext = project_heads(
        seg_row.astype(F32), turn, pieces, w_heads.reshape(model_width, -1), held
    )
    sums, joined_own = attend_heads(bounds, q_ext, k_ext, v_ext, row_count)
    output, d_joined, dh_one, norms_part, packed = feed_forward(
        tokens, exchange(joined_own, 3), cotangent, full_out, full_gate, full_up, full_down, norms
    )
    depth = model_width // shards
    ff_blocks = full_gate.shape[1] // model_width
    owned = lax.psum_scatter(
        packed.reshape(-1, model_width), ("shard", "seq"), scatter_dimension=0, tiled=True
    )

    dout = exchange(d_joined, 4)
    d_heads = attend_back_heads(bounds, q_ext, k_ext, v_ext, sums, dout, turn)
    w_lanes = w_heads.reshape(model_width, -1)
    w_own = jnp.concatenate(
        [w_lanes[:, at : at + HD] for at in range(0, w_lanes.shape[1], LANES)], axis=1
    )
    input_grad, columns, norm_sums = scatter_gradients(d_heads, pieces, w_own, dh_one, norms_part, shards)
    columns, owned = lax.optimization_barrier((columns, owned))
    shared = gather_rows(owned)
    grad_gate, grad_up, grad_down, grad_out, grad_qkv = unpack_gradients(shared, columns, ff_blocks)
    shard = lax.axis_index("shard")
    norm_sums = lax.dynamic_slice_in_dim(norm_sums, shard * depth, depth, 1)
    return (
        output,
        input_grad,
        grad_qkv,
        grad_out,
        grad_gate,
        grad_up,
        grad_down,
        norm_sums[0],
        norm_sums[1],
        norm_sums[2],
        norm_sums[3],
    )


def solution(mesh):
    in_specs = (
        P("shard", "seq", None),
        P("shard", None),
        P("shard", "seq"),
        P("shard", "seq", None),
        P("shard", None),
        P("shard", None),
        P("shard", None),
        P("shard", None),
        P("shard", None),
        P("shard"),
        P("shard"),
        P("shard"),
        P("shard"),
    )
    out_specs = (
        P("shard", "seq", None),
        P("shard", "seq", None),
        P("shard", None),
        P("shard", None),
        P("shard", None),
        P("shard", None),
        P("shard", None),
        P("shard"),
        P("shard"),
        P("shard"),
        P("shard"),
    )
    body = functools.partial(local_heads, mesh.shape["shard"]) if (mesh.shape["seq"], mesh.shape["shard"]) == (SEQ_SIZE, GROUPS) else local
    return jax.shard_map(body, mesh=mesh, in_specs=in_specs, out_specs=out_specs, check_vma=False)
```

```python
import functools
import math

import jax
import jax.numpy as jnp
from jax import lax
from jax.experimental import pallas as pl
from jax.experimental.pallas import tpu as pltpu
from jax.sharding import PartitionSpec as P

HEADS = 12
HD = 64


EPS = 1e-05
ROPE_BASE = 1000.0


def rope_tables(pos_block):
    half_dim = HD // 2
    freqs = jnp.exp(jnp.arange(half_dim, dtype=jnp.float32) * (-math.log(ROPE_BASE) / half_dim))
    angle = pos_block.astype(jnp.float32)[..., None] * freqs
    return (jnp.cos(angle)[:, :, None, :], jnp.sin(angle)[:, :, None, :])


def rotate(heads, cos_b, sin_b):
    half_dim = heads.shape[-1] // 2
    first = heads[..., :half_dim]
    second = heads[..., half_dim:]
    return jnp.concatenate(
        [first * cos_b - second * sin_b, second * cos_b + first * sin_b], axis=-1
    )


def rotate_back(grads, cos_b, sin_b):
    half_dim = grads.shape[-1] // 2
    first = grads[..., :half_dim]
    second = grads[..., half_dim:]
    return jnp.concatenate(
        [first * cos_b + second * sin_b, second * cos_b - first * sin_b], axis=-1
    )


def norm_fwd(values, gain, bias):
    mean_val = jnp.mean(values, axis=-1, keepdims=True)
    centered = values - mean_val
    variance = jnp.mean(centered * centered, axis=-1, keepdims=True)
    inverse = lax.rsqrt(variance + EPS)
    normed = centered * inverse
    return (normed * gain + bias, normed, inverse)


def norm_back(grad_in, normed, inverse, gain):
    scaled = grad_in * gain
    return inverse * (
        scaled
        - jnp.mean(scaled, axis=-1, keepdims=True)
        - normed * jnp.mean(scaled * normed, axis=-1, keepdims=True)
    )


def head_split(block_rows, seq_count, row_count):
    return block_rows.reshape(seq_count, row_count, HEADS, HD)


def attend(q_heads, q_seg, k_full, v_full, seg_all, block, score_scale):
    seq_count, row_count = (q_heads.shape[0], q_heads.shape[1])
    block_count = k_full.shape[1] // block

    def attend_step(carry, index):
        row_total, value_sum = carry
        start = index * block
        k_part = head_split(lax.dynamic_slice_in_dim(k_full, start, block, 1), seq_count, block)
        v_part = head_split(lax.dynamic_slice_in_dim(v_full, start, block, 1), seq_count, block)
        seg_part = lax.dynamic_slice_in_dim(seg_all, start, block, 1)
        raw = (
            jnp.einsum("sqhd,skhd->shqk", q_heads, k_part, preferred_element_type=jnp.float32)
            * score_scale
        )
        same_doc = q_seg[:, None, :, None] == seg_part[:, None, None, :]
        expo = jnp.where(same_doc, jnp.exp(raw), 0.0)
        row_total = row_total + jnp.sum(expo, axis=-1)
        value_sum = value_sum + jnp.einsum(
            "shqk,skhd->sqhd", expo.astype(jnp.bfloat16), v_part, preferred_element_type=jnp.float32
        )
        return ((row_total, value_sum), None)

    start_carry = (
        jnp.zeros((seq_count, HEADS, row_count), jnp.float32),
        jnp.zeros((seq_count, row_count, HEADS, HD), jnp.float32),
    )
    final, unused = lax.scan(attend_step, start_carry, jnp.arange(block_count, dtype=jnp.int32))
    return final


def back_keys(q_heads, g_heads, delta, q_seg, k_full, v_full, seg_all, block, score_scale):
    seq_count, row_count = (q_heads.shape[0], q_heads.shape[1])
    full_len = k_full.shape[1]
    block_count = full_len // block

    def back_step(carry, index):
        start = index * block
        k_part = head_split(lax.dynamic_slice_in_dim(k_full, start, block, 1), seq_count, block)
        v_part = head_split(lax.dynamic_slice_in_dim(v_full, start, block, 1), seq_count, block)
        seg_part = lax.dynamic_slice_in_dim(seg_all, start, block, 1)
        raw = (
            jnp.einsum("sqhd,skhd->shqk", q_heads, k_part, preferred_element_type=jnp.float32)
            * score_scale
        )
        same_doc = q_seg[:, None, :, None] == seg_part[:, None, None, :]
        expo = jnp.where(same_doc, jnp.exp(raw), 0.0)
        prob_grad = jnp.einsum(
            "sqhd,skhd->shqk", g_heads, v_part, preferred_element_type=jnp.float32
        )
        d_score = (expo * (prob_grad - delta[..., None])).astype(jnp.bfloat16)
        q_grad = carry[0] + jnp.einsum(
            "shqk,skhd->sqhd", d_score, k_part, preferred_element_type=jnp.float32
        )
        k_grad = (
            jnp.einsum("shqk,sqhd->skhd", d_score, q_heads, preferred_element_type=jnp.float32)
            * score_scale
        )
        v_grad = jnp.einsum(
            "shqk,sqhd->skhd",
            expo.astype(jnp.bfloat16),
            g_heads,
            preferred_element_type=jnp.float32,
        )
        k_store = lax.dynamic_update_slice_in_dim(
            carry[1], k_grad.reshape(seq_count, block, HEADS * HD), start, 1
        )
        v_store = lax.dynamic_update_slice_in_dim(
            carry[2], v_grad.reshape(seq_count, block, HEADS * HD), start, 1
        )
        return ((q_grad, k_store, v_store), None)

    q_zero = jnp.zeros((seq_count, row_count, HEADS, HD), jnp.float32)
    kv_zero = jnp.zeros((seq_count, full_len, HEADS * HD), jnp.float32)
    start_carry = (q_zero, kv_zero, kv_zero)
    final, unused = lax.scan(back_step, start_carry, jnp.arange(block_count, dtype=jnp.int32))
    return (final[0] * score_scale,) + tuple(final[1:])


def local(
    tokens,
    segments,
    positions,
    cotangent,
    w_qkv,
    w_out,
    w_gate,
    w_up,
    w_down,
    ln1_gain,
    ln1_bias,
    ln2_gain,
    ln2_bias,
):
    seq_count, row_count, model_width = tokens.shape
    score_scale = HD ** (-0.5)
    q_seg = lax.dynamic_slice_in_dim(segments, lax.axis_index("seq") * row_count, row_count, 1)
    gathered = (
        lax.all_gather(w_qkv, "shard", axis=0, tiled=True),
        lax.all_gather(w_out, "shard", axis=0, tiled=True),
        lax.all_gather(w_gate, "shard", axis=0, tiled=True),
        lax.all_gather(w_up, "shard", axis=0, tiled=True),
        lax.all_gather(w_down, "shard", axis=0, tiled=True),
        lax.all_gather(ln1_gain, "shard", axis=0, tiled=True),
        lax.all_gather(ln1_bias, "shard", axis=0, tiled=True),
        lax.all_gather(ln2_gain, "shard", axis=0, tiled=True),
        lax.all_gather(ln2_bias, "shard", axis=0, tiled=True),
    )
    full_qkv, full_out, full_gate, full_up, full_down, gain_one, bias_one, gain_two, bias_two = (
        gathered
    )
    cos_b, sin_b = rope_tables(positions)
    qkv_all = jnp.einsum("scd,de->sce", tokens, full_qkv, preferred_element_type=jnp.float32)
    q_heads = rotate(
        head_split(qkv_all[..., :model_width], seq_count, row_count), cos_b, sin_b
    ).astype(jnp.bfloat16)
    k_heads = rotate(
        head_split(qkv_all[..., model_width : 2 * model_width], seq_count, row_count), cos_b, sin_b
    ).astype(jnp.bfloat16)
    v_heads = head_split(qkv_all[..., 2 * model_width :], seq_count, row_count).astype(jnp.bfloat16)
    k_local = k_heads.reshape(seq_count, row_count, model_width)
    v_local = v_heads.reshape(seq_count, row_count, model_width)
    k_full, v_full = (
        lax.all_gather(k_local, "seq", axis=1, tiled=True),
        lax.all_gather(v_local, "seq", axis=1, tiled=True),
    )
    row_total, value_sum = attend(q_heads, q_seg, k_full, v_full, segments, row_count, score_scale)
    denom = jnp.transpose(row_total, (0, 2, 1))[..., None]
    attn_out = value_sum / denom
    joined = attn_out.reshape(seq_count, row_count, model_width).astype(jnp.bfloat16)
    tokens_f = tokens.astype(jnp.float32)
    h_one = tokens_f + jnp.einsum(
        "sci,io->sco", joined, full_out, preferred_element_type=jnp.float32
    )
    x_one, normed_one, inverse_one = norm_fwd(
        h_one, gain_one.astype(jnp.float32), bias_one.astype(jnp.float32)
    )
    x_low = x_one.astype(jnp.bfloat16)
    gate_pre = jnp.einsum("scd,df->scf", x_low, full_gate, preferred_element_type=jnp.float32)
    up_pre = jnp.einsum("scd,df->scf", x_low, full_up, preferred_element_type=jnp.float32)
    sigma = jax.nn.sigmoid(gate_pre)
    smooth = gate_pre * sigma
    hidden = (smooth * up_pre).astype(jnp.bfloat16)
    h_two = x_one + jnp.einsum("scf,fd->scd", hidden, full_down, preferred_element_type=jnp.float32)
    result, normed_two, inverse_two = norm_fwd(
        h_two, gain_two.astype(jnp.float32), bias_two.astype(jnp.float32)
    )
    output = result.astype(jnp.bfloat16)
    regathered = (
        lax.all_gather(w_qkv, "shard", axis=0, tiled=True),
        lax.all_gather(w_out, "shard", axis=0, tiled=True),
        lax.all_gather(w_gate, "shard", axis=0, tiled=True),
        lax.all_gather(w_up, "shard", axis=0, tiled=True),
        lax.all_gather(w_down, "shard", axis=0, tiled=True),
        lax.all_gather(ln1_gain, "shard", axis=0, tiled=True),
        lax.all_gather(ln2_gain, "shard", axis=0, tiled=True),
    )
    back_qkv, back_out, back_gate, back_up, back_down, back_gain_one, back_gain_two = regathered
    back_k, back_v = (
        lax.all_gather(k_local, "seq", axis=1, tiled=True),
        lax.all_gather(v_local, "seq", axis=1, tiled=True),
    )
    cot_f = cotangent.astype(jnp.float32)
    grad_gain_two = jnp.sum(cot_f * normed_two, axis=(0, 1))
    grad_bias_two = jnp.sum(cot_f, axis=(0, 1))
    dh_two = norm_back(cot_f, normed_two, inverse_two, back_gain_two.astype(jnp.float32))
    dm_low = dh_two.astype(jnp.bfloat16)
    grad_down = jnp.einsum("scf,scd->fd", hidden, dm_low, preferred_element_type=jnp.float32)
    d_hidden = jnp.einsum("scd,fd->scf", dm_low, back_down, preferred_element_type=jnp.float32)
    d_up = (d_hidden * smooth).astype(jnp.bfloat16)
    d_gate = (d_hidden * up_pre * sigma * (1.0 + gate_pre * (1.0 - sigma))).astype(jnp.bfloat16)
    grad_gate = jnp.einsum("scd,scf->df", x_low, d_gate, preferred_element_type=jnp.float32)
    grad_up = jnp.einsum("scd,scf->df", x_low, d_up, preferred_element_type=jnp.float32)
    dx_one = (
        dh_two
        + jnp.einsum("scf,df->scd", d_gate, back_gate, preferred_element_type=jnp.float32)
        + jnp.einsum("scf,df->scd", d_up, back_up, preferred_element_type=jnp.float32)
    )
    grad_gain_one = jnp.sum(dx_one * normed_one, axis=(0, 1))
    grad_bias_one = jnp.sum(dx_one, axis=(0, 1))
    dh_one = norm_back(dx_one, normed_one, inverse_one, back_gain_one.astype(jnp.float32))
    d_attn = dh_one.astype(jnp.bfloat16)
    grad_out = jnp.einsum("sci,sco->io", joined, d_attn, preferred_element_type=jnp.float32)
    d_joined = jnp.einsum(
        "sco,io->sci", d_attn, back_out, preferred_element_type=jnp.float32
    ).astype(jnp.bfloat16)
    d_heads = head_split(d_joined, seq_count, row_count).astype(jnp.float32)
    g_heads = (d_heads / denom).astype(jnp.bfloat16)
    delta = jnp.transpose(jnp.sum(d_heads * attn_out, axis=-1) / denom[..., 0], (0, 2, 1))
    q_grad, k_all, v_all = back_keys(
        q_heads, g_heads, delta, q_seg, back_k, back_v, segments, row_count, score_scale
    )
    k_sum, v_sum = (
        lax.psum_scatter(k_all.astype(jnp.bfloat16), "seq", scatter_dimension=1, tiled=True).astype(
            jnp.float32
        ),
        lax.psum_scatter(v_all.astype(jnp.bfloat16), "seq", scatter_dimension=1, tiled=True).astype(
            jnp.float32
        ),
    )
    k_grad = head_split(k_sum, seq_count, row_count)
    v_grad = head_split(v_sum, seq_count, row_count)
    q_back = rotate_back(q_grad, cos_b, sin_b).reshape(seq_count, row_count, model_width)
    k_back = rotate_back(k_grad, cos_b, sin_b).reshape(seq_count, row_count, model_width)
    d_qkv = jnp.concatenate(
        [q_back, k_back, v_grad.reshape(seq_count, row_count, model_width)], axis=-1
    ).astype(jnp.bfloat16)
    grad_qkv = jnp.einsum("scd,sce->de", tokens, d_qkv, preferred_element_type=jnp.float32)
    d_tokens = dh_one + jnp.einsum(
        "sce,de->scd", d_qkv, back_qkv, preferred_element_type=jnp.float32
    )
    input_grad = d_tokens.astype(jnp.bfloat16)
    owned = (
        lax.psum_scatter(
            grad_qkv.astype(jnp.bfloat16), "shard", scatter_dimension=0, tiled=True
        ).astype(jnp.float32),
        lax.psum_scatter(
            grad_out.astype(jnp.bfloat16), "shard", scatter_dimension=0, tiled=True
        ).astype(jnp.float32),
        lax.psum_scatter(
            grad_gate.astype(jnp.bfloat16), "shard", scatter_dimension=0, tiled=True
        ).astype(jnp.float32),
        lax.psum_scatter(
            grad_up.astype(jnp.bfloat16), "shard", scatter_dimension=0, tiled=True
        ).astype(jnp.float32),
        lax.psum_scatter(
            grad_down.astype(jnp.bfloat16), "shard", scatter_dimension=0, tiled=True
        ).astype(jnp.float32),
        lax.psum_scatter(
            grad_gain_one.astype(jnp.bfloat16), "shard", scatter_dimension=0, tiled=True
        ).astype(jnp.float32),
        lax.psum_scatter(
            grad_bias_one.astype(jnp.bfloat16), "shard", scatter_dimension=0, tiled=True
        ).astype(jnp.float32),
        lax.psum_scatter(
            grad_gain_two.astype(jnp.bfloat16), "shard", scatter_dimension=0, tiled=True
        ).astype(jnp.float32),
        lax.psum_scatter(
            grad_bias_two.astype(jnp.bfloat16), "shard", scatter_dimension=0, tiled=True
        ).astype(jnp.float32),
    )
    summed = (
        lax.psum(owned[0].astype(jnp.bfloat16), "seq").astype(jnp.float32),
        lax.psum(owned[1].astype(jnp.bfloat16), "seq").astype(jnp.float32),
        lax.psum(owned[2].astype(jnp.bfloat16), "seq").astype(jnp.float32),
        lax.psum(owned[3].astype(jnp.bfloat16), "seq").astype(jnp.float32),
        lax.psum(owned[4].astype(jnp.bfloat16), "seq").astype(jnp.float32),
        lax.psum(owned[5].astype(jnp.bfloat16), "seq").astype(jnp.float32),
        lax.psum(owned[6].astype(jnp.bfloat16), "seq").astype(jnp.float32),
        lax.psum(owned[7].astype(jnp.bfloat16), "seq").astype(jnp.float32),
        lax.psum(owned[8].astype(jnp.bfloat16), "seq").astype(jnp.float32),
    )
    return (
        output,
        input_grad,
        summed[0],
        summed[1],
        summed[2],
        summed[3],
        summed[4],
        summed[5],
        summed[6],
        summed[7],
        summed[8],
    )


SEQS_HELD = 2
SEQ_SIZE = 8
GROUPS = 4
LANES = 128
LOG2E = 1.4426950408889634
LN2 = 0.6931471805599453
FAR = 2.0**30
F32 = jnp.float32
BF16 = jnp.bfloat16
VMEM_LIMIT = 60 * 1024 * 1024
FEED_LIMIT = 63 * 1024 * 1024
BY_MESH = pl.DeviceIdType.MESH
BY_LANES = (((1,), (1,)), ((), ()))


def packed_heads(rows):
    return rows + rows // 2


def unpack_heads(block):
    rows = block.shape[0] * 2 // 3
    last = block[rows:]
    third = jnp.concatenate([last[:, :HD], last[:, HD:]], axis=0)
    return jnp.concatenate([block[:rows], third], axis=1)


def pack_heads(value):
    rows = value.shape[0]
    third = value[:, 2 * HD :]
    return value[:, : 2 * HD], jnp.concatenate([third[: rows // 2], third[rows // 2 :]], axis=1)


def flip(index, bit):
    return index + bit - 2 * bit * lax.rem(lax.div(index, bit), 2)


def gather_kernel(
    chunks, by_z, tok_ref, w_ref, n_ref, place_ref, freq_ref, all_ref, w_all_ref, n_all_ref, turn_ref, send, recv, kept, w_send, w_recv
):
    me = lax.axis_index("seq")
    shard = lax.axis_index("shard")
    shards = w_all_ref.shape[0]
    half = lax.div(me, GROUPS)
    y_near, z_near, partner = flip(me, 1), flip(me, 2), flip(me, 4)
    barrier = pltpu.get_barrier_semaphore()
    for device in (y_near, z_near, partner):
        pl.semaphore_signal(barrier, inc=1, device_id={"seq": device}, device_id_type=BY_MESH)
    for step in range(1, shards):
        pl.semaphore_signal(
            barrier, inc=1, device_id={"shard": lax.rem(shard + step, shards)}, device_id_type=BY_MESH
        )
    pl.semaphore_wait(barrier, 2 + shards)

    part = tok_ref.shape[1] // chunks
    started = []

    def go(source, target, slot, device):
        copy = pltpu.make_async_remote_copy(
            src_ref=source,
            dst_ref=target,
            send_sem=send.at[slot],
            recv_sem=recv.at[slot],
            device_id={"seq": device},
            device_id_type=BY_MESH,
        )
        copy.start()
        started.append(copy)
        return copy

    def rows(chunk):
        return pl.ds(chunk * part, part)

    def relay(piece, chunk, slot, device):
        return go(all_ref.at[piece, rows(chunk)], all_ref.at[piece, rows(chunk)], slot * chunks + chunk, device)

    def own(which, chunk, slot, device):
        return go(tok_ref.at[which, rows(chunk)], all_ref.at[me, rows(chunk)], slot * chunks + chunk, device)

    crossing = [own(1 - half, chunk, 0, partner) for chunk in range(chunks)]
    own_y, own_z = [], []
    for chunk in range(chunks):
        own_y.append(own(half, chunk, 1, y_near))
        own_z.append(own(half, chunk, 2, z_near))
    weights = []
    for step in range(1, shards):
        copy = pltpu.make_async_remote_copy(
            src_ref=w_ref,
            dst_ref=w_all_ref.at[shard],
            send_sem=w_send.at[step],
            recv_sem=w_recv.at[step],
            device_id={"shard": lax.rem(shard + step, shards)},
            device_id_type=BY_MESH,
        )
        copy.start()
        weights.append(copy)
        copy = pltpu.make_async_remote_copy(
            src_ref=n_ref,
            dst_ref=n_all_ref.at[shard],
            send_sem=w_send.at[shards + step],
            recv_sem=w_recv.at[shards + step],
            device_id={"shard": lax.rem(shard + step, shards)},
            device_id_type=BY_MESH,
        )
        copy.start()
        weights.append(copy)
    keep_n = pltpu.make_async_copy(n_ref, n_all_ref.at[shard], kept.at[2])
    keep_n.start()
    keep_tok = pltpu.make_async_copy(tok_ref.at[half], all_ref.at[me], kept.at[0])
    keep_tok.start()
    keep_w = pltpu.make_async_copy(w_ref, w_all_ref.at[shard], kept.at[1])
    keep_w.start()

    def turn_piece(index, carry):
        count = turn_ref.shape[0] // place_ref.shape[0]
        lane = lax.broadcasted_iota(jnp.int32, (count, LANES), 1)
        place = jnp.transpose(jnp.broadcast_to(place_ref[index], (LANES, count)))
        angle = place * freq_ref[...]
        turn_ref[pl.ds(pl.multiple_of(index * count, count), count), :] = jnp.where(
            lane < HD, jnp.cos(angle), jnp.sin(angle)
        )
        return carry

    lax.fori_loop(0, place_ref.shape[0], turn_piece, 0)

    cross_y, cross_z, corner = [], [], []
    for chunk in range(chunks):
        own_y[chunk].wait_recv()
        if chunk < by_z:
            corner.append(relay(y_near, chunk, 5, z_near))
        own_z[chunk].wait_recv()
        if chunk >= by_z:
            corner.append(relay(z_near, chunk, 5, y_near))
        crossing[chunk].wait_recv()
        cross_y.append(relay(partner, chunk, 3, y_near))
        cross_z.append(relay(partner, chunk, 4, z_near))
    for chunk in range(chunks):
        cross_y[chunk].wait_recv()
        if chunk < by_z:
            corner.append(relay(flip(y_near, 4), chunk, 6, z_near))
        cross_z[chunk].wait_recv()
        if chunk >= by_z:
            corner.append(relay(flip(z_near, 4), chunk, 6, y_near))
    for copy in corner:
        copy.wait_recv()
    for copy in weights:
        copy.wait()
    keep_tok.wait()
    keep_w.wait()
    keep_n.wait()
    for copy in started:
        copy.wait_send()


def gather_tokens(tokens, w_part, norms, place, freq, shards, chunks=8, by_z=3):
    seqs, rows, width = tokens.shape
    anywhere = pl.BlockSpec(memory_space=pl.ANY)
    vmem = pl.BlockSpec(memory_space=pltpu.VMEM)
    return pl.pallas_call(
        functools.partial(gather_kernel, chunks, by_z),
        out_shape=(
            jax.ShapeDtypeStruct((SEQ_SIZE, rows, width), tokens.dtype),
            jax.ShapeDtypeStruct((shards,) + w_part.shape, w_part.dtype),
            jax.ShapeDtypeStruct((shards,) + norms.shape, norms.dtype),
            jax.ShapeDtypeStruct((place.shape[0] * place.shape[2], LANES), F32),
        ),
        in_specs=[anywhere, anywhere, anywhere, vmem, vmem],
        out_specs=(anywhere, anywhere, anywhere, vmem),
        scratch_shapes=[
            pltpu.SemaphoreType.DMA((7 * chunks,)),
            pltpu.SemaphoreType.DMA((7 * chunks,)),
            pltpu.SemaphoreType.DMA((3,)),
            pltpu.SemaphoreType.DMA((2 * shards,)),
            pltpu.SemaphoreType.DMA((2 * shards,)),
        ],
        compiler_params=pltpu.CompilerParams(collective_id=1, has_side_effects=True),
        name="gather_tokens",
    )(tokens, w_part, norms, place, freq)


def project_kernel(seg_ref, turn_ref, x_ref, w_ref, q_ref, k_ref, v_ref):
    rows = x_ref.shape[1]
    held = q_ref.shape[0]
    lane = lax.broadcasted_iota(jnp.int32, (rows, LANES), 1)
    seg = jnp.transpose(jnp.broadcast_to(seg_ref[0], (LANES, rows)))
    turn = turn_ref[...]
    cos_b = jnp.where(lane < HD, turn, 0.0)
    sin_b = jnp.where(lane < HD, pltpu.roll(turn, HD, 1), 0.0)
    sin_b = jnp.where(lane < HD // 2, -sin_b, sin_b)
    same = seg == (lane - HD).astype(F32)
    q_tail = jnp.where(same, 1.0, 0.0)
    k_tail = jnp.where(same | (lane < HD), 0.0, -FAR)
    v_tail = jnp.where(lane < HD, 0.0, 1.0)
    scale = HD ** (-0.5) * LOG2E
    q_cos, q_sin = cos_b * scale, sin_b * scale
    width = held * LANES
    for part in range(3):
        mixed = jnp.dot(x_ref[0], w_ref[:, part * width : (part + 1) * width], preferred_element_type=F32)
        for head in range(held):
            value = mixed[:, head * LANES : (head + 1) * LANES]
            if part == 0:
                value = value * q_cos + pltpu.roll(value, HD // 2, 1) * q_sin + q_tail
                q_ref[head] = value.astype(BF16)
            elif part == 1:
                value = value * cos_b + pltpu.roll(value, HD // 2, 1) * sin_b + k_tail
                k_ref[head] = value.astype(BF16)
            else:
                v_ref[head] = (value + v_tail).astype(BF16)


def project_heads(seg_row, turn, pieces, w_full, held):
    count, rows, width = pieces.shape
    length = count * rows
    row_spec = pl.BlockSpec((1, 1, rows), lambda i: (i, 0, 0))
    head_spec = pl.BlockSpec((held, rows, LANES), lambda i: (0, i, 0))
    head_shape = jax.ShapeDtypeStruct((held, length, LANES), BF16)
    return pl.pallas_call(
        project_kernel,
        out_shape=(head_shape, head_shape, head_shape),
        grid=(count,),
        in_specs=[
            row_spec,
            pl.BlockSpec((rows, LANES), lambda i: (i, 0)),
            pl.BlockSpec((1, rows, width), lambda i: (i, 0, 0)),
            pl.BlockSpec(w_full.shape, lambda i: (0, 0)),
        ],
        out_specs=(head_spec, head_spec, head_spec),
        compiler_params=pltpu.CompilerParams(vmem_limit_bytes=VMEM_LIMIT),
        cost_estimate=pl.CostEstimate(
            flops=2 * length * width * w_full.shape[1],
            bytes_accessed=length * (width * 2 + held * LANES * 6 + LANES * 4),
            transcendentals=length * LANES,
        ),
        name="project_heads",
    )(seg_row.reshape(count, 1, rows), turn, pieces, w_full)


def document_bounds(seg_row, rows):
    first = seg_row[::rows]
    last = seg_row[rows - 1 :: rows]
    low = jnp.sum((seg_row[None, :] < first[:, None]).astype(jnp.int32), axis=1)
    high = jnp.sum((seg_row[None, :] <= last[:, None]).astype(jnp.int32), axis=1)
    return low, high


def windows(bounds, length, window, align):
    low = bounds[0] // align * align
    count = (bounds[1] - low + window - 1) // window
    return jnp.minimum(low, length - count * window), count


def attend_kernel(window, align, low_ref, count_ref, q_ref, k_ref, v_ref, sum_ref, joined_ref):
    block = pl.program_id(0)
    low = low_ref[block]
    sum_ref[...] = jnp.zeros_like(sum_ref)

    def step(index, carry):
        start = pl.multiple_of(low + index * window, align)
        for head in range(q_ref.shape[0]):
            k_part = k_ref[head, pl.ds(start, window), :]
            v_part = v_ref[head, pl.ds(start, window), :]
            score = lax.dot_general(q_ref[head], k_part, BY_LANES, preferred_element_type=F32)
            expo = jnp.exp2(score).astype(BF16)
            sum_ref[head] += jnp.dot(expo, v_part, preferred_element_type=F32)
        return carry

    lax.fori_loop(0, count_ref[block], step, 0)
    rows = q_ref.shape[1]
    parts = [sum_ref[head][:, :HD] / sum_ref[head][:, HD : HD + 1] for head in range(q_ref.shape[0])]
    first, last = pack_heads(jnp.concatenate(parts, axis=1))
    joined_ref[0, :rows] = first.astype(BF16)
    joined_ref[0, rows:] = last.astype(BF16)


def attend_heads(bounds, q_ext, k_ext, v_ext, rows, window=1024, align=16):
    heads, length, lanes = q_ext.shape
    low, count = windows(bounds, length, window, align)
    whole = pl.BlockSpec((heads, length, lanes), lambda i, *_: (0, 0, 0))
    part = pl.BlockSpec((heads, rows, lanes), lambda i, *_: (0, i, 0))
    return pl.pallas_call(
        functools.partial(attend_kernel, window, align),
        out_shape=(
            jax.ShapeDtypeStruct((heads, length, lanes), F32),
            jax.ShapeDtypeStruct((length // rows, packed_heads(rows), LANES), BF16),
        ),
        grid_spec=pltpu.PrefetchScalarGridSpec(
            num_scalar_prefetch=2,
            grid=(length // rows,),
            in_specs=[part, whole, whole],
            out_specs=(part, pl.BlockSpec((1, packed_heads(rows), LANES), lambda i, *_: (i, 0, 0))),
        ),
        compiler_params=pltpu.CompilerParams(vmem_limit_bytes=VMEM_LIMIT),
        cost_estimate=pl.CostEstimate(
            flops=heads * length * length * 4 * lanes // 2,
            bytes_accessed=heads * length * lanes * 10,
            transcendentals=heads * length * length // 2,
        ),
        name="attend_heads",
    )(low, count, q_ext, k_ext, v_ext)


def attend_back_kernel(
    align,
    low_ref,
    count_ref,
    q_ref,
    sum_ref,
    dout_ref,
    turn_ref,
    k_ref,
    v_ref,
    d_ref,
    dq_ref,
    dkv_ref,
    g_ref,
    gt_ref,
    qt_ref,
):
    block = pl.program_id(0)
    heads, rows, lanes = q_ref.shape
    width = heads * HD

    @pl.when(block == 0)
    def _():
        dkv_ref[...] = jnp.zeros_like(dkv_ref)

    dq_ref[...] = jnp.zeros_like(dq_ref)
    half_lane = lax.broadcasted_iota(jnp.int32, (rows, HD), 1)
    dout_all = unpack_heads(dout_ref[0].astype(F32))
    for head in range(heads):
        dout = dout_all[:, head * HD : (head + 1) * HD]
        sums = sum_ref[head]
        total = sums[:, HD : HD + 1]
        g_low = dout / total
        delta = -jnp.sum(dout * sums[:, :HD], axis=1, keepdims=True) / (total * total)
        high = delta.astype(BF16).astype(F32)
        middle = (delta - high).astype(BF16).astype(F32)
        tail = jnp.where(
            half_lane == 0,
            high,
            jnp.where(half_lane == 1, middle, jnp.where(half_lane == 2, delta - high - middle, 0.0)),
        )
        g_ext = jnp.concatenate([g_low, tail], axis=1)
        g_ref[head] = g_ext.astype(BF16)
        gt_ref[head] = jnp.transpose(g_ext)[:HD].astype(BF16)
        qt_ref[head] = jnp.transpose(q_ref[head].astype(F32))[:HD].astype(BF16)

    low = low_ref[block]

    def step(window, low, index, carry):
        start = pl.multiple_of(low + index * window, align)
        for head in range(heads):
            k_part = k_ref[head, pl.ds(start, window), :]
            v_part = v_ref[head, pl.ds(start, window), :]
            score = lax.dot_general(q_ref[head], k_part, BY_LANES, preferred_element_type=F32)
            slope = lax.dot_general(g_ref[head], v_part, BY_LANES, preferred_element_type=F32)
            expo = jnp.exp2(score)
            d_score = (expo * slope).astype(BF16)
            expo = expo.astype(BF16)
            dq_ref[head] += jnp.dot(d_score, k_part, preferred_element_type=F32)
            dkv_ref[head, :HD, pl.ds(start, window)] += jnp.dot(qt_ref[head], d_score, preferred_element_type=F32)
            dkv_ref[head, HD:, pl.ds(start, window)] += jnp.dot(gt_ref[head], expo, preferred_element_type=F32)
        return carry

    units = count_ref[block]
    many = lax.div(units, 4)
    rest = lax.rem(units, 4)
    lax.fori_loop(0, many, functools.partial(step, 4 * align, low), 0)
    low = low + many * 4 * align

    @pl.when(rest >= 2)
    def _():
        step(2 * align, low, 0, 0)

    @pl.when(lax.rem(rest, 2) == 1)
    def _():
        step(align, low + lax.div(rest, 2) * 2 * align, 0, 0)

    lane = lax.broadcasted_iota(jnp.int32, (rows, lanes), 1)

    def turn_back(value, turn):
        swapped = jnp.where(lane < HD // 2, pltpu.roll(value, lanes - HD // 2, 1), pltpu.roll(value, HD // 2, 1))
        sine = pltpu.roll(turn, HD, 1)
        sine = jnp.where(lane < HD // 2, sine, -sine)
        return (value * turn + swapped * sine)[:, :HD]

    here = turn_ref[pl.ds(pl.multiple_of(block * rows, rows), rows), :]
    for head in range(heads):
        turned = turn_back(dq_ref[head] * HD ** (-0.5), here)
        d_ref[block, :, head * HD : (head + 1) * HD] = turned.astype(BF16)

    @pl.when(block == pl.num_programs(0) - 1)
    def _():
        def finish(piece, carry):
            start = pl.multiple_of(piece * rows, rows)
            turn = turn_ref[pl.ds(start, rows), :]
            for head in range(heads):
                both = jnp.transpose(dkv_ref[head, :, pl.ds(start, rows)])
                at = width + head * HD
                d_ref[piece, :, at : at + HD] = (turn_back(both, turn) * LN2).astype(BF16)
                d_ref[piece, :, width + at : width + at + HD] = both[:, HD:].astype(BF16)
            return carry

        lax.fori_loop(0, d_ref.shape[0], finish, 0)


def attend_back_heads(bounds, q_ext, k_ext, v_ext, sums, dout, turn, align=128):
    heads, length, lanes = q_ext.shape
    count_blocks = dout.shape[0]
    rows, width = length // count_blocks, heads * HD
    low, count = windows(bounds, length, align, align)
    whole = pl.BlockSpec((heads, length, lanes), lambda i, *_: (0, 0, 0))
    part = pl.BlockSpec((heads, rows, lanes), lambda i, *_: (0, i, 0))
    return pl.pallas_call(
        functools.partial(attend_back_kernel, align),
        out_shape=jax.ShapeDtypeStruct((count_blocks, rows, 3 * width), BF16),
        grid_spec=pltpu.PrefetchScalarGridSpec(
            num_scalar_prefetch=2,
            grid=(count_blocks,),
            in_specs=[
                part,
                part,
                pl.BlockSpec((1,) + dout.shape[1:], lambda i, *_: (i, 0, 0)),
                pl.BlockSpec((length, lanes), lambda i, *_: (0, 0)),
                whole,
                whole,
            ],
            out_specs=pl.BlockSpec((count_blocks, rows, 3 * width), lambda i, *_: (0, 0, 0)),
            scratch_shapes=[
                pltpu.VMEM((heads, rows, lanes), F32),
                pltpu.VMEM((heads, 2 * HD, length), F32),
                pltpu.VMEM((heads, rows, lanes), BF16),
                pltpu.VMEM((heads, HD, rows), BF16),
                pltpu.VMEM((heads, HD, rows), BF16),
            ],
        ),
        compiler_params=pltpu.CompilerParams(vmem_limit_bytes=VMEM_LIMIT),
        cost_estimate=pl.CostEstimate(
            flops=heads * length * length * 10 * lanes // 2,
            bytes_accessed=heads * length * lanes * 20,
            transcendentals=heads * length * length // 2,
        ),
        name="attend_back_heads",
    )(low, count, q_ext, sums, dout, turn, k_ext, v_ext)


def scatter_kernel(
    chunks,
    by_z,
    d_hbm,
    x_hbm,
    w_ref,
    dh_hbm,
    norm_ref,
    out_hbm,
    gw_all_ref,
    norm_out_ref,
    d_ref,
    x_ref,
    part_ref,
    gw_sum,
    gw_ref,
    dh_ref,
    out_ref,
    got_y,
    got_z,
    relay_y,
    relay_z,
    sent_y,
    sent_z,
    cross_out,
    cross_in,
    gw_got,
    gw_mine,
    gw_pair,
    gw_final,
    norm_got,
    norm_sent,
    send,
    recv,
    gw_send,
    gw_recv,
    norm_send,
    norm_recv,
    kept,
):
    me = lax.axis_index("seq")
    shard = lax.axis_index("shard")
    shards = gw_ref.shape[0]
    half = lax.div(me, GROUPS)
    y_near, z_near, partner = flip(me, 1), flip(me, 2), flip(me, 4)
    corner = flip(y_near, 2)
    barrier = pltpu.get_barrier_semaphore()
    for n in range(1, SEQ_SIZE):
        pl.semaphore_signal(
            barrier, inc=1, device_id={"seq": lax.rem(me + n, SEQ_SIZE)}, device_id_type=BY_MESH
        )
    for step in range(1, shards):
        pl.semaphore_signal(
            barrier, inc=1, device_id={"shard": lax.rem(shard + step, shards)}, device_id_type=BY_MESH
        )
    pl.semaphore_wait(barrier, SEQ_SIZE + shards - 2)

    started = []

    def go(source, target, sends, receives, slot, where):
        copy = pltpu.make_async_remote_copy(
            src_ref=source,
            dst_ref=target,
            send_sem=sends.at[slot],
            recv_sem=receives.at[slot],
            device_id=where,
            device_id_type=BY_MESH,
        )
        copy.start()
        started.append(copy)
        return copy

    rows = part_ref.shape[1] // chunks

    def band(chunk):
        return pl.ds(chunk * rows, rows)

    def piece(device, far):
        return flip(device, 4) if far else device

    def slot(kind, far, chunk):
        return (kind * 2 + (0 if far else 1)) * chunks + chunk

    def other(mask):
        index = 0
        for bit in (1, 2, 4):
            here, there = lax.rem(lax.div(me, bit), 2), lax.rem(lax.div(mask, bit), 2)
            index = index + bit * (here + there - 2 * here * there)
        return index

    masks = (7, 6, 5, 3, 2, 1, 4, 0)

    def fetch(mask, place):
        return pltpu.make_async_copy(d_hbm.at[other(mask)], d_ref.at[other(mask)], kept.at[8 + place])

    for place, mask in enumerate(masks):
        fetch(mask, place).start()
    loads = [
        pltpu.make_async_copy(dh_hbm, dh_ref, kept.at[4]),
        pltpu.make_async_copy(x_hbm, x_ref, kept.at[5]),
    ]
    for copy in loads:
        copy.start()

    def project(count, first, place):
        def body(n, carry):
            mask = first(n)
            fetch(mask, place + n).wait()
            index = other(mask)
            part_ref[index] = lax.dot_general(
                d_ref[index], w_ref[...], BY_LANES, preferred_element_type=F32
            ).astype(BF16)
            return carry

        lax.fori_loop(0, count, body, 0)

    norm_seq = [
        go(norm_ref, norm_got.at[n], norm_send, norm_recv, n, {"seq": lax.rem(me + n + 1, SEQ_SIZE)})
        for n in range(SEQ_SIZE - 1)
    ]

    from_corner, direct = {}, {}

    def send_pieces(far):
        for chunk in range(chunks):
            over_z = chunk < by_z
            from_corner[far, chunk] = go(
                part_ref.at[piece(corner, far), band(chunk)],
                (relay_y if over_z else relay_z).at[0 if far else 1, chunk if over_z else chunk - by_z],
                send,
                recv,
                slot(0, far, chunk),
                {"seq": y_near if over_z else z_near},
            )
        for chunk in range(chunks):
            over_z = chunk < by_z
            direct[far, chunk] = go(
                part_ref.at[piece(y_near if over_z else z_near, far), band(chunk)],
                (got_y if over_z else got_z).at[0 if far else 1, band(chunk)],
                send,
                recv,
                slot(1 if over_z else 2, far, chunk),
                {"seq": y_near if over_z else z_near},
            )

    project(3, lambda n: 7 - n, 0)
    send_pieces(True)
    project(3, lambda n: 3 - n, 3)
    project(2, lambda n: 4 - 4 * n, 6)
    relayed = {}

    def relay(far, chunk):
        over_z = chunk < by_z
        target = z_near if over_z else y_near
        index = chunk if over_z else chunk - by_z
        which = 0 if far else 1
        from_corner[far, chunk].wait_recv()
        source = relay_y if over_z else relay_z
        buffer = sent_y if over_z else sent_z
        passed = part_ref[piece(target, far), band(chunk)].astype(F32)
        buffer[which, index] = (source[which, index].astype(F32) + passed).astype(BF16)
        relayed[far, chunk] = go(
            buffer.at[which, index],
            (got_z if over_z else got_y).at[which, band(chunk)],
            send,
            recv,
            slot(2 if over_z else 1, far, chunk),
            {"seq": target},
        )

    def total(far, chunk):
        which = 0 if far else 1
        direct[far, chunk].wait_recv()
        relayed[far, chunk].wait_recv()
        return part_ref[piece(me, far), band(chunk)].astype(F32) + got_y[which, band(chunk)].astype(F32) + got_z[which, band(chunk)].astype(F32)

    for chunk in range(chunks):
        relay(True, chunk)
    send_pieces(False)
    for copy in loads:
        copy.wait()
    gw_sum[...] = jnp.zeros_like(gw_sum)

    def grow(n, carry):
        gw_sum[...] += lax.dot_general(
            x_ref[n], d_ref[n], (((0,), (0,)), ((), ())), preferred_element_type=F32
        )
        return carry

    lax.fori_loop(0, d_ref.shape[0], grow, 0)
    depth = gw_ref.shape[1]
    for owner in range(shards):
        gw_ref[owner] = gw_sum[owner * depth : (owner + 1) * depth, :].astype(BF16)
    gw_one = [
        go(
            gw_ref.at[lax.rem(shard + step, shards)],
            gw_got.at[step - 1],
            gw_send,
            gw_recv,
            step - 1,
            {"shard": lax.rem(shard + step, shards)},
        )
        for step in range(1, shards)
    ]
    norm_total = norm_ref[...]
    for n, copy in enumerate(norm_seq):
        copy.wait_recv()
        norm_total = norm_total + norm_got[n]
    norm_sent[...] = norm_total
    for copy in gw_one:
        copy.wait_recv()
    summed = gw_ref[shard].astype(F32)
    for step in range(1, shards):
        summed = summed + gw_got[step - 1].astype(F32)
    gw_mine[...] = summed.astype(BF16)
    gw_two = go(gw_mine, gw_pair, gw_send, gw_recv, shards - 1, {"seq": partner})
    norm_shard = [
        go(
            norm_sent,
            norm_got.at[SEQ_SIZE - 2 + step],
            norm_send,
            norm_recv,
            SEQ_SIZE - 2 + step,
            {"shard": lax.rem(shard + step, shards)},
        )
        for step in range(1, shards)
    ]
    crossing = []
    for chunk in range(chunks):
        cross_out[band(chunk)] = total(True, chunk).astype(BF16)
        crossing.append(
            go(cross_out.at[band(chunk)], cross_in.at[band(chunk)], send, recv, slot(3, True, chunk), {"seq": partner})
        )
    for chunk in range(chunks):
        relay(False, chunk)
    gw_two.wait_recv()
    gw_final[...] = (gw_mine[...].astype(F32) + gw_pair[...].astype(F32)).astype(BF16)
    group = lax.rem(me, GROUPS)
    gw_three = [
        go(gw_final, gw_all_ref.at[group], gw_send, gw_recv, shards + n, {"seq": device})
        for n, device in enumerate((y_near, z_near, corner))
    ]
    keep = pltpu.make_async_copy(gw_final, gw_all_ref.at[group], kept.at[0])
    keep.start()
    for chunk in range(chunks):
        out_ref[0, band(chunk)] = (total(False, chunk) + dh_ref[half, band(chunk)]).astype(BF16)
    out_near = pltpu.make_async_copy(out_ref.at[0], out_hbm.at[half], kept.at[2])
    out_near.start()
    norm_total = norm_sent[...]
    for step, copy in enumerate(norm_shard):
        copy.wait_recv()
        norm_total = norm_total + norm_got[SEQ_SIZE - 1 + step]
    norm_out_ref[...] = norm_total
    for chunk in range(chunks):
        crossing[chunk].wait_recv()
        other = 1 - half
        out_ref[1, band(chunk)] = (cross_in[band(chunk)].astype(F32) + dh_ref[other, band(chunk)]).astype(BF16)
    out_far = pltpu.make_async_copy(out_ref.at[1], out_hbm.at[1 - half], kept.at[3])
    out_far.start()
    for copy in gw_three:
        copy.wait_recv()
    keep.wait()
    out_near.wait()
    out_far.wait()
    for copy in started:
        copy.wait_send()


def scatter_gradients(d_heads, pieces, w_own, dh_one, norms, shards, chunks=4, by_z=3):
    _, rows, width = pieces.shape
    columns = d_heads.shape[2]
    depth = width // shards
    part = rows // chunks
    hbm = pl.BlockSpec(memory_space=pltpu.HBM)
    vmem = pl.BlockSpec(memory_space=pltpu.VMEM)
    dma = pltpu.SemaphoreType.DMA
    return pl.pallas_call(
        functools.partial(scatter_kernel, chunks, by_z),
        out_shape=(
            jax.ShapeDtypeStruct(dh_one.shape, BF16),
            jax.ShapeDtypeStruct((GROUPS, depth, columns), BF16),
            jax.ShapeDtypeStruct(norms.shape, F32),
        ),
        in_specs=[hbm, hbm, vmem, hbm, vmem],
        out_specs=(hbm, vmem, vmem),
        scratch_shapes=[
            pltpu.VMEM(d_heads.shape, BF16),
            pltpu.VMEM(pieces.shape, BF16),
            pltpu.VMEM(pieces.shape, BF16),
            pltpu.VMEM((width, columns), F32),
            pltpu.VMEM((shards, depth, columns), BF16),
            pltpu.VMEM(dh_one.shape, F32),
            pltpu.VMEM((2, rows, width), BF16),
            pltpu.VMEM((2, rows, width), BF16),
            pltpu.VMEM((2, rows, width), BF16),
            pltpu.VMEM((2, by_z, part, width), BF16),
            pltpu.VMEM((2, chunks - by_z, part, width), BF16),
            pltpu.VMEM((2, by_z, part, width), BF16),
            pltpu.VMEM((2, chunks - by_z, part, width), BF16),
            pltpu.VMEM((rows, width), BF16),
            pltpu.VMEM((rows, width), BF16),
            pltpu.VMEM((shards - 1, depth, columns), BF16),
            pltpu.VMEM((depth, columns), BF16),
            pltpu.VMEM((depth, columns), BF16),
            pltpu.VMEM((depth, columns), BF16),
            pltpu.VMEM((SEQ_SIZE + shards - 2,) + norms.shape, F32),
            pltpu.VMEM(norms.shape, F32),
            dma((7 * chunks,)),
            dma((7 * chunks,)),
            dma((shards + 3,)),
            dma((shards + 3,)),
            dma((SEQ_SIZE + shards - 2,)),
            dma((SEQ_SIZE + shards - 2,)),
            dma((8 + SEQ_SIZE,)),
        ],
        compiler_params=pltpu.CompilerParams(
            collective_id=2, has_side_effects=True, vmem_limit_bytes=VMEM_LIMIT
        ),
        cost_estimate=pl.CostEstimate(flops=60 * 10**9, bytes_accessed=64 * 2**20, transcendentals=0),
        name="scatter_gradients",
    )(d_heads, pieces, w_own, dh_one, norms)


def padded_rows(blocks, depth):
    return pl.cdiv((3 * blocks + 1) * depth, SEQ_SIZE * 16) * SEQ_SIZE * 16


def feed_forward_kernel(
    tokens_ref,
    joined_ref,
    cot_ref,
    out_hbm,
    gate_hbm,
    up_hbm,
    down_hbm,
    norms_ref,
    output_ref,
    dout_ref,
    dh_ref,
    norm_sums_ref,
    packed_ref,
    w_out,
    w_gate,
    w_up,
    w_down,
    flow,
    hat_one,
    inverse_one,
    x_low,
    x_turned,
    dm_low,
    gate_kept,
    up_kept,
    d_both,
    hidden_kept,
    staged,
    loads,
    stores,
):
    seqs, rows, width = dh_ref.shape
    shards = packed_ref.shape[0]
    depth = width // shards
    blocks = gate_hbm.shape[1] // width
    weights = ((out_hbm, w_out), (gate_hbm, w_gate), (up_hbm, w_up), (down_hbm, w_down))
    fetch = [pltpu.make_async_copy(src, dst, loads.at[n]) for n, (src, dst) in enumerate(weights)]
    tokens_in = pltpu.make_async_copy(tokens_ref, flow, loads.at[4])
    tokens_in.start()
    for copy in fetch:
        copy.start()
    gain_one, bias_one, gain_two, bias_two = (norms_ref[n : n + 1, :] for n in range(4))

    def mean(value):
        return jnp.sum(value, axis=-1, keepdims=True) * (1.0 / width)

    def rows_of(seq):
        return pl.ds(pl.multiple_of(seq * rows, rows), rows)

    fetch[0].wait()
    tokens_in.wait()

    def enter(seq, carry):
        h_one = flow[seq].astype(F32)
        for group in range(GROUPS):
            h_one = h_one + jnp.dot(
                unpack_heads(joined_ref[seq * GROUPS + group]),
                w_out[group * depth : (group + 1) * depth, :],
                preferred_element_type=F32,
            )
        centered = h_one - mean(h_one)
        inverse = lax.rsqrt(mean(centered * centered) + EPS)
        normed = centered * inverse
        hat_one[seq] = normed
        inverse_one[seq] = inverse
        x_one = normed * gain_one + bias_one
        dh_ref[seq] = x_one
        x_low[seq] = x_one.astype(BF16)
        x_turned[:, rows_of(seq)] = jnp.transpose(x_one).astype(BF16)
        return carry

    lax.fori_loop(0, seqs, enter, 0)
    cot_in = pltpu.make_async_copy(cot_ref, flow, loads.at[4])
    cot_in.start()
    for copy in fetch[1:]:
        copy.wait()

    def forward(step, carry):
        block, seq = lax.div(step, seqs), lax.rem(step, seqs)
        at = pl.ds(pl.multiple_of(block * width, width), width)
        gate = jnp.dot(x_low[seq], w_gate[:, at], preferred_element_type=F32)
        up = jnp.dot(x_low[seq], w_up[:, at], preferred_element_type=F32)
        gate_kept[block, seq] = gate.astype(gate_kept.dtype)
        up_kept[block, seq] = up.astype(up_kept.dtype)
        hidden = (gate * jax.nn.sigmoid(gate) * up).astype(BF16)
        dh_ref[seq] += jnp.dot(hidden, w_down[at, :], preferred_element_type=F32)
        return carry

    lax.fori_loop(0, blocks * seqs, forward, 0)

    cot_in.wait()
    def turn(seq, carry):
        gain_two_sum, bias_two_sum = carry
        h_two = dh_ref[seq]
        centered = h_two - mean(h_two)
        inverse = lax.rsqrt(mean(centered * centered) + EPS)
        normed = centered * inverse
        cot = flow[seq].astype(F32)
        flow[seq] = (normed * gain_two + bias_two).astype(BF16)
        gain_two_sum = gain_two_sum + jnp.sum(cot * normed, axis=0, keepdims=True)
        bias_two_sum = bias_two_sum + jnp.sum(cot, axis=0, keepdims=True)
        scaled = cot * gain_two
        dh_two = inverse * (scaled - mean(scaled) - normed * mean(scaled * normed))
        dh_ref[seq] = dh_two
        dm_low[rows_of(seq), :] = dh_two.astype(BF16)
        return gain_two_sum, bias_two_sum

    empty = jnp.zeros((1, width), F32)
    gain_two_sum, bias_two_sum = lax.fori_loop(0, seqs, turn, (empty, empty))
    output_out = pltpu.make_async_copy(flow, output_ref, loads.at[4])
    output_out.start()

    def store(kind, block):
        if kind < 2:
            start = pl.multiple_of((kind * blocks + block) * depth, depth)
            return [
                pltpu.make_async_copy(
                    staged.at[kind, pl.ds(shard * depth, depth)],
                    packed_ref.at[shard, pl.ds(start, depth)],
                    stores.at[kind, shard],
                )
                for shard in range(shards)
            ]
        start = 2 * blocks * depth
        return [
            pltpu.make_async_copy(
                staged.at[2], packed_ref.at[block, pl.ds(start, width)], stores.at[2, 0]
            )
        ]

    def backward(block, carry):
        at = pl.ds(pl.multiple_of(block * width, width), width)
        def rows_back(seq, carry):
            here = rows_of(seq)
            d_hidden = lax.dot_general(dm_low[here, :], w_down[at, :], BY_LANES, preferred_element_type=F32)
            gate = gate_kept[block, seq].astype(F32)
            up = up_kept[block, seq].astype(F32)
            sigma = jax.nn.sigmoid(gate)
            smooth = gate * sigma
            hidden_kept[here, :] = (smooth * up).astype(BF16)
            dg = (d_hidden * up * (sigma + smooth * (1.0 - sigma))).astype(BF16)
            du = (d_hidden * smooth).astype(BF16)
            d_both[0, here, :] = dg
            d_both[1, here, :] = du
            dh_ref[seq] += lax.dot_general(dg, w_gate[:, at], BY_LANES, preferred_element_type=F32)
            dh_ref[seq] += lax.dot_general(du, w_up[:, at], BY_LANES, preferred_element_type=F32)
            return carry

        lax.fori_loop(0, seqs, rows_back, 0)

        @pl.when(block > 0)
        def _():
            for kind in range(3):
                for copy in store(kind, block - 1):
                    copy.wait()

        def grow(kind, carry):
            staged[kind] = jnp.dot(x_turned[...], d_both[kind], preferred_element_type=F32).astype(BF16)
            return carry

        lax.fori_loop(0, 2, grow, 0)
        staged[2] = lax.dot_general(
            hidden_kept[...], dm_low[...], (((0,), (0,)), ((), ())), preferred_element_type=F32
        ).astype(BF16)
        for kind in range(3):
            for copy in store(kind, block):
                copy.start()
        return carry

    lax.fori_loop(0, blocks, backward, 0)

    def leave(seq, carry):
        gain_one_sum, bias_one_sum = carry
        dx_one = dh_ref[seq]
        normed = hat_one[seq]
        gain_one_sum = gain_one_sum + jnp.sum(dx_one * normed, axis=0, keepdims=True)
        bias_one_sum = bias_one_sum + jnp.sum(dx_one, axis=0, keepdims=True)
        scaled = dx_one * gain_one
        dh_one = inverse_one[seq] * (scaled - mean(scaled) - normed * mean(scaled * normed))
        dh_ref[seq] = dh_one
        d_attn = dh_one.astype(BF16)
        d_both[0, rows_of(seq), :] = d_attn
        for group in range(GROUPS):
            dout = lax.dot_general(
                d_attn, w_out[group * depth : (group + 1) * depth, :], BY_LANES, preferred_element_type=F32
            )
            first, last = pack_heads(dout)
            dout_ref[seq * GROUPS + group, :rows] = first.astype(BF16)
            dout_ref[seq * GROUPS + group, rows:] = last.astype(BF16)
        return gain_one_sum, bias_one_sum

    gain_one_sum, bias_one_sum = lax.fori_loop(0, seqs, leave, (empty, empty))
    for kind in range(3):
        for copy in store(kind, blocks - 1):
            copy.wait()
    def grow_out(group, carry):
        grad = jnp.zeros((depth, width), F32)
        for seq in range(seqs):
            grad = grad + lax.dot_general(
                unpack_heads(joined_ref[seq * GROUPS + group]),
                d_both[0, seq * rows : (seq + 1) * rows, :],
                (((0,), (0,)), ((), ())),
                preferred_element_type=F32,
            )
        staged[0, pl.ds(pl.multiple_of(group * depth, depth), depth), :] = grad.astype(BF16)
        return carry

    lax.fori_loop(0, GROUPS, grow_out, 0)
    last = [
        pltpu.make_async_copy(
            staged.at[0, pl.ds(shard * depth, depth)],
            packed_ref.at[shard, pl.ds(3 * blocks * depth, depth)],
            stores.at[0, shard],
        )
        for shard in range(shards)
    ]
    used = (3 * blocks + 1) * depth
    rest = packed_ref.shape[1] - used
    staged[1, :rest, :] = jnp.zeros((rest, width), BF16)
    last += [
        pltpu.make_async_copy(
            staged.at[1, pl.ds(0, rest)], packed_ref.at[shard, pl.ds(used, rest)], stores.at[1, shard]
        )
        for shard in range(shards)
    ]
    for copy in last:
        copy.start()
    norm_sums_ref[0:1, :] = gain_one_sum
    norm_sums_ref[1:2, :] = bias_one_sum
    norm_sums_ref[2:3, :] = gain_two_sum
    norm_sums_ref[3:4, :] = bias_two_sum
    for copy in last:
        copy.wait()
    output_out.wait()


def feed_forward(tokens, joined, cotangent, w_out, w_gate, w_up, w_down, norms, kept=BF16):
    seqs, rows, width = tokens.shape
    total = seqs * rows
    hidden = w_gate.shape[1]
    blocks = hidden // width
    depth = width // GROUPS
    vmem = pl.BlockSpec(memory_space=pltpu.VMEM)
    hbm = pl.BlockSpec(memory_space=pltpu.HBM)
    dma = pltpu.SemaphoreType.DMA
    return pl.pallas_call(
        feed_forward_kernel,
        out_shape=(
            jax.ShapeDtypeStruct(tokens.shape, BF16),
            jax.ShapeDtypeStruct(joined.shape, BF16),
            jax.ShapeDtypeStruct(tokens.shape, F32),
            jax.ShapeDtypeStruct((4, width), F32),
            jax.ShapeDtypeStruct((GROUPS, padded_rows(blocks, depth), width), BF16),
        ),
        in_specs=[hbm, vmem, hbm, hbm, hbm, hbm, hbm, vmem],
        out_specs=(hbm, vmem, vmem, vmem, hbm),
        scratch_shapes=[
            pltpu.VMEM(w_out.shape, BF16),
            pltpu.VMEM(w_gate.shape, BF16),
            pltpu.VMEM(w_up.shape, BF16),
            pltpu.VMEM(w_down.shape, BF16),
            pltpu.VMEM(tokens.shape, BF16),
            pltpu.VMEM(tokens.shape, F32),
            pltpu.VMEM((seqs, rows, 1), F32),
            pltpu.VMEM(tokens.shape, BF16),
            pltpu.VMEM((width, total), BF16),
            pltpu.VMEM((total, width), BF16),
            pltpu.VMEM((blocks, seqs, rows, width), kept),
            pltpu.VMEM((blocks, seqs, rows, width), kept),
            pltpu.VMEM((2, total, width), BF16),
            pltpu.VMEM((total, width), BF16),
            pltpu.VMEM((3, width, width), BF16),
            dma((5,)),
            dma((3, GROUPS)),
        ],
        compiler_params=pltpu.CompilerParams(vmem_limit_bytes=FEED_LIMIT),
        cost_estimate=pl.CostEstimate(
            flops=6 * total * width * (3 * hidden + width),
            bytes_accessed=2 * 2 * (3 * hidden + width) * width + 20 * total * width,
            transcendentals=2 * total * hidden,
        ),
        name="feed_forward",
    )(tokens, joined, cotangent, w_out, w_gate, w_up, w_down, norms)


def gather_rows_kernel(chunks, by_z, own_ref, rows_ref, send, recv, kept):
    me = lax.axis_index("seq")
    y_near, z_near, partner = flip(me, 1), flip(me, 2), flip(me, 4)
    barrier = pltpu.get_barrier_semaphore()
    for device in (y_near, z_near, partner):
        pl.semaphore_signal(barrier, inc=1, device_id={"seq": device}, device_id_type=BY_MESH)
    pl.semaphore_wait(barrier, 3)
    count = own_ref.shape[0]
    part = count // chunks
    started = []

    def go(source, target, slot, device):
        copy = pltpu.make_async_remote_copy(
            src_ref=source,
            dst_ref=target,
            send_sem=send.at[slot],
            recv_sem=recv.at[slot],
            device_id={"seq": device},
            device_id_type=BY_MESH,
        )
        copy.start()
        started.append(copy)
        return copy

    def band(device, chunk):
        return rows_ref.at[pl.ds(device * count + chunk * part, part)]

    def own(chunk, slot, device):
        return go(own_ref.at[pl.ds(chunk * part, part)], band(me, chunk), slot * chunks + chunk, device)

    def relay(device, chunk, slot, target):
        return go(band(device, chunk), band(device, chunk), slot * chunks + chunk, target)

    crossing = [own(chunk, 0, partner) for chunk in range(chunks)]
    own_y, own_z = [], []
    for chunk in range(chunks):
        own_y.append(own(chunk, 1, y_near))
        own_z.append(own(chunk, 2, z_near))
    keep = pltpu.make_async_copy(own_ref, rows_ref.at[pl.ds(me * count, count)], kept)
    keep.start()
    cross_y, cross_z, corner = [], [], []
    for chunk in range(chunks):
        own_y[chunk].wait_recv()
        if chunk < by_z:
            corner.append(relay(y_near, chunk, 5, z_near))
        own_z[chunk].wait_recv()
        if chunk >= by_z:
            corner.append(relay(z_near, chunk, 5, y_near))
        crossing[chunk].wait_recv()
        cross_y.append(relay(partner, chunk, 3, y_near))
        cross_z.append(relay(partner, chunk, 4, z_near))
    for chunk in range(chunks):
        cross_y[chunk].wait_recv()
        if chunk < by_z:
            corner.append(relay(flip(y_near, 4), chunk, 6, z_near))
        cross_z[chunk].wait_recv()
        if chunk >= by_z:
            corner.append(relay(flip(z_near, 4), chunk, 6, y_near))
    for copy in corner:
        copy.wait_recv()
    keep.wait()
    for copy in started:
        copy.wait_send()


def gather_rows(owned, chunks=8, by_z=3):
    hbm = pl.BlockSpec(memory_space=pltpu.HBM)
    dma = pltpu.SemaphoreType.DMA
    return pl.pallas_call(
        functools.partial(gather_rows_kernel, chunks, by_z),
        out_shape=jax.ShapeDtypeStruct((SEQ_SIZE * owned.shape[0], owned.shape[1]), BF16),
        in_specs=[hbm],
        out_specs=hbm,
        scratch_shapes=[dma((7 * chunks,)), dma((7 * chunks,)), dma],
        compiler_params=pltpu.CompilerParams(collective_id=5, has_side_effects=True),
        name="gather_rows",
    )(owned)


def unpack_kernel(gate_rows, up_rows, down_rows, out_rows, columns, gate_ref, up_ref, down_ref, out_ref, qkv_ref):
    gate_ref[...] = gate_rows[...].astype(F32)
    up_ref[...] = up_rows[...].astype(F32)
    down_ref[...] = down_rows[...].astype(F32)

    @pl.when(pl.program_id(0) == 0)
    def _():
        out_ref[...] = out_rows[...].astype(F32)
        groups, _, width = columns.shape
        width = width // 3
        for group in range(groups):
            for part in range(3):
                at = (part * groups + group) * width
                qkv_ref[:, at : at + width] = columns[group, :, part * width : (part + 1) * width].astype(F32)


def unpack_gradients(rows, columns, blocks):
    groups, depth, thirds = columns.shape
    width = rows.shape[1]
    piece = [
        pl.BlockSpec((depth, width), lambda i, first=first, step=step: (first + step * i, 0))
        for first, step in ((0, 1), (blocks, 1), (2 * blocks, 1), (3 * blocks, 0))
    ]
    return pl.pallas_call(
        unpack_kernel,
        out_shape=(
            jax.ShapeDtypeStruct((depth, blocks * width), F32),
            jax.ShapeDtypeStruct((depth, blocks * width), F32),
            jax.ShapeDtypeStruct((blocks * depth, width), F32),
            jax.ShapeDtypeStruct((depth, width), F32),
            jax.ShapeDtypeStruct((depth, groups * thirds), F32),
        ),
        grid=(blocks,),
        in_specs=piece + [pl.BlockSpec(columns.shape, lambda i: (0, 0, 0))],
        out_specs=(
            pl.BlockSpec((depth, width), lambda i: (0, i)),
            pl.BlockSpec((depth, width), lambda i: (0, i)),
            pl.BlockSpec((depth, width), lambda i: (i, 0)),
            pl.BlockSpec((depth, width), lambda i: (0, 0)),
            pl.BlockSpec((depth, groups * thirds), lambda i: (0, 0)),
        ),
        name="unpack_gradients",
    )(rows, rows, rows, rows, columns)


def document_places(seg_row):
    length = seg_row.shape[0]
    ids = jnp.arange(LANES - HD, dtype=jnp.int32)[:, None]
    starts = jnp.sum((seg_row[None, :] < ids).astype(jnp.int32), axis=1, keepdims=True)
    start = jnp.sum(jnp.where(seg_row[None, :] == ids, starts, 0), axis=0)
    return jnp.arange(length, dtype=jnp.int32) - start


def exchange_kernel(sent_ref, taken_ref, send, recv, kept):
    me = lax.axis_index("seq")
    barrier = pltpu.get_barrier_semaphore()
    others = [lax.rem(me + step, SEQ_SIZE) for step in range(1, SEQ_SIZE)]
    for device in others:
        pl.semaphore_signal(barrier, inc=1, device_id={"seq": device}, device_id_type=BY_MESH)
    pl.semaphore_wait(barrier, SEQ_SIZE - 1)
    copies = []
    for step, device in enumerate(others):
        copy = pltpu.make_async_remote_copy(
            src_ref=sent_ref.at[device],
            dst_ref=taken_ref.at[me],
            send_sem=send.at[step],
            recv_sem=recv.at[step],
            device_id={"seq": device},
            device_id_type=BY_MESH,
        )
        copy.start()
        copies.append(copy)
    keep = pltpu.make_async_copy(sent_ref.at[me], taken_ref.at[me], kept)
    keep.start()
    keep.wait()
    for copy in copies:
        copy.wait()


def exchange(blocks, collective_id):
    hbm = pl.BlockSpec(memory_space=pltpu.HBM)
    dma = pltpu.SemaphoreType.DMA
    return pl.pallas_call(
        exchange_kernel,
        out_shape=jax.ShapeDtypeStruct(blocks.shape, blocks.dtype),
        in_specs=[hbm],
        out_specs=hbm,
        scratch_shapes=[dma((SEQ_SIZE - 1,)), dma((SEQ_SIZE - 1,)), dma],
        compiler_params=pltpu.CompilerParams(collective_id=collective_id, has_side_effects=True),
        name="exchange",
    )(blocks)


def head_columns(w_qkv, group, held):
    depth = w_qkv.shape[0]
    split = w_qkv.reshape(depth, 3, GROUPS, held, HD)
    mine = lax.dynamic_index_in_dim(split, group, 2, keepdims=False)
    second = mine * jnp.array([1, 1, 0], w_qkv.dtype)[None, :, None, None]
    return jnp.concatenate([mine, second], axis=-1).reshape(depth, 3 * held * 2 * HD)


def local_heads(
    shards,
    tokens,
    segments,
    positions,
    cotangent,
    w_qkv,
    w_out,
    w_gate,
    w_up,
    w_down,
    ln1_gain,
    ln1_bias,
    ln2_gain,
    ln2_bias,
):
    seq_count, row_count, model_width = tokens.shape
    held = HEADS // GROUPS
    length = row_count * SEQ_SIZE
    me = lax.axis_index("seq")
    seg_row = lax.dynamic_index_in_dim(segments, me // GROUPS, 0, keepdims=False)

    def gather(shard):
        return lax.all_gather(shard, "shard", axis=0, tiled=True)

    freqs = jnp.exp(jnp.arange(HD // 2, dtype=F32) * (-math.log(ROPE_BASE) / (HD // 2)))
    freq = jnp.tile(freqs, LANES // (HD // 2))[None]
    place = document_places(seg_row).astype(F32).reshape(SEQ_SIZE, 1, row_count)
    norm_rows = jnp.stack([ln1_gain, ln1_bias, ln2_gain, ln2_bias]).astype(F32)
    pieces, w_heads, norms, turn = gather_tokens(
        tokens, head_columns(w_qkv, me % GROUPS, held), norm_rows, place, freq, shards
    )
    norms = jnp.transpose(norms, (1, 0, 2)).reshape(4, model_width)
    full_out, full_gate, full_up, full_down = (gather(w) for w in (w_out, w_gate, w_up, w_down))
    bounds = document_bounds(seg_row, row_count)
    q_ext, k_ext, v_ext = project_heads(
        seg_row.astype(F32), turn, pieces, w_heads.reshape(model_width, -1), held
    )
    sums, joined_own = attend_heads(bounds, q_ext, k_ext, v_ext, row_count)
    output, d_joined, dh_one, norms_part, packed = feed_forward(
        tokens, exchange(joined_own, 3), cotangent, full_out, full_gate, full_up, full_down, norms
    )
    depth = model_width // shards
    ff_blocks = full_gate.shape[1] // model_width
    owned = lax.psum_scatter(
        packed.reshape(-1, model_width), ("shard", "seq"), scatter_dimension=0, tiled=True
    )

    dout = exchange(d_joined, 4)
    d_heads = attend_back_heads(bounds, q_ext, k_ext, v_ext, sums, dout, turn)
    w_lanes = w_heads.reshape(model_width, -1)
    w_own = jnp.concatenate(
        [w_lanes[:, at : at + HD] for at in range(0, w_lanes.shape[1], LANES)], axis=1
    )
    input_grad, columns, norm_sums = scatter_gradients(d_heads, pieces, w_own, dh_one, norms_part, shards)
    columns, owned = lax.optimization_barrier((columns, owned))
    shared = gather_rows(owned)
    grad_gate, grad_up, grad_down, grad_out, grad_qkv = unpack_gradients(shared, columns, ff_blocks)
    shard = lax.axis_index("shard")
    norm_sums = lax.dynamic_slice_in_dim(norm_sums, shard * depth, depth, 1)
    return (
        output,
        input_grad,
        grad_qkv,
        grad_out,
        grad_gate,
        grad_up,
        grad_down,
        norm_sums[0],
        norm_sums[1],
        norm_sums[2],
        norm_sums[3],
    )


def solution(mesh):
    in_specs = (
        P("shard", "seq", None),
        P("shard", None),
        P("shard", "seq"),
        P("shard", "seq", None),
        P("shard", None),
        P("shard", None),
        P("shard", None),
        P("shard", None),
        P("shard", None),
        P("shard"),
        P("shard"),
        P("shard"),
        P("shard"),
    )
    out_specs = (
        P("shard", "seq", None),
        P("shard", "seq", None),
        P("shard", None),
        P("shard", None),
        P("shard", None),
        P("shard", None),
        P("shard", None),
        P("shard"),
        P("shard"),
        P("shard"),
        P("shard"),
    )
    body = functools.partial(local_heads, mesh.shape["shard"]) if (mesh.shape["seq"], mesh.shape["shard"]) == (SEQ_SIZE, GROUPS) else local
    return jax.shard_map(body, mesh=mesh, in_specs=in_specs, out_specs=out_specs, check_vma=False)
```

```python
import functools
import math

import jax
import jax.numpy as jnp
from jax import lax
from jax.experimental import pallas as pl
from jax.experimental.pallas import tpu as pltpu
from jax.sharding import PartitionSpec as P

HEADS = 12
HD = 64


EPS = 1e-05
ROPE_BASE = 1000.0


def rope_tables(pos_block):
    half_dim = HD // 2
    freqs = jnp.exp(jnp.arange(half_dim, dtype=jnp.float32) * (-math.log(ROPE_BASE) / half_dim))
    angle = pos_block.astype(jnp.float32)[..., None] * freqs
    return (jnp.cos(angle)[:, :, None, :], jnp.sin(angle)[:, :, None, :])


def rotate(heads, cos_b, sin_b):
    half_dim = heads.shape[-1] // 2
    first = heads[..., :half_dim]
    second = heads[..., half_dim:]
    return jnp.concatenate(
        [first * cos_b - second * sin_b, second * cos_b + first * sin_b], axis=-1
    )


def rotate_back(grads, cos_b, sin_b):
    half_dim = grads.shape[-1] // 2
    first = grads[..., :half_dim]
    second = grads[..., half_dim:]
    return jnp.concatenate(
        [first * cos_b + second * sin_b, second * cos_b - first * sin_b], axis=-1
    )


def norm_fwd(values, gain, bias):
    mean_val = jnp.mean(values, axis=-1, keepdims=True)
    centered = values - mean_val
    variance = jnp.mean(centered * centered, axis=-1, keepdims=True)
    inverse = lax.rsqrt(variance + EPS)
    normed = centered * inverse
    return (normed * gain + bias, normed, inverse)


def norm_back(grad_in, normed, inverse, gain):
    scaled = grad_in * gain
    return inverse * (
        scaled
        - jnp.mean(scaled, axis=-1, keepdims=True)
        - normed * jnp.mean(scaled * normed, axis=-1, keepdims=True)
    )


def head_split(block_rows, seq_count, row_count):
    return block_rows.reshape(seq_count, row_count, HEADS, HD)


def attend(q_heads, q_seg, k_full, v_full, seg_all, block, score_scale):
    seq_count, row_count = (q_heads.shape[0], q_heads.shape[1])
    block_count = k_full.shape[1] // block

    def attend_step(carry, index):
        row_total, value_sum = carry
        start = index * block
        k_part = head_split(lax.dynamic_slice_in_dim(k_full, start, block, 1), seq_count, block)
        v_part = head_split(lax.dynamic_slice_in_dim(v_full, start, block, 1), seq_count, block)
        seg_part = lax.dynamic_slice_in_dim(seg_all, start, block, 1)
        raw = (
            jnp.einsum("sqhd,skhd->shqk", q_heads, k_part, preferred_element_type=jnp.float32)
            * score_scale
        )
        same_doc = q_seg[:, None, :, None] == seg_part[:, None, None, :]
        expo = jnp.where(same_doc, jnp.exp(raw), 0.0)
        row_total = row_total + jnp.sum(expo, axis=-1)
        value_sum = value_sum + jnp.einsum(
            "shqk,skhd->sqhd", expo.astype(jnp.bfloat16), v_part, preferred_element_type=jnp.float32
        )
        return ((row_total, value_sum), None)

    start_carry = (
        jnp.zeros((seq_count, HEADS, row_count), jnp.float32),
        jnp.zeros((seq_count, row_count, HEADS, HD), jnp.float32),
    )
    final, unused = lax.scan(attend_step, start_carry, jnp.arange(block_count, dtype=jnp.int32))
    return final


def back_keys(q_heads, g_heads, delta, q_seg, k_full, v_full, seg_all, block, score_scale):
    seq_count, row_count = (q_heads.shape[0], q_heads.shape[1])
    full_len = k_full.shape[1]
    block_count = full_len // block

    def back_step(carry, index):
        start = index * block
        k_part = head_split(lax.dynamic_slice_in_dim(k_full, start, block, 1), seq_count, block)
        v_part = head_split(lax.dynamic_slice_in_dim(v_full, start, block, 1), seq_count, block)
        seg_part = lax.dynamic_slice_in_dim(seg_all, start, block, 1)
        raw = (
            jnp.einsum("sqhd,skhd->shqk", q_heads, k_part, preferred_element_type=jnp.float32)
            * score_scale
        )
        same_doc = q_seg[:, None, :, None] == seg_part[:, None, None, :]
        expo = jnp.where(same_doc, jnp.exp(raw), 0.0)
        prob_grad = jnp.einsum(
            "sqhd,skhd->shqk", g_heads, v_part, preferred_element_type=jnp.float32
        )
        d_score = (expo * (prob_grad - delta[..., None])).astype(jnp.bfloat16)
        q_grad = carry[0] + jnp.einsum(
            "shqk,skhd->sqhd", d_score, k_part, preferred_element_type=jnp.float32
        )
        k_grad = (
            jnp.einsum("shqk,sqhd->skhd", d_score, q_heads, preferred_element_type=jnp.float32)
            * score_scale
        )
        v_grad = jnp.einsum(
            "shqk,sqhd->skhd",
            expo.astype(jnp.bfloat16),
            g_heads,
            preferred_element_type=jnp.float32,
        )
        k_store = lax.dynamic_update_slice_in_dim(
            carry[1], k_grad.reshape(seq_count, block, HEADS * HD), start, 1
        )
        v_store = lax.dynamic_update_slice_in_dim(
            carry[2], v_grad.reshape(seq_count, block, HEADS * HD), start, 1
        )
        return ((q_grad, k_store, v_store), None)

    q_zero = jnp.zeros((seq_count, row_count, HEADS, HD), jnp.float32)
    kv_zero = jnp.zeros((seq_count, full_len, HEADS * HD), jnp.float32)
    start_carry = (q_zero, kv_zero, kv_zero)
    final, unused = lax.scan(back_step, start_carry, jnp.arange(block_count, dtype=jnp.int32))
    return (final[0] * score_scale,) + tuple(final[1:])


def local(
    tokens,
    segments,
    positions,
    cotangent,
    w_qkv,
    w_out,
    w_gate,
    w_up,
    w_down,
    ln1_gain,
    ln1_bias,
    ln2_gain,
    ln2_bias,
):
    seq_count, row_count, model_width = tokens.shape
    score_scale = HD ** (-0.5)
    q_seg = lax.dynamic_slice_in_dim(segments, lax.axis_index("seq") * row_count, row_count, 1)
    gathered = (
        lax.all_gather(w_qkv, "shard", axis=0, tiled=True),
        lax.all_gather(w_out, "shard", axis=0, tiled=True),
        lax.all_gather(w_gate, "shard", axis=0, tiled=True),
        lax.all_gather(w_up, "shard", axis=0, tiled=True),
        lax.all_gather(w_down, "shard", axis=0, tiled=True),
        lax.all_gather(ln1_gain, "shard", axis=0, tiled=True),
        lax.all_gather(ln1_bias, "shard", axis=0, tiled=True),
        lax.all_gather(ln2_gain, "shard", axis=0, tiled=True),
        lax.all_gather(ln2_bias, "shard", axis=0, tiled=True),
    )
    full_qkv, full_out, full_gate, full_up, full_down, gain_one, bias_one, gain_two, bias_two = (
        gathered
    )
    cos_b, sin_b = rope_tables(positions)
    qkv_all = jnp.einsum("scd,de->sce", tokens, full_qkv, preferred_element_type=jnp.float32)
    q_heads = rotate(
        head_split(qkv_all[..., :model_width], seq_count, row_count), cos_b, sin_b
    ).astype(jnp.bfloat16)
    k_heads = rotate(
        head_split(qkv_all[..., model_width : 2 * model_width], seq_count, row_count), cos_b, sin_b
    ).astype(jnp.bfloat16)
    v_heads = head_split(qkv_all[..., 2 * model_width :], seq_count, row_count).astype(jnp.bfloat16)
    k_local = k_heads.reshape(seq_count, row_count, model_width)
    v_local = v_heads.reshape(seq_count, row_count, model_width)
    k_full, v_full = (
        lax.all_gather(k_local, "seq", axis=1, tiled=True),
        lax.all_gather(v_local, "seq", axis=1, tiled=True),
    )
    row_total, value_sum = attend(q_heads, q_seg, k_full, v_full, segments, row_count, score_scale)
    denom = jnp.transpose(row_total, (0, 2, 1))[..., None]
    attn_out = value_sum / denom
    joined = attn_out.reshape(seq_count, row_count, model_width).astype(jnp.bfloat16)
    tokens_f = tokens.astype(jnp.float32)
    h_one = tokens_f + jnp.einsum(
        "sci,io->sco", joined, full_out, preferred_element_type=jnp.float32
    )
    x_one, normed_one, inverse_one = norm_fwd(
        h_one, gain_one.astype(jnp.float32), bias_one.astype(jnp.float32)
    )
    x_low = x_one.astype(jnp.bfloat16)
    gate_pre = jnp.einsum("scd,df->scf", x_low, full_gate, preferred_element_type=jnp.float32)
    up_pre = jnp.einsum("scd,df->scf", x_low, full_up, preferred_element_type=jnp.float32)
    sigma = jax.nn.sigmoid(gate_pre)
    smooth = gate_pre * sigma
    hidden = (smooth * up_pre).astype(jnp.bfloat16)
    h_two = x_one + jnp.einsum("scf,fd->scd", hidden, full_down, preferred_element_type=jnp.float32)
    result, normed_two, inverse_two = norm_fwd(
        h_two, gain_two.astype(jnp.float32), bias_two.astype(jnp.float32)
    )
    output = result.astype(jnp.bfloat16)
    regathered = (
        lax.all_gather(w_qkv, "shard", axis=0, tiled=True),
        lax.all_gather(w_out, "shard", axis=0, tiled=True),
        lax.all_gather(w_gate, "shard", axis=0, tiled=True),
        lax.all_gather(w_up, "shard", axis=0, tiled=True),
        lax.all_gather(w_down, "shard", axis=0, tiled=True),
        lax.all_gather(ln1_gain, "shard", axis=0, tiled=True),
        lax.all_gather(ln2_gain, "shard", axis=0, tiled=True),
    )
    back_qkv, back_out, back_gate, back_up, back_down, back_gain_one, back_gain_two = regathered
    back_k, back_v = (
        lax.all_gather(k_local, "seq", axis=1, tiled=True),
        lax.all_gather(v_local, "seq", axis=1, tiled=True),
    )
    cot_f = cotangent.astype(jnp.float32)
    grad_gain_two = jnp.sum(cot_f * normed_two, axis=(0, 1))
    grad_bias_two = jnp.sum(cot_f, axis=(0, 1))
    dh_two = norm_back(cot_f, normed_two, inverse_two, back_gain_two.astype(jnp.float32))
    dm_low = dh_two.astype(jnp.bfloat16)
    grad_down = jnp.einsum("scf,scd->fd", hidden, dm_low, preferred_element_type=jnp.float32)
    d_hidden = jnp.einsum("scd,fd->scf", dm_low, back_down, preferred_element_type=jnp.float32)
    d_up = (d_hidden * smooth).astype(jnp.bfloat16)
    d_gate = (d_hidden * up_pre * sigma * (1.0 + gate_pre * (1.0 - sigma))).astype(jnp.bfloat16)
    grad_gate = jnp.einsum("scd,scf->df", x_low, d_gate, preferred_element_type=jnp.float32)
    grad_up = jnp.einsum("scd,scf->df", x_low, d_up, preferred_element_type=jnp.float32)
    dx_one = (
        dh_two
        + jnp.einsum("scf,df->scd", d_gate, back_gate, preferred_element_type=jnp.float32)
        + jnp.einsum("scf,df->scd", d_up, back_up, preferred_element_type=jnp.float32)
    )
    grad_gain_one = jnp.sum(dx_one * normed_one, axis=(0, 1))
    grad_bias_one = jnp.sum(dx_one, axis=(0, 1))
    dh_one = norm_back(dx_one, normed_one, inverse_one, back_gain_one.astype(jnp.float32))
    d_attn = dh_one.astype(jnp.bfloat16)
    grad_out = jnp.einsum("sci,sco->io", joined, d_attn, preferred_element_type=jnp.float32)
    d_joined = jnp.einsum(
        "sco,io->sci", d_attn, back_out, preferred_element_type=jnp.float32
    ).astype(jnp.bfloat16)
    d_heads = head_split(d_joined, seq_count, row_count).astype(jnp.float32)
    g_heads = (d_heads / denom).astype(jnp.bfloat16)
    delta = jnp.transpose(jnp.sum(d_heads * attn_out, axis=-1) / denom[..., 0], (0, 2, 1))
    q_grad, k_all, v_all = back_keys(
        q_heads, g_heads, delta, q_seg, back_k, back_v, segments, row_count, score_scale
    )
    k_sum, v_sum = (
        lax.psum_scatter(k_all.astype(jnp.bfloat16), "seq", scatter_dimension=1, tiled=True).astype(
            jnp.float32
        ),
        lax.psum_scatter(v_all.astype(jnp.bfloat16), "seq", scatter_dimension=1, tiled=True).astype(
            jnp.float32
        ),
    )
    k_grad = head_split(k_sum, seq_count, row_count)
    v_grad = head_split(v_sum, seq_count, row_count)
    q_back = rotate_back(q_grad, cos_b, sin_b).reshape(seq_count, row_count, model_width)
    k_back = rotate_back(k_grad, cos_b, sin_b).reshape(seq_count, row_count, model_width)
    d_qkv = jnp.concatenate(
        [q_back, k_back, v_grad.reshape(seq_count, row_count, model_width)], axis=-1
    ).astype(jnp.bfloat16)
    grad_qkv = jnp.einsum("scd,sce->de", tokens, d_qkv, preferred_element_type=jnp.float32)
    d_tokens = dh_one + jnp.einsum(
        "sce,de->scd", d_qkv, back_qkv, preferred_element_type=jnp.float32
    )
    input_grad = d_tokens.astype(jnp.bfloat16)
    owned = (
        lax.psum_scatter(
            grad_qkv.astype(jnp.bfloat16), "shard", scatter_dimension=0, tiled=True
        ).astype(jnp.float32),
        lax.psum_scatter(
            grad_out.astype(jnp.bfloat16), "shard", scatter_dimension=0, tiled=True
        ).astype(jnp.float32),
        lax.psum_scatter(
            grad_gate.astype(jnp.bfloat16), "shard", scatter_dimension=0, tiled=True
        ).astype(jnp.float32),
        lax.psum_scatter(
            grad_up.astype(jnp.bfloat16), "shard", scatter_dimension=0, tiled=True
        ).astype(jnp.float32),
        lax.psum_scatter(
            grad_down.astype(jnp.bfloat16), "shard", scatter_dimension=0, tiled=True
        ).astype(jnp.float32),
        lax.psum_scatter(
            grad_gain_one.astype(jnp.bfloat16), "shard", scatter_dimension=0, tiled=True
        ).astype(jnp.float32),
        lax.psum_scatter(
            grad_bias_one.astype(jnp.bfloat16), "shard", scatter_dimension=0, tiled=True
        ).astype(jnp.float32),
        lax.psum_scatter(
            grad_gain_two.astype(jnp.bfloat16), "shard", scatter_dimension=0, tiled=True
        ).astype(jnp.float32),
        lax.psum_scatter(
            grad_bias_two.astype(jnp.bfloat16), "shard", scatter_dimension=0, tiled=True
        ).astype(jnp.float32),
    )
    summed = (
        lax.psum(owned[0].astype(jnp.bfloat16), "seq").astype(jnp.float32),
        lax.psum(owned[1].astype(jnp.bfloat16), "seq").astype(jnp.float32),
        lax.psum(owned[2].astype(jnp.bfloat16), "seq").astype(jnp.float32),
        lax.psum(owned[3].astype(jnp.bfloat16), "seq").astype(jnp.float32),
        lax.psum(owned[4].astype(jnp.bfloat16), "seq").astype(jnp.float32),
        lax.psum(owned[5].astype(jnp.bfloat16), "seq").astype(jnp.float32),
        lax.psum(owned[6].astype(jnp.bfloat16), "seq").astype(jnp.float32),
        lax.psum(owned[7].astype(jnp.bfloat16), "seq").astype(jnp.float32),
        lax.psum(owned[8].astype(jnp.bfloat16), "seq").astype(jnp.float32),
    )
    return (
        output,
        input_grad,
        summed[0],
        summed[1],
        summed[2],
        summed[3],
        summed[4],
        summed[5],
        summed[6],
        summed[7],
        summed[8],
    )


SEQS_HELD = 2
SEQ_SIZE = 8
GROUPS = 4
LANES = 128
LOG2E = 1.4426950408889634
LN2 = 0.6931471805599453
FAR = 2.0**30
F32 = jnp.float32
BF16 = jnp.bfloat16
VMEM_LIMIT = 60 * 1024 * 1024
FEED_LIMIT = 63 * 1024 * 1024
BY_MESH = pl.DeviceIdType.MESH
BY_LANES = (((1,), (1,)), ((), ()))


def packed_heads(rows):
    return rows + rows // 2


def unpack_heads(block):
    rows = block.shape[0] * 2 // 3
    last = block[rows:]
    third = jnp.concatenate([last[:, :HD], last[:, HD:]], axis=0)
    return jnp.concatenate([block[:rows], third], axis=1)


def pack_heads(value):
    rows = value.shape[0]
    third = value[:, 2 * HD :]
    return value[:, : 2 * HD], jnp.concatenate([third[: rows // 2], third[rows // 2 :]], axis=1)


def flip(index, bit):
    return index + bit - 2 * bit * lax.rem(lax.div(index, bit), 2)


def gather_kernel(
    chunks, by_z, tok_ref, w_ref, n_ref, place_ref, freq_ref, all_ref, w_all_ref, n_all_ref, turn_ref, send, recv, kept, w_send, w_recv
):
    me = lax.axis_index("seq")
    shard = lax.axis_index("shard")
    shards = w_all_ref.shape[0]
    half = lax.div(me, GROUPS)
    y_near, z_near, partner = flip(me, 1), flip(me, 2), flip(me, 4)
    barrier = pltpu.get_barrier_semaphore()
    for device in (y_near, z_near, partner):
        pl.semaphore_signal(barrier, inc=1, device_id={"seq": device}, device_id_type=BY_MESH)
    for step in range(1, shards):
        pl.semaphore_signal(
            barrier, inc=1, device_id={"shard": lax.rem(shard + step, shards)}, device_id_type=BY_MESH
        )
    pl.semaphore_wait(barrier, 2 + shards)

    part = tok_ref.shape[1] // chunks
    started = []

    def go(source, target, slot, device):
        copy = pltpu.make_async_remote_copy(
            src_ref=source,
            dst_ref=target,
            send_sem=send.at[slot],
            recv_sem=recv.at[slot],
            device_id={"seq": device},
            device_id_type=BY_MESH,
        )
        copy.start()
        started.append(copy)
        return copy

    def rows(chunk):
        return pl.ds(chunk * part, part)

    def relay(piece, chunk, slot, device):
        return go(all_ref.at[piece, rows(chunk)], all_ref.at[piece, rows(chunk)], slot * chunks + chunk, device)

    def own(which, chunk, slot, device):
        return go(tok_ref.at[which, rows(chunk)], all_ref.at[me, rows(chunk)], slot * chunks + chunk, device)

    own_y, own_z, crossing = [], [], []
    for chunk in range(chunks):
        own_y.append(own(half, chunk, 1, y_near))
        crossing.append(own(1 - half, chunk, 0, partner))
        own_z.append(own(half, chunk, 2, z_near))
    weights = []
    for step in range(1, shards):
        copy = pltpu.make_async_remote_copy(
            src_ref=w_ref,
            dst_ref=w_all_ref.at[shard],
            send_sem=w_send.at[step],
            recv_sem=w_recv.at[step],
            device_id={"shard": lax.rem(shard + step, shards)},
            device_id_type=BY_MESH,
        )
        copy.start()
        weights.append(copy)
        copy = pltpu.make_async_remote_copy(
            src_ref=n_ref,
            dst_ref=n_all_ref.at[shard],
            send_sem=w_send.at[shards + step],
            recv_sem=w_recv.at[shards + step],
            device_id={"shard": lax.rem(shard + step, shards)},
            device_id_type=BY_MESH,
        )
        copy.start()
        weights.append(copy)
    keep_n = pltpu.make_async_copy(n_ref, n_all_ref.at[shard], kept.at[2])
    keep_n.start()
    keep_tok = pltpu.make_async_copy(tok_ref.at[half], all_ref.at[me], kept.at[0])
    keep_tok.start()
    keep_w = pltpu.make_async_copy(w_ref, w_all_ref.at[shard], kept.at[1])
    keep_w.start()

    def turn_piece(index, carry):
        count = turn_ref.shape[0] // place_ref.shape[0]
        lane = lax.broadcasted_iota(jnp.int32, (count, LANES), 1)
        place = jnp.transpose(jnp.broadcast_to(place_ref[index], (LANES, count)))
        angle = place * freq_ref[...]
        turn_ref[pl.ds(pl.multiple_of(index * count, count), count), :] = jnp.where(
            lane < HD, jnp.cos(angle), jnp.sin(angle)
        )
        return carry

    lax.fori_loop(0, place_ref.shape[0], turn_piece, 0)

    cross_y, cross_z, corner = [], [], []
    for chunk in range(chunks):
        own_y[chunk].wait_recv()
        if chunk < by_z:
            corner.append(relay(y_near, chunk, 5, z_near))
        own_z[chunk].wait_recv()
        if chunk >= by_z:
            corner.append(relay(z_near, chunk, 5, y_near))
        crossing[chunk].wait_recv()
        cross_y.append(relay(partner, chunk, 3, y_near))
        cross_z.append(relay(partner, chunk, 4, z_near))
    for chunk in range(chunks):
        cross_y[chunk].wait_recv()
        if chunk < by_z:
            corner.append(relay(flip(y_near, 4), chunk, 6, z_near))
        cross_z[chunk].wait_recv()
        if chunk >= by_z:
            corner.append(relay(flip(z_near, 4), chunk, 6, y_near))
    for copy in corner:
        copy.wait_recv()
    for copy in weights:
        copy.wait()
    keep_tok.wait()
    keep_w.wait()
    keep_n.wait()
    for copy in started:
        copy.wait_send()


def gather_tokens(tokens, w_part, norms, place, freq, shards, chunks=8, by_z=2):
    seqs, rows, width = tokens.shape
    anywhere = pl.BlockSpec(memory_space=pl.ANY)
    vmem = pl.BlockSpec(memory_space=pltpu.VMEM)
    return pl.pallas_call(
        functools.partial(gather_kernel, chunks, by_z),
        out_shape=(
            jax.ShapeDtypeStruct((SEQ_SIZE, rows, width), tokens.dtype),
            jax.ShapeDtypeStruct((shards,) + w_part.shape, w_part.dtype),
            jax.ShapeDtypeStruct((shards,) + norms.shape, norms.dtype),
            jax.ShapeDtypeStruct((place.shape[0] * place.shape[2], LANES), F32),
        ),
        in_specs=[anywhere, anywhere, anywhere, vmem, vmem],
        out_specs=(anywhere, anywhere, anywhere, vmem),
        scratch_shapes=[
            pltpu.SemaphoreType.DMA((7 * chunks,)),
            pltpu.SemaphoreType.DMA((7 * chunks,)),
            pltpu.SemaphoreType.DMA((3,)),
            pltpu.SemaphoreType.DMA((2 * shards,)),
            pltpu.SemaphoreType.DMA((2 * shards,)),
        ],
        compiler_params=pltpu.CompilerParams(collective_id=1, has_side_effects=True),
        name="gather_tokens",
    )(tokens, w_part, norms, place, freq)


def project_kernel(seg_ref, turn_ref, x_ref, w_ref, q_ref, k_ref, v_ref):
    rows = x_ref.shape[1]
    held = q_ref.shape[0]
    lane = lax.broadcasted_iota(jnp.int32, (rows, LANES), 1)
    seg = jnp.transpose(jnp.broadcast_to(seg_ref[0], (LANES, rows)))
    turn = turn_ref[...]
    cos_b = jnp.where(lane < HD, turn, 0.0)
    sin_b = jnp.where(lane < HD, pltpu.roll(turn, HD, 1), 0.0)
    sin_b = jnp.where(lane < HD // 2, -sin_b, sin_b)
    same = seg == (lane - HD).astype(F32)
    q_tail = jnp.where(same, 1.0, 0.0)
    k_tail = jnp.where(same | (lane < HD), 0.0, -FAR)
    v_tail = jnp.where(lane < HD, 0.0, 1.0)
    scale = HD ** (-0.5) * LOG2E
    q_cos, q_sin = cos_b * scale, sin_b * scale
    width = held * LANES
    for part in range(3):
        mixed = jnp.dot(x_ref[0], w_ref[:, part * width : (part + 1) * width], preferred_element_type=F32)
        for head in range(held):
            value = mixed[:, head * LANES : (head + 1) * LANES]
            if part == 0:
                value = value * q_cos + pltpu.roll(value, HD // 2, 1) * q_sin + q_tail
                q_ref[head] = value.astype(BF16)
            elif part == 1:
                value = value * cos_b + pltpu.roll(value, HD // 2, 1) * sin_b + k_tail
                k_ref[head] = value.astype(BF16)
            else:
                v_ref[head] = (value + v_tail).astype(BF16)


def project_heads(seg_row, turn, pieces, w_full, held):
    count, rows, width = pieces.shape
    length = count * rows
    row_spec = pl.BlockSpec((1, 1, rows), lambda i: (i, 0, 0))
    head_spec = pl.BlockSpec((held, rows, LANES), lambda i: (0, i, 0))
    head_shape = jax.ShapeDtypeStruct((held, length, LANES), BF16)
    return pl.pallas_call(
        project_kernel,
        out_shape=(head_shape, head_shape, head_shape),
        grid=(count,),
        in_specs=[
            row_spec,
            pl.BlockSpec((rows, LANES), lambda i: (i, 0)),
            pl.BlockSpec((1, rows, width), lambda i: (i, 0, 0)),
            pl.BlockSpec(w_full.shape, lambda i: (0, 0)),
        ],
        out_specs=(head_spec, head_spec, head_spec),
        compiler_params=pltpu.CompilerParams(vmem_limit_bytes=VMEM_LIMIT),
        cost_estimate=pl.CostEstimate(
            flops=2 * length * width * w_full.shape[1],
            bytes_accessed=length * (width * 2 + held * LANES * 6 + LANES * 4),
            transcendentals=length * LANES,
        ),
        name="project_heads",
    )(seg_row.reshape(count, 1, rows), turn, pieces, w_full)


def document_bounds(seg_row, rows):
    first = seg_row[::rows]
    last = seg_row[rows - 1 :: rows]
    low = jnp.sum((seg_row[None, :] < first[:, None]).astype(jnp.int32), axis=1)
    high = jnp.sum((seg_row[None, :] <= last[:, None]).astype(jnp.int32), axis=1)
    return low, high


def windows(bounds, length, window, align):
    low = bounds[0] // align * align
    count = (bounds[1] - low + window - 1) // window
    return jnp.minimum(low, length - count * window), count


def attend_kernel(window, align, low_ref, count_ref, q_ref, k_ref, v_ref, sum_ref, joined_ref):
    block = pl.program_id(0)
    low = low_ref[block]
    sum_ref[...] = jnp.zeros_like(sum_ref)

    def step(index, carry):
        start = pl.multiple_of(low + index * window, align)
        for head in range(q_ref.shape[0]):
            k_part = k_ref[head, pl.ds(start, window), :]
            v_part = v_ref[head, pl.ds(start, window), :]
            score = lax.dot_general(q_ref[head], k_part, BY_LANES, preferred_element_type=F32)
            expo = jnp.exp2(score).astype(BF16)
            sum_ref[head] += jnp.dot(expo, v_part, preferred_element_type=F32)
        return carry

    lax.fori_loop(0, count_ref[block], step, 0)
    rows = q_ref.shape[1]
    parts = [sum_ref[head][:, :HD] / sum_ref[head][:, HD : HD + 1] for head in range(q_ref.shape[0])]
    first, last = pack_heads(jnp.concatenate(parts, axis=1))
    joined_ref[0, :rows] = first.astype(BF16)
    joined_ref[0, rows:] = last.astype(BF16)


def attend_heads(bounds, q_ext, k_ext, v_ext, rows, window=1024, align=16):
    heads, length, lanes = q_ext.shape
    low, count = windows(bounds, length, window, align)
    whole = pl.BlockSpec((heads, length, lanes), lambda i, *_: (0, 0, 0))
    part = pl.BlockSpec((heads, rows, lanes), lambda i, *_: (0, i, 0))
    return pl.pallas_call(
        functools.partial(attend_kernel, window, align),
        out_shape=(
            jax.ShapeDtypeStruct((heads, length, lanes), F32),
            jax.ShapeDtypeStruct((length // rows, packed_heads(rows), LANES), BF16),
        ),
        grid_spec=pltpu.PrefetchScalarGridSpec(
            num_scalar_prefetch=2,
            grid=(length // rows,),
            in_specs=[part, whole, whole],
            out_specs=(part, pl.BlockSpec((1, packed_heads(rows), LANES), lambda i, *_: (i, 0, 0))),
        ),
        compiler_params=pltpu.CompilerParams(vmem_limit_bytes=VMEM_LIMIT),
        cost_estimate=pl.CostEstimate(
            flops=heads * length * length * 4 * lanes // 2,
            bytes_accessed=heads * length * lanes * 10,
            transcendentals=heads * length * length // 2,
        ),
        name="attend_heads",
    )(low, count, q_ext, k_ext, v_ext)


def attend_back_kernel(
    align,
    low_ref,
    count_ref,
    q_ref,
    sum_ref,
    dout_ref,
    turn_ref,
    k_ref,
    v_ref,
    d_ref,
    dq_ref,
    dkv_ref,
    g_ref,
    gt_ref,
    qt_ref,
):
    block = pl.program_id(0)
    heads, rows, lanes = q_ref.shape
    width = heads * HD

    @pl.when(block == 0)
    def _():
        dkv_ref[...] = jnp.zeros_like(dkv_ref)

    dq_ref[...] = jnp.zeros_like(dq_ref)
    half_lane = lax.broadcasted_iota(jnp.int32, (rows, HD), 1)
    dout_all = unpack_heads(dout_ref[0].astype(F32))
    for head in range(heads):
        dout = dout_all[:, head * HD : (head + 1) * HD]
        sums = sum_ref[head]
        total = sums[:, HD : HD + 1]
        g_low = dout / total
        delta = -jnp.sum(dout * sums[:, :HD], axis=1, keepdims=True) / (total * total)
        high = delta.astype(BF16).astype(F32)
        middle = (delta - high).astype(BF16).astype(F32)
        tail = jnp.where(
            half_lane == 0,
            high,
            jnp.where(half_lane == 1, middle, jnp.where(half_lane == 2, delta - high - middle, 0.0)),
        )
        g_ext = jnp.concatenate([g_low, tail], axis=1)
        g_ref[head] = g_ext.astype(BF16)
        gt_ref[head] = jnp.transpose(g_ext)[:HD].astype(BF16)
        qt_ref[head] = jnp.transpose(q_ref[head].astype(F32))[:HD].astype(BF16)

    low = low_ref[block]

    def step(window, low, index, carry):
        start = pl.multiple_of(low + index * window, align)
        for head in range(heads):
            k_part = k_ref[head, pl.ds(start, window), :]
            v_part = v_ref[head, pl.ds(start, window), :]
            score = lax.dot_general(q_ref[head], k_part, BY_LANES, preferred_element_type=F32)
            slope = lax.dot_general(g_ref[head], v_part, BY_LANES, preferred_element_type=F32)
            expo = jnp.exp2(score)
            d_score = (expo * slope).astype(BF16)
            expo = expo.astype(BF16)
            dq_ref[head] += jnp.dot(d_score, k_part, preferred_element_type=F32)
            dkv_ref[head, :HD, pl.ds(start, window)] += jnp.dot(qt_ref[head], d_score, preferred_element_type=F32)
            dkv_ref[head, HD:, pl.ds(start, window)] += jnp.dot(gt_ref[head], expo, preferred_element_type=F32)
        return carry

    units = count_ref[block]
    many = lax.div(units, 4)
    rest = lax.rem(units, 4)
    lax.fori_loop(0, many, functools.partial(step, 4 * align, low), 0)
    low = low + many * 4 * align

    @pl.when(rest >= 2)
    def _():
        step(2 * align, low, 0, 0)

    @pl.when(lax.rem(rest, 2) == 1)
    def _():
        step(align, low + lax.div(rest, 2) * 2 * align, 0, 0)

    lane = lax.broadcasted_iota(jnp.int32, (rows, lanes), 1)

    def turn_back(value, turn):
        swapped = jnp.where(lane < HD // 2, pltpu.roll(value, lanes - HD // 2, 1), pltpu.roll(value, HD // 2, 1))
        sine = pltpu.roll(turn, HD, 1)
        sine = jnp.where(lane < HD // 2, sine, -sine)
        return (value * turn + swapped * sine)[:, :HD]

    here = turn_ref[pl.ds(pl.multiple_of(block * rows, rows), rows), :]
    for head in range(heads):
        turned = turn_back(dq_ref[head] * HD ** (-0.5), here)
        d_ref[block, :, head * HD : (head + 1) * HD] = turned.astype(BF16)

    @pl.when(block == pl.num_programs(0) - 1)
    def _():
        def finish(piece, carry):
            start = pl.multiple_of(piece * rows, rows)
            turn = turn_ref[pl.ds(start, rows), :]
            for head in range(heads):
                both = jnp.transpose(dkv_ref[head, :, pl.ds(start, rows)])
                at = width + head * HD
                d_ref[piece, :, at : at + HD] = (turn_back(both, turn) * LN2).astype(BF16)
                d_ref[piece, :, width + at : width + at + HD] = both[:, HD:].astype(BF16)
            return carry

        lax.fori_loop(0, d_ref.shape[0], finish, 0)


def attend_back_heads(bounds, q_ext, k_ext, v_ext, sums, dout, turn, align=128):
    heads, length, lanes = q_ext.shape
    count_blocks = dout.shape[0]
    rows, width = length // count_blocks, heads * HD
    low, count = windows(bounds, length, align, align)
    whole = pl.BlockSpec((heads, length, lanes), lambda i, *_: (0, 0, 0))
    part = pl.BlockSpec((heads, rows, lanes), lambda i, *_: (0, i, 0))
    return pl.pallas_call(
        functools.partial(attend_back_kernel, align),
        out_shape=jax.ShapeDtypeStruct((count_blocks, rows, 3 * width), BF16),
        grid_spec=pltpu.PrefetchScalarGridSpec(
            num_scalar_prefetch=2,
            grid=(count_blocks,),
            in_specs=[
                part,
                part,
                pl.BlockSpec((1,) + dout.shape[1:], lambda i, *_: (i, 0, 0)),
                pl.BlockSpec((length, lanes), lambda i, *_: (0, 0)),
                whole,
                whole,
            ],
            out_specs=pl.BlockSpec((count_blocks, rows, 3 * width), lambda i, *_: (0, 0, 0)),
            scratch_shapes=[
                pltpu.VMEM((heads, rows, lanes), F32),
                pltpu.VMEM((heads, 2 * HD, length), F32),
                pltpu.VMEM((heads, rows, lanes), BF16),
                pltpu.VMEM((heads, HD, rows), BF16),
                pltpu.VMEM((heads, HD, rows), BF16),
            ],
        ),
        compiler_params=pltpu.CompilerParams(vmem_limit_bytes=VMEM_LIMIT),
        cost_estimate=pl.CostEstimate(
            flops=heads * length * length * 10 * lanes // 2,
            bytes_accessed=heads * length * lanes * 20,
            transcendentals=heads * length * length // 2,
        ),
        name="attend_back_heads",
    )(low, count, q_ext, sums, dout, turn, k_ext, v_ext)


def scatter_kernel(
    chunks,
    by_z,
    d_hbm,
    x_hbm,
    w_ref,
    dh_hbm,
    norm_ref,
    out_hbm,
    gw_all_ref,
    norm_out_ref,
    d_ref,
    x_ref,
    part_ref,
    gw_sum,
    gw_ref,
    dh_ref,
    out_ref,
    got_y,
    got_z,
    relay_y,
    relay_z,
    sent_y,
    sent_z,
    cross_out,
    cross_in,
    gw_got,
    gw_mine,
    gw_pair,
    gw_final,
    norm_got,
    norm_sent,
    send,
    recv,
    gw_send,
    gw_recv,
    norm_send,
    norm_recv,
    kept,
):
    me = lax.axis_index("seq")
    shard = lax.axis_index("shard")
    shards = gw_ref.shape[0]
    half = lax.div(me, GROUPS)
    y_near, z_near, partner = flip(me, 1), flip(me, 2), flip(me, 4)
    corner = flip(y_near, 2)
    barrier = pltpu.get_barrier_semaphore()
    for n in range(1, SEQ_SIZE):
        pl.semaphore_signal(
            barrier, inc=1, device_id={"seq": lax.rem(me + n, SEQ_SIZE)}, device_id_type=BY_MESH
        )
    for step in range(1, shards):
        pl.semaphore_signal(
            barrier, inc=1, device_id={"shard": lax.rem(shard + step, shards)}, device_id_type=BY_MESH
        )
    pl.semaphore_wait(barrier, SEQ_SIZE + shards - 2)

    started = []

    def go(source, target, sends, receives, slot, where):
        copy = pltpu.make_async_remote_copy(
            src_ref=source,
            dst_ref=target,
            send_sem=sends.at[slot],
            recv_sem=receives.at[slot],
            device_id=where,
            device_id_type=BY_MESH,
        )
        copy.start()
        started.append(copy)
        return copy

    rows = part_ref.shape[1] // chunks

    def band(chunk):
        return pl.ds(chunk * rows, rows)

    def piece(device, far):
        return flip(device, 4) if far else device

    def slot(kind, far, chunk):
        return (kind * 2 + (0 if far else 1)) * chunks + chunk

    def other(mask):
        index = 0
        for bit in (1, 2, 4):
            here, there = lax.rem(lax.div(me, bit), 2), lax.rem(lax.div(mask, bit), 2)
            index = index + bit * (here + there - 2 * here * there)
        return index

    masks = (7, 6, 5, 3, 2, 1, 4, 0)

    def fetch(mask, place):
        return pltpu.make_async_copy(d_hbm.at[other(mask)], d_ref.at[other(mask)], kept.at[8 + place])

    for place, mask in enumerate(masks):
        fetch(mask, place).start()
    loads = [
        pltpu.make_async_copy(dh_hbm, dh_ref, kept.at[4]),
        pltpu.make_async_copy(x_hbm, x_ref, kept.at[5]),
    ]
    for copy in loads:
        copy.start()

    def project(count, first, place):
        def body(n, carry):
            mask = first(n)
            fetch(mask, place + n).wait()
            index = other(mask)
            part_ref[index] = lax.dot_general(
                d_ref[index], w_ref[...], BY_LANES, preferred_element_type=F32
            ).astype(BF16)
            return carry

        lax.fori_loop(0, count, body, 0)

    norm_seq = [
        go(norm_ref, norm_got.at[n], norm_send, norm_recv, n, {"seq": lax.rem(me + n + 1, SEQ_SIZE)})
        for n in range(SEQ_SIZE - 1)
    ]

    from_corner, direct = {}, {}

    def send_pieces(far):
        for chunk in range(chunks):
            over_z = chunk < by_z
            from_corner[far, chunk] = go(
                part_ref.at[piece(corner, far), band(chunk)],
                (relay_y if over_z else relay_z).at[0 if far else 1, chunk if over_z else chunk - by_z],
                send,
                recv,
                slot(0, far, chunk),
                {"seq": y_near if over_z else z_near},
            )
        for chunk in range(chunks):
            over_z = chunk < by_z
            direct[far, chunk] = go(
                part_ref.at[piece(y_near if over_z else z_near, far), band(chunk)],
                (got_y if over_z else got_z).at[0 if far else 1, band(chunk)],
                send,
                recv,
                slot(1 if over_z else 2, far, chunk),
                {"seq": y_near if over_z else z_near},
            )

    project(3, lambda n: 7 - n, 0)
    send_pieces(True)
    project(3, lambda n: 3 - n, 3)
    project(2, lambda n: 4 - 4 * n, 6)
    relayed = {}

    def relay(far, chunk):
        over_z = chunk < by_z
        target = z_near if over_z else y_near
        index = chunk if over_z else chunk - by_z
        which = 0 if far else 1
        from_corner[far, chunk].wait_recv()
        source = relay_y if over_z else relay_z
        buffer = sent_y if over_z else sent_z
        passed = part_ref[piece(target, far), band(chunk)].astype(F32)
        buffer[which, index] = (source[which, index].astype(F32) + passed).astype(BF16)
        relayed[far, chunk] = go(
            buffer.at[which, index],
            (got_z if over_z else got_y).at[which, band(chunk)],
            send,
            recv,
            slot(2 if over_z else 1, far, chunk),
            {"seq": target},
        )

    def total(far, chunk):
        which = 0 if far else 1
        direct[far, chunk].wait_recv()
        relayed[far, chunk].wait_recv()
        return part_ref[piece(me, far), band(chunk)].astype(F32) + got_y[which, band(chunk)].astype(F32) + got_z[which, band(chunk)].astype(F32)

    for chunk in range(chunks):
        relay(True, chunk)
    send_pieces(False)
    for copy in loads:
        copy.wait()
    gw_sum[...] = jnp.zeros_like(gw_sum)

    def grow(n, carry):
        gw_sum[...] += lax.dot_general(
            x_ref[n], d_ref[n], (((0,), (0,)), ((), ())), preferred_element_type=F32
        )
        return carry

    lax.fori_loop(0, d_ref.shape[0], grow, 0)
    depth = gw_ref.shape[1]
    for owner in range(shards):
        gw_ref[owner] = gw_sum[owner * depth : (owner + 1) * depth, :].astype(BF16)
    gw_one = [
        go(
            gw_ref.at[lax.rem(shard + step, shards)],
            gw_got.at[step - 1],
            gw_send,
            gw_recv,
            step - 1,
            {"shard": lax.rem(shard + step, shards)},
        )
        for step in range(1, shards)
    ]
    norm_total = norm_ref[...]
    for n, copy in enumerate(norm_seq):
        copy.wait_recv()
        norm_total = norm_total + norm_got[n]
    norm_sent[...] = norm_total
    for copy in gw_one:
        copy.wait_recv()
    summed = gw_ref[shard].astype(F32)
    for step in range(1, shards):
        summed = summed + gw_got[step - 1].astype(F32)
    gw_mine[...] = summed.astype(BF16)
    gw_two = go(gw_mine, gw_pair, gw_send, gw_recv, shards - 1, {"seq": partner})
    norm_shard = [
        go(
            norm_sent,
            norm_got.at[SEQ_SIZE - 2 + step],
            norm_send,
            norm_recv,
            SEQ_SIZE - 2 + step,
            {"shard": lax.rem(shard + step, shards)},
        )
        for step in range(1, shards)
    ]
    crossing = []
    for chunk in range(chunks):
        cross_out[band(chunk)] = total(True, chunk).astype(BF16)
        crossing.append(
            go(cross_out.at[band(chunk)], cross_in.at[band(chunk)], send, recv, slot(3, True, chunk), {"seq": partner})
        )
    for chunk in range(chunks):
        relay(False, chunk)
    gw_two.wait_recv()
    gw_final[...] = (gw_mine[...].astype(F32) + gw_pair[...].astype(F32)).astype(BF16)
    group = lax.rem(me, GROUPS)
    gw_three = [
        go(gw_final, gw_all_ref.at[group], gw_send, gw_recv, shards + n, {"seq": device})
        for n, device in enumerate((y_near, z_near, corner))
    ]
    keep = pltpu.make_async_copy(gw_final, gw_all_ref.at[group], kept.at[0])
    keep.start()
    for chunk in range(chunks):
        out_ref[0, band(chunk)] = (total(False, chunk) + dh_ref[half, band(chunk)]).astype(BF16)
    out_near = pltpu.make_async_copy(out_ref.at[0], out_hbm.at[half], kept.at[2])
    out_near.start()
    norm_total = norm_sent[...]
    for step, copy in enumerate(norm_shard):
        copy.wait_recv()
        norm_total = norm_total + norm_got[SEQ_SIZE - 1 + step]
    norm_out_ref[...] = norm_total
    for chunk in range(chunks):
        crossing[chunk].wait_recv()
        other = 1 - half
        out_ref[1, band(chunk)] = (cross_in[band(chunk)].astype(F32) + dh_ref[other, band(chunk)]).astype(BF16)
    out_far = pltpu.make_async_copy(out_ref.at[1], out_hbm.at[1 - half], kept.at[3])
    out_far.start()
    for copy in gw_three:
        copy.wait_recv()
    keep.wait()
    out_near.wait()
    out_far.wait()
    for copy in started:
        copy.wait_send()


def scatter_gradients(d_heads, pieces, w_own, dh_one, norms, shards, chunks=4, by_z=3):
    _, rows, width = pieces.shape
    columns = d_heads.shape[2]
    depth = width // shards
    part = rows // chunks
    hbm = pl.BlockSpec(memory_space=pltpu.HBM)
    vmem = pl.BlockSpec(memory_space=pltpu.VMEM)
    dma = pltpu.SemaphoreType.DMA
    return pl.pallas_call(
        functools.partial(scatter_kernel, chunks, by_z),
        out_shape=(
            jax.ShapeDtypeStruct(dh_one.shape, BF16),
            jax.ShapeDtypeStruct((GROUPS, depth, columns), BF16),
            jax.ShapeDtypeStruct(norms.shape, F32),
        ),
        in_specs=[hbm, hbm, vmem, hbm, vmem],
        out_specs=(hbm, vmem, vmem),
        scratch_shapes=[
            pltpu.VMEM(d_heads.shape, BF16),
            pltpu.VMEM(pieces.shape, BF16),
            pltpu.VMEM(pieces.shape, BF16),
            pltpu.VMEM((width, columns), F32),
            pltpu.VMEM((shards, depth, columns), BF16),
            pltpu.VMEM(dh_one.shape, F32),
            pltpu.VMEM((2, rows, width), BF16),
            pltpu.VMEM((2, rows, width), BF16),
            pltpu.VMEM((2, rows, width), BF16),
            pltpu.VMEM((2, by_z, part, width), BF16),
            pltpu.VMEM((2, chunks - by_z, part, width), BF16),
            pltpu.VMEM((2, by_z, part, width), BF16),
            pltpu.VMEM((2, chunks - by_z, part, width), BF16),
            pltpu.VMEM((rows, width), BF16),
            pltpu.VMEM((rows, width), BF16),
            pltpu.VMEM((shards - 1, depth, columns), BF16),
            pltpu.VMEM((depth, columns), BF16),
            pltpu.VMEM((depth, columns), BF16),
            pltpu.VMEM((depth, columns), BF16),
            pltpu.VMEM((SEQ_SIZE + shards - 2,) + norms.shape, F32),
            pltpu.VMEM(norms.shape, F32),
            dma((7 * chunks,)),
            dma((7 * chunks,)),
            dma((shards + 3,)),
            dma((shards + 3,)),
            dma((SEQ_SIZE + shards - 2,)),
            dma((SEQ_SIZE + shards - 2,)),
            dma((8 + SEQ_SIZE,)),
        ],
        compiler_params=pltpu.CompilerParams(
            collective_id=2, has_side_effects=True, vmem_limit_bytes=VMEM_LIMIT
        ),
        cost_estimate=pl.CostEstimate(flops=60 * 10**9, bytes_accessed=64 * 2**20, transcendentals=0),
        name="scatter_gradients",
    )(d_heads, pieces, w_own, dh_one, norms)


def padded_rows(blocks, depth):
    return pl.cdiv((3 * blocks + 1) * depth, SEQ_SIZE * 16) * SEQ_SIZE * 16


def feed_forward_kernel(
    tokens_ref,
    joined_ref,
    cot_ref,
    out_hbm,
    gate_hbm,
    up_hbm,
    down_hbm,
    norms_ref,
    output_ref,
    dout_ref,
    dh_ref,
    norm_sums_ref,
    packed_ref,
    w_out,
    w_gate,
    w_up,
    w_down,
    flow,
    hat_one,
    inverse_one,
    x_low,
    x_turned,
    dm_low,
    gate_kept,
    up_kept,
    d_both,
    hidden_kept,
    staged,
    loads,
    stores,
):
    seqs, rows, width = dh_ref.shape
    shards = packed_ref.shape[0]
    depth = width // shards
    blocks = gate_hbm.shape[1] // width
    weights = ((out_hbm, w_out), (gate_hbm, w_gate), (up_hbm, w_up), (down_hbm, w_down))
    fetch = [pltpu.make_async_copy(src, dst, loads.at[n]) for n, (src, dst) in enumerate(weights)]
    tokens_in = pltpu.make_async_copy(tokens_ref, flow, loads.at[4])
    tokens_in.start()
    for copy in fetch:
        copy.start()
    gain_one, bias_one, gain_two, bias_two = (norms_ref[n : n + 1, :] for n in range(4))

    def mean(value):
        return jnp.sum(value, axis=-1, keepdims=True) * (1.0 / width)

    def rows_of(seq):
        return pl.ds(pl.multiple_of(seq * rows, rows), rows)

    fetch[0].wait()
    tokens_in.wait()

    def enter(seq, carry):
        h_one = flow[seq].astype(F32)
        for group in range(GROUPS):
            h_one = h_one + jnp.dot(
                unpack_heads(joined_ref[seq * GROUPS + group]),
                w_out[group * depth : (group + 1) * depth, :],
                preferred_element_type=F32,
            )
        centered = h_one - mean(h_one)
        inverse = lax.rsqrt(mean(centered * centered) + EPS)
        normed = centered * inverse
        hat_one[seq] = normed
        inverse_one[seq] = inverse
        x_one = normed * gain_one + bias_one
        dh_ref[seq] = x_one
        x_low[seq] = x_one.astype(BF16)
        x_turned[:, rows_of(seq)] = jnp.transpose(x_one).astype(BF16)
        return carry

    lax.fori_loop(0, seqs, enter, 0)
    cot_in = pltpu.make_async_copy(cot_ref, flow, loads.at[4])
    cot_in.start()
    for copy in fetch[1:]:
        copy.wait()

    def forward(step, carry):
        block, seq = lax.div(step, seqs), lax.rem(step, seqs)
        at = pl.ds(pl.multiple_of(block * width, width), width)
        gate = jnp.dot(x_low[seq], w_gate[:, at], preferred_element_type=F32)
        up = jnp.dot(x_low[seq], w_up[:, at], preferred_element_type=F32)
        gate_kept[block, seq] = gate.astype(gate_kept.dtype)
        up_kept[block, seq] = up.astype(up_kept.dtype)
        hidden = (gate * jax.nn.sigmoid(gate) * up).astype(BF16)
        dh_ref[seq] += jnp.dot(hidden, w_down[at, :], preferred_element_type=F32)
        return carry

    lax.fori_loop(0, blocks * seqs, forward, 0)

    cot_in.wait()
    def turn(seq, carry):
        gain_two_sum, bias_two_sum = carry
        h_two = dh_ref[seq]
        centered = h_two - mean(h_two)
        inverse = lax.rsqrt(mean(centered * centered) + EPS)
        normed = centered * inverse
        cot = flow[seq].astype(F32)
        flow[seq] = (normed * gain_two + bias_two).astype(BF16)
        gain_two_sum = gain_two_sum + jnp.sum(cot * normed, axis=0, keepdims=True)
        bias_two_sum = bias_two_sum + jnp.sum(cot, axis=0, keepdims=True)
        scaled = cot * gain_two
        dh_two = inverse * (scaled - mean(scaled) - normed * mean(scaled * normed))
        dh_ref[seq] = dh_two
        dm_low[rows_of(seq), :] = dh_two.astype(BF16)
        return gain_two_sum, bias_two_sum

    empty = jnp.zeros((1, width), F32)
    gain_two_sum, bias_two_sum = lax.fori_loop(0, seqs, turn, (empty, empty))
    output_out = pltpu.make_async_copy(flow, output_ref, loads.at[4])
    output_out.start()

    def store(kind, block):
        if kind < 2:
            start = pl.multiple_of((kind * blocks + block) * depth, depth)
            return [
                pltpu.make_async_copy(
                    staged.at[kind, pl.ds(shard * depth, depth)],
                    packed_ref.at[shard, pl.ds(start, depth)],
                    stores.at[kind, shard],
                )
                for shard in range(shards)
            ]
        start = 2 * blocks * depth
        return [
            pltpu.make_async_copy(
                staged.at[2], packed_ref.at[block, pl.ds(start, width)], stores.at[2, 0]
            )
        ]

    def backward(block, carry):
        at = pl.ds(pl.multiple_of(block * width, width), width)
        def rows_back(seq, carry):
            here = rows_of(seq)
            d_hidden = lax.dot_general(dm_low[here, :], w_down[at, :], BY_LANES, preferred_element_type=F32)
            gate = gate_kept[block, seq].astype(F32)
            up = up_kept[block, seq].astype(F32)
            sigma = jax.nn.sigmoid(gate)
            smooth = gate * sigma
            hidden_kept[here, :] = (smooth * up).astype(BF16)
            dg = (d_hidden * up * (sigma + smooth * (1.0 - sigma))).astype(BF16)
            du = (d_hidden * smooth).astype(BF16)
            d_both[0, here, :] = dg
            d_both[1, here, :] = du
            dh_ref[seq] += lax.dot_general(dg, w_gate[:, at], BY_LANES, preferred_element_type=F32)
            dh_ref[seq] += lax.dot_general(du, w_up[:, at], BY_LANES, preferred_element_type=F32)
            return carry

        lax.fori_loop(0, seqs, rows_back, 0)

        @pl.when(block > 0)
        def _():
            for kind in range(3):
                for copy in store(kind, block - 1):
                    copy.wait()

        def grow(kind, carry):
            staged[kind] = jnp.dot(x_turned[...], d_both[kind], preferred_element_type=F32).astype(BF16)
            return carry

        lax.fori_loop(0, 2, grow, 0)
        staged[2] = lax.dot_general(
            hidden_kept[...], dm_low[...], (((0,), (0,)), ((), ())), preferred_element_type=F32
        ).astype(BF16)
        for kind in range(3):
            for copy in store(kind, block):
                copy.start()
        return carry

    lax.fori_loop(0, blocks, backward, 0)

    def leave(seq, carry):
        gain_one_sum, bias_one_sum = carry
        dx_one = dh_ref[seq]
        normed = hat_one[seq]
        gain_one_sum = gain_one_sum + jnp.sum(dx_one * normed, axis=0, keepdims=True)
        bias_one_sum = bias_one_sum + jnp.sum(dx_one, axis=0, keepdims=True)
        scaled = dx_one * gain_one
        dh_one = inverse_one[seq] * (scaled - mean(scaled) - normed * mean(scaled * normed))
        dh_ref[seq] = dh_one
        d_attn = dh_one.astype(BF16)
        d_both[0, rows_of(seq), :] = d_attn
        for group in range(GROUPS):
            dout = lax.dot_general(
                d_attn, w_out[group * depth : (group + 1) * depth, :], BY_LANES, preferred_element_type=F32
            )
            first, last = pack_heads(dout)
            dout_ref[seq * GROUPS + group, :rows] = first.astype(BF16)
            dout_ref[seq * GROUPS + group, rows:] = last.astype(BF16)
        return gain_one_sum, bias_one_sum

    gain_one_sum, bias_one_sum = lax.fori_loop(0, seqs, leave, (empty, empty))
    for kind in range(3):
        for copy in store(kind, blocks - 1):
            copy.wait()
    def grow_out(group, carry):
        grad = jnp.zeros((depth, width), F32)
        for seq in range(seqs):
            grad = grad + lax.dot_general(
                unpack_heads(joined_ref[seq * GROUPS + group]),
                d_both[0, seq * rows : (seq + 1) * rows, :],
                (((0,), (0,)), ((), ())),
                preferred_element_type=F32,
            )
        staged[0, pl.ds(pl.multiple_of(group * depth, depth), depth), :] = grad.astype(BF16)
        return carry

    lax.fori_loop(0, GROUPS, grow_out, 0)
    last = [
        pltpu.make_async_copy(
            staged.at[0, pl.ds(shard * depth, depth)],
            packed_ref.at[shard, pl.ds(3 * blocks * depth, depth)],
            stores.at[0, shard],
        )
        for shard in range(shards)
    ]
    used = (3 * blocks + 1) * depth
    rest = packed_ref.shape[1] - used
    staged[1, :rest, :] = jnp.zeros((rest, width), BF16)
    last += [
        pltpu.make_async_copy(
            staged.at[1, pl.ds(0, rest)], packed_ref.at[shard, pl.ds(used, rest)], stores.at[1, shard]
        )
        for shard in range(shards)
    ]
    for copy in last:
        copy.start()
    norm_sums_ref[0:1, :] = gain_one_sum
    norm_sums_ref[1:2, :] = bias_one_sum
    norm_sums_ref[2:3, :] = gain_two_sum
    norm_sums_ref[3:4, :] = bias_two_sum
    for copy in last:
        copy.wait()
    output_out.wait()


def feed_forward(tokens, joined, cotangent, w_out, w_gate, w_up, w_down, norms, kept=BF16):
    seqs, rows, width = tokens.shape
    total = seqs * rows
    hidden = w_gate.shape[1]
    blocks = hidden // width
    depth = width // GROUPS
    vmem = pl.BlockSpec(memory_space=pltpu.VMEM)
    hbm = pl.BlockSpec(memory_space=pltpu.HBM)
    dma = pltpu.SemaphoreType.DMA
    return pl.pallas_call(
        feed_forward_kernel,
        out_shape=(
            jax.ShapeDtypeStruct(tokens.shape, BF16),
            jax.ShapeDtypeStruct(joined.shape, BF16),
            jax.ShapeDtypeStruct(tokens.shape, F32),
            jax.ShapeDtypeStruct((4, width), F32),
            jax.ShapeDtypeStruct((GROUPS, padded_rows(blocks, depth), width), BF16),
        ),
        in_specs=[hbm, vmem, hbm, hbm, hbm, hbm, hbm, vmem],
        out_specs=(hbm, vmem, vmem, vmem, hbm),
        scratch_shapes=[
            pltpu.VMEM(w_out.shape, BF16),
            pltpu.VMEM(w_gate.shape, BF16),
            pltpu.VMEM(w_up.shape, BF16),
            pltpu.VMEM(w_down.shape, BF16),
            pltpu.VMEM(tokens.shape, BF16),
            pltpu.VMEM(tokens.shape, F32),
            pltpu.VMEM((seqs, rows, 1), F32),
            pltpu.VMEM(tokens.shape, BF16),
            pltpu.VMEM((width, total), BF16),
            pltpu.VMEM((total, width), BF16),
            pltpu.VMEM((blocks, seqs, rows, width), kept),
            pltpu.VMEM((blocks, seqs, rows, width), kept),
            pltpu.VMEM((2, total, width), BF16),
            pltpu.VMEM((total, width), BF16),
            pltpu.VMEM((3, width, width), BF16),
            dma((5,)),
            dma((3, GROUPS)),
        ],
        compiler_params=pltpu.CompilerParams(vmem_limit_bytes=FEED_LIMIT),
        cost_estimate=pl.CostEstimate(
            flops=6 * total * width * (3 * hidden + width),
            bytes_accessed=2 * 2 * (3 * hidden + width) * width + 20 * total * width,
            transcendentals=2 * total * hidden,
        ),
        name="feed_forward",
    )(tokens, joined, cotangent, w_out, w_gate, w_up, w_down, norms)


def gather_rows_kernel(chunks, by_z, own_ref, rows_ref, send, recv, kept):
    me = lax.axis_index("seq")
    y_near, z_near, partner = flip(me, 1), flip(me, 2), flip(me, 4)
    barrier = pltpu.get_barrier_semaphore()
    for device in (y_near, z_near, partner):
        pl.semaphore_signal(barrier, inc=1, device_id={"seq": device}, device_id_type=BY_MESH)
    pl.semaphore_wait(barrier, 3)
    count = own_ref.shape[0]
    part = count // chunks
    started = []

    def go(source, target, slot, device):
        copy = pltpu.make_async_remote_copy(
            src_ref=source,
            dst_ref=target,
            send_sem=send.at[slot],
            recv_sem=recv.at[slot],
            device_id={"seq": device},
            device_id_type=BY_MESH,
        )
        copy.start()
        started.append(copy)
        return copy

    def band(device, chunk):
        return rows_ref.at[pl.ds(device * count + chunk * part, part)]

    def own(chunk, slot, device):
        return go(own_ref.at[pl.ds(chunk * part, part)], band(me, chunk), slot * chunks + chunk, device)

    def relay(device, chunk, slot, target):
        return go(band(device, chunk), band(device, chunk), slot * chunks + chunk, target)

    own_y, own_z, crossing = [], [], []
    for chunk in range(chunks):
        own_y.append(own(chunk, 1, y_near))
        crossing.append(own(chunk, 0, partner))
        own_z.append(own(chunk, 2, z_near))
    keep = pltpu.make_async_copy(own_ref, rows_ref.at[pl.ds(me * count, count)], kept)
    keep.start()
    cross_y, cross_z, corner = [], [], []
    for chunk in range(chunks):
        own_y[chunk].wait_recv()
        if chunk < by_z:
            corner.append(relay(y_near, chunk, 5, z_near))
        own_z[chunk].wait_recv()
        if chunk >= by_z:
            corner.append(relay(z_near, chunk, 5, y_near))
        crossing[chunk].wait_recv()
        cross_y.append(relay(partner, chunk, 3, y_near))
        cross_z.append(relay(partner, chunk, 4, z_near))
    for chunk in range(chunks):
        cross_y[chunk].wait_recv()
        if chunk < by_z:
            corner.append(relay(flip(y_near, 4), chunk, 6, z_near))
        cross_z[chunk].wait_recv()
        if chunk >= by_z:
            corner.append(relay(flip(z_near, 4), chunk, 6, y_near))
    for copy in corner:
        copy.wait_recv()
    keep.wait()
    for copy in started:
        copy.wait_send()


def gather_rows(owned, chunks=8, by_z=2):
    hbm = pl.BlockSpec(memory_space=pltpu.HBM)
    dma = pltpu.SemaphoreType.DMA
    return pl.pallas_call(
        functools.partial(gather_rows_kernel, chunks, by_z),
        out_shape=jax.ShapeDtypeStruct((SEQ_SIZE * owned.shape[0], owned.shape[1]), BF16),
        in_specs=[hbm],
        out_specs=hbm,
        scratch_shapes=[dma((7 * chunks,)), dma((7 * chunks,)), dma],
        compiler_params=pltpu.CompilerParams(collective_id=5, has_side_effects=True),
        name="gather_rows",
    )(owned)


def unpack_kernel(gate_rows, up_rows, down_rows, out_rows, columns, gate_ref, up_ref, down_ref, out_ref, qkv_ref):
    gate_ref[...] = gate_rows[...].astype(F32)
    up_ref[...] = up_rows[...].astype(F32)
    down_ref[...] = down_rows[...].astype(F32)

    @pl.when(pl.program_id(0) == 0)
    def _():
        out_ref[...] = out_rows[...].astype(F32)
        groups, _, width = columns.shape
        width = width // 3
        for group in range(groups):
            for part in range(3):
                at = (part * groups + group) * width
                qkv_ref[:, at : at + width] = columns[group, :, part * width : (part + 1) * width].astype(F32)


def unpack_gradients(rows, columns, blocks):
    groups, depth, thirds = columns.shape
    width = rows.shape[1]
    piece = [
        pl.BlockSpec((depth, width), lambda i, first=first, step=step: (first + step * i, 0))
        for first, step in ((0, 1), (blocks, 1), (2 * blocks, 1), (3 * blocks, 0))
    ]
    return pl.pallas_call(
        unpack_kernel,
        out_shape=(
            jax.ShapeDtypeStruct((depth, blocks * width), F32),
            jax.ShapeDtypeStruct((depth, blocks * width), F32),
            jax.ShapeDtypeStruct((blocks * depth, width), F32),
            jax.ShapeDtypeStruct((depth, width), F32),
            jax.ShapeDtypeStruct((depth, groups * thirds), F32),
        ),
        grid=(blocks,),
        in_specs=piece + [pl.BlockSpec(columns.shape, lambda i: (0, 0, 0))],
        out_specs=(
            pl.BlockSpec((depth, width), lambda i: (0, i)),
            pl.BlockSpec((depth, width), lambda i: (0, i)),
            pl.BlockSpec((depth, width), lambda i: (i, 0)),
            pl.BlockSpec((depth, width), lambda i: (0, 0)),
            pl.BlockSpec((depth, groups * thirds), lambda i: (0, 0)),
        ),
        name="unpack_gradients",
    )(rows, rows, rows, rows, columns)


def document_places(seg_row):
    length = seg_row.shape[0]
    ids = jnp.arange(LANES - HD, dtype=jnp.int32)[:, None]
    starts = jnp.sum((seg_row[None, :] < ids).astype(jnp.int32), axis=1, keepdims=True)
    start = jnp.sum(jnp.where(seg_row[None, :] == ids, starts, 0), axis=0)
    return jnp.arange(length, dtype=jnp.int32) - start


def exchange_kernel(sent_ref, taken_ref, send, recv, kept):
    me = lax.axis_index("seq")
    barrier = pltpu.get_barrier_semaphore()
    others = [lax.rem(me + step, SEQ_SIZE) for step in range(1, SEQ_SIZE)]
    for device in others:
        pl.semaphore_signal(barrier, inc=1, device_id={"seq": device}, device_id_type=BY_MESH)
    pl.semaphore_wait(barrier, SEQ_SIZE - 1)
    copies = []
    for step, device in enumerate(others):
        copy = pltpu.make_async_remote_copy(
            src_ref=sent_ref.at[device],
            dst_ref=taken_ref.at[me],
            send_sem=send.at[step],
            recv_sem=recv.at[step],
            device_id={"seq": device},
            device_id_type=BY_MESH,
        )
        copy.start()
        copies.append(copy)
    keep = pltpu.make_async_copy(sent_ref.at[me], taken_ref.at[me], kept)
    keep.start()
    keep.wait()
    for copy in copies:
        copy.wait()


def exchange(blocks, collective_id):
    hbm = pl.BlockSpec(memory_space=pltpu.HBM)
    dma = pltpu.SemaphoreType.DMA
    return pl.pallas_call(
        exchange_kernel,
        out_shape=jax.ShapeDtypeStruct(blocks.shape, blocks.dtype),
        in_specs=[hbm],
        out_specs=hbm,
        scratch_shapes=[dma((SEQ_SIZE - 1,)), dma((SEQ_SIZE - 1,)), dma],
        compiler_params=pltpu.CompilerParams(collective_id=collective_id, has_side_effects=True),
        name="exchange",
    )(blocks)


def head_columns(w_qkv, group, held):
    depth = w_qkv.shape[0]
    split = w_qkv.reshape(depth, 3, GROUPS, held, HD)
    mine = lax.dynamic_index_in_dim(split, group, 2, keepdims=False)
    second = mine * jnp.array([1, 1, 0], w_qkv.dtype)[None, :, None, None]
    return jnp.concatenate([mine, second], axis=-1).reshape(depth, 3 * held * 2 * HD)


def local_heads(
    shards,
    tokens,
    segments,
    positions,
    cotangent,
    w_qkv,
    w_out,
    w_gate,
    w_up,
    w_down,
    ln1_gain,
    ln1_bias,
    ln2_gain,
    ln2_bias,
):
    seq_count, row_count, model_width = tokens.shape
    held = HEADS // GROUPS
    length = row_count * SEQ_SIZE
    me = lax.axis_index("seq")
    seg_row = lax.dynamic_index_in_dim(segments, me // GROUPS, 0, keepdims=False)

    def gather(shard):
        return lax.all_gather(shard, "shard", axis=0, tiled=True)

    freqs = jnp.exp(jnp.arange(HD // 2, dtype=F32) * (-math.log(ROPE_BASE) / (HD // 2)))
    freq = jnp.tile(freqs, LANES // (HD // 2))[None]
    place = document_places(seg_row).astype(F32).reshape(SEQ_SIZE, 1, row_count)
    norm_rows = jnp.stack([ln1_gain, ln1_bias, ln2_gain, ln2_bias]).astype(F32)
    pieces, w_heads, norms, turn = gather_tokens(
        tokens, head_columns(w_qkv, me % GROUPS, held), norm_rows, place, freq, shards
    )
    norms = jnp.transpose(norms, (1, 0, 2)).reshape(4, model_width)
    full_out, full_gate, full_up, full_down = (gather(w) for w in (w_out, w_gate, w_up, w_down))
    bounds = document_bounds(seg_row, row_count)
    q_ext, k_ext, v_ext = project_heads(
        seg_row.astype(F32), turn, pieces, w_heads.reshape(model_width, -1), held
    )
    sums, joined_own = attend_heads(bounds, q_ext, k_ext, v_ext, row_count)
    output, d_joined, dh_one, norms_part, packed = feed_forward(
        tokens, exchange(joined_own, 3), cotangent, full_out, full_gate, full_up, full_down, norms
    )
    depth = model_width // shards
    ff_blocks = full_gate.shape[1] // model_width
    owned = lax.psum_scatter(
        packed.reshape(-1, model_width), ("shard", "seq"), scatter_dimension=0, tiled=True
    )

    dout = exchange(d_joined, 4)
    d_heads = attend_back_heads(bounds, q_ext, k_ext, v_ext, sums, dout, turn)
    w_lanes = w_heads.reshape(model_width, -1)
    w_own = jnp.concatenate(
        [w_lanes[:, at : at + HD] for at in range(0, w_lanes.shape[1], LANES)], axis=1
    )
    input_grad, columns, norm_sums = scatter_gradients(d_heads, pieces, w_own, dh_one, norms_part, shards)
    columns, owned = lax.optimization_barrier((columns, owned))
    shared = gather_rows(owned)
    grad_gate, grad_up, grad_down, grad_out, grad_qkv = unpack_gradients(shared, columns, ff_blocks)
    shard = lax.axis_index("shard")
    norm_sums = lax.dynamic_slice_in_dim(norm_sums, shard * depth, depth, 1)
    return (
        output,
        input_grad,
        grad_qkv,
        grad_out,
        grad_gate,
        grad_up,
        grad_down,
        norm_sums[0],
        norm_sums[1],
        norm_sums[2],
        norm_sums[3],
    )


def solution(mesh):
    in_specs = (
        P("shard", "seq", None),
        P("shard", None),
        P("shard", "seq"),
        P("shard", "seq", None),
        P("shard", None),
        P("shard", None),
        P("shard", None),
        P("shard", None),
        P("shard", None),
        P("shard"),
        P("shard"),
        P("shard"),
        P("shard"),
    )
    out_specs = (
        P("shard", "seq", None),
        P("shard", "seq", None),
        P("shard", None),
        P("shard", None),
        P("shard", None),
        P("shard", None),
        P("shard", None),
        P("shard"),
        P("shard"),
        P("shard"),
        P("shard"),
    )
    body = functools.partial(local_heads, mesh.shape["shard"]) if (mesh.shape["seq"], mesh.shape["shard"]) == (SEQ_SIZE, GROUPS) else local
    return jax.shard_map(body, mesh=mesh, in_specs=in_specs, out_specs=out_specs, check_vma=False)
```
